32 devices in a mesh: fsdp: 4 (over x, core), ctx: 2 (over y), tp: 4 (over z).
Axes of the slice: x: 2, y: 2, z: 4, core: 2. Of those that a mesh axis runs over, the one named last changes fastest.
Arguments:
- inputs: bfloat16 [8, 1024, 1024], P('fsdp', 'ctx'), may hold values from -6 to 6
- encoder: bfloat16 [8, 512, 1024], P('fsdp', 'ctx'), may hold values from -6 to 6
- lengths: int32 [8], P('fsdp'), may hold values from 256 to 1024, as said below
- cotangent: bfloat16 [8, 1024, 1024], P('fsdp', 'ctx'), may hold values from -6 to 6
- norm_self: bfloat16 [1024], P(('fsdp', 'ctx')), may hold values from 0.5 to 1.5
- self_query: bfloat16 [1024, 1024], P(('fsdp', 'ctx'), 'tp'), may hold values from -0.046875 to 0.046875
- self_key_matrix: bfloat16 [1024, 512], P(('fsdp', 'ctx'), 'tp'), may hold values from -0.1875 to 0.1875
- self_value_matrix: bfloat16 [1024, 512], P(('fsdp', 'ctx'), 'tp'), may hold values from -0.1875 to 0.1875
- self_out: bfloat16 [1024, 1024], P(('fsdp', 'ctx'), 'tp'), may hold values from -0.75 to 0.75
- bias_table: bfloat16 [32, 16], P(('fsdp', 'ctx'), 'tp'), may hold values from -4 to 4
- norm_cross: bfloat16 [1024], P(('fsdp', 'ctx')), may hold values from 0.5 to 1.5
- cross_query: bfloat16 [1024, 1024], P(('fsdp', 'ctx'), 'tp'), may hold values from -0.046875 to 0.046875
- cross_key_matrix: bfloat16 [1024, 512], P(('fsdp', 'ctx'), 'tp'), may hold values from -0.1875 to 0.1875
- cross_value_matrix: bfloat16 [1024, 512], P(('fsdp', 'ctx'), 'tp'), may hold values from -0.1875 to 0.1875
- cross_out: bfloat16 [1024, 1024], P(('fsdp', 'ctx'), 'tp'), may hold values from -0.75 to 0.75
- norm_feed: bfloat16 [1024], P(('fsdp', 'ctx')), may hold values from 0.5 to 1.5
- feed_gate: bfloat16 [1024, 2816], P(('fsdp', 'ctx'), 'tp'), may hold values from -0.1875 to 0.1875
- feed_up: bfloat16 [1024, 2816], P(('fsdp', 'ctx'), 'tp'), may hold values from -0.1875 to 0.1875
- feed_out: bfloat16 [1024, 2816], P(('fsdp', 'ctx'), 'tp'), may hold values from -0.109375 to 0.109375
Outputs:
- output: bfloat16 [8, 1024, 1024], P('fsdp', 'ctx')
- grad_inputs: float32 [8, 1024, 1024], P('fsdp', 'ctx')
- grad_encoder: float32 [8, 512, 1024], P('fsdp', 'ctx')
- grad_norm_self: float32 [1024], P(('fsdp', 'ctx'))
- grad_self_query: float32 [1024, 1024], P(('fsdp', 'ctx'), 'tp')
- grad_self_key: float32 [1024, 512], P(('fsdp', 'ctx'), 'tp')
- grad_self_value: float32 [1024, 512], P(('fsdp', 'ctx'), 'tp')
- grad_self_out: float32 [1024, 1024], P(('fsdp', 'ctx'), 'tp')
- grad_bias_table: float32 [32, 16], P(('fsdp', 'ctx'), 'tp')
- grad_norm_cross: float32 [1024], P(('fsdp', 'ctx'))
- grad_cross_query: float32 [1024, 1024], P(('fsdp', 'ctx'), 'tp')
- grad_cross_key: float32 [1024, 512], P(('fsdp', 'ctx'), 'tp')
- grad_cross_value: float32 [1024, 512], P(('fsdp', 'ctx'), 'tp')
- grad_cross_out: float32 [1024, 1024], P(('fsdp', 'ctx'), 'tp')
- grad_norm_feed: float32 [1024], P(('fsdp', 'ctx'))
- grad_feed_gate: float32 [1024, 2816], P(('fsdp', 'ctx'), 'tp')
- grad_feed_up: float32 [1024, 2816], P(('fsdp', 'ctx'), 'tp')
- grad_feed_out: float32 [1024, 2816], P(('fsdp', 'ctx'), 'tp')
The draws below stay inside these ranges and needn't reach their ends.
Inputs may be any that keep to these rules, and one draw needn't show every extreme that they name: `lengths`: number of real tokens of each sequence; slots from there on are padding; some sequence is full and some has the fewest.
All inputs are finite; a program needn't handle non-finite values.
Results may differ from the reference program's by a relative error of at most 0.03.
The reference program's roundings to bfloat16 on the way count: a program that leaves them out, or rounds other values in their place, can miss the bound.
Values may be sent and summed in bfloat16 or wider, within the bound.
A program may use at most 192 MiB of HBM per device.

```python
import math
from functools import partial
import jax
import jax.numpy as jnp
from jax import lax

MODEL_WIDTH = 1024
QUERY_HEADS = 16
HEAD_SIZE = 64
FF = 2816
KEY_VALUE_HEADS = 8
BUCKETS = 32
MAXDIST = 128
ENC_LEN = 512
SEQUENCE_SLOTS = 1024
SEQ_ALL = 8


def draw_lengths(key, part):
    key_draw, key_long, key_short = jax.random.split(key, 3)
    values = jax.random.randint(key_draw, (SEQ_ALL,), SEQUENCE_SLOTS // 4, SEQUENCE_SLOTS + 1)
    longest = jax.random.randint(key_long, (), 0, SEQ_ALL)
    offset = jax.random.randint(key_short, (), 1, SEQ_ALL)
    shortest = (longest + offset) % SEQ_ALL
    values = values.at[longest].set(SEQUENCE_SLOTS)
    values = values.at[shortest].set(SEQUENCE_SLOTS // 4)
    return values.astype(jnp.int32)


def block_levels(own_key, dims, cuts, least, high):
    loudness = 1.0
    for dim, shards_of in cuts:
        draws = jax.random.uniform(jax.random.fold_in(jax.random.fold_in(own_key, 6), dim), (shards_of,), jnp.float32, least / len(cuts), high / len(cuts))
        loudness = loudness * jnp.repeat(jnp.exp(draws), dims[dim] // shards_of).reshape((-1,) + (1,) * (len(dims) - 1 - dim))
    return loudness


def normal_values(own_key, shape, width, reach, cuts=(), held_as=jnp.bfloat16):
    factor_of = block_levels(own_key, shape, cuts, -0.22, 0.18) if cuts else 1.0
    array = jax.random.normal(own_key, shape, jnp.float32) * width * factor_of
    return jnp.minimum(jnp.maximum(array, -reach), reach).astype(held_as)


def setup_inputs(seed: int = 0) -> dict:
    key_list = jax.random.split(jax.random.key(seed), 20)
    return {
        "inputs": normal_values(key_list[0], (SEQ_ALL, SEQUENCE_SLOTS, MODEL_WIDTH), 1.0, 6.0, ((0, 4), (1, 2))),
        "encoder": normal_values(key_list[1], (SEQ_ALL, ENC_LEN, MODEL_WIDTH), 1.0, 6.0, ((0, 4), (1, 2))),
        "lengths": draw_lengths(jax.random.fold_in(key_list[19], 71), 0),
        "cotangent": normal_values(key_list[3], (SEQ_ALL, SEQUENCE_SLOTS, MODEL_WIDTH), 1.0, 6.0, ((0, 4), (1, 2))),
        "norm_self": jnp.clip(1.0 + 0.1 * jax.random.normal(key_list[4], (MODEL_WIDTH,), jnp.float32), 0.5, 1.5).astype(jnp.bfloat16),
        "self_query": normal_values(key_list[5], (MODEL_WIDTH, QUERY_HEADS * HEAD_SIZE), (MODEL_WIDTH * HEAD_SIZE // 4) ** -0.5, 0.046875, ((0, 8), (1, 4))),
        "self_key_matrix": normal_values(key_list[6], (MODEL_WIDTH, KEY_VALUE_HEADS * HEAD_SIZE), MODEL_WIDTH ** -0.5, 0.1875, ((0, 8), (1, 4))),
        "self_value_matrix": normal_values(key_list[7], (MODEL_WIDTH, KEY_VALUE_HEADS * HEAD_SIZE), MODEL_WIDTH ** -0.5, 0.1875, ((0, 8), (1, 4))),
        "self_out": normal_values(key_list[8], (MODEL_WIDTH, QUERY_HEADS * HEAD_SIZE), (QUERY_HEADS * HEAD_SIZE // 16) ** -0.5, 0.75, ((0, 8), (1, 4))),
        "bias_table": normal_values(key_list[9], (BUCKETS, QUERY_HEADS), 1.0, 4.0, ((0, 8), (1, 4))),
        "norm_cross": jnp.clip(1.0 + 0.1 * jax.random.normal(key_list[10], (MODEL_WIDTH,), jnp.float32), 0.5, 1.5).astype(jnp.bfloat16),
        "cross_query": normal_values(key_list[11], (MODEL_WIDTH, QUERY_HEADS * HEAD_SIZE), (MODEL_WIDTH * HEAD_SIZE // 4) ** -0.5, 0.046875, ((0, 8), (1, 4))),
        "cross_key_matrix": normal_values(key_list[12], (MODEL_WIDTH, KEY_VALUE_HEADS * HEAD_SIZE), MODEL_WIDTH ** -0.5, 0.1875, ((0, 8), (1, 4))),
        "cross_value_matrix": normal_values(key_list[13], (MODEL_WIDTH, KEY_VALUE_HEADS * HEAD_SIZE), MODEL_WIDTH ** -0.5, 0.1875, ((0, 8), (1, 4))),
        "cross_out": normal_values(key_list[14], (MODEL_WIDTH, QUERY_HEADS * HEAD_SIZE), (QUERY_HEADS * HEAD_SIZE // 16) ** -0.5, 0.75, ((0, 8), (1, 4))),
        "norm_feed": jnp.clip(1.0 + 0.1 * jax.random.normal(key_list[15], (MODEL_WIDTH,), jnp.float32), 0.5, 1.5).astype(jnp.bfloat16),
        "feed_gate": normal_values(key_list[16], (MODEL_WIDTH, FF), MODEL_WIDTH ** -0.5, 0.1875, ((0, 8), (1, 4))),
        "feed_up": normal_values(key_list[17], (MODEL_WIDTH, FF), MODEL_WIDTH ** -0.5, 0.1875, ((0, 8), (1, 4))),
        "feed_out": normal_values(key_list[18], (MODEL_WIDTH, FF), FF ** -0.5, 0.109375, ((0, 8), (1, 4))),
    }


@jax.custom_vjp
def low(v):
    return lax.optimization_barrier(v.astype(jnp.bfloat16)).astype(jnp.float32)

@jax.custom_vjp
def low_back(v):
    return v

def low_keep(v):
    return (low(v), None)

def low_pass(kept, grad):
    return (grad,)

def back_keep(v):
    return (v, None)

def back_low(kept, grad):
    return (low(grad),)
low.defvjp(low_keep, low_pass)
low_back.defvjp(back_keep, back_low)
EPSILON = 1e-06
MASKED = -1000000000.0
TOP_PRECISION = lax.Precision.HIGHEST

def bucket_index(distance):
    exact_count = BUCKETS // 2
    counter = jnp.zeros(distance.shape, jnp.int32)
    for level_index in range(1, BUCKETS - exact_count):
        border = math.ceil(exact_count * (MAXDIST / exact_count) ** (level_index / (BUCKETS - exact_count)))
        counter = counter + (distance >= border).astype(jnp.int32)
    return jnp.where(distance < exact_count, distance, exact_count + counter)

def rms_scale(values, gain_row):
    inverse = lax.rsqrt(lax.optimization_barrier(jnp.mean(values * values, axis=-1, keepdims=True)) + EPSILON)
    return values * inverse * gain_row

def project(operand_array, weight_arrays):
    return jnp.einsum('mwy,yq->mwq', operand_array, weight_arrays, precision=TOP_PRECISION)

def project_back(operand_array, weight_arrays):
    return jnp.einsum('jxe,me->jxm', operand_array, weight_arrays, precision=TOP_PRECISION)

def relative_bias(bias_weights):
    distance = jnp.arange(SEQUENCE_SLOTS, dtype=jnp.int32)
    one_hot = (bucket_index(distance)[:, None] == jnp.arange(BUCKETS, dtype=jnp.int32)[None, :]).astype(jnp.float32)
    per_distance = jnp.dot(one_hot, bias_weights, precision=TOP_PRECISION)
    offsets = jnp.maximum(distance[:, None] - distance[None, :], 0)
    spread_rows = jnp.take(per_distance, offsets, axis=0)
    return jnp.transpose(spread_rows, (2, 0, 1)).reshape(KEY_VALUE_HEADS, QUERY_HEADS // KEY_VALUE_HEADS, SEQUENCE_SLOTS, SEQUENCE_SLOTS)

def attend(queries, key_rows, value_rows, bias, lengths):
    row_total_count = queries.shape[1]
    key_total_count = key_rows.shape[1]

    def one_sequence(piece_list):
        query_sequence = piece_list[0].reshape(row_total_count, KEY_VALUE_HEADS, QUERY_HEADS // KEY_VALUE_HEADS, HEAD_SIZE)
        key_sequence = piece_list[1].reshape(key_total_count, KEY_VALUE_HEADS, HEAD_SIZE)
        value_sequence = piece_list[2].reshape(key_total_count, KEY_VALUE_HEADS, HEAD_SIZE)
        scores = low_back(jnp.einsum('ignd,jgd->gnij', query_sequence, key_sequence, precision=TOP_PRECISION))
        if bias is not None:
            positions = jnp.arange(row_total_count, dtype=jnp.int32)
            allowed = (positions[None, :] <= positions[:, None]) & (positions[None, :] < piece_list[3])
            scores = jnp.where(allowed, scores + bias, MASKED)
        weights_row = low(jax.nn.softmax(scores, axis=-1))
        output = low(low_back(jnp.einsum('gnij,jgd->ignd', weights_row, value_sequence, precision=TOP_PRECISION)))
        return output.reshape(row_total_count, QUERY_HEADS * HEAD_SIZE)
    if bias is None:
        sources = (queries, key_rows, value_rows)
    else:
        sources = (queries, key_rows, value_rows, lengths)
    return lax.map(jax.checkpoint(one_sequence), sources)

def layer(lengths, hidden_in, encoder_in, gain_one, query_one, key_one, value_one, out_one, bias_weights, gain_two, query_two, key_two, value_two, out_two, gain_three, gate_three, up_three, down_three):
    self_in = low(rms_scale(hidden_in, gain_one))
    self_q = low(low_back(project(self_in, query_one)))
    self_k = low(low_back(project(self_in, key_one)))
    self_v = low(low_back(project(self_in, value_one)))
    self_att = attend(self_q, self_k, self_v, relative_bias(bias_weights), lengths)
    hidden_two = hidden_in + low_back(project_back(self_att, out_one))
    cross_in = low(rms_scale(hidden_two, gain_two))
    cross_q = low(low_back(project(cross_in, query_two)))
    cross_k = low(low_back(project(encoder_in, key_two)))
    cross_v = low(low_back(project(encoder_in, value_two)))
    cross_att = attend(cross_q, cross_k, cross_v, None, None)
    hidden_three = hidden_two + low_back(project_back(cross_att, out_two))
    feed_in = low(rms_scale(hidden_three, gain_three))
    gate_value = low_back(project(feed_in, gate_three))
    up_value = low_back(project(feed_in, up_three))
    feed_hidden = low(jax.nn.gelu(gate_value, approximate=True) * up_value)
    return hidden_three + low_back(project_back(feed_hidden, down_three))

def reference(inputs, encoder, lengths, cotangent, norm_self, self_query, self_key_matrix, self_value_matrix, self_out, bias_table, norm_cross, cross_query, cross_key_matrix, cross_value_matrix, cross_out, norm_feed, feed_gate, feed_up, feed_out):
    floats = tuple((argument.astype(jnp.float32) for argument in (inputs, encoder, norm_self, self_query, self_key_matrix, self_value_matrix, self_out, bias_table, norm_cross, cross_query, cross_key_matrix, cross_value_matrix, cross_out, norm_feed, feed_gate, feed_up, feed_out)))
    output, pullback = jax.vjp(partial(layer, lengths), *floats)
    positions = jnp.arange(SEQUENCE_SLOTS, dtype=jnp.int32)
    valid_rows = (positions[None, :] < lengths[:, None]).astype(jnp.float32)
    grads = pullback(cotangent.astype(jnp.float32) * valid_rows[:, :, None])
    return (output.astype(jnp.bfloat16), grads[0], grads[1], grads[2], grads[3], grads[4], grads[5], grads[6], grads[7], grads[8], grads[9], grads[10], grads[11], grads[12], grads[13], grads[14], grads[15], grads[16])
```

```python
import functools
import math

import jax
import jax.numpy as jnp
from jax import lax
from jax.experimental import pallas as pl
from jax.experimental.pallas import tpu as pltpu
from jax.sharding import PartitionSpec as P

HEAD_SIZE = 64
BUCKETS = 32
MAXDIST = 128


EPSILON = 1e-06
MASKED = -1000000000.0
TOP_PRECISION = lax.Precision.HIGHEST


def rms_scale(values, gain_row):
    inverse = lax.rsqrt(jnp.mean(values * values, axis=-1, keepdims=True) + EPSILON)
    return values * inverse * gain_row


def gated_product(gate_in, up_in):
    return jax.nn.gelu(gate_in, approximate=True) * up_in


def project(operand_array, weight_arrays):
    return jnp.einsum(
        "spd,dk->spk", operand_array, weight_arrays, preferred_element_type=jnp.float32
    )


def project_back(grad_cols, weight_arrays):
    return jnp.einsum("spk,dk->spd", grad_cols, weight_arrays, preferred_element_type=jnp.float32)


def weight_grad(operand_array, grad_cols):
    return jnp.einsum("spd,spk->dk", operand_array, grad_cols, preferred_element_type=jnp.float32)


def bucket_index(distance):
    exact_count = BUCKETS // 2
    counter = jnp.zeros(distance.shape, jnp.int32)
    for level_index in range(1, BUCKETS - exact_count):
        border = math.ceil(
            exact_count * (MAXDIST / exact_count) ** (level_index / (BUCKETS - exact_count))
        )
        counter = counter + (distance >= border).astype(jnp.int32)
    return jnp.where(distance < exact_count, distance, exact_count + counter)


def reduce_rows(partial_sum):
    return lax.psum(partial_sum, "tp")


def block_scores(queries, key_rows, bias_rows, allowed):
    scores = jnp.einsum("gpkrd,gjkd->gkrpj", queries, key_rows, preferred_element_type=jnp.float32)
    if bias_rows is not None:
        scores = jnp.where(allowed[:, None, None], scores + bias_rows[None], MASKED)
    return scores


def forward_block(queries, key_rows, value_rows, bias_rows, allowed):
    scores = block_scores(queries, key_rows, bias_rows, allowed)
    row_peak = jnp.max(scores, axis=-1, keepdims=True)
    log_total = row_peak + jnp.log(jnp.sum(jnp.exp(scores - row_peak), axis=-1, keepdims=True))
    weights_low = jnp.exp(scores - log_total).astype(jnp.bfloat16)
    output = jnp.einsum(
        "gkrpj,gjkd->gpkrd", weights_low, value_rows, preferred_element_type=jnp.float32
    )
    return (output.astype(jnp.bfloat16), log_total)


def backward_block(queries, key_rows, value_rows, bias_rows, allowed, log_total, grad_out):
    scores = block_scores(queries, key_rows, bias_rows, allowed)
    softmax_rows = jnp.exp(scores - log_total)
    grad_probs = jnp.einsum(
        "gpkrd,gjkd->gkrpj", grad_out, value_rows, preferred_element_type=jnp.float32
    )
    grad_scores = softmax_rows * (
        grad_probs - jnp.sum(grad_probs * softmax_rows, axis=-1, keepdims=True)
    )
    scores_low = grad_scores.astype(jnp.bfloat16)
    grad_query = jnp.einsum(
        "gkrpj,gjkd->gpkrd", scores_low, key_rows, preferred_element_type=jnp.float32
    )
    grad_key = jnp.einsum(
        "gkrpj,gpkrd->gjkd", scores_low, queries, preferred_element_type=jnp.float32
    )
    grad_value = jnp.einsum(
        "gkrpj,gpkrd->gjkd",
        softmax_rows.astype(jnp.bfloat16),
        grad_out,
        preferred_element_type=jnp.float32,
    )
    if bias_rows is None:
        grad_bias = jnp.zeros((1,), jnp.float32)
    else:
        grad_bias = jnp.sum(grad_scores, axis=0)
    return (grad_query.astype(jnp.bfloat16), grad_key, grad_value, grad_bias)


def block_shapes(queries, key_rows, block_seqs):
    seq_count, row_total_count, query_cols = queries.shape
    key_total_count, key_cols = (key_rows.shape[1], key_rows.shape[2])
    kv_heads = key_cols // HEAD_SIZE
    repeats = query_cols // key_cols
    blocks = seq_count // block_seqs
    query_shape = (blocks, block_seqs, row_total_count, kv_heads, repeats, HEAD_SIZE)
    key_shape = (blocks, block_seqs, key_total_count, kv_heads, HEAD_SIZE)
    mask_shape = (blocks, block_seqs, row_total_count, key_total_count)
    return (query_shape, key_shape, mask_shape)


def attention_forward(queries, key_rows, value_rows, bias_rows, allowed, block_seqs):
    query_shape, key_shape, mask_shape = block_shapes(queries, key_rows, block_seqs)
    sources = (
        queries.reshape(query_shape),
        key_rows.reshape(key_shape),
        value_rows.reshape(key_shape),
    )
    if allowed is not None:
        sources = sources + (allowed.reshape(mask_shape),)

    def one_block(piece_list):
        mask_block = piece_list[3] if allowed is not None else None
        return forward_block(piece_list[0], piece_list[1], piece_list[2], bias_rows, mask_block)

    outputs, log_totals = lax.map(one_block, sources)
    return (outputs.reshape(queries.shape), log_totals)


def attention_backward(
    queries, key_rows, value_rows, bias_rows, allowed, log_totals, grad_out, block_seqs
):
    query_shape, key_shape, mask_shape = block_shapes(queries, key_rows, block_seqs)
    sources = (
        queries.reshape(query_shape),
        key_rows.reshape(key_shape),
        value_rows.reshape(key_shape),
        log_totals,
        grad_out.reshape(query_shape),
    )
    if allowed is not None:
        sources = sources + (allowed.reshape(mask_shape),)
    if bias_rows is None:
        initial = jnp.zeros((1,), jnp.float32)
    else:
        initial = jnp.zeros(bias_rows.shape, jnp.float32)

    def one_block(running, piece_list):
        mask_block = piece_list[5] if allowed is not None else None
        grad_query, grad_key, grad_value, grad_bias = backward_block(
            piece_list[0],
            piece_list[1],
            piece_list[2],
            bias_rows,
            mask_block,
            piece_list[3],
            piece_list[4],
        )
        return (running + grad_bias, (grad_query, grad_key, grad_value))

    bias_total, grad_list = lax.scan(one_block, initial, sources)
    return (
        grad_list[0].reshape(queries.shape),
        grad_list[1].reshape(key_rows.shape),
        grad_list[2].reshape(value_rows.shape),
        bias_total,
    )


def shards(
    inputs,
    encoder,
    lengths,
    cotangent,
    norm_self,
    self_query,
    self_key_matrix,
    self_value_matrix,
    self_out,
    bias_table,
    norm_cross,
    cross_query,
    cross_key_matrix,
    cross_value_matrix,
    cross_out,
    norm_feed,
    feed_gate,
    feed_up,
    feed_out,
):
    self_group = (
        lax.all_gather(norm_self, ("fsdp", "ctx"), axis=0, tiled=True),
        lax.all_gather(self_query, ("fsdp", "ctx"), axis=0, tiled=True),
        lax.all_gather(self_key_matrix, ("fsdp", "ctx"), axis=0, tiled=True),
        lax.all_gather(self_value_matrix, ("fsdp", "ctx"), axis=0, tiled=True),
        lax.all_gather(self_out, ("fsdp", "ctx"), axis=0, tiled=True),
        lax.all_gather(bias_table, ("fsdp", "ctx"), axis=0, tiled=True),
    )
    seq_count, row_total_count = (inputs.shape[0], inputs.shape[1])
    block_seqs = max((trial for trial in (1, 2, 3, 4) if seq_count % trial == 0))
    start_row = lax.axis_index("ctx") * row_total_count
    key_total_count = row_total_count * lax.axis_size("ctx")
    row_pos = start_row + jnp.arange(row_total_count, dtype=jnp.int32)
    col_pos = jnp.arange(key_total_count, dtype=jnp.int32)
    buckets = bucket_index(jnp.maximum(row_pos[:, None] - col_pos[None, :], 0))
    one_hot = (buckets[:, :, None] == jnp.arange(BUCKETS, dtype=jnp.int32)[None, None, :]).astype(
        jnp.float32
    )
    causal = col_pos[None, :] <= row_pos[:, None]
    allowed = causal[None] & (col_pos[None, None, :] < lengths[:, None, None])
    hidden_in = inputs.astype(jnp.float32)
    normed_one, norm_pull_one = jax.vjp(rms_scale, hidden_in, self_group[0].astype(jnp.float32))
    self_in = normed_one.astype(jnp.bfloat16)
    self_q = project(self_in, self_group[1]).astype(jnp.bfloat16)
    self_k = project(self_in, self_group[2]).astype(jnp.bfloat16)
    self_v = project(self_in, self_group[3]).astype(jnp.bfloat16)
    keys_self, values_self = (
        lax.all_gather(self_k, "ctx", axis=1, tiled=True),
        lax.all_gather(self_v, "ctx", axis=1, tiled=True),
    )
    heads_local = self_group[1].shape[1] // HEAD_SIZE
    kv_local = self_group[2].shape[1] // HEAD_SIZE
    table_rows = self_group[5].astype(jnp.float32)
    bias_rows = jnp.einsum("ijb,bh->hij", one_hot, table_rows, precision=TOP_PRECISION).reshape(
        kv_local, heads_local // kv_local, row_total_count, key_total_count
    )
    self_att, lse_self = attention_forward(
        self_q, keys_self, values_self, bias_rows, allowed, block_seqs
    )
    hidden_two = hidden_in + reduce_rows(project_back(self_att, self_group[4]))
    cross_group = (
        lax.all_gather(norm_cross, ("fsdp", "ctx"), axis=0, tiled=True),
        lax.all_gather(cross_query, ("fsdp", "ctx"), axis=0, tiled=True),
        lax.all_gather(cross_key_matrix, ("fsdp", "ctx"), axis=0, tiled=True),
        lax.all_gather(cross_value_matrix, ("fsdp", "ctx"), axis=0, tiled=True),
        lax.all_gather(cross_out, ("fsdp", "ctx"), axis=0, tiled=True),
    )
    normed_two, norm_pull_two = jax.vjp(rms_scale, hidden_two, cross_group[0].astype(jnp.float32))
    cross_in = normed_two.astype(jnp.bfloat16)
    cross_q = project(cross_in, cross_group[1]).astype(jnp.bfloat16)
    enc_keys = project(encoder, cross_group[2]).astype(jnp.bfloat16)
    enc_values = project(encoder, cross_group[3]).astype(jnp.bfloat16)
    keys_cross, values_cross = (
        lax.all_gather(enc_keys, "ctx", axis=1, tiled=True),
        lax.all_gather(enc_values, "ctx", axis=1, tiled=True),
    )
    cross_att, lse_cross = attention_forward(
        cross_q, keys_cross, values_cross, None, None, block_seqs
    )
    hidden_three = hidden_two + reduce_rows(project_back(cross_att, cross_group[4]))
    feed_group = (
        lax.all_gather(norm_feed, ("fsdp", "ctx"), axis=0, tiled=True),
        lax.all_gather(feed_gate, ("fsdp", "ctx"), axis=0, tiled=True),
        lax.all_gather(feed_up, ("fsdp", "ctx"), axis=0, tiled=True),
        lax.all_gather(feed_out, ("fsdp", "ctx"), axis=0, tiled=True),
    )
    normed_three, norm_pull_three = jax.vjp(
        rms_scale, hidden_three, feed_group[0].astype(jnp.float32)
    )
    feed_in = normed_three.astype(jnp.bfloat16)
    gate_value = project(feed_in, feed_group[1])
    up_value = project(feed_in, feed_group[2])
    gated_value, gated_pull = jax.vjp(gated_product, gate_value, up_value)
    feed_hidden = gated_value.astype(jnp.bfloat16)
    hidden_four = hidden_three + reduce_rows(project_back(feed_hidden, feed_group[3]))
    output = hidden_four.astype(jnp.bfloat16)
    valid_rows = (row_pos[None, :] < lengths[:, None]).astype(jnp.float32)
    grad_full = cotangent.astype(jnp.float32) * valid_rows[:, :, None]
    branch_low = grad_full.astype(jnp.bfloat16)
    grad_hidden = grad_full
    grad_feed_out = weight_grad(branch_low, feed_hidden)
    grad_gated = project(branch_low, feed_group[3])
    grad_gate, grad_up = gated_pull(grad_gated)
    gate_low = grad_gate.astype(jnp.bfloat16)
    up_low = grad_up.astype(jnp.bfloat16)
    grad_feed_gate = weight_grad(feed_in, gate_low)
    grad_feed_up = weight_grad(feed_in, up_low)
    grad_feed_in = reduce_rows(
        project_back(gate_low, feed_group[1]) + project_back(up_low, feed_group[2])
    )
    grad_three, grad_gain_three = norm_pull_three(grad_feed_in)
    grad_hidden = grad_hidden + grad_three
    feed_grads = (
        lax.psum_scatter(
            grad_gain_three.astype(jnp.bfloat16), ("fsdp", "ctx"), scatter_dimension=0, tiled=True
        ).astype(jnp.float32),
        lax.psum_scatter(
            grad_feed_gate.astype(jnp.bfloat16), ("fsdp", "ctx"), scatter_dimension=0, tiled=True
        ).astype(jnp.float32),
        lax.psum_scatter(
            grad_feed_up.astype(jnp.bfloat16), ("fsdp", "ctx"), scatter_dimension=0, tiled=True
        ).astype(jnp.float32),
        lax.psum_scatter(
            grad_feed_out.astype(jnp.bfloat16), ("fsdp", "ctx"), scatter_dimension=0, tiled=True
        ).astype(jnp.float32),
    )
    cross_low = grad_hidden.astype(jnp.bfloat16)
    grad_cross_out = weight_grad(cross_low, cross_att)
    grad_cross_att = project(cross_low, cross_group[4]).astype(jnp.bfloat16)
    grad_cq, grad_ck_part, grad_cv_part, unused_bias = attention_backward(
        cross_q, keys_cross, values_cross, None, None, lse_cross, grad_cross_att, block_seqs
    )
    grad_ck, grad_cv = (
        lax.psum_scatter(
            grad_ck_part.astype(jnp.bfloat16), "ctx", scatter_dimension=1, tiled=True
        ).astype(jnp.float32),
        lax.psum_scatter(
            grad_cv_part.astype(jnp.bfloat16), "ctx", scatter_dimension=1, tiled=True
        ).astype(jnp.float32),
    )
    ck_low = grad_ck.astype(jnp.bfloat16)
    cv_low = grad_cv.astype(jnp.bfloat16)
    grad_cross_query = weight_grad(cross_in, grad_cq)
    grad_cross_key = weight_grad(encoder, ck_low)
    grad_cross_value = weight_grad(encoder, cv_low)
    grad_cross_in, grad_encoder = reduce_rows(
        (
            project_back(grad_cq, cross_group[1]),
            project_back(ck_low, cross_group[2]) + project_back(cv_low, cross_group[3]),
        )
    )
    grad_two, grad_gain_two = norm_pull_two(grad_cross_in)
    grad_hidden = grad_hidden + grad_two
    cross_grads = (
        lax.psum_scatter(
            grad_gain_two.astype(jnp.bfloat16), ("fsdp", "ctx"), scatter_dimension=0, tiled=True
        ).astype(jnp.float32),
        lax.psum_scatter(
            grad_cross_query.astype(jnp.bfloat16), ("fsdp", "ctx"), scatter_dimension=0, tiled=True
        ).astype(jnp.float32),
        lax.psum_scatter(
            grad_cross_key.astype(jnp.bfloat16), ("fsdp", "ctx"), scatter_dimension=0, tiled=True
        ).astype(jnp.float32),
        lax.psum_scatter(
            grad_cross_value.astype(jnp.bfloat16), ("fsdp", "ctx"), scatter_dimension=0, tiled=True
        ).astype(jnp.float32),
        lax.psum_scatter(
            grad_cross_out.astype(jnp.bfloat16), ("fsdp", "ctx"), scatter_dimension=0, tiled=True
        ).astype(jnp.float32),
    )
    self_low = grad_hidden.astype(jnp.bfloat16)
    grad_self_out = weight_grad(self_low, self_att)
    grad_self_att = project(self_low, self_group[4]).astype(jnp.bfloat16)
    grad_sq, grad_sk_part, grad_sv_part, bias_total = attention_backward(
        self_q, keys_self, values_self, bias_rows, allowed, lse_self, grad_self_att, block_seqs
    )
    grad_sk, grad_sv = (
        lax.psum_scatter(
            grad_sk_part.astype(jnp.bfloat16), "ctx", scatter_dimension=1, tiled=True
        ).astype(jnp.float32),
        lax.psum_scatter(
            grad_sv_part.astype(jnp.bfloat16), "ctx", scatter_dimension=1, tiled=True
        ).astype(jnp.float32),
    )
    sk_low = grad_sk.astype(jnp.bfloat16)
    sv_low = grad_sv.astype(jnp.bfloat16)
    grad_table = jnp.einsum(
        "ijb,hij->bh",
        one_hot,
        bias_total.reshape(heads_local, row_total_count, key_total_count),
        precision=TOP_PRECISION,
    )
    grad_self_query = weight_grad(self_in, grad_sq)
    grad_self_key = weight_grad(self_in, sk_low)
    grad_self_value = weight_grad(self_in, sv_low)
    grad_self_in = reduce_rows(
        project_back(grad_sq, self_group[1])
        + project_back(sk_low, self_group[2])
        + project_back(sv_low, self_group[3])
    )
    grad_one, grad_gain_one = norm_pull_one(grad_self_in)
    grad_inputs = grad_hidden + grad_one
    self_grads = (
        lax.psum_scatter(
            grad_gain_one.astype(jnp.bfloat16), ("fsdp", "ctx"), scatter_dimension=0, tiled=True
        ).astype(jnp.float32),
        lax.psum_scatter(
            grad_self_query.astype(jnp.bfloat16), ("fsdp", "ctx"), scatter_dimension=0, tiled=True
        ).astype(jnp.float32),
        lax.psum_scatter(
            grad_self_key.astype(jnp.bfloat16), ("fsdp", "ctx"), scatter_dimension=0, tiled=True
        ).astype(jnp.float32),
        lax.psum_scatter(
            grad_self_value.astype(jnp.bfloat16), ("fsdp", "ctx"), scatter_dimension=0, tiled=True
        ).astype(jnp.float32),
        lax.psum_scatter(
            grad_self_out.astype(jnp.bfloat16), ("fsdp", "ctx"), scatter_dimension=0, tiled=True
        ).astype(jnp.float32),
        lax.psum_scatter(
            grad_table.astype(jnp.bfloat16), ("fsdp", "ctx"), scatter_dimension=0, tiled=True
        ).astype(jnp.float32),
    )
    gain_shares = jnp.stack((self_grads[0], cross_grads[0], feed_grads[0]), axis=0)
    return (
        output,
        grad_inputs,
        grad_encoder,
        gain_shares[0],
        self_grads[1],
        self_grads[2],
        self_grads[3],
        self_grads[4],
        self_grads[5],
        gain_shares[1],
        cross_grads[1],
        cross_grads[2],
        cross_grads[3],
        cross_grads[4],
        gain_shares[2],
        feed_grads[1],
        feed_grads[2],
        feed_grads[3],
    )


MESH = pl.DeviceIdType.MESH
DEPTH = 4
LINKS = {("x", 0): 0, ("y", 0): 1, ("z", 1): 2, ("z", -1): 3, ("c", 0): 4}
SIZES = {"x": 2, "y": 2, "z": DEPTH}


class Place:
    def __init__(self):
        row = lax.axis_index("fsdp")
        self.y = lax.axis_index("ctx")
        self.z = lax.axis_index("tp")
        self.x = lax.div(row, 2)
        self.c = lax.rem(row, 2)

    def link(self, axis, d):
        x, y, z, c = self.x, self.y, self.z, self.c
        if axis == "x":
            x = 1 - x
        elif axis == "y":
            y = 1 - y
        elif axis == "z":
            z = z + d
        else:
            c = 1 - c
        return (x * 2 + c, y, z)

    def has(self, link):
        if link == ("z", 1):
            return self.z < DEPTH - 1
        if link == ("z", -1):
            return self.z > 0
        return None

    def source(self, src):
        x = 1 - self.x if src.get("x") else self.x
        y = 1 - self.y if src.get("y") else self.y
        return x, y, self.z + src.get("z", 0)

    def exists(self, src):
        off = src.get("z", 0)
        if off < 0:
            return self.z >= -off
        if off > 0:
            return self.z < DEPTH - off
        return None


def arrivals(order):
    events = []
    for k, axis in enumerate(order):
        sources = [{}]
        for a in order[:k]:
            choice = (0, -1, 1, -2, 2, -3, 3) if a == "z" else (0, 1)
            sources = [dict(b, **{a: o}) for o in choice for b in sources]
        for o in (-1, 1, -2, 2, -3, 3) if axis == "z" else (1,):
            for b in sources:
                src = dict(b, **{axis: o})
                d = 0 if axis != "z" else (1 if o < 0 else -1)
                events.append((k, sum(abs(v) for v in src.values()), src, d))
    return events


def onward(order, k, d):
    out = [("z", d)] if k >= 0 and order[k] == "z" else []
    for a in order[k + 1 :]:
        out += [("z", 1), ("z", -1)] if a == "z" else [(a, 0)]
    return out


def when(cond, action):
    if cond is None:
        action()
    else:
        pl.when(cond)(action)


def number(x, y, z):
    return (x * 2 + y) * DEPTH + z


def greet(place):
    barrier = pltpu.get_barrier_semaphore()

    def signal(link):
        pl.semaphore_signal(
            barrier, inc=1, device_id=place.link(*link), device_id_type=MESH
        )

    for link in LINKS:
        when(place.has(link), functools.partial(signal, link))
    ends = jnp.where(place.z < DEPTH - 1, 1, 0) + jnp.where(place.z > 0, 1, 0)
    pl.semaphore_wait(barrier, ends + 3)


def remote(src, dst, send, recv, device):
    return pltpu.make_async_remote_copy(
        src_ref=src, dst_ref=dst, send_sem=send, recv_sem=recv,
        device_id=device, device_id_type=MESH,
    )


def gather_kernel(orders, rows, count, *refs):
    ins, outs = refs[:count], refs[count : 2 * count]
    send, recv, core_recv, local_sem = refs[2 * count :]
    place = Place()
    greet(place)
    me = (place.x, place.y, place.z)

    def slot(j, xyz, c):
        x, y, z = xyz
        if len(orders[j]) == 1:
            return outs[j].at[y if orders[j] == "y" else z]
        at = ((x * 2 + c) * 2 + y) * rows[j]
        return outs[j].at[z, pl.ds(pl.multiple_of(at, rows[j]), rows[j]), :]

    def copy(j, xyz, link, own):
        here = slot(j, xyz, place.c)
        arrived = core_recv if link[0] == "c" else recv
        i = number(*xyz)
        return remote(
            ins[j] if own else here, here, send.at[j, i, LINKS[link]], arrived.at[j, i],
            place.link(*link),
        )

    def routes(j, k, d):
        links = onward(orders[j], k, d)
        return links + [("c", 0)] if len(orders[j]) == 3 else links

    for stage in range(2):
        for j in range(count):
            for link in routes(j, -1, 0):
                if (link[0] == "c") == (stage == 1):
                    when(place.has(link), copy(j, me, link, True).start)
    local = []
    for j in range(count):
        local.append(pltpu.make_async_copy(ins[j], slot(j, me, place.c), local_sem.at[j]))
        local[-1].start()
    events = [
        (k, hops, j, src, d)
        for j in range(count)
        for k, hops, src, d in arrivals(orders[j])
    ]
    events.sort(key=lambda e: (e[0], e[1]))
    for k, hops, j, src, d in events:
        xyz = place.source(src)

        def step():
            copy(j, xyz, ("x", 0), True).wait_recv()
            for link in routes(j, k, d):
                when(place.has(link), copy(j, xyz, link, False).start)

        when(place.exists(src), step)
    for c in local:
        c.wait()
    for j in range(count):
        for link in routes(j, -1, 0):
            when(place.has(link), copy(j, me, link, True).wait_send)
    for k, hops, j, src, d in events:
        xyz = place.source(src)

        def finish():
            for link in routes(j, k, d):
                when(place.has(link), copy(j, xyz, link, False).wait_send)

        when(place.exists(src), finish)
    for j in range(count):
        if len(orders[j]) == 3:

            def from_core(i, carry):
                xyz = (lax.div(i, 2 * DEPTH), lax.rem(lax.div(i, DEPTH), 2), lax.rem(i, DEPTH))
                there = slot(j, xyz, 1 - place.c)
                remote(
                    ins[j], there, send.at[j, i, 4], core_recv.at[j, i], place.link("c", 0)
                ).wait_recv()
                return carry

            lax.fori_loop(0, 4 * DEPTH, from_core, 0)


def gather(arrays, orders, number_id, name):
    count = len(arrays)
    rows = [a.shape[0] for a in arrays]
    outs = [
        jax.ShapeDtypeStruct(
            (SIZES[o],) + a.shape if len(o) == 1 else (DEPTH, 8 * a.shape[0], a.shape[1]),
            a.dtype,
        )
        for a, o in zip(arrays, orders)
    ]
    dma = pltpu.SemaphoreType.DMA
    return pl.pallas_call(
        functools.partial(gather_kernel, orders, rows, count),
        out_shape=outs,
        in_specs=[pl.BlockSpec(memory_space=pltpu.VMEM)] * count,
        out_specs=[pl.BlockSpec(memory_space=pl.ANY)] * count,
        scratch_shapes=[
            dma((count, 4 * DEPTH, 5)), dma((count, 4 * DEPTH)), dma((count, 4 * DEPTH)),
            dma((count,)),
        ],
        compiler_params=pltpu.CompilerParams(collective_id=number_id, has_side_effects=True),
        name=name,
    )(*arrays)


def child_slots(order):
    starts, total, before = [], 0, 1
    for a in order:
        starts.append(total)
        total += before * (DEPTH + 1 if a == "z" else 1)
        before *= SIZES[a]
    return starts, total


def child_slot(order, starts, m, xyz, tail):
    at = 0
    for a in order[:m]:
        at = at * SIZES[a] + xyz["xyz".index(a)]
    if order[m] == "z":
        at = at * (DEPTH + 1) + tail
    return starts[m] + at


def scatter_kernel(orders, rows, count, *refs):
    ins, outs = refs[:count], refs[count : 2 * count]
    sums, gifts, kids = (refs[i * count : (i + 1) * count] for i in (2, 3, 4))
    load_sem, give_sem, gift_sem, up_sem, kid_sem = refs[5 * count :]
    place = Place()
    greet(place)
    me = (place.x, place.y, place.z)
    plans = [child_slots(o) for o in orders]
    partner = place.link("c", 0)

    def slot(j, xyz, c):
        x, y, z = xyz
        at = ((x * 2 + c) * 2 + y) * rows[j]
        return ins[j].at[z, pl.ds(pl.multiple_of(at, rows[j]), rows[j]), :]

    def load(j, xyz):
        i = number(*xyz)
        return pltpu.make_async_copy(slot(j, xyz, place.c), sums[j].at[i], load_sem.at[j, i])

    def give(j, xyz):
        i = number(*xyz)
        return remote(
            slot(j, xyz, 1 - place.c), gifts[j].at[i], give_sem.at[j, i], gift_sem.at[j, i],
            partner,
        )

    def up(j, xyz, k, d):
        axis = orders[j][k]
        tail = xyz[2]
        if axis == "z" and d < 0:
            tail = jnp.where(xyz[2] == place.z - d, DEPTH, xyz[2])
        at = child_slot(orders[j], plans[j][0], k, xyz, tail)
        i = number(*xyz)
        return remote(
            sums[j].at[i], kids[j].at[at], up_sem.at[j, i], kid_sem.at[j, at],
            place.link(axis, -d),
        )

    def kid(j, m, xyz, tail):
        at = child_slot(orders[j], plans[j][0], m, xyz, tail)
        ref = kids[j].at[at]
        remote(ref, ref, up_sem.at[j, 0], kid_sem.at[j, at], partner).wait_recv()
        return ref

    def add(j, i, terms, out=None):
        total = sums[j].at[i]
        step = min(rows[j], 16)

        def body(q, carry):
            at = pl.ds(pl.multiple_of(q * step, step), step)
            value = total[at, :].astype(jnp.float32)
            for term in terms:
                value = value + term[at, :].astype(jnp.float32)
            if out is None:
                total[at, :] = value.astype(total.dtype)
            else:
                out[at, :] = value.astype(out.dtype)
            return carry

        lax.fori_loop(0, rows[j] // step, body, 0)

    def collect(j, xyz, k, d, out=None):
        i = number(*xyz)
        order = orders[j]
        load(j, xyz).wait()
        give(j, xyz).wait_recv()
        always, sometimes = [], []
        if k >= 0 and order[k] == "z":
            sometimes.append((k, ("z", d), xyz[2]))
        for m in range(k + 1, len(order)):
            if order[m] == "z":
                sometimes += [(m, ("z", 1), xyz[2]), (m, ("z", -1), DEPTH)]
            else:
                always.append(m)
        for m, link, tail in sometimes:

            def more():
                add(j, i, [kid(j, m, xyz, tail)])

            when(place.has(link), more)
        add(j, i, [gifts[j].at[i]] + [kid(j, m, xyz, 0) for m in always], out)

    events = [
        (k, hops, j, src, d)
        for j in range(count)
        for k, hops, src, d in arrivals(orders[j])
    ]
    events.sort(key=lambda e: (-e[0], -e[1]))
    for k, hops, j, src, d in events:
        xyz = place.source(src)

        def begin():
            give(j, xyz).start()
            load(j, xyz).start()

        when(place.exists(src), begin)
    for j in range(count):
        give(j, me).start()
        load(j, me).start()
    for k, hops, j, src, d in events:
        xyz = place.source(src)

        def step():
            collect(j, xyz, k, d)
            up(j, xyz, k, d).start()

        when(place.exists(src), step)
    for j in range(count):
        collect(j, me, -1, 0, outs[j])
    for k, hops, j, src, d in events:
        xyz = place.source(src)

        def finish():
            up(j, xyz, k, d).wait_send()
            give(j, xyz).wait_send()

        when(place.exists(src), finish)
    for j in range(count):
        give(j, me).wait_send()


def scatter(arrays, orders, number_id, name):
    count = len(arrays)
    rows = [a.shape[1] // 8 for a in arrays]
    plans = [child_slots(o)[1] for o in orders]
    dma = pltpu.SemaphoreType.DMA

    def room(slots):
        return [
            pltpu.VMEM((n, r, a.shape[2]), a.dtype) for n, r, a in zip(slots, rows, arrays)
        ]

    full = [4 * DEPTH] * count
    return pl.pallas_call(
        functools.partial(scatter_kernel, orders, rows, count),
        out_shape=[
            jax.ShapeDtypeStruct((r, a.shape[2]), jnp.float32) for r, a in zip(rows, arrays)
        ],
        in_specs=[pl.BlockSpec(memory_space=pl.ANY)] * count,
        out_specs=[pl.BlockSpec(memory_space=pltpu.VMEM)] * count,
        scratch_shapes=room(full) + room(full) + room(plans)
        + [dma((count, 4 * DEPTH))] * 4 + [dma((count, max(plans)))],
        compiler_params=pltpu.CompilerParams(
            collective_id=number_id, has_side_effects=True, vmem_limit_bytes=67043328
        ),
        name=name,
    )(*arrays)


WIDTH = 1024
QROWS = 256
KEYS = 1024
ENC_ROWS = 512
SPAN = 1280
CHUNK = 128
VMEM_MOST = 64000000
ROWS_OF = (((0,), (0,)), ((), ()))
LAST = (((1,), (1,)), ((), ()))
PLAIN = (((1,), (0,)), ((), ()))


def mm(a, b, dims=PLAIN):
    return lax.dot_general(a, b, dims, preferred_element_type=jnp.float32)


def norm_rows(v, gain):
    return v * lax.rsqrt(jnp.mean(v * v, axis=-1, keepdims=True) + EPSILON) * gain


def norm_back(v, gain, e):
    r = lax.rsqrt(jnp.mean(v * v, axis=-1, keepdims=True) + EPSILON)
    ev = e * v
    gain_grad = jnp.sum(ev * r, axis=0, keepdims=True)
    back = r * gain * e - v * (r * r * r) * jnp.mean(ev * gain, axis=-1, keepdims=True)
    return back, gain_grad


def head_rows(cols, a):
    return jnp.concatenate(
        [cols[:, a * 128 : a * 128 + 64], cols[:, a * 128 + 64 : a * 128 + 128]], axis=0
    )


def attend(q, kv, p_ref, s_ref, ot_ref, keys, add_bias):
    for a in range(2):
        q2 = head_rows(q, a)
        k = kv[:, a * 64 : a * 64 + 64]
        v = kv[:, 128 + a * 64 : 192 + a * 64]
        if add_bias is not None:
            add_bias(a, None, None)
        peak = None
        for c in range(keys // CHUNK):
            rows = pl.ds(c * CHUNK, CHUNK)
            s = mm(k[c * CHUNK : (c + 1) * CHUNK], q2, LAST)
            if add_bias is not None:
                s = add_bias(a, c, s)
            s_ref[rows, :] = s
            top = jnp.max(s, axis=0, keepdims=True)
            peak = top if peak is None else jnp.maximum(peak, top)
        total = jnp.zeros_like(peak)
        for c in range(keys // CHUNK):
            rows = pl.ds(c * CHUNK, CHUNK)
            e = jnp.exp(s_ref[rows, :] - peak)
            s_ref[rows, :] = e
            total = total + jnp.sum(e, axis=0, keepdims=True)
        inverse = 1.0 / total
        for c in range(keys // CHUNK):
            rows = pl.ds(c * CHUNK, CHUNK)
            p_ref[0, a, rows, :] = (s_ref[rows, :] * inverse).astype(jnp.bfloat16)
        ot = mm(v, p_ref[0, a], ROWS_OF)
        ot_ref[a * 128 : a * 128 + 64, :] = ot[:, :QROWS]
        ot_ref[a * 128 + 64 : a * 128 + 128, :] = ot[:, QROWS:]
    return jnp.transpose(ot_ref[...]).astype(jnp.bfloat16)


def attend_back(q, kv, p_ref, do, dkv_ref, d_ref, ds_ref, qt_ref, keys, take_bias):
    for a in range(2):
        q2 = head_rows(q, a)
        do2 = head_rows(do, a)
        k = kv[:, a * 64 : a * 64 + 64]
        v = kv[:, 128 + a * 64 : 192 + a * 64]
        total = jnp.zeros((1, 2 * QROWS), jnp.float32)
        for c in range(keys // CHUNK):
            rows = pl.ds(c * CHUNK, CHUNK)
            dp = mm(v[c * CHUNK : (c + 1) * CHUNK], do2, LAST)
            d_ref[rows, :] = dp
            total = total + jnp.sum(
                dp * p_ref[0, a, rows, :].astype(jnp.float32), axis=0, keepdims=True
            )
        for c in range(keys // CHUNK):
            rows = pl.ds(c * CHUNK, CHUNK)
            ds = p_ref[0, a, rows, :].astype(jnp.float32) * (d_ref[rows, :] - total)
            if take_bias is not None:
                take_bias(a, c, ds)
            ds_ref[rows, :] = ds.astype(jnp.bfloat16)
        if take_bias is not None:
            take_bias(a, None, None)
        dkv_ref[0, :, a * 64 : a * 64 + 64] = mm(ds_ref[...], q2).astype(jnp.bfloat16)
        dkv_ref[0, :, 128 + a * 64 : 192 + a * 64] = mm(p_ref[0, a], do2).astype(jnp.bfloat16)
        qt = mm(k, ds_ref[...], ROWS_OF)
        qt_ref[a * 128 : a * 128 + 64, :] = qt[:, :QROWS]
        qt_ref[a * 128 + 64 : a * 128 + 128, :] = qt[:, QROWS:]
    return jnp.transpose(qt_ref[...]).astype(jnp.bfloat16)


def self_forward_kernel(
    info, table, x_ref, gain_ref, w_ref, wkv_ref, bucket_ref,
    x2_ref, h_ref, q_ref, kv_ref, p_ref, o_ref,
    h1_ref, s_ref, strip_ref, ot_ref,
):
    first = pl.multiple_of(info[0], QROWS)
    length = info[1]

    @pl.when(pl.program_id(0) == 0)
    def _():
        for c in range(KEYS // QROWS):
            rows = pl.ds(c * QROWS, QROWS)
            h1_ref[rows, :] = norm_rows(
                x_ref[rows, :].astype(jnp.float32), gain_ref[...]
            ).astype(jnp.bfloat16)
        x2_ref[...] = x_ref[pl.ds(first, QROWS), :].astype(jnp.float32)
        h_ref[...] = h1_ref[pl.ds(first, QROWS), :]

    kv = mm(h1_ref[...], wkv_ref[0]).astype(jnp.bfloat16)
    kv_ref[0] = kv
    q = mm(h1_ref[pl.ds(first, QROWS), :], w_ref[0, :, :QROWS]).astype(jnp.bfloat16)
    q_ref[0] = q
    lane = lax.broadcasted_iota(jnp.int32, (1, 2 * QROWS), 1)
    lane = jnp.where(lane < QROWS, lane, lane - QROWS)
    last_key = jnp.minimum(lane + first, length - 1)

    def add_bias(a, c, s):
        if c is None:
            for b in range(2):
                head = pl.program_id(0) * 4 + 2 * a + b
                bucket = bucket_ref[...]
                near = jnp.full((8, SPAN), table[BUCKETS - 1, head], jnp.float32)
                for i in range(BUCKETS - 1):
                    near = jnp.where(bucket == i, table[i, head], near)
                for g in range(16):
                    shift = (SPAN - (120 - 8 * g)) % SPAN
                    strip_ref[b, 8 * g : 8 * g + 8, :] = (
                        pltpu.roll(near, shift, 1) if shift else near
                    )
            return None
        cols = pl.ds(CHUNK * (7 - c), QROWS)
        bias = jnp.concatenate([strip_ref[0, :, cols], strip_ref[1, :, cols]], axis=1)
        key = lax.broadcasted_iota(jnp.int32, s.shape, 0) + c * CHUNK
        return jnp.where(key <= last_key, s + bias, MASKED)

    o = attend(q, kv, p_ref, s_ref, ot_ref, KEYS, add_bias)
    o_ref[0] = o
    x2_ref[...] += mm(o, w_ref[0, :, QROWS:], LAST)


def cross_forward_kernel(
    x2_ref, enc_ref, gain_ref, w_ref, wkv_ref,
    x3_ref, h_ref, q_ref, kv_ref, p_ref, o_ref,
    s_ref, ot_ref,
):
    @pl.when(pl.program_id(0) == 0)
    def _():
        x3_ref[...] = x2_ref[...]
        h_ref[...] = norm_rows(x2_ref[...], gain_ref[...]).astype(jnp.bfloat16)

    kv = mm(enc_ref[...], wkv_ref[0]).astype(jnp.bfloat16)
    kv_ref[0] = kv
    q = mm(h_ref[...], w_ref[0, :, :QROWS]).astype(jnp.bfloat16)
    q_ref[0] = q
    o = attend(q, kv, p_ref, s_ref, ot_ref, ENC_ROWS, None)
    o_ref[0] = o
    x3_ref[...] += mm(o, w_ref[0, :, QROWS:], LAST)


def feed_kernel(
    info, x3_ref, cot_ref, gain_ref, wg_ref, wu_ref, wo_ref,
    out_ref, g3_ref, gg_ref, gu_ref, go_ref, gn_ref,
    h_ref, ht_ref, g_ref, gt_ref, y_ref, dh_ref,
):
    step = pl.program_id(0)

    @pl.when(step == 0)
    def _():
        h = norm_rows(x3_ref[...], gain_ref[...]).astype(jnp.bfloat16)
        h_ref[...] = h
        ht_ref[...] = jnp.transpose(h)
        row = lax.broadcasted_iota(jnp.int32, (QROWS, 1), 0) + info[0]
        g4 = jnp.where(row < info[1], cot_ref[...].astype(jnp.float32), 0.0)
        g = g4.astype(jnp.bfloat16)
        g_ref[...] = g
        gt_ref[...] = jnp.transpose(g)
        y_ref[...] = x3_ref[...]
        dh_ref[...] = jnp.zeros_like(dh_ref)

    gate = mm(h_ref[...], wg_ref[0])
    up = mm(h_ref[...], wu_ref[0])
    root = math.sqrt(2.0 / math.pi)
    square = gate * gate
    th = jnp.tanh(root * (gate + 0.044715 * gate * square))
    half = 0.5 * (1.0 + th)
    gelu = gate * half
    slope = half + 0.5 * gate * (1.0 - th * th) * (root * (1.0 + 3 * 0.044715 * square))
    hidden = (gelu * up).astype(jnp.bfloat16)
    y_ref[...] += mm(hidden, wo_ref[0], LAST)
    go_ref[0] = mm(gt_ref[...], hidden).astype(jnp.bfloat16)
    dhid = mm(g_ref[...], wo_ref[0])
    dup = (dhid * gelu).astype(jnp.bfloat16)
    dgate = (dhid * up * slope).astype(jnp.bfloat16)
    gg_ref[0] = mm(ht_ref[...], dgate).astype(jnp.bfloat16)
    gu_ref[0] = mm(ht_ref[...], dup).astype(jnp.bfloat16)
    dh_ref[...] += mm(dgate, wg_ref[0], LAST) + mm(dup, wu_ref[0], LAST)

    @pl.when(step == pl.num_programs(0) - 1)
    def _():
        out_ref[...] = y_ref[...].astype(jnp.bfloat16)
        back, gain_grad = norm_back(x3_ref[...], gain_ref[...], dh_ref[...])
        g3_ref[...] = g_ref[...].astype(jnp.float32) + back
        gn_ref[...] = gain_grad


def cross_backward_kernel(
    g3_ref, x2_ref, h_ref, gain_ref, w_ref, q_ref, kv_ref, p_ref, o_ref,
    g2_ref, dkv_ref, gw_ref, gn_ref,
    g_ref, gt_ref, ht_ref, dh_ref, d_ref, ds_ref, qt_ref,
):
    step = pl.program_id(0)

    @pl.when(step == 0)
    def _():
        g = g3_ref[...].astype(jnp.bfloat16)
        g_ref[...] = g
        gt_ref[...] = jnp.transpose(g)
        ht_ref[...] = jnp.transpose(h_ref[...])
        dh_ref[...] = jnp.zeros_like(dh_ref)

    do = mm(g_ref[...], w_ref[0, :, QROWS:]).astype(jnp.bfloat16)
    gw_ref[0, :, QROWS:] = mm(gt_ref[...], o_ref[0]).astype(jnp.bfloat16)
    dq = attend_back(
        q_ref[0], kv_ref[0], p_ref, do, dkv_ref, d_ref, ds_ref, qt_ref, ENC_ROWS, None
    )
    gw_ref[0, :, :QROWS] = mm(ht_ref[...], dq).astype(jnp.bfloat16)
    dh_ref[...] += mm(dq, w_ref[0, :, :QROWS], LAST)

    @pl.when(step == pl.num_programs(0) - 1)
    def _():
        back, gain_grad = norm_back(x2_ref[...], gain_ref[...], dh_ref[...])
        g2_ref[...] = g3_ref[...] + back
        gn_ref[...] = gain_grad


def self_backward_kernel(
    g2_ref, h_ref, w_ref, q_ref, kv_ref, p_ref, o_ref,
    dh_ref, dkv_ref, gw_ref, near_ref,
    g_ref, gt_ref, ht_ref, d_ref, ds_ref, qt_ref, strip_ref,
):
    @pl.when(pl.program_id(0) == 0)
    def _():
        g = g2_ref[...].astype(jnp.bfloat16)
        g_ref[...] = g
        gt_ref[...] = jnp.transpose(g)
        ht_ref[...] = jnp.transpose(h_ref[...])
        dh_ref[...] = jnp.zeros_like(dh_ref)

    def take_bias(a, c, ds):
        if c is None:
            for b in range(2):
                total = jnp.zeros((8, SPAN), jnp.float32)
                for g in range(16):
                    part = strip_ref[b, 8 * g : 8 * g + 8, :]
                    shift = 120 - 8 * g
                    total = total + (pltpu.roll(part, shift, 1) if shift else part)
                near_ref[0, 2 * a + b] = total
            return
        if c == 0:
            strip_ref[...] = jnp.zeros_like(strip_ref)
        cols = pl.ds(CHUNK * (7 - c), QROWS)
        strip_ref[0, :, cols] += ds[:, :QROWS]
        strip_ref[1, :, cols] += ds[:, QROWS:]

    do = mm(g_ref[...], w_ref[0, :, QROWS:]).astype(jnp.bfloat16)
    gw_ref[0, :, QROWS:] = mm(gt_ref[...], o_ref[0]).astype(jnp.bfloat16)
    dq = attend_back(
        q_ref[0], kv_ref[0], p_ref, do, dkv_ref, d_ref, ds_ref, qt_ref, KEYS, take_bias
    )
    gw_ref[0, :, :QROWS] = mm(ht_ref[...], dq).astype(jnp.bfloat16)
    dh_ref[...] += mm(dq, w_ref[0, :, :QROWS], LAST)


def last_kernel(
    dh_part_ref, dkv_ref, x_ref, h_ref, gain_ref, g2_ref, ws_ref, wc_ref, dkvc_ref, enc_ref,
    gx_ref, genc_ref, gw_ref, gn_ref,
    ht_ref, et_ref, dh_ref, de_ref,
):
    step = pl.program_id(0)

    @pl.when(step == 0)
    def _():
        ht_ref[...] = jnp.transpose(h_ref[...])
        et_ref[...] = jnp.transpose(enc_ref[...])
        dh_ref[...] = dh_part_ref[...]
        de_ref[...] = jnp.zeros_like(de_ref)

    dkv = dkv_ref[0]
    dkvc = dkvc_ref[0]
    gw_ref[0, :, :QROWS] = mm(ht_ref[...], dkv).astype(jnp.bfloat16)
    gw_ref[0, :, QROWS:] = mm(et_ref[...], dkvc).astype(jnp.bfloat16)
    dh_ref[...] += mm(dkv, ws_ref[0], LAST)
    de_ref[...] += mm(dkvc, wc_ref[0], LAST)

    @pl.when(step == pl.num_programs(0) - 1)
    def _():
        back, gain_grad = norm_back(
            x_ref[...].astype(jnp.float32), gain_ref[...], dh_ref[...]
        )
        gx_ref[...] = (g2_ref[...] + back).astype(jnp.bfloat16)
        genc_ref[...] = de_ref[...].astype(jnp.bfloat16)
        gn_ref[...] = gain_grad


def whole(shape):
    zeros = (0,) * len(shape)
    return pl.BlockSpec(shape, lambda t: zeros)


def part(shape, column=0):
    tail = (0,) * (len(shape) - 2)
    return pl.BlockSpec(shape, lambda t: (t,) + tail + (column,))


SCALARS = pl.BlockSpec(memory_space=pltpu.SMEM)
F32 = jnp.float32
LOW = jnp.bfloat16


def run_heads(kernel, name, ins, specs, outs, out_specs, scratch, flops, steps=4):
    moved = sum(math.prod(a.shape) * a.dtype.itemsize for a in list(ins) + list(outs))
    return pl.pallas_call(
        kernel,
        grid=(steps,),
        in_specs=specs,
        out_specs=out_specs,
        out_shape=outs,
        scratch_shapes=scratch,
        compiler_params=pltpu.CompilerParams(
            dimension_semantics=("arbitrary",), vmem_limit_bytes=VMEM_MOST
        ),
        cost_estimate=pl.CostEstimate(flops=flops, bytes_accessed=moved, transcendentals=0),
        name=name,
    )(*ins)


def shape_of(shape, dtype):
    return jax.ShapeDtypeStruct(shape, dtype)


def self_forward(info, x, gain, w1, w3, table, bucket):
    return run_heads(
        self_forward_kernel, "self_forward",
        (info, table, x, gain, w1, w3, bucket),
        [SCALARS, SCALARS, whole((KEYS, WIDTH)), whole((1, WIDTH)), part((1, WIDTH, 512)),
         part((1, WIDTH, 256)), whole((8, SPAN))],
        [shape_of((QROWS, WIDTH), F32), shape_of((QROWS, WIDTH), LOW),
         shape_of((4, QROWS, 256), LOW), shape_of((4, KEYS, 256), LOW),
         shape_of((4, 2, KEYS, 512), LOW), shape_of((4, QROWS, 256), LOW)],
        [whole((QROWS, WIDTH)), whole((QROWS, WIDTH)), part((1, QROWS, 256)),
         part((1, KEYS, 256)), part((1, 2, KEYS, 512)), part((1, QROWS, 256))],
        [pltpu.VMEM((KEYS, WIDTH), LOW), pltpu.VMEM((KEYS, 512), F32),
         pltpu.VMEM((2, CHUNK, SPAN), F32), pltpu.VMEM((256, QROWS), F32)],
        5 * 10**9,
    )


def cross_forward(x2, enc, gain, w2, w3):
    return run_heads(
        cross_forward_kernel, "cross_forward",
        (x2, enc, gain, w2, w3),
        [whole((QROWS, WIDTH)), whole((ENC_ROWS, WIDTH)), whole((1, WIDTH)),
         part((1, WIDTH, 512)), part((1, WIDTH, 256), 1)],
        [shape_of((QROWS, WIDTH), F32), shape_of((QROWS, WIDTH), LOW),
         shape_of((4, QROWS, 256), LOW), shape_of((4, ENC_ROWS, 256), LOW),
         shape_of((4, 2, ENC_ROWS, 512), LOW), shape_of((4, QROWS, 256), LOW)],
        [whole((QROWS, WIDTH)), whole((QROWS, WIDTH)), part((1, QROWS, 256)),
         part((1, ENC_ROWS, 256)), part((1, 2, ENC_ROWS, 512)), part((1, QROWS, 256))],
        [pltpu.VMEM((ENC_ROWS, 512), F32), pltpu.VMEM((256, QROWS), F32)],
        3 * 10**9,
    )


def feed(info, x3, cot, gain, wg, wu, wo):
    units = wg.shape[2]
    wide = part((1, WIDTH, units))
    return run_heads(
        feed_kernel, "feed",
        (info, x3, cot, gain, wg, wu, wo),
        [SCALARS, whole((QROWS, WIDTH)), whole((QROWS, WIDTH)), whole((1, WIDTH)),
         wide, wide, wide],
        [shape_of((QROWS, WIDTH), LOW), shape_of((QROWS, WIDTH), F32)]
        + [shape_of((4, WIDTH, units), LOW)] * 3
        + [shape_of((1, WIDTH), F32)],
        [whole((QROWS, WIDTH)), whole((QROWS, WIDTH)), wide, wide, wide, whole((1, WIDTH))],
        [pltpu.VMEM((QROWS, WIDTH), LOW), pltpu.VMEM((WIDTH, QROWS), LOW),
         pltpu.VMEM((QROWS, WIDTH), LOW), pltpu.VMEM((WIDTH, QROWS), LOW),
         pltpu.VMEM((QROWS, WIDTH), F32), pltpu.VMEM((QROWS, WIDTH), F32)],
        13 * 10**9,
    )


def cross_backward(g3, x2, h, gain, w2, q, kv, p, o):
    return run_heads(
        cross_backward_kernel, "cross_backward",
        (g3, x2, h, gain, w2, q, kv, p, o),
        [whole((QROWS, WIDTH)), whole((QROWS, WIDTH)), whole((QROWS, WIDTH)),
         whole((1, WIDTH)), part((1, WIDTH, 512)), part((1, QROWS, 256)),
         part((1, ENC_ROWS, 256)), part((1, 2, ENC_ROWS, 512)), part((1, QROWS, 256))],
        [shape_of((QROWS, WIDTH), F32), shape_of((4, ENC_ROWS, 256), LOW),
         shape_of((4, WIDTH, 512), LOW), shape_of((1, WIDTH), F32)],
        [whole((QROWS, WIDTH)), part((1, ENC_ROWS, 256)), part((1, WIDTH, 512)),
         whole((1, WIDTH))],
        [pltpu.VMEM((QROWS, WIDTH), LOW), pltpu.VMEM((WIDTH, QROWS), LOW),
         pltpu.VMEM((WIDTH, QROWS), LOW), pltpu.VMEM((QROWS, WIDTH), F32),
         pltpu.VMEM((ENC_ROWS, 512), F32), pltpu.VMEM((ENC_ROWS, 512), LOW),
         pltpu.VMEM((256, QROWS), F32)],
        5 * 10**9,
    )


def self_backward(g2, h, w1, q, kv, p, o):
    return run_heads(
        self_backward_kernel, "self_backward",
        (g2, h, w1, q, kv, p, o),
        [whole((QROWS, WIDTH)), whole((QROWS, WIDTH)), part((1, WIDTH, 512)),
         part((1, QROWS, 256)), part((1, KEYS, 256)), part((1, 2, KEYS, 512)),
         part((1, QROWS, 256))],
        [shape_of((QROWS, WIDTH), F32), shape_of((4, KEYS, 256), LOW),
         shape_of((4, WIDTH, 512), LOW), shape_of((4, 4, 8, SPAN), F32)],
        [whole((QROWS, WIDTH)), part((1, KEYS, 256)), part((1, WIDTH, 512)),
         part((1, 4, 8, SPAN))],
        [pltpu.VMEM((QROWS, WIDTH), LOW), pltpu.VMEM((WIDTH, QROWS), LOW),
         pltpu.VMEM((WIDTH, QROWS), LOW), pltpu.VMEM((KEYS, 512), F32),
         pltpu.VMEM((KEYS, 512), LOW), pltpu.VMEM((256, QROWS), F32),
         pltpu.VMEM((2, CHUNK, SPAN), F32)],
        6 * 10**9,
    )


def last_grads(dh, dkv, x, h, gain, g2, w3, dkvc, enc):
    rows = enc.shape[0]
    return run_heads(
        last_kernel, "last_grads",
        (dh, dkv, x, h, gain, g2, w3, w3, dkvc, enc),
        [whole((QROWS, WIDTH)), part((1, QROWS, 256)), whole((QROWS, WIDTH)),
         whole((QROWS, WIDTH)), whole((1, WIDTH)), whole((QROWS, WIDTH)),
         part((1, WIDTH, 256)), part((1, WIDTH, 256), 1), part((1, rows, 256)),
         whole((rows, WIDTH))],
        [shape_of((QROWS, WIDTH), LOW), shape_of((rows, WIDTH), LOW),
         shape_of((4, WIDTH, 512), LOW), shape_of((1, WIDTH), F32)],
        [whole((QROWS, WIDTH)), whole((rows, WIDTH)), part((1, WIDTH, 512)),
         whole((1, WIDTH))],
        [pltpu.VMEM((WIDTH, QROWS), LOW), pltpu.VMEM((WIDTH, rows), LOW),
         pltpu.VMEM((QROWS, WIDTH), F32), pltpu.VMEM((rows, WIDTH), F32)],
        3 * 10**9,
    )


ORDERS = ("xzy", "yzx", "zyx", "xzy", "yzx", "zxy", "zxy")
SMALL_ROWS = 16
LANES = 128


def small_rows(gains, table):
    flat = jnp.pad(table.reshape(1, -1).astype(F32), ((0, 0), (0, LANES - table.size)))
    rows = jnp.concatenate([g.reshape(1, LANES).astype(F32) for g in gains] + [flat], axis=0)
    return jnp.pad(rows, ((0, SMALL_ROWS - 4), (0, 0)))


def swap(value, axis, pairs):
    return lax.ppermute(value, axis, pairs)


def share_rows(grads, y, half):
    n = grads.shape[1] // 2
    away = lax.dynamic_slice_in_dim(grads, (1 - y) * n, n, 1)
    got = swap(away, "ctx", [(0, 1), (1, 0)])
    mine = lax.dynamic_slice_in_dim(grads, y * n, n, 1).astype(F32)
    n = n // 2
    away = (
        lax.dynamic_slice_in_dim(mine, (1 - half) * n, n, 1)
        + lax.dynamic_slice_in_dim(got, (1 - half) * n, n, 1).astype(F32)
    ).astype(LOW)
    second = swap(away, "tp", [(0, 1), (1, 0), (2, 3), (3, 2)])
    total = (
        lax.dynamic_slice_in_dim(mine, half * n, n, 1)
        + lax.dynamic_slice_in_dim(got, half * n, n, 1).astype(F32)
        + second.astype(F32)
    )
    return total.astype(LOW)


def tokens_split(
    inputs, encoder, lengths, cotangent,
    norm_self, self_query, self_key_matrix, self_value_matrix, self_out, bias_table,
    norm_cross, cross_query, cross_key_matrix, cross_value_matrix, cross_out,
    norm_feed, feed_gate, feed_up, feed_out,
):
    y = lax.axis_index("ctx")
    t = lax.axis_index("tp")
    seq, half = lax.div(t, 2), lax.rem(t, 2)
    first = y * (2 * QROWS) + half * QROWS
    info = jnp.stack([first, lax.dynamic_index_in_dim(lengths, seq, 0, False)])
    x_seq = lax.dynamic_index_in_dim(inputs, seq, 0, False)
    enc_seq = lax.dynamic_index_in_dim(encoder, seq, 0, False)
    x_own = lax.dynamic_slice_in_dim(x_seq, half * QROWS, QROWS, 0)
    cot = lax.dynamic_slice(cotangent, (seq, half * QROWS, 0), (1, QROWS, WIDTH))[0]
    packed = (
        feed_gate, feed_up, feed_out,
        jnp.concatenate([self_query, self_out], axis=1),
        jnp.concatenate([cross_query, cross_out], axis=1),
        jnp.concatenate(
            [self_key_matrix, self_value_matrix, cross_key_matrix, cross_value_matrix], axis=1
        ),
        small_rows((norm_self, norm_cross, norm_feed), bias_table),
        x_seq, enc_seq,
    )
    wg, wu, wo, w1, w2, w3, small, x_all, enc_all = gather(
        packed, ORDERS + ("y", "y"), 1, "gather_weights"
    )
    small = small.reshape(4, 8, SMALL_ROWS, LANES)
    gains = jnp.transpose(small[0, :, :3], (1, 0, 2)).reshape(3, 1, WIDTH)
    table = jnp.transpose(
        small[:, :, 3, :16].reshape(4, 8, 4, 4), (1, 2, 0, 3)
    ).reshape(BUCKETS, 16)
    x_all = x_all.reshape(KEYS, WIDTH)
    enc_all = enc_all.reshape(ENC_ROWS, WIDTH)

    distance = jnp.maximum(
        first + jnp.arange(SPAN)[None, :] - (SPAN - 264) - jnp.arange(8)[:, None], 0
    )
    bucket = bucket_index(distance)
    x2, h1, q1, kv1, p1, o1 = self_forward(info, x_all, gains[0], w1, w3, table, bucket)
    x3, h2, q2, kv2, p2, o2 = cross_forward(x2, enc_all, gains[1], w2, w3)
    out, g3, gg, gu, go, gn3 = feed(info, x3, cot, gains[2], wg, wu, wo)
    g2, dkv2, gw2, gn2 = cross_backward(g3, x2, h2, gains[1], w2, q2, kv2, p2, o2)
    dh, dkv1, gw1, near = self_backward(g2, h1, w1, q1, kv1, p1, o1)
    dkvc = share_rows(dkv2, y, half)
    dkv = share_rows(dkv1, y, half)
    enc_own = lax.dynamic_slice_in_dim(enc_seq, half * (QROWS // 2), QROWS // 2, 0)
    gx, genc, gw3, gn1 = last_grads(
        dh, dkv, x_own, h1, gains[0], g2, w3, dkvc, enc_own
    )
    one_hot = (bucket[:, :, None] == jnp.arange(BUCKETS, dtype=jnp.int32)).astype(F32)
    grad_table = jnp.einsum(
        "hrm,rmb->bh", near.reshape(16, 8, SPAN), one_hot, precision=TOP_PRECISION
    )
    gain_grads = jnp.concatenate([gn1, gn2, gn3], axis=0).reshape(3, 8, LANES)
    gain_grads = jnp.broadcast_to(jnp.transpose(gain_grads, (1, 0, 2))[None], (4, 8, 3, LANES))
    table_grads = jnp.transpose(grad_table.reshape(8, 4, 4, 4), (2, 0, 1, 3)).reshape(4, 8, 1, 16)
    table_grads = jnp.pad(table_grads, ((0, 0), (0, 0), (0, 0), (0, LANES - 16)))
    small_grads = jnp.pad(
        jnp.concatenate([gain_grads, table_grads], axis=2),
        ((0, 0), (0, 0), (0, SMALL_ROWS - 4), (0, 0)),
    ).reshape(4, 8 * SMALL_ROWS, LANES)
    gg, gu, go, gw1, gw2, gw3, gs = scatter(
        (gg, gu, go, gw1, gw2, gw3, small_grads), ORDERS, 2, "scatter_grads"
    )
    out, gx, genc = gather((out, gx, genc), ("z", "z", "z"), 3, "gather_rows")
    return (
        out.reshape(inputs.shape),
        gx.reshape(inputs.shape).astype(F32),
        genc.reshape(encoder.shape).astype(F32),
        gs[0], gw1[:, :256], gw3[:, :128], gw3[:, 128:256], gw1[:, 256:],
        gs[3, :16].reshape(4, 4),
        gs[1], gw2[:, :256], gw3[:, 256:384], gw3[:, 384:], gw2[:, 256:],
        gs[2], gg, gu, go,
    )


def solution(mesh):
    sizes = (mesh.shape["fsdp"], mesh.shape["ctx"], mesh.shape["tp"])
    return jax.shard_map(
        tokens_split if sizes == (4, 2, DEPTH) else shards,
        mesh=mesh,
        in_specs=(
            P("fsdp", "ctx", None),
            P("fsdp", "ctx", None),
            P("fsdp"),
            P("fsdp", "ctx", None),
            P(("fsdp", "ctx")),
            P(("fsdp", "ctx"), "tp"),
            P(("fsdp", "ctx"), "tp"),
            P(("fsdp", "ctx"), "tp"),
            P(("fsdp", "ctx"), "tp"),
            P(("fsdp", "ctx"), "tp"),
            P(("fsdp", "ctx")),
            P(("fsdp", "ctx"), "tp"),
            P(("fsdp", "ctx"), "tp"),
            P(("fsdp", "ctx"), "tp"),
            P(("fsdp", "ctx"), "tp"),
            P(("fsdp", "ctx")),
            P(("fsdp", "ctx"), "tp"),
            P(("fsdp", "ctx"), "tp"),
            P(("fsdp", "ctx"), "tp"),
        ),
        out_specs=(
            P("fsdp", "ctx", None),
            P("fsdp", "ctx", None),
            P("fsdp", "ctx", None),
            P(("fsdp", "ctx")),
            P(("fsdp", "ctx"), "tp"),
            P(("fsdp", "ctx"), "tp"),
            P(("fsdp", "ctx"), "tp"),
            P(("fsdp", "ctx"), "tp"),
            P(("fsdp", "ctx"), "tp"),
            P(("fsdp", "ctx")),
            P(("fsdp", "ctx"), "tp"),
            P(("fsdp", "ctx"), "tp"),
            P(("fsdp", "ctx"), "tp"),
            P(("fsdp", "ctx"), "tp"),
            P(("fsdp", "ctx")),
            P(("fsdp", "ctx"), "tp"),
            P(("fsdp", "ctx"), "tp"),
            P(("fsdp", "ctx"), "tp"),
        ),
        check_vma=False,
    )
```

```python
import functools
import math

import jax
import jax.numpy as jnp
from jax import lax
from jax.experimental import pallas as pl
from jax.experimental.pallas import tpu as pltpu
from jax.sharding import PartitionSpec as P

HEAD_SIZE = 64
BUCKETS = 32
MAXDIST = 128


EPSILON = 1e-06
MASKED = -1000000000.0
TOP_PRECISION = lax.Precision.HIGHEST


def rms_scale(values, gain_row):
    inverse = lax.rsqrt(jnp.mean(values * values, axis=-1, keepdims=True) + EPSILON)
    return values * inverse * gain_row


def gated_product(gate_in, up_in):
    return jax.nn.gelu(gate_in, approximate=True) * up_in


def project(operand_array, weight_arrays):
    return jnp.einsum(
        "spd,dk->spk", operand_array, weight_arrays, preferred_element_type=jnp.float32
    )


def project_back(grad_cols, weight_arrays):
    return jnp.einsum("spk,dk->spd", grad_cols, weight_arrays, preferred_element_type=jnp.float32)


def weight_grad(operand_array, grad_cols):
    return jnp.einsum("spd,spk->dk", operand_array, grad_cols, preferred_element_type=jnp.float32)


def bucket_index(distance):
    exact_count = BUCKETS // 2
    counter = jnp.zeros(distance.shape, jnp.int32)
    for level_index in range(1, BUCKETS - exact_count):
        border = math.ceil(
            exact_count * (MAXDIST / exact_count) ** (level_index / (BUCKETS - exact_count))
        )
        counter = counter + (distance >= border).astype(jnp.int32)
    return jnp.where(distance < exact_count, distance, exact_count + counter)


def reduce_rows(partial_sum):
    return lax.psum(partial_sum, "tp")


def block_scores(queries, key_rows, bias_rows, allowed):
    scores = jnp.einsum("gpkrd,gjkd->gkrpj", queries, key_rows, preferred_element_type=jnp.float32)
    if bias_rows is not None:
        scores = jnp.where(allowed[:, None, None], scores + bias_rows[None], MASKED)
    return scores


def forward_block(queries, key_rows, value_rows, bias_rows, allowed):
    scores = block_scores(queries, key_rows, bias_rows, allowed)
    row_peak = jnp.max(scores, axis=-1, keepdims=True)
    log_total = row_peak + jnp.log(jnp.sum(jnp.exp(scores - row_peak), axis=-1, keepdims=True))
    weights_low = jnp.exp(scores - log_total).astype(jnp.bfloat16)
    output = jnp.einsum(
        "gkrpj,gjkd->gpkrd", weights_low, value_rows, preferred_element_type=jnp.float32
    )
    return (output.astype(jnp.bfloat16), log_total)


def backward_block(queries, key_rows, value_rows, bias_rows, allowed, log_total, grad_out):
    scores = block_scores(queries, key_rows, bias_rows, allowed)
    softmax_rows = jnp.exp(scores - log_total)
    grad_probs = jnp.einsum(
        "gpkrd,gjkd->gkrpj", grad_out, value_rows, preferred_element_type=jnp.float32
    )
    grad_scores = softmax_rows * (
        grad_probs - jnp.sum(grad_probs * softmax_rows, axis=-1, keepdims=True)
    )
    scores_low = grad_scores.astype(jnp.bfloat16)
    grad_query = jnp.einsum(
        "gkrpj,gjkd->gpkrd", scores_low, key_rows, preferred_element_type=jnp.float32
    )
    grad_key = jnp.einsum(
        "gkrpj,gpkrd->gjkd", scores_low, queries, preferred_element_type=jnp.float32
    )
    grad_value = jnp.einsum(
        "gkrpj,gpkrd->gjkd",
        softmax_rows.astype(jnp.bfloat16),
        grad_out,
        preferred_element_type=jnp.float32,
    )
    if bias_rows is None:
        grad_bias = jnp.zeros((1,), jnp.float32)
    else:
        grad_bias = jnp.sum(grad_scores, axis=0)
    return (grad_query.astype(jnp.bfloat16), grad_key, grad_value, grad_bias)


def block_shapes(queries, key_rows, block_seqs):
    seq_count, row_total_count, query_cols = queries.shape
    key_total_count, key_cols = (key_rows.shape[1], key_rows.shape[2])
    kv_heads = key_cols // HEAD_SIZE
    repeats = query_cols // key_cols
    blocks = seq_count // block_seqs
    query_shape = (blocks, block_seqs, row_total_count, kv_heads, repeats, HEAD_SIZE)
    key_shape = (blocks, block_seqs, key_total_count, kv_heads, HEAD_SIZE)
    mask_shape = (blocks, block_seqs, row_total_count, key_total_count)
    return (query_shape, key_shape, mask_shape)


def attention_forward(queries, key_rows, value_rows, bias_rows, allowed, block_seqs):
    query_shape, key_shape, mask_shape = block_shapes(queries, key_rows, block_seqs)
    sources = (
        queries.reshape(query_shape),
        key_rows.reshape(key_shape),
        value_rows.reshape(key_shape),
    )
    if allowed is not None:
        sources = sources + (allowed.reshape(mask_shape),)

    def one_block(piece_list):
        mask_block = piece_list[3] if allowed is not None else None
        return forward_block(piece_list[0], piece_list[1], piece_list[2], bias_rows, mask_block)

    outputs, log_totals = lax.map(one_block, sources)
    return (outputs.reshape(queries.shape), log_totals)


def attention_backward(
    queries, key_rows, value_rows, bias_rows, allowed, log_totals, grad_out, block_seqs
):
    query_shape, key_shape, mask_shape = block_shapes(queries, key_rows, block_seqs)
    sources = (
        queries.reshape(query_shape),
        key_rows.reshape(key_shape),
        value_rows.reshape(key_shape),
        log_totals,
        grad_out.reshape(query_shape),
    )
    if allowed is not None:
        sources = sources + (allowed.reshape(mask_shape),)
    if bias_rows is None:
        initial = jnp.zeros((1,), jnp.float32)
    else:
        initial = jnp.zeros(bias_rows.shape, jnp.float32)

    def one_block(running, piece_list):
        mask_block = piece_list[5] if allowed is not None else None
        grad_query, grad_key, grad_value, grad_bias = backward_block(
            piece_list[0],
            piece_list[1],
            piece_list[2],
            bias_rows,
            mask_block,
            piece_list[3],
            piece_list[4],
        )
        return (running + grad_bias, (grad_query, grad_key, grad_value))

    bias_total, grad_list = lax.scan(one_block, initial, sources)
    return (
        grad_list[0].reshape(queries.shape),
        grad_list[1].reshape(key_rows.shape),
        grad_list[2].reshape(value_rows.shape),
        bias_total,
    )


def shards(
    inputs,
    encoder,
    lengths,
    cotangent,
    norm_self,
    self_query,
    self_key_matrix,
    self_value_matrix,
    self_out,
    bias_table,
    norm_cross,
    cross_query,
    cross_key_matrix,
    cross_value_matrix,
    cross_out,
    norm_feed,
    feed_gate,
    feed_up,
    feed_out,
):
    self_group = (
        lax.all_gather(norm_self, ("fsdp", "ctx"), axis=0, tiled=True),
        lax.all_gather(self_query, ("fsdp", "ctx"), axis=0, tiled=True),
        lax.all_gather(self_key_matrix, ("fsdp", "ctx"), axis=0, tiled=True),
        lax.all_gather(self_value_matrix, ("fsdp", "ctx"), axis=0, tiled=True),
        lax.all_gather(self_out, ("fsdp", "ctx"), axis=0, tiled=True),
        lax.all_gather(bias_table, ("fsdp", "ctx"), axis=0, tiled=True),
    )
    seq_count, row_total_count = (inputs.shape[0], inputs.shape[1])
    block_seqs = max((trial for trial in (1, 2, 3, 4) if seq_count % trial == 0))
    start_row = lax.axis_index("ctx") * row_total_count
    key_total_count = row_total_count * lax.axis_size("ctx")
    row_pos = start_row + jnp.arange(row_total_count, dtype=jnp.int32)
    col_pos = jnp.arange(key_total_count, dtype=jnp.int32)
    buckets = bucket_index(jnp.maximum(row_pos[:, None] - col_pos[None, :], 0))
    one_hot = (buckets[:, :, None] == jnp.arange(BUCKETS, dtype=jnp.int32)[None, None, :]).astype(
        jnp.float32
    )
    causal = col_pos[None, :] <= row_pos[:, None]
    allowed = causal[None] & (col_pos[None, None, :] < lengths[:, None, None])
    hidden_in = inputs.astype(jnp.float32)
    normed_one, norm_pull_one = jax.vjp(rms_scale, hidden_in, self_group[0].astype(jnp.float32))
    self_in = normed_one.astype(jnp.bfloat16)
    self_q = project(self_in, self_group[1]).astype(jnp.bfloat16)
    self_k = project(self_in, self_group[2]).astype(jnp.bfloat16)
    self_v = project(self_in, self_group[3]).astype(jnp.bfloat16)
    keys_self, values_self = (
        lax.all_gather(self_k, "ctx", axis=1, tiled=True),
        lax.all_gather(self_v, "ctx", axis=1, tiled=True),
    )
    heads_local = self_group[1].shape[1] // HEAD_SIZE
    kv_local = self_group[2].shape[1] // HEAD_SIZE
    table_rows = self_group[5].astype(jnp.float32)
    bias_rows = jnp.einsum("ijb,bh->hij", one_hot, table_rows, precision=TOP_PRECISION).reshape(
        kv_local, heads_local // kv_local, row_total_count, key_total_count
    )
    self_att, lse_self = attention_forward(
        self_q, keys_self, values_self, bias_rows, allowed, block_seqs
    )
    hidden_two = hidden_in + reduce_rows(project_back(self_att, self_group[4]))
    cross_group = (
        lax.all_gather(norm_cross, ("fsdp", "ctx"), axis=0, tiled=True),
        lax.all_gather(cross_query, ("fsdp", "ctx"), axis=0, tiled=True),
        lax.all_gather(cross_key_matrix, ("fsdp", "ctx"), axis=0, tiled=True),
        lax.all_gather(cross_value_matrix, ("fsdp", "ctx"), axis=0, tiled=True),
        lax.all_gather(cross_out, ("fsdp", "ctx"), axis=0, tiled=True),
    )
    normed_two, norm_pull_two = jax.vjp(rms_scale, hidden_two, cross_group[0].astype(jnp.float32))
    cross_in = normed_two.astype(jnp.bfloat16)
    cross_q = project(cross_in, cross_group[1]).astype(jnp.bfloat16)
    enc_keys = project(encoder, cross_group[2]).astype(jnp.bfloat16)
    enc_values = project(encoder, cross_group[3]).astype(jnp.bfloat16)
    keys_cross, values_cross = (
        lax.all_gather(enc_keys, "ctx", axis=1, tiled=True),
        lax.all_gather(enc_values, "ctx", axis=1, tiled=True),
    )
    cross_att, lse_cross = attention_forward(
        cross_q, keys_cross, values_cross, None, None, block_seqs
    )
    hidden_three = hidden_two + reduce_rows(project_back(cross_att, cross_group[4]))
    feed_group = (
        lax.all_gather(norm_feed, ("fsdp", "ctx"), axis=0, tiled=True),
        lax.all_gather(feed_gate, ("fsdp", "ctx"), axis=0, tiled=True),
        lax.all_gather(feed_up, ("fsdp", "ctx"), axis=0, tiled=True),
        lax.all_gather(feed_out, ("fsdp", "ctx"), axis=0, tiled=True),
    )
    normed_three, norm_pull_three = jax.vjp(
        rms_scale, hidden_three, feed_group[0].astype(jnp.float32)
    )
    feed_in = normed_three.astype(jnp.bfloat16)
    gate_value = project(feed_in, feed_group[1])
    up_value = project(feed_in, feed_group[2])
    gated_value, gated_pull = jax.vjp(gated_product, gate_value, up_value)
    feed_hidden = gated_value.astype(jnp.bfloat16)
    hidden_four = hidden_three + reduce_rows(project_back(feed_hidden, feed_group[3]))
    output = hidden_four.astype(jnp.bfloat16)
    valid_rows = (row_pos[None, :] < lengths[:, None]).astype(jnp.float32)
    grad_full = cotangent.astype(jnp.float32) * valid_rows[:, :, None]
    branch_low = grad_full.astype(jnp.bfloat16)
    grad_hidden = grad_full
    grad_feed_out = weight_grad(branch_low, feed_hidden)
    grad_gated = project(branch_low, feed_group[3])
    grad_gate, grad_up = gated_pull(grad_gated)
    gate_low = grad_gate.astype(jnp.bfloat16)
    up_low = grad_up.astype(jnp.bfloat16)
    grad_feed_gate = weight_grad(feed_in, gate_low)
    grad_feed_up = weight_grad(feed_in, up_low)
    grad_feed_in = reduce_rows(
        project_back(gate_low, feed_group[1]) + project_back(up_low, feed_group[2])
    )
    grad_three, grad_gain_three = norm_pull_three(grad_feed_in)
    grad_hidden = grad_hidden + grad_three
    feed_grads = (
        lax.psum_scatter(
            grad_gain_three.astype(jnp.bfloat16), ("fsdp", "ctx"), scatter_dimension=0, tiled=True
        ).astype(jnp.float32),
        lax.psum_scatter(
            grad_feed_gate.astype(jnp.bfloat16), ("fsdp", "ctx"), scatter_dimension=0, tiled=True
        ).astype(jnp.float32),
        lax.psum_scatter(
            grad_feed_up.astype(jnp.bfloat16), ("fsdp", "ctx"), scatter_dimension=0, tiled=True
        ).astype(jnp.float32),
        lax.psum_scatter(
            grad_feed_out.astype(jnp.bfloat16), ("fsdp", "ctx"), scatter_dimension=0, tiled=True
        ).astype(jnp.float32),
    )
    cross_low = grad_hidden.astype(jnp.bfloat16)
    grad_cross_out = weight_grad(cross_low, cross_att)
    grad_cross_att = project(cross_low, cross_group[4]).astype(jnp.bfloat16)
    grad_cq, grad_ck_part, grad_cv_part, unused_bias = attention_backward(
        cross_q, keys_cross, values_cross, None, None, lse_cross, grad_cross_att, block_seqs
    )
    grad_ck, grad_cv = (
        lax.psum_scatter(
            grad_ck_part.astype(jnp.bfloat16), "ctx", scatter_dimension=1, tiled=True
        ).astype(jnp.float32),
        lax.psum_scatter(
            grad_cv_part.astype(jnp.bfloat16), "ctx", scatter_dimension=1, tiled=True
        ).astype(jnp.float32),
    )
    ck_low = grad_ck.astype(jnp.bfloat16)
    cv_low = grad_cv.astype(jnp.bfloat16)
    grad_cross_query = weight_grad(cross_in, grad_cq)
    grad_cross_key = weight_grad(encoder, ck_low)
    grad_cross_value = weight_grad(encoder, cv_low)
    grad_cross_in, grad_encoder = reduce_rows(
        (
            project_back(grad_cq, cross_group[1]),
            project_back(ck_low, cross_group[2]) + project_back(cv_low, cross_group[3]),
        )
    )
    grad_two, grad_gain_two = norm_pull_two(grad_cross_in)
    grad_hidden = grad_hidden + grad_two
    cross_grads = (
        lax.psum_scatter(
            grad_gain_two.astype(jnp.bfloat16), ("fsdp", "ctx"), scatter_dimension=0, tiled=True
        ).astype(jnp.float32),
        lax.psum_scatter(
            grad_cross_query.astype(jnp.bfloat16), ("fsdp", "ctx"), scatter_dimension=0, tiled=True
        ).astype(jnp.float32),
        lax.psum_scatter(
            grad_cross_key.astype(jnp.bfloat16), ("fsdp", "ctx"), scatter_dimension=0, tiled=True
        ).astype(jnp.float32),
        lax.psum_scatter(
            grad_cross_value.astype(jnp.bfloat16), ("fsdp", "ctx"), scatter_dimension=0, tiled=True
        ).astype(jnp.float32),
        lax.psum_scatter(
            grad_cross_out.astype(jnp.bfloat16), ("fsdp", "ctx"), scatter_dimension=0, tiled=True
        ).astype(jnp.float32),
    )
    self_low = grad_hidden.astype(jnp.bfloat16)
    grad_self_out = weight_grad(self_low, self_att)
    grad_self_att = project(self_low, self_group[4]).astype(jnp.bfloat16)
    grad_sq, grad_sk_part, grad_sv_part, bias_total = attention_backward(
        self_q, keys_self, values_self, bias_rows, allowed, lse_self, grad_self_att, block_seqs
    )
    grad_sk, grad_sv = (
        lax.psum_scatter(
            grad_sk_part.astype(jnp.bfloat16), "ctx", scatter_dimension=1, tiled=True
        ).astype(jnp.float32),
        lax.psum_scatter(
            grad_sv_part.astype(jnp.bfloat16), "ctx", scatter_dimension=1, tiled=True
        ).astype(jnp.float32),
    )
    sk_low = grad_sk.astype(jnp.bfloat16)
    sv_low = grad_sv.astype(jnp.bfloat16)
    grad_table = jnp.einsum(
        "ijb,hij->bh",
        one_hot,
        bias_total.reshape(heads_local, row_total_count, key_total_count),
        precision=TOP_PRECISION,
    )
    grad_self_query = weight_grad(self_in, grad_sq)
    grad_self_key = weight_grad(self_in, sk_low)
    grad_self_value = weight_grad(self_in, sv_low)
    grad_self_in = reduce_rows(
        project_back(grad_sq, self_group[1])
        + project_back(sk_low, self_group[2])
        + project_back(sv_low, self_group[3])
    )
    grad_one, grad_gain_one = norm_pull_one(grad_self_in)
    grad_inputs = grad_hidden + grad_one
    self_grads = (
        lax.psum_scatter(
            grad_gain_one.astype(jnp.bfloat16), ("fsdp", "ctx"), scatter_dimension=0, tiled=True
        ).astype(jnp.float32),
        lax.psum_scatter(
            grad_self_query.astype(jnp.bfloat16), ("fsdp", "ctx"), scatter_dimension=0, tiled=True
        ).astype(jnp.float32),
        lax.psum_scatter(
            grad_self_key.astype(jnp.bfloat16), ("fsdp", "ctx"), scatter_dimension=0, tiled=True
        ).astype(jnp.float32),
        lax.psum_scatter(
            grad_self_value.astype(jnp.bfloat16), ("fsdp", "ctx"), scatter_dimension=0, tiled=True
        ).astype(jnp.float32),
        lax.psum_scatter(
            grad_self_out.astype(jnp.bfloat16), ("fsdp", "ctx"), scatter_dimension=0, tiled=True
        ).astype(jnp.float32),
        lax.psum_scatter(
            grad_table.astype(jnp.bfloat16), ("fsdp", "ctx"), scatter_dimension=0, tiled=True
        ).astype(jnp.float32),
    )
    gain_shares = jnp.stack((self_grads[0], cross_grads[0], feed_grads[0]), axis=0)
    return (
        output,
        grad_inputs,
        grad_encoder,
        gain_shares[0],
        self_grads[1],
        self_grads[2],
        self_grads[3],
        self_grads[4],
        self_grads[5],
        gain_shares[1],
        cross_grads[1],
        cross_grads[2],
        cross_grads[3],
        cross_grads[4],
        gain_shares[2],
        feed_grads[1],
        feed_grads[2],
        feed_grads[3],
    )


MESH = pl.DeviceIdType.MESH
DEPTH = 4
LINKS = {("x", 0): 0, ("y", 0): 1, ("z", 1): 2, ("z", -1): 3, ("c", 0): 4}
SIZES = {"x": 2, "y": 2, "z": DEPTH}


class Place:
    def __init__(self):
        row = lax.axis_index("fsdp")
        self.y = lax.axis_index("ctx")
        self.z = lax.axis_index("tp")
        self.x = lax.div(row, 2)
        self.c = lax.rem(row, 2)

    def link(self, axis, d):
        x, y, z, c = self.x, self.y, self.z, self.c
        if axis == "x":
            x = 1 - x
        elif axis == "y":
            y = 1 - y
        elif axis == "z":
            z = z + d
        else:
            c = 1 - c
        return (x * 2 + c, y, z)

    def has(self, link):
        if link == ("z", 1):
            return self.z < DEPTH - 1
        if link == ("z", -1):
            return self.z > 0
        return None

    def source(self, src):
        x = 1 - self.x if src.get("x") else self.x
        y = 1 - self.y if src.get("y") else self.y
        return x, y, self.z + src.get("z", 0)

    def exists(self, src):
        off = src.get("z", 0)
        if off < 0:
            return self.z >= -off
        if off > 0:
            return self.z < DEPTH - off
        return None


def arrivals(order):
    events = []
    for k, axis in enumerate(order):
        sources = [{}]
        for a in order[:k]:
            choice = (0, -1, 1, -2, 2, -3, 3) if a == "z" else (0, 1)
            sources = [dict(b, **{a: o}) for o in choice for b in sources]
        for o in (-1, 1, -2, 2, -3, 3) if axis == "z" else (1,):
            for b in sources:
                src = dict(b, **{axis: o})
                d = 0 if axis != "z" else (1 if o < 0 else -1)
                events.append((k, sum(abs(v) for v in src.values()), src, d))
    return events


def onward(order, k, d):
    out = [("z", d)] if k >= 0 and order[k] == "z" else []
    for a in order[k + 1 :]:
        out += [("z", 1), ("z", -1)] if a == "z" else [(a, 0)]
    return out


def when(cond, action):
    if cond is None:
        action()
    else:
        pl.when(cond)(action)


def number(x, y, z):
    return (x * 2 + y) * DEPTH + z


def greet(place):
    barrier = pltpu.get_barrier_semaphore()

    def signal(link):
        pl.semaphore_signal(
            barrier, inc=1, device_id=place.link(*link), device_id_type=MESH
        )

    for link in LINKS:
        when(place.has(link), functools.partial(signal, link))
    ends = jnp.where(place.z < DEPTH - 1, 1, 0) + jnp.where(place.z > 0, 1, 0)
    pl.semaphore_wait(barrier, ends + 3)


def remote(src, dst, send, recv, device):
    return pltpu.make_async_remote_copy(
        src_ref=src, dst_ref=dst, send_sem=send, recv_sem=recv,
        device_id=device, device_id_type=MESH,
    )


class Gather:
    def __init__(self, place, orders, rows, ins, outs, sems):
        self.place, self.orders, self.rows, self.ins, self.outs = place, orders, rows, ins, outs
        self.send, self.recv, self.core_recv, self.local_sem = sems
        self.me = (place.x, place.y, place.z)
        self.arrivals = [
            (k, hops, j, src, d)
            for j in range(len(orders))
            for k, hops, src, d in arrivals(orders[j])
        ]
        self.arrivals.sort(key=lambda e: (e[0], e[1]))

    @staticmethod
    def scratch(count):
        dma = pltpu.SemaphoreType.DMA
        return [
            dma((count, 4 * DEPTH, 5)), dma((count, 4 * DEPTH)), dma((count, 4 * DEPTH)),
            dma((count,)),
        ]

    def slot(self, j, xyz, c):
        x, y, z = xyz
        if len(self.orders[j]) == 1:
            return self.outs[j].at[y if self.orders[j] == "y" else z]
        at = ((x * 2 + c) * 2 + y) * self.rows[j]
        return self.outs[j].at[z, pl.ds(pl.multiple_of(at, self.rows[j]), self.rows[j]), :]

    def copy(self, j, xyz, link, own):
        here = self.slot(j, xyz, self.place.c)
        arrived = self.core_recv if link[0] == "c" else self.recv
        i = number(*xyz)
        return remote(
            self.ins[j] if own else here, here, self.send.at[j, i, LINKS[link]],
            arrived.at[j, i], self.place.link(*link),
        )

    def routes(self, j, k, d):
        links = onward(self.orders[j], k, d)
        return links + [("c", 0)] if len(self.orders[j]) == 3 else links

    def local(self, j):
        return pltpu.make_async_copy(
            self.ins[j], self.slot(j, self.me, self.place.c), self.local_sem.at[j]
        )

    def start(self, first=()):
        count = len(self.orders)
        turn = list(first) + [j for j in range(count) if j not in first]
        for stage in range(2):
            for j in turn:
                for link in self.routes(j, -1, 0):
                    if (link[0] == "c") == (stage == 1):
                        when(self.place.has(link), self.copy(j, self.me, link, True).start)
        for j in range(count):
            self.local(j).start()

    def steps(self):
        for e, (k, hops, j, src, d) in enumerate(self.arrivals):
            xyz = self.place.source(src)

            def step(k=k, j=j, d=d, xyz=xyz, src=src):
                def run():
                    self.copy(j, xyz, ("x", 0), True).wait_recv()
                    for link in self.routes(j, k, d):
                        when(self.place.has(link), self.copy(j, xyz, link, False).start)

                when(self.place.exists(src), run)

            yield (e + 1) / len(self.arrivals), step

    def finish(self):
        count = len(self.orders)
        for j in range(count):
            self.local(j).wait()
            for link in self.routes(j, -1, 0):
                when(self.place.has(link), self.copy(j, self.me, link, True).wait_send)
        for k, hops, j, src, d in self.arrivals:
            xyz = self.place.source(src)

            def run():
                for link in self.routes(j, k, d):
                    when(self.place.has(link), self.copy(j, xyz, link, False).wait_send)

            when(self.place.exists(src), run)
        for j in range(count):
            if len(self.orders[j]) == 3:

                def from_core(i, carry):
                    xyz = (
                        lax.div(i, 2 * DEPTH), lax.rem(lax.div(i, DEPTH), 2), lax.rem(i, DEPTH)
                    )
                    remote(
                        self.ins[j], self.slot(j, xyz, 1 - self.place.c), self.send.at[j, i, 4],
                        self.core_recv.at[j, i], self.place.link("c", 0),
                    ).wait_recv()
                    return carry

                lax.fori_loop(0, 4 * DEPTH, from_core, 0)


def child_slots(order):
    starts, total, before = [], 0, 1
    for a in order:
        starts.append(total)
        total += before * (DEPTH + 1 if a == "z" else 1)
        before *= SIZES[a]
    return starts, total


def child_slot(order, starts, m, xyz, tail):
    at = 0
    for a in order[:m]:
        at = at * SIZES[a] + xyz["xyz".index(a)]
    if order[m] == "z":
        at = at * (DEPTH + 1) + tail
    return starts[m] + at


def add_rows(out, terms, rows):
    step = min(rows, 16)

    def body(q, carry):
        at = pl.ds(pl.multiple_of(q * step, step), step)
        value = terms[0][at, :].astype(jnp.float32)
        for term in terms[1:]:
            value = value + term[at, :].astype(jnp.float32)
        out[at, :] = value.astype(out.dtype)
        return carry

    lax.fori_loop(0, rows // step, body, 0)


class Scatter:
    def __init__(self, place, orders, rows, ins, outs, scratch):
        self.place, self.orders, self.rows, self.ins, self.outs = place, orders, rows, ins, outs
        n = len(orders)
        self.sums, self.gifts, self.kids = (scratch[i * n : (i + 1) * n] for i in range(3))
        self.load_sem, self.give_sem, self.gift_sem, self.up_sem, self.kid_sem = scratch[3 * n :]
        self.me = (place.x, place.y, place.z)
        self.plans = [child_slots(o) for o in orders]
        self.partner = place.link("c", 0)
        self.events = [
            (k, hops, j, src, d)
            for j in range(n)
            for k, hops, src, d in arrivals(orders[j])
        ]
        self.events.sort(key=lambda e: (-e[0], -e[1]))

    @staticmethod
    def scratch(arrays, rows, orders):
        plans = [child_slots(o)[1] for o in orders]
        count = len(arrays)
        dma = pltpu.SemaphoreType.DMA

        def room(slots):
            return [
                pltpu.VMEM((n, r, a.shape[2]), a.dtype) for n, r, a in zip(slots, rows, arrays)
            ]

        full = [4 * DEPTH] * count
        return (
            room(full) + room(full) + room(plans)
            + [dma((count, 4 * DEPTH))] * 4 + [dma((count, max(plans)))]
        )

    def slot(self, j, xyz, c):
        x, y, z = xyz
        at = ((x * 2 + c) * 2 + y) * self.rows[j]
        return self.ins[j].at[z, pl.ds(pl.multiple_of(at, self.rows[j]), self.rows[j]), :]

    def load(self, j, xyz):
        i = number(*xyz)
        return pltpu.make_async_copy(
            self.slot(j, xyz, self.place.c), self.sums[j].at[i], self.load_sem.at[j, i]
        )

    def give(self, j, xyz):
        i = number(*xyz)
        return remote(
            self.slot(j, xyz, 1 - self.place.c), self.gifts[j].at[i], self.give_sem.at[j, i],
            self.gift_sem.at[j, i], self.partner,
        )

    def up(self, j, xyz, k, d):
        axis = self.orders[j][k]
        tail = xyz[2]
        if axis == "z" and d < 0:
            tail = jnp.where(xyz[2] == self.place.z - d, DEPTH, xyz[2])
        at = child_slot(self.orders[j], self.plans[j][0], k, xyz, tail)
        i = number(*xyz)
        return remote(
            self.sums[j].at[i], self.kids[j].at[at], self.up_sem.at[j, i],
            self.kid_sem.at[j, at], self.place.link(axis, -d),
        )

    def kid(self, j, m, xyz, tail):
        at = child_slot(self.orders[j], self.plans[j][0], m, xyz, tail)
        ref = self.kids[j].at[at]
        remote(ref, ref, self.up_sem.at[j, 0], self.kid_sem.at[j, at], self.partner).wait_recv()
        return ref

    def collect(self, j, xyz, k, d, out=None):
        i = number(*xyz)
        order = self.orders[j]
        total = self.sums[j].at[i]
        self.load(j, xyz).wait()
        self.give(j, xyz).wait_recv()
        always, sometimes = [], []
        if k >= 0 and order[k] == "z":
            sometimes.append((k, ("z", d), xyz[2]))
        for m in range(k + 1, len(order)):
            if order[m] == "z":
                sometimes += [(m, ("z", 1), xyz[2]), (m, ("z", -1), DEPTH)]
            else:
                always.append(m)
        for m, link, tail in sometimes:

            def more():
                add_rows(total, [total, self.kid(j, m, xyz, tail)], self.rows[j])

            when(self.place.has(link), more)
        terms = [total, self.gifts[j].at[i]] + [self.kid(j, m, xyz, 0) for m in always]
        add_rows(total if out is None else out, terms, self.rows[j])

    def start(self):
        for k, hops, j, src, d in self.events:
            xyz = self.place.source(src)

            def begin():
                self.give(j, xyz).start()
                self.load(j, xyz).start()

            when(self.place.exists(src), begin)
        for j in range(len(self.orders)):
            self.give(j, self.me).start()
            self.load(j, self.me).start()

    def steps(self):
        count = len(self.events)
        for e, (k, hops, j, src, d) in enumerate(self.events):
            xyz = self.place.source(src)

            def step(k=k, j=j, d=d, xyz=xyz, src=src):
                def run():
                    self.collect(j, xyz, k, d)
                    self.up(j, xyz, k, d).start()

                when(self.place.exists(src), run)

            yield (e + 1) / (count + 1), step
        for j in range(len(self.orders)):

            def last(j=j):
                self.collect(j, self.me, -1, 0, self.outs[j])

            yield 1.0, last

    def finish(self):
        for k, hops, j, src, d in self.events:
            xyz = self.place.source(src)

            def run():
                self.up(j, xyz, k, d).wait_send()
                self.give(j, xyz).wait_send()

            when(self.place.exists(src), run)
        for j in range(len(self.orders)):
            self.give(j, self.me).wait_send()


class Share:
    def __init__(self, place, rows, ins, outs, scratch):
        self.place, self.rows, self.ins, self.outs = place, rows, ins, outs
        n = len(rows)
        self.first, self.second, self.sums = (scratch[i * n : (i + 1) * n] for i in range(3))
        self.send, self.recv = scratch[3 * n :]
        self.half = lax.rem(place.z, 2)
        self.over_y = place.link("y", 0)
        self.over_z = place.link("z", 1 - 2 * self.half)

    @staticmethod
    def scratch(rows):
        dma = pltpu.SemaphoreType.DMA
        out = []
        for slots in (8, 4, 4):
            out += [pltpu.VMEM((slots, n, 256), jnp.bfloat16) for n in rows]
        return out + [dma((len(rows), 12)), dma((len(rows), 12))]

    def block(self, j, t, y, half):
        n = self.rows[j]
        return self.ins[j].at[t, pl.ds(pl.multiple_of((y * 2 + half) * n, n), n), :]

    def early(self, j, t, s):
        if t < 2:
            src, device = self.block(j, t, 1 - self.place.y, s), self.over_y
        else:
            src, device = self.block(j, t, s, 1 - self.half), self.over_z
        i = t * 2 + s
        return remote(src, self.first[j].at[i], self.send.at[j, i], self.recv.at[j, i], device)

    def late(self, j, t):
        return remote(
            self.sums[j].at[t], self.second[j].at[t], self.send.at[j, 8 + t],
            self.recv.at[j, 8 + t], self.over_z if t < 2 else self.over_y,
        )

    def start(self):
        for j in range(len(self.rows)):
            for s in range(2):
                for t in range(4):
                    self.early(j, t, s).start()

    def steps(self):
        for j in range(len(self.rows)):
            for t in range(4):

                def pass_on(j=j, t=t):
                    for s in range(2):
                        self.early(j, t, s).wait_recv()
                    if t < 2:
                        away = 1 - self.half
                        mine = self.block(j, t, self.place.y, away)
                    else:
                        away = 1 - self.place.y
                        mine = self.block(j, t, away, self.half)
                    add_rows(
                        self.sums[j].at[t], [mine, self.first[j].at[t * 2 + away]], self.rows[j]
                    )
                    self.late(j, t).start()

                yield 0.25, pass_on
        for j in range(len(self.rows)):
            for t in range(4):

                def total(j=j, t=t):
                    self.late(j, t).wait_recv()
                    kept = self.half if t < 2 else self.place.y
                    mine = self.block(j, t, self.place.y, self.half)
                    add_rows(
                        self.outs[j].at[t],
                        [mine, self.first[j].at[t * 2 + kept], self.second[j].at[t]],
                        self.rows[j],
                    )

                yield 0.5, total

    def finish(self):
        for j in range(len(self.rows)):
            for t in range(4):
                for s in range(2):
                    self.early(j, t, s).wait_send()
                self.late(j, t).wait_send()


def run_steps(parts):
    steps = []
    for plan, begin, length in parts:
        steps += [(begin + length * at, step) for at, step in plan.steps()]
    steps.sort(key=lambda s: s[0])
    for _, step in steps:
        step()


HBM = pl.BlockSpec(memory_space=pl.ANY)
INSIDE = pl.BlockSpec(memory_space=pltpu.VMEM)


def comm_call(kernel, name, number_id, ins, in_specs, outs, out_specs, scratch):
    return pl.pallas_call(
        kernel,
        out_shape=outs,
        in_specs=in_specs,
        out_specs=out_specs,
        scratch_shapes=scratch,
        compiler_params=pltpu.CompilerParams(
            collective_id=number_id, has_side_effects=True, vmem_limit_bytes=67043328
        ),
        name=name,
    )(*ins)


def gathered(a, order):
    if len(order) == 1:
        return jax.ShapeDtypeStruct((SIZES[order],) + a.shape, a.dtype)
    return jax.ShapeDtypeStruct((DEPTH, 8 * a.shape[0], a.shape[1]), a.dtype)


def gather(arrays, orders, name):
    count = len(arrays)
    rows = [a.shape[0] for a in arrays]

    def kernel(*refs):
        place = Place()
        ins, outs, sems = refs[:count], refs[count : 2 * count], refs[2 * count :]
        plan = Gather(place, orders, rows, ins, outs, sems)
        greet(place)
        plan.start()
        run_steps([(plan, 0.0, 1.0)])
        plan.finish()

    return comm_call(
        kernel, name, 1, arrays, [INSIDE] * count,
        [gathered(a, o) for a, o in zip(arrays, orders)], [HBM] * count,
        Gather.scratch(count),
    )


def scattered(arrays):
    return [
        jax.ShapeDtypeStruct((a.shape[1] // 8, a.shape[2]), jnp.float32) for a in arrays
    ]


def scatter_and_share(arrays, orders, shared, name):
    n, m = len(arrays), len(shared)
    rows = [a.shape[1] // 8 for a in arrays]
    own = [a.shape[1] // 4 for a in shared]
    room = Scatter.scratch(arrays, rows, orders)

    def kernel(*refs):
        place = Place()
        ins, outs, scratch = refs[: n + m], refs[n + m : 2 * (n + m)], refs[2 * (n + m) :]
        plan = Scatter(place, orders, rows, ins[:n], outs[:n], scratch[: len(room)])
        share = Share(place, own, ins[n:], outs[n:], scratch[len(room) :])
        greet(place)
        share.start()
        plan.start()
        run_steps([(plan, 0.0, 80.0), (share, 0.0, 80.0)])
        share.finish()
        plan.finish()

    return comm_call(
        kernel, name, 2, arrays + shared, [HBM] * n + [INSIDE] * m,
        scattered(arrays)
        + [jax.ShapeDtypeStruct((4, r, 256), jnp.bfloat16) for r in own],
        [INSIDE] * (n + m), room + Share.scratch(own),
    )


def scatter_and_rows(arrays, orders, rows_in, name):
    n, m = len(arrays), len(rows_in)
    rows = [a.shape[1] // 8 for a in arrays]
    room = Scatter.scratch(arrays, rows, orders)

    def kernel(*refs):
        place = Place()
        ins, outs, scratch = refs[: n + m], refs[n + m : 2 * (n + m)], refs[2 * (n + m) :]
        plan = Scatter(place, orders, rows, ins[:n], outs[:n], scratch[: len(room)])
        lines = Gather(
            place, ["z"] * m, [a.shape[0] for a in rows_in], ins[n:], outs[n:],
            scratch[len(room) :],
        )
        greet(place)
        lines.start()
        plan.start()
        run_steps([(plan, 0.0, 70.0), (lines, 0.0, 60.0)])
        lines.finish()
        plan.finish()

    return comm_call(
        kernel, name, 3, arrays + rows_in, [HBM] * n + [INSIDE] * m,
        scattered(arrays) + [gathered(a, "z") for a in rows_in],
        [INSIDE] * n + [HBM] * m, room + Gather.scratch(m),
    )


WIDTH = 1024
QROWS = 256
KEYS = 1024
ENC_ROWS = 512
SPAN = 1280
CHUNK = 128
VMEM_MOST = 64000000
ROWS_OF = (((0,), (0,)), ((), ()))
LAST = (((1,), (1,)), ((), ()))
PLAIN = (((1,), (0,)), ((), ()))


def mm(a, b, dims=PLAIN):
    return lax.dot_general(a, b, dims, preferred_element_type=jnp.float32)


def norm_rows(v, gain):
    return v * lax.rsqrt(jnp.mean(v * v, axis=-1, keepdims=True) + EPSILON) * gain


def norm_back(v, gain, e):
    r = lax.rsqrt(jnp.mean(v * v, axis=-1, keepdims=True) + EPSILON)
    ev = e * v
    gain_grad = jnp.sum(ev * r, axis=0, keepdims=True)
    back = r * gain * e - v * (r * r * r) * jnp.mean(ev * gain, axis=-1, keepdims=True)
    return back, gain_grad


def head_rows(cols, a):
    return jnp.concatenate(
        [cols[:, a * 128 : a * 128 + 64], cols[:, a * 128 + 64 : a * 128 + 128]], axis=0
    )


def attend(q, kv, p_ref, s_ref, ot_ref, keys, add_bias):
    for a in range(2):
        q2 = head_rows(q, a)
        k = kv[:, a * 64 : a * 64 + 64]
        v = kv[:, 128 + a * 64 : 192 + a * 64]
        if add_bias is not None:
            add_bias(a, None, None)
        peak = None
        for c in range(keys // CHUNK):
            rows = pl.ds(c * CHUNK, CHUNK)
            s = mm(k[c * CHUNK : (c + 1) * CHUNK], q2, LAST)
            if add_bias is not None:
                s = add_bias(a, c, s)
            s_ref[rows, :] = s
            top = jnp.max(s, axis=0, keepdims=True)
            peak = top if peak is None else jnp.maximum(peak, top)
        total = jnp.zeros_like(peak)
        for c in range(keys // CHUNK):
            rows = pl.ds(c * CHUNK, CHUNK)
            e = jnp.exp(s_ref[rows, :] - peak)
            s_ref[rows, :] = e
            total = total + jnp.sum(e, axis=0, keepdims=True)
        inverse = 1.0 / total
        for c in range(keys // CHUNK):
            rows = pl.ds(c * CHUNK, CHUNK)
            p_ref[0, a, rows, :] = (s_ref[rows, :] * inverse).astype(jnp.bfloat16)
        ot = mm(v, p_ref[0, a], ROWS_OF)
        ot_ref[a * 128 : a * 128 + 64, :] = ot[:, :QROWS]
        ot_ref[a * 128 + 64 : a * 128 + 128, :] = ot[:, QROWS:]
    return jnp.transpose(ot_ref[...]).astype(jnp.bfloat16)


def attend_back(q, kv, p_ref, do, dkv_ref, d_ref, ds_ref, qt_ref, keys, take_bias):
    for a in range(2):
        q2 = head_rows(q, a)
        do2 = head_rows(do, a)
        k = kv[:, a * 64 : a * 64 + 64]
        v = kv[:, 128 + a * 64 : 192 + a * 64]
        total = jnp.zeros((1, 2 * QROWS), jnp.float32)
        for c in range(keys // CHUNK):
            rows = pl.ds(c * CHUNK, CHUNK)
            dp = mm(v[c * CHUNK : (c + 1) * CHUNK], do2, LAST)
            d_ref[rows, :] = dp
            total = total + jnp.sum(
                dp * p_ref[0, a, rows, :].astype(jnp.float32), axis=0, keepdims=True
            )
        for c in range(keys // CHUNK):
            rows = pl.ds(c * CHUNK, CHUNK)
            ds = p_ref[0, a, rows, :].astype(jnp.float32) * (d_ref[rows, :] - total)
            if take_bias is not None:
                take_bias(a, c, ds)
            ds_ref[rows, :] = ds.astype(jnp.bfloat16)
        if take_bias is not None:
            take_bias(a, None, None)
        dkv_ref[0, :, a * 64 : a * 64 + 64] = mm(ds_ref[...], q2).astype(jnp.bfloat16)
        dkv_ref[0, :, 128 + a * 64 : 192 + a * 64] = mm(p_ref[0, a], do2).astype(jnp.bfloat16)
        qt = mm(k, ds_ref[...], ROWS_OF)
        qt_ref[a * 128 : a * 128 + 64, :] = qt[:, :QROWS]
        qt_ref[a * 128 + 64 : a * 128 + 128, :] = qt[:, QROWS:]
    return jnp.transpose(qt_ref[...]).astype(jnp.bfloat16)


def self_forward_kernel(
    info, table, x_ref, gain_ref, w_ref, wkv_ref, bucket_ref,
    x2_ref, h_ref, q_ref, kv_ref, p_ref, o_ref,
    h1_ref, s_ref, strip_ref, ot_ref,
):
    first = pl.multiple_of(info[0], QROWS)
    length = info[1]

    @pl.when(pl.program_id(0) == 0)
    def _():
        for c in range(KEYS // QROWS):
            rows = pl.ds(c * QROWS, QROWS)
            h1_ref[rows, :] = norm_rows(
                x_ref[rows, :].astype(jnp.float32), gain_ref[...]
            ).astype(jnp.bfloat16)
        x2_ref[...] = x_ref[pl.ds(first, QROWS), :].astype(jnp.float32)
        h_ref[...] = h1_ref[pl.ds(first, QROWS), :]

    kv = mm(h1_ref[...], wkv_ref[0]).astype(jnp.bfloat16)
    kv_ref[0] = kv
    q = mm(h1_ref[pl.ds(first, QROWS), :], w_ref[0, :, :QROWS]).astype(jnp.bfloat16)
    q_ref[0] = q
    lane = lax.broadcasted_iota(jnp.int32, (1, 2 * QROWS), 1)
    lane = jnp.where(lane < QROWS, lane, lane - QROWS)
    last_key = jnp.minimum(lane + first, length - 1)

    def add_bias(a, c, s):
        if c is None:
            for b in range(2):
                head = pl.program_id(0) * 4 + 2 * a + b
                bucket = bucket_ref[...]
                near = jnp.full((8, SPAN), table[BUCKETS - 1, head], jnp.float32)
                for i in range(BUCKETS - 1):
                    near = jnp.where(bucket == i, table[i, head], near)
                for g in range(16):
                    shift = (SPAN - (120 - 8 * g)) % SPAN
                    strip_ref[b, 8 * g : 8 * g + 8, :] = (
                        pltpu.roll(near, shift, 1) if shift else near
                    )
            return None
        cols = pl.ds(CHUNK * (7 - c), QROWS)
        bias = jnp.concatenate([strip_ref[0, :, cols], strip_ref[1, :, cols]], axis=1)
        key = lax.broadcasted_iota(jnp.int32, s.shape, 0) + c * CHUNK
        return jnp.where(key <= last_key, s + bias, MASKED)

    o = attend(q, kv, p_ref, s_ref, ot_ref, KEYS, add_bias)
    o_ref[0] = o
    x2_ref[...] += mm(o, w_ref[0, :, QROWS:], LAST)


def cross_forward_kernel(
    x2_ref, enc_ref, gain_ref, w_ref, wkv_ref,
    x3_ref, h_ref, q_ref, kv_ref, p_ref, o_ref,
    s_ref, ot_ref,
):
    @pl.when(pl.program_id(0) == 0)
    def _():
        x3_ref[...] = x2_ref[...]
        h_ref[...] = norm_rows(x2_ref[...], gain_ref[...]).astype(jnp.bfloat16)

    kv = mm(enc_ref[...], wkv_ref[0]).astype(jnp.bfloat16)
    kv_ref[0] = kv
    q = mm(h_ref[...], w_ref[0, :, :QROWS]).astype(jnp.bfloat16)
    q_ref[0] = q
    o = attend(q, kv, p_ref, s_ref, ot_ref, ENC_ROWS, None)
    o_ref[0] = o
    x3_ref[...] += mm(o, w_ref[0, :, QROWS:], LAST)


def feed_kernel(
    info, x3_ref, cot_ref, gain_ref, wg_ref, wu_ref, wo_ref,
    out_ref, g3_ref, gg_ref, gu_ref, go_ref, gn_ref,
    h_ref, ht_ref, g_ref, gt_ref, y_ref, dh_ref,
):
    step = pl.program_id(0)

    @pl.when(step == 0)
    def _():
        h = norm_rows(x3_ref[...], gain_ref[...]).astype(jnp.bfloat16)
        h_ref[...] = h
        ht_ref[...] = jnp.transpose(h)
        row = lax.broadcasted_iota(jnp.int32, (QROWS, 1), 0) + info[0]
        g4 = jnp.where(row < info[1], cot_ref[...].astype(jnp.float32), 0.0)
        g = g4.astype(jnp.bfloat16)
        g_ref[...] = g
        gt_ref[...] = jnp.transpose(g)
        y_ref[...] = x3_ref[...]
        dh_ref[...] = jnp.zeros_like(dh_ref)

    gate = mm(h_ref[...], wg_ref[0])
    up = mm(h_ref[...], wu_ref[0])
    root = math.sqrt(2.0 / math.pi)
    square = gate * gate
    th = jnp.tanh(root * (gate + 0.044715 * gate * square))
    half = 0.5 * (1.0 + th)
    gelu = gate * half
    slope = half + 0.5 * gate * (1.0 - th * th) * (root * (1.0 + 3 * 0.044715 * square))
    hidden = (gelu * up).astype(jnp.bfloat16)
    y_ref[...] += mm(hidden, wo_ref[0], LAST)
    go_ref[0] = mm(gt_ref[...], hidden).astype(jnp.bfloat16)
    dhid = mm(g_ref[...], wo_ref[0])
    dup = (dhid * gelu).astype(jnp.bfloat16)
    dgate = (dhid * up * slope).astype(jnp.bfloat16)
    gg_ref[0] = mm(ht_ref[...], dgate).astype(jnp.bfloat16)
    gu_ref[0] = mm(ht_ref[...], dup).astype(jnp.bfloat16)
    dh_ref[...] += mm(dgate, wg_ref[0], LAST) + mm(dup, wu_ref[0], LAST)

    @pl.when(step == pl.num_programs(0) - 1)
    def _():
        out_ref[...] = y_ref[...].astype(jnp.bfloat16)
        back, gain_grad = norm_back(x3_ref[...], gain_ref[...], dh_ref[...])
        g3_ref[...] = g_ref[...].astype(jnp.float32) + back
        gn_ref[...] = gain_grad


def cross_backward_kernel(
    g3_ref, x2_ref, h_ref, gain_ref, w_ref, q_ref, kv_ref, p_ref, o_ref,
    g2_ref, dkv_ref, gw_ref, gn_ref,
    g_ref, gt_ref, ht_ref, dh_ref, d_ref, ds_ref, qt_ref,
):
    step = pl.program_id(0)

    @pl.when(step == 0)
    def _():
        g = g3_ref[...].astype(jnp.bfloat16)
        g_ref[...] = g
        gt_ref[...] = jnp.transpose(g)
        ht_ref[...] = jnp.transpose(h_ref[...])
        dh_ref[...] = jnp.zeros_like(dh_ref)

    do = mm(g_ref[...], w_ref[0, :, QROWS:]).astype(jnp.bfloat16)
    gw_ref[0, :, QROWS:] = mm(gt_ref[...], o_ref[0]).astype(jnp.bfloat16)
    dq = attend_back(
        q_ref[0], kv_ref[0], p_ref, do, dkv_ref, d_ref, ds_ref, qt_ref, ENC_ROWS, None
    )
    gw_ref[0, :, :QROWS] = mm(ht_ref[...], dq).astype(jnp.bfloat16)
    dh_ref[...] += mm(dq, w_ref[0, :, :QROWS], LAST)

    @pl.when(step == pl.num_programs(0) - 1)
    def _():
        back, gain_grad = norm_back(x2_ref[...], gain_ref[...], dh_ref[...])
        g2_ref[...] = g3_ref[...] + back
        gn_ref[...] = gain_grad


def self_backward_kernel(
    g2_ref, h_ref, w_ref, q_ref, kv_ref, p_ref, o_ref,
    dh_ref, dkv_ref, gw_ref, near_ref,
    g_ref, gt_ref, ht_ref, d_ref, ds_ref, qt_ref, strip_ref,
):
    @pl.when(pl.program_id(0) == 0)
    def _():
        g = g2_ref[...].astype(jnp.bfloat16)
        g_ref[...] = g
        gt_ref[...] = jnp.transpose(g)
        ht_ref[...] = jnp.transpose(h_ref[...])
        dh_ref[...] = jnp.zeros_like(dh_ref)

    def take_bias(a, c, ds):
        if c is None:
            for b in range(2):
                total = jnp.zeros((8, SPAN), jnp.float32)
                for g in range(16):
                    part = strip_ref[b, 8 * g : 8 * g + 8, :]
                    shift = 120 - 8 * g
                    total = total + (pltpu.roll(part, shift, 1) if shift else part)
                near_ref[0, 2 * a + b] = total
            return
        if c == 0:
            strip_ref[...] = jnp.zeros_like(strip_ref)
        cols = pl.ds(CHUNK * (7 - c), QROWS)
        strip_ref[0, :, cols] += ds[:, :QROWS]
        strip_ref[1, :, cols] += ds[:, QROWS:]

    do = mm(g_ref[...], w_ref[0, :, QROWS:]).astype(jnp.bfloat16)
    gw_ref[0, :, QROWS:] = mm(gt_ref[...], o_ref[0]).astype(jnp.bfloat16)
    dq = attend_back(
        q_ref[0], kv_ref[0], p_ref, do, dkv_ref, d_ref, ds_ref, qt_ref, KEYS, take_bias
    )
    gw_ref[0, :, :QROWS] = mm(ht_ref[...], dq).astype(jnp.bfloat16)
    dh_ref[...] += mm(dq, w_ref[0, :, :QROWS], LAST)


def last_kernel(
    dh_part_ref, dkv_ref, x_ref, h_ref, gain_ref, g2_ref, ws_ref, wc_ref, dkvc_ref, enc_ref,
    gx_ref, genc_ref, gw_ref, gn_ref,
    ht_ref, et_ref, dh_ref, de_ref,
):
    step = pl.program_id(0)

    @pl.when(step == 0)
    def _():
        ht_ref[...] = jnp.transpose(h_ref[...])
        et_ref[...] = jnp.transpose(enc_ref[...])
        dh_ref[...] = dh_part_ref[...]
        de_ref[...] = jnp.zeros_like(de_ref)

    dkv = dkv_ref[0]
    dkvc = dkvc_ref[0]
    gw_ref[0, :, :QROWS] = mm(ht_ref[...], dkv).astype(jnp.bfloat16)
    gw_ref[0, :, QROWS:] = mm(et_ref[...], dkvc).astype(jnp.bfloat16)
    dh_ref[...] += mm(dkv, ws_ref[0], LAST)
    de_ref[...] += mm(dkvc, wc_ref[0], LAST)

    @pl.when(step == pl.num_programs(0) - 1)
    def _():
        back, gain_grad = norm_back(
            x_ref[...].astype(jnp.float32), gain_ref[...], dh_ref[...]
        )
        gx_ref[...] = (g2_ref[...] + back).astype(jnp.bfloat16)
        genc_ref[...] = de_ref[...].astype(jnp.bfloat16)
        gn_ref[...] = gain_grad


def whole(shape):
    zeros = (0,) * len(shape)
    return pl.BlockSpec(shape, lambda t: zeros)


def part(shape, column=0):
    tail = (0,) * (len(shape) - 2)
    return pl.BlockSpec(shape, lambda t: (t,) + tail + (column,))


SCALARS = pl.BlockSpec(memory_space=pltpu.SMEM)
F32 = jnp.float32
LOW = jnp.bfloat16


def run_heads(kernel, name, ins, specs, outs, out_specs, scratch, flops, steps=4):
    moved = sum(math.prod(a.shape) * a.dtype.itemsize for a in list(ins) + list(outs))
    return pl.pallas_call(
        kernel,
        grid=(steps,),
        in_specs=specs,
        out_specs=out_specs,
        out_shape=outs,
        scratch_shapes=scratch,
        compiler_params=pltpu.CompilerParams(
            dimension_semantics=("arbitrary",), vmem_limit_bytes=VMEM_MOST
        ),
        cost_estimate=pl.CostEstimate(flops=flops, bytes_accessed=moved, transcendentals=0),
        name=name,
    )(*ins)


def shape_of(shape, dtype):
    return jax.ShapeDtypeStruct(shape, dtype)


def self_forward(info, x, gain, w1, w3, table, bucket):
    return run_heads(
        self_forward_kernel, "self_forward",
        (info, table, x, gain, w1, w3, bucket),
        [SCALARS, SCALARS, whole((KEYS, WIDTH)), whole((1, WIDTH)), part((1, WIDTH, 512)),
         part((1, WIDTH, 256)), whole((8, SPAN))],
        [shape_of((QROWS, WIDTH), F32), shape_of((QROWS, WIDTH), LOW),
         shape_of((4, QROWS, 256), LOW), shape_of((4, KEYS, 256), LOW),
         shape_of((4, 2, KEYS, 512), LOW), shape_of((4, QROWS, 256), LOW)],
        [whole((QROWS, WIDTH)), whole((QROWS, WIDTH)), part((1, QROWS, 256)),
         part((1, KEYS, 256)), part((1, 2, KEYS, 512)), part((1, QROWS, 256))],
        [pltpu.VMEM((KEYS, WIDTH), LOW), pltpu.VMEM((KEYS, 512), F32),
         pltpu.VMEM((2, CHUNK, SPAN), F32), pltpu.VMEM((256, QROWS), F32)],
        5 * 10**9,
    )


def cross_forward(x2, enc, gain, w2, w3):
    return run_heads(
        cross_forward_kernel, "cross_forward",
        (x2, enc, gain, w2, w3),
        [whole((QROWS, WIDTH)), whole((ENC_ROWS, WIDTH)), whole((1, WIDTH)),
         part((1, WIDTH, 512)), part((1, WIDTH, 256), 1)],
        [shape_of((QROWS, WIDTH), F32), shape_of((QROWS, WIDTH), LOW),
         shape_of((4, QROWS, 256), LOW), shape_of((4, ENC_ROWS, 256), LOW),
         shape_of((4, 2, ENC_ROWS, 512), LOW), shape_of((4, QROWS, 256), LOW)],
        [whole((QROWS, WIDTH)), whole((QROWS, WIDTH)), part((1, QROWS, 256)),
         part((1, ENC_ROWS, 256)), part((1, 2, ENC_ROWS, 512)), part((1, QROWS, 256))],
        [pltpu.VMEM((ENC_ROWS, 512), F32), pltpu.VMEM((256, QROWS), F32)],
        3 * 10**9,
    )


def feed(info, x3, cot, gain, wg, wu, wo):
    units = wg.shape[2]
    wide = part((1, WIDTH, units))
    return run_heads(
        feed_kernel, "feed",
        (info, x3, cot, gain, wg, wu, wo),
        [SCALARS, whole((QROWS, WIDTH)), whole((QROWS, WIDTH)), whole((1, WIDTH)),
         wide, wide, wide],
        [shape_of((QROWS, WIDTH), LOW), shape_of((QROWS, WIDTH), F32)]
        + [shape_of((4, WIDTH, units), LOW)] * 3
        + [shape_of((1, WIDTH), F32)],
        [whole((QROWS, WIDTH)), whole((QROWS, WIDTH)), wide, wide, wide, whole((1, WIDTH))],
        [pltpu.VMEM((QROWS, WIDTH), LOW), pltpu.VMEM((WIDTH, QROWS), LOW),
         pltpu.VMEM((QROWS, WIDTH), LOW), pltpu.VMEM((WIDTH, QROWS), LOW),
         pltpu.VMEM((QROWS, WIDTH), F32), pltpu.VMEM((QROWS, WIDTH), F32)],
        13 * 10**9,
    )


def cross_backward(g3, x2, h, gain, w2, q, kv, p, o):
    return run_heads(
        cross_backward_kernel, "cross_backward",
        (g3, x2, h, gain, w2, q, kv, p, o),
        [whole((QROWS, WIDTH)), whole((QROWS, WIDTH)), whole((QROWS, WIDTH)),
         whole((1, WIDTH)), part((1, WIDTH, 512)), part((1, QROWS, 256)),
         part((1, ENC_ROWS, 256)), part((1, 2, ENC_ROWS, 512)), part((1, QROWS, 256))],
        [shape_of((QROWS, WIDTH), F32), shape_of((4, ENC_ROWS, 256), LOW),
         shape_of((4, WIDTH, 512), LOW), shape_of((1, WIDTH), F32)],
        [whole((QROWS, WIDTH)), part((1, ENC_ROWS, 256)), part((1, WIDTH, 512)),
         whole((1, WIDTH))],
        [pltpu.VMEM((QROWS, WIDTH), LOW), pltpu.VMEM((WIDTH, QROWS), LOW),
         pltpu.VMEM((WIDTH, QROWS), LOW), pltpu.VMEM((QROWS, WIDTH), F32),
         pltpu.VMEM((ENC_ROWS, 512), F32), pltpu.VMEM((ENC_ROWS, 512), LOW),
         pltpu.VMEM((256, QROWS), F32)],
        5 * 10**9,
    )


def self_backward(g2, h, w1, q, kv, p, o):
    return run_heads(
        self_backward_kernel, "self_backward",
        (g2, h, w1, q, kv, p, o),
        [whole((QROWS, WIDTH)), whole((QROWS, WIDTH)), part((1, WIDTH, 512)),
         part((1, QROWS, 256)), part((1, KEYS, 256)), part((1, 2, KEYS, 512)),
         part((1, QROWS, 256))],
        [shape_of((QROWS, WIDTH), F32), shape_of((4, KEYS, 256), LOW),
         shape_of((4, WIDTH, 512), LOW), shape_of((4, 4, 8, SPAN), F32)],
        [whole((QROWS, WIDTH)), part((1, KEYS, 256)), part((1, WIDTH, 512)),
         part((1, 4, 8, SPAN))],
        [pltpu.VMEM((QROWS, WIDTH), LOW), pltpu.VMEM((WIDTH, QROWS), LOW),
         pltpu.VMEM((WIDTH, QROWS), LOW), pltpu.VMEM((KEYS, 512), F32),
         pltpu.VMEM((KEYS, 512), LOW), pltpu.VMEM((256, QROWS), F32),
         pltpu.VMEM((2, CHUNK, SPAN), F32)],
        6 * 10**9,
    )


def last_grads(dh, dkv, x, h, gain, g2, w3, dkvc, enc):
    rows = enc.shape[0]
    return run_heads(
        last_kernel, "last_grads",
        (dh, dkv, x, h, gain, g2, w3, w3, dkvc, enc),
        [whole((QROWS, WIDTH)), part((1, QROWS, 256)), whole((QROWS, WIDTH)),
         whole((QROWS, WIDTH)), whole((1, WIDTH)), whole((QROWS, WIDTH)),
         part((1, WIDTH, 256)), part((1, WIDTH, 256), 1), part((1, rows, 256)),
         whole((rows, WIDTH))],
        [shape_of((QROWS, WIDTH), LOW), shape_of((rows, WIDTH), LOW),
         shape_of((4, WIDTH, 512), LOW), shape_of((1, WIDTH), F32)],
        [whole((QROWS, WIDTH)), whole((rows, WIDTH)), part((1, WIDTH, 512)),
         whole((1, WIDTH))],
        [pltpu.VMEM((WIDTH, QROWS), LOW), pltpu.VMEM((WIDTH, rows), LOW),
         pltpu.VMEM((QROWS, WIDTH), F32), pltpu.VMEM((rows, WIDTH), F32)],
        3 * 10**9,
    )


GATHER_ORDERS = ("yzx", "yzx", "zxy", "yxz", "zxy", "zxy", "zxy")
FEED_ORDERS = ("xzy", "zyx", "yzx")
HEAD_ORDERS = ("zyx", "zxy", "zyx", "zxy")
SMALL_ROWS = 16
LANES = 128


def small_rows(gains, table):
    flat = jnp.pad(table.reshape(1, -1).astype(F32), ((0, 0), (0, LANES - table.size)))
    rows = jnp.concatenate([g.reshape(1, LANES).astype(F32) for g in gains] + [flat], axis=0)
    return jnp.pad(rows, ((0, SMALL_ROWS - 4), (0, 0)))


def rows_along_tp(own, t):
    found = [own]
    for k in range(1, DEPTH):
        found.append(lax.ppermute(own, "tp", [(i, (i + k) % DEPTH) for i in range(DEPTH)]))
    found = jnp.stack(found)
    return jnp.stack(
        [lax.dynamic_index_in_dim(found, (t - i + DEPTH) % DEPTH, 0, False) for i in range(DEPTH)]
    )


def tokens_split(
    inputs, encoder, lengths, cotangent,
    norm_self, self_query, self_key_matrix, self_value_matrix, self_out, bias_table,
    norm_cross, cross_query, cross_key_matrix, cross_value_matrix, cross_out,
    norm_feed, feed_gate, feed_up, feed_out,
):
    y = lax.axis_index("ctx")
    t = lax.axis_index("tp")
    seq, half = lax.div(t, 2), lax.rem(t, 2)
    first = y * (2 * QROWS) + half * QROWS
    info = jnp.stack([first, lax.dynamic_index_in_dim(lengths, seq, 0, False)])
    x_seq = lax.dynamic_index_in_dim(inputs, seq, 0, False)
    enc_seq = lax.dynamic_index_in_dim(encoder, seq, 0, False)
    x_own = lax.dynamic_slice_in_dim(x_seq, half * QROWS, QROWS, 0)
    cot = lax.dynamic_slice(cotangent, (seq, half * QROWS, 0), (1, QROWS, WIDTH))[0]
    packed = (
        feed_gate, feed_up, feed_out,
        jnp.concatenate([self_query, self_out], axis=1),
        jnp.concatenate([cross_query, cross_out], axis=1),
        jnp.concatenate(
            [self_key_matrix, self_value_matrix, cross_key_matrix, cross_value_matrix], axis=1
        ),
        small_rows((norm_self, norm_cross, norm_feed), bias_table),
        x_seq, enc_seq,
    )
    wg, wu, wo, w1, w2, w3, small, x_all, enc_all = gather(
        packed, GATHER_ORDERS + ("y", "y"), "gather_weights"
    )
    small = small.reshape(4, 8, SMALL_ROWS, LANES)
    gains = jnp.transpose(small[0, :, :3], (1, 0, 2)).reshape(3, 1, WIDTH)
    table = jnp.transpose(
        small[:, :, 3, :16].reshape(4, 8, 4, 4), (1, 2, 0, 3)
    ).reshape(BUCKETS, 16)
    x_all = x_all.reshape(KEYS, WIDTH)
    enc_all = enc_all.reshape(ENC_ROWS, WIDTH)

    distance = jnp.maximum(
        first + jnp.arange(SPAN)[None, :] - (SPAN - 264) - jnp.arange(8)[:, None], 0
    )
    bucket = bucket_index(distance)
    x2, h1, q1, kv1, p1, o1 = self_forward(info, x_all, gains[0], w1, w3, table, bucket)
    x3, h2, q2, kv2, p2, o2 = cross_forward(x2, enc_all, gains[1], w2, w3)
    out, g3, gg, gu, go, gn3 = feed(info, x3, cot, gains[2], wg, wu, wo)
    out = rows_along_tp(out, t)
    g2, dkv2, gw2, gn2 = cross_backward(g3, x2, h2, gains[1], w2, q2, kv2, p2, o2)
    dh, dkv1, gw1, near = self_backward(g2, h1, w1, q1, kv1, p1, o1)
    gg, gu, go, dkv, dkvc = scatter_and_share(
        (gg, gu, go), FEED_ORDERS, (dkv1, dkv2), "scatter_feed"
    )
    enc_own = lax.dynamic_slice_in_dim(enc_seq, half * (QROWS // 2), QROWS // 2, 0)
    gx, genc, gw3, gn1 = last_grads(
        dh, dkv, x_own, h1, gains[0], g2, w3, dkvc, enc_own
    )
    one_hot = (bucket[:, :, None] == jnp.arange(BUCKETS, dtype=jnp.int32)).astype(F32)
    grad_table = jnp.einsum(
        "hrm,rmb->bh", near.reshape(16, 8, SPAN), one_hot, precision=TOP_PRECISION
    )
    gain_grads = jnp.concatenate([gn1, gn2, gn3], axis=0).reshape(3, 8, LANES)
    gain_grads = jnp.broadcast_to(jnp.transpose(gain_grads, (1, 0, 2))[None], (4, 8, 3, LANES))
    table_grads = jnp.transpose(grad_table.reshape(8, 4, 4, 4), (2, 0, 1, 3)).reshape(4, 8, 1, 16)
    table_grads = jnp.pad(table_grads, ((0, 0), (0, 0), (0, 0), (0, LANES - 16)))
    small_grads = jnp.pad(
        jnp.concatenate([gain_grads, table_grads], axis=2),
        ((0, 0), (0, 0), (0, SMALL_ROWS - 4), (0, 0)),
    ).reshape(4, 8 * SMALL_ROWS, LANES)
    gw1, gw2, gw3, gs, gx, genc = scatter_and_rows(
        (gw1, gw2, gw3, small_grads), HEAD_ORDERS, (gx, genc), "scatter_heads"
    )
    return (
        out.reshape(inputs.shape),
        gx.reshape(inputs.shape).astype(F32),
        genc.reshape(encoder.shape).astype(F32),
        gs[0], gw1[:, :256], gw3[:, :128], gw3[:, 128:256], gw1[:, 256:],
        gs[3, :16].reshape(4, 4),
        gs[1], gw2[:, :256], gw3[:, 256:384], gw3[:, 384:], gw2[:, 256:],
        gs[2], gg, gu, go,
    )


def solution(mesh):
    sizes = (mesh.shape["fsdp"], mesh.shape["ctx"], mesh.shape["tp"])
    return jax.shard_map(
        tokens_split if sizes == (4, 2, DEPTH) else shards,
        mesh=mesh,
        in_specs=(
            P("fsdp", "ctx", None),
            P("fsdp", "ctx", None),
            P("fsdp"),
            P("fsdp", "ctx", None),
            P(("fsdp", "ctx")),
            P(("fsdp", "ctx"), "tp"),
            P(("fsdp", "ctx"), "tp"),
            P(("fsdp", "ctx"), "tp"),
            P(("fsdp", "ctx"), "tp"),
            P(("fsdp", "ctx"), "tp"),
            P(("fsdp", "ctx")),
            P(("fsdp", "ctx"), "tp"),
            P(("fsdp", "ctx"), "tp"),
            P(("fsdp", "ctx"), "tp"),
            P(("fsdp", "ctx"), "tp"),
            P(("fsdp", "ctx")),
            P(("fsdp", "ctx"), "tp"),
            P(("fsdp", "ctx"), "tp"),
            P(("fsdp", "ctx"), "tp"),
        ),
        out_specs=(
            P("fsdp", "ctx", None),
            P("fsdp", "ctx", None),
            P("fsdp", "ctx", None),
            P(("fsdp", "ctx")),
            P(("fsdp", "ctx"), "tp"),
            P(("fsdp", "ctx"), "tp"),
            P(("fsdp", "ctx"), "tp"),
            P(("fsdp", "ctx"), "tp"),
            P(("fsdp", "ctx"), "tp"),
            P(("fsdp", "ctx")),
            P(("fsdp", "ctx"), "tp"),
            P(("fsdp", "ctx"), "tp"),
            P(("fsdp", "ctx"), "tp"),
            P(("fsdp", "ctx"), "tp"),
            P(("fsdp", "ctx")),
            P(("fsdp", "ctx"), "tp"),
            P(("fsdp", "ctx"), "tp"),
            P(("fsdp", "ctx"), "tp"),
        ),
        check_vma=False,
    )
```

```python
import functools
import math

import jax
import jax.numpy as jnp
from jax import lax
from jax.experimental import pallas as pl
from jax.experimental.pallas import tpu as pltpu
from jax.sharding import PartitionSpec as P

HEAD_SIZE = 64
BUCKETS = 32
MAXDIST = 128


EPSILON = 1e-06
MASKED = -1000000000.0
TOP_PRECISION = lax.Precision.HIGHEST


def rms_scale(values, gain_row):
    inverse = lax.rsqrt(jnp.mean(values * values, axis=-1, keepdims=True) + EPSILON)
    return values * inverse * gain_row


def gated_product(gate_in, up_in):
    return jax.nn.gelu(gate_in, approximate=True) * up_in


def project(operand_array, weight_arrays):
    return jnp.einsum(
        "spd,dk->spk", operand_array, weight_arrays, preferred_element_type=jnp.float32
    )


def project_back(grad_cols, weight_arrays):
    return jnp.einsum("spk,dk->spd", grad_cols, weight_arrays, preferred_element_type=jnp.float32)


def weight_grad(operand_array, grad_cols):
    return jnp.einsum("spd,spk->dk", operand_array, grad_cols, preferred_element_type=jnp.float32)


def bucket_index(distance):
    exact_count = BUCKETS // 2
    counter = jnp.zeros(distance.shape, jnp.int32)
    for level_index in range(1, BUCKETS - exact_count):
        border = math.ceil(
            exact_count * (MAXDIST / exact_count) ** (level_index / (BUCKETS - exact_count))
        )
        counter = counter + (distance >= border).astype(jnp.int32)
    return jnp.where(distance < exact_count, distance, exact_count + counter)


def reduce_rows(partial_sum):
    return lax.psum(partial_sum, "tp")


def block_scores(queries, key_rows, bias_rows, allowed):
    scores = jnp.einsum("gpkrd,gjkd->gkrpj", queries, key_rows, preferred_element_type=jnp.float32)
    if bias_rows is not None:
        scores = jnp.where(allowed[:, None, None], scores + bias_rows[None], MASKED)
    return scores


def forward_block(queries, key_rows, value_rows, bias_rows, allowed):
    scores = block_scores(queries, key_rows, bias_rows, allowed)
    row_peak = jnp.max(scores, axis=-1, keepdims=True)
    log_total = row_peak + jnp.log(jnp.sum(jnp.exp(scores - row_peak), axis=-1, keepdims=True))
    weights_low = jnp.exp(scores - log_total).astype(jnp.bfloat16)
    output = jnp.einsum(
        "gkrpj,gjkd->gpkrd", weights_low, value_rows, preferred_element_type=jnp.float32
    )
    return (output.astype(jnp.bfloat16), log_total)


def backward_block(queries, key_rows, value_rows, bias_rows, allowed, log_total, grad_out):
    scores = block_scores(queries, key_rows, bias_rows, allowed)
    softmax_rows = jnp.exp(scores - log_total)
    grad_probs = jnp.einsum(
        "gpkrd,gjkd->gkrpj", grad_out, value_rows, preferred_element_type=jnp.float32
    )
    grad_scores = softmax_rows * (
        grad_probs - jnp.sum(grad_probs * softmax_rows, axis=-1, keepdims=True)
    )
    scores_low = grad_scores.astype(jnp.bfloat16)
    grad_query = jnp.einsum(
        "gkrpj,gjkd->gpkrd", scores_low, key_rows, preferred_element_type=jnp.float32
    )
    grad_key = jnp.einsum(
        "gkrpj,gpkrd->gjkd", scores_low, queries, preferred_element_type=jnp.float32
    )
    grad_value = jnp.einsum(
        "gkrpj,gpkrd->gjkd",
        softmax_rows.astype(jnp.bfloat16),
        grad_out,
        preferred_element_type=jnp.float32,
    )
    if bias_rows is None:
        grad_bias = jnp.zeros((1,), jnp.float32)
    else:
        grad_bias = jnp.sum(grad_scores, axis=0)
    return (grad_query.astype(jnp.bfloat16), grad_key, grad_value, grad_bias)


def block_shapes(queries, key_rows, block_seqs):
    seq_count, row_total_count, query_cols = queries.shape
    key_total_count, key_cols = (key_rows.shape[1], key_rows.shape[2])
    kv_heads = key_cols // HEAD_SIZE
    repeats = query_cols // key_cols
    blocks = seq_count // block_seqs
    query_shape = (blocks, block_seqs, row_total_count, kv_heads, repeats, HEAD_SIZE)
    key_shape = (blocks, block_seqs, key_total_count, kv_heads, HEAD_SIZE)
    mask_shape = (blocks, block_seqs, row_total_count, key_total_count)
    return (query_shape, key_shape, mask_shape)


def attention_forward(queries, key_rows, value_rows, bias_rows, allowed, block_seqs):
    query_shape, key_shape, mask_shape = block_shapes(queries, key_rows, block_seqs)
    sources = (
        queries.reshape(query_shape),
        key_rows.reshape(key_shape),
        value_rows.reshape(key_shape),
    )
    if allowed is not None:
        sources = sources + (allowed.reshape(mask_shape),)

    def one_block(piece_list):
        mask_block = piece_list[3] if allowed is not None else None
        return forward_block(piece_list[0], piece_list[1], piece_list[2], bias_rows, mask_block)

    outputs, log_totals = lax.map(one_block, sources)
    return (outputs.reshape(queries.shape), log_totals)


def attention_backward(
    queries, key_rows, value_rows, bias_rows, allowed, log_totals, grad_out, block_seqs
):
    query_shape, key_shape, mask_shape = block_shapes(queries, key_rows, block_seqs)
    sources = (
        queries.reshape(query_shape),
        key_rows.reshape(key_shape),
        value_rows.reshape(key_shape),
        log_totals,
        grad_out.reshape(query_shape),
    )
    if allowed is not None:
        sources = sources + (allowed.reshape(mask_shape),)
    if bias_rows is None:
        initial = jnp.zeros((1,), jnp.float32)
    else:
        initial = jnp.zeros(bias_rows.shape, jnp.float32)

    def one_block(running, piece_list):
        mask_block = piece_list[5] if allowed is not None else None
        grad_query, grad_key, grad_value, grad_bias = backward_block(
            piece_list[0],
            piece_list[1],
            piece_list[2],
            bias_rows,
            mask_block,
            piece_list[3],
            piece_list[4],
        )
        return (running + grad_bias, (grad_query, grad_key, grad_value))

    bias_total, grad_list = lax.scan(one_block, initial, sources)
    return (
        grad_list[0].reshape(queries.shape),
        grad_list[1].reshape(key_rows.shape),
        grad_list[2].reshape(value_rows.shape),
        bias_total,
    )


def shards(
    inputs,
    encoder,
    lengths,
    cotangent,
    norm_self,
    self_query,
    self_key_matrix,
    self_value_matrix,
    self_out,
    bias_table,
    norm_cross,
    cross_query,
    cross_key_matrix,
    cross_value_matrix,
    cross_out,
    norm_feed,
    feed_gate,
    feed_up,
    feed_out,
):
    self_group = (
        lax.all_gather(norm_self, ("fsdp", "ctx"), axis=0, tiled=True),
        lax.all_gather(self_query, ("fsdp", "ctx"), axis=0, tiled=True),
        lax.all_gather(self_key_matrix, ("fsdp", "ctx"), axis=0, tiled=True),
        lax.all_gather(self_value_matrix, ("fsdp", "ctx"), axis=0, tiled=True),
        lax.all_gather(self_out, ("fsdp", "ctx"), axis=0, tiled=True),
        lax.all_gather(bias_table, ("fsdp", "ctx"), axis=0, tiled=True),
    )
    seq_count, row_total_count = (inputs.shape[0], inputs.shape[1])
    block_seqs = max((trial for trial in (1, 2, 3, 4) if seq_count % trial == 0))
    start_row = lax.axis_index("ctx") * row_total_count
    key_total_count = row_total_count * lax.axis_size("ctx")
    row_pos = start_row + jnp.arange(row_total_count, dtype=jnp.int32)
    col_pos = jnp.arange(key_total_count, dtype=jnp.int32)
    buckets = bucket_index(jnp.maximum(row_pos[:, None] - col_pos[None, :], 0))
    one_hot = (buckets[:, :, None] == jnp.arange(BUCKETS, dtype=jnp.int32)[None, None, :]).astype(
        jnp.float32
    )
    causal = col_pos[None, :] <= row_pos[:, None]
    allowed = causal[None] & (col_pos[None, None, :] < lengths[:, None, None])
    hidden_in = inputs.astype(jnp.float32)
    normed_one, norm_pull_one = jax.vjp(rms_scale, hidden_in, self_group[0].astype(jnp.float32))
    self_in = normed_one.astype(jnp.bfloat16)
    self_q = project(self_in, self_group[1]).astype(jnp.bfloat16)
    self_k = project(self_in, self_group[2]).astype(jnp.bfloat16)
    self_v = project(self_in, self_group[3]).astype(jnp.bfloat16)
    keys_self, values_self = (
        lax.all_gather(self_k, "ctx", axis=1, tiled=True),
        lax.all_gather(self_v, "ctx", axis=1, tiled=True),
    )
    heads_local = self_group[1].shape[1] // HEAD_SIZE
    kv_local = self_group[2].shape[1] // HEAD_SIZE
    table_rows = self_group[5].astype(jnp.float32)
    bias_rows = jnp.einsum("ijb,bh->hij", one_hot, table_rows, precision=TOP_PRECISION).reshape(
        kv_local, heads_local // kv_local, row_total_count, key_total_count
    )
    self_att, lse_self = attention_forward(
        self_q, keys_self, values_self, bias_rows, allowed, block_seqs
    )
    hidden_two = hidden_in + reduce_rows(project_back(self_att, self_group[4]))
    cross_group = (
        lax.all_gather(norm_cross, ("fsdp", "ctx"), axis=0, tiled=True),
        lax.all_gather(cross_query, ("fsdp", "ctx"), axis=0, tiled=True),
        lax.all_gather(cross_key_matrix, ("fsdp", "ctx"), axis=0, tiled=True),
        lax.all_gather(cross_value_matrix, ("fsdp", "ctx"), axis=0, tiled=True),
        lax.all_gather(cross_out, ("fsdp", "ctx"), axis=0, tiled=True),
    )
    normed_two, norm_pull_two = jax.vjp(rms_scale, hidden_two, cross_group[0].astype(jnp.float32))
    cross_in = normed_two.astype(jnp.bfloat16)
    cross_q = project(cross_in, cross_group[1]).astype(jnp.bfloat16)
    enc_keys = project(encoder, cross_group[2]).astype(jnp.bfloat16)
    enc_values = project(encoder, cross_group[3]).astype(jnp.bfloat16)
    keys_cross, values_cross = (
        lax.all_gather(enc_keys, "ctx", axis=1, tiled=True),
        lax.all_gather(enc_values, "ctx", axis=1, tiled=True),
    )
    cross_att, lse_cross = attention_forward(
        cross_q, keys_cross, values_cross, None, None, block_seqs
    )
    hidden_three = hidden_two + reduce_rows(project_back(cross_att, cross_group[4]))
    feed_group = (
        lax.all_gather(norm_feed, ("fsdp", "ctx"), axis=0, tiled=True),
        lax.all_gather(feed_gate, ("fsdp", "ctx"), axis=0, tiled=True),
        lax.all_gather(feed_up, ("fsdp", "ctx"), axis=0, tiled=True),
        lax.all_gather(feed_out, ("fsdp", "ctx"), axis=0, tiled=True),
    )
    normed_three, norm_pull_three = jax.vjp(
        rms_scale, hidden_three, feed_group[0].astype(jnp.float32)
    )
    feed_in = normed_three.astype(jnp.bfloat16)
    gate_value = project(feed_in, feed_group[1])
    up_value = project(feed_in, feed_group[2])
    gated_value, gated_pull = jax.vjp(gated_product, gate_value, up_value)
    feed_hidden = gated_value.astype(jnp.bfloat16)
    hidden_four = hidden_three + reduce_rows(project_back(feed_hidden, feed_group[3]))
    output = hidden_four.astype(jnp.bfloat16)
    valid_rows = (row_pos[None, :] < lengths[:, None]).astype(jnp.float32)
    grad_full = cotangent.astype(jnp.float32) * valid_rows[:, :, None]
    branch_low = grad_full.astype(jnp.bfloat16)
    grad_hidden = grad_full
    grad_feed_out = weight_grad(branch_low, feed_hidden)
    grad_gated = project(branch_low, feed_group[3])
    grad_gate, grad_up = gated_pull(grad_gated)
    gate_low = grad_gate.astype(jnp.bfloat16)
    up_low = grad_up.astype(jnp.bfloat16)
    grad_feed_gate = weight_grad(feed_in, gate_low)
    grad_feed_up = weight_grad(feed_in, up_low)
    grad_feed_in = reduce_rows(
        project_back(gate_low, feed_group[1]) + project_back(up_low, feed_group[2])
    )
    grad_three, grad_gain_three = norm_pull_three(grad_feed_in)
    grad_hidden = grad_hidden + grad_three
    feed_grads = (
        lax.psum_scatter(
            grad_gain_three.astype(jnp.bfloat16), ("fsdp", "ctx"), scatter_dimension=0, tiled=True
        ).astype(jnp.float32),
        lax.psum_scatter(
            grad_feed_gate.astype(jnp.bfloat16), ("fsdp", "ctx"), scatter_dimension=0, tiled=True
        ).astype(jnp.float32),
        lax.psum_scatter(
            grad_feed_up.astype(jnp.bfloat16), ("fsdp", "ctx"), scatter_dimension=0, tiled=True
        ).astype(jnp.float32),
        lax.psum_scatter(
            grad_feed_out.astype(jnp.bfloat16), ("fsdp", "ctx"), scatter_dimension=0, tiled=True
        ).astype(jnp.float32),
    )
    cross_low = grad_hidden.astype(jnp.bfloat16)
    grad_cross_out = weight_grad(cross_low, cross_att)
    grad_cross_att = project(cross_low, cross_group[4]).astype(jnp.bfloat16)
    grad_cq, grad_ck_part, grad_cv_part, unused_bias = attention_backward(
        cross_q, keys_cross, values_cross, None, None, lse_cross, grad_cross_att, block_seqs
    )
    grad_ck, grad_cv = (
        lax.psum_scatter(
            grad_ck_part.astype(jnp.bfloat16), "ctx", scatter_dimension=1, tiled=True
        ).astype(jnp.float32),
        lax.psum_scatter(
            grad_cv_part.astype(jnp.bfloat16), "ctx", scatter_dimension=1, tiled=True
        ).astype(jnp.float32),
    )
    ck_low = grad_ck.astype(jnp.bfloat16)
    cv_low = grad_cv.astype(jnp.bfloat16)
    grad_cross_query = weight_grad(cross_in, grad_cq)
    grad_cross_key = weight_grad(encoder, ck_low)
    grad_cross_value = weight_grad(encoder, cv_low)
    grad_cross_in, grad_encoder = reduce_rows(
        (
            project_back(grad_cq, cross_group[1]),
            project_back(ck_low, cross_group[2]) + project_back(cv_low, cross_group[3]),
        )
    )
    grad_two, grad_gain_two = norm_pull_two(grad_cross_in)
    grad_hidden = grad_hidden + grad_two
    cross_grads = (
        lax.psum_scatter(
            grad_gain_two.astype(jnp.bfloat16), ("fsdp", "ctx"), scatter_dimension=0, tiled=True
        ).astype(jnp.float32),
        lax.psum_scatter(
            grad_cross_query.astype(jnp.bfloat16), ("fsdp", "ctx"), scatter_dimension=0, tiled=True
        ).astype(jnp.float32),
        lax.psum_scatter(
            grad_cross_key.astype(jnp.bfloat16), ("fsdp", "ctx"), scatter_dimension=0, tiled=True
        ).astype(jnp.float32),
        lax.psum_scatter(
            grad_cross_value.astype(jnp.bfloat16), ("fsdp", "ctx"), scatter_dimension=0, tiled=True
        ).astype(jnp.float32),
        lax.psum_scatter(
            grad_cross_out.astype(jnp.bfloat16), ("fsdp", "ctx"), scatter_dimension=0, tiled=True
        ).astype(jnp.float32),
    )
    self_low = grad_hidden.astype(jnp.bfloat16)
    grad_self_out = weight_grad(self_low, self_att)
    grad_self_att = project(self_low, self_group[4]).astype(jnp.bfloat16)
    grad_sq, grad_sk_part, grad_sv_part, bias_total = attention_backward(
        self_q, keys_self, values_self, bias_rows, allowed, lse_self, grad_self_att, block_seqs
    )
    grad_sk, grad_sv = (
        lax.psum_scatter(
            grad_sk_part.astype(jnp.bfloat16), "ctx", scatter_dimension=1, tiled=True
        ).astype(jnp.float32),
        lax.psum_scatter(
            grad_sv_part.astype(jnp.bfloat16), "ctx", scatter_dimension=1, tiled=True
        ).astype(jnp.float32),
    )
    sk_low = grad_sk.astype(jnp.bfloat16)
    sv_low = grad_sv.astype(jnp.bfloat16)
    grad_table = jnp.einsum(
        "ijb,hij->bh",
        one_hot,
        bias_total.reshape(heads_local, row_total_count, key_total_count),
        precision=TOP_PRECISION,
    )
    grad_self_query = weight_grad(self_in, grad_sq)
    grad_self_key = weight_grad(self_in, sk_low)
    grad_self_value = weight_grad(self_in, sv_low)
    grad_self_in = reduce_rows(
        project_back(grad_sq, self_group[1])
        + project_back(sk_low, self_group[2])
        + project_back(sv_low, self_group[3])
    )
    grad_one, grad_gain_one = norm_pull_one(grad_self_in)
    grad_inputs = grad_hidden + grad_one
    self_grads = (
        lax.psum_scatter(
            grad_gain_one.astype(jnp.bfloat16), ("fsdp", "ctx"), scatter_dimension=0, tiled=True
        ).astype(jnp.float32),
        lax.psum_scatter(
            grad_self_query.astype(jnp.bfloat16), ("fsdp", "ctx"), scatter_dimension=0, tiled=True
        ).astype(jnp.float32),
        lax.psum_scatter(
            grad_self_key.astype(jnp.bfloat16), ("fsdp", "ctx"), scatter_dimension=0, tiled=True
        ).astype(jnp.float32),
        lax.psum_scatter(
            grad_self_value.astype(jnp.bfloat16), ("fsdp", "ctx"), scatter_dimension=0, tiled=True
        ).astype(jnp.float32),
        lax.psum_scatter(
            grad_self_out.astype(jnp.bfloat16), ("fsdp", "ctx"), scatter_dimension=0, tiled=True
        ).astype(jnp.float32),
        lax.psum_scatter(
            grad_table.astype(jnp.bfloat16), ("fsdp", "ctx"), scatter_dimension=0, tiled=True
        ).astype(jnp.float32),
    )
    gain_shares = jnp.stack((self_grads[0], cross_grads[0], feed_grads[0]), axis=0)
    return (
        output,
        grad_inputs,
        grad_encoder,
        gain_shares[0],
        self_grads[1],
        self_grads[2],
        self_grads[3],
        self_grads[4],
        self_grads[5],
        gain_shares[1],
        cross_grads[1],
        cross_grads[2],
        cross_grads[3],
        cross_grads[4],
        gain_shares[2],
        feed_grads[1],
        feed_grads[2],
        feed_grads[3],
    )


MESH = pl.DeviceIdType.MESH
DEPTH = 4
LINKS = {("x", 0): 0, ("y", 0): 1, ("z", 1): 2, ("z", -1): 3, ("c", 0): 4}
SIZES = {"x": 2, "y": 2, "z": DEPTH}


class Place:
    def __init__(self):
        row = lax.axis_index("fsdp")
        self.y = lax.axis_index("ctx")
        self.z = lax.axis_index("tp")
        self.x = lax.div(row, 2)
        self.c = lax.rem(row, 2)

    def link(self, axis, d):
        x, y, z, c = self.x, self.y, self.z, self.c
        if axis == "x":
            x = 1 - x
        elif axis == "y":
            y = 1 - y
        elif axis == "z":
            z = z + d
        else:
            c = 1 - c
        return (x * 2 + c, y, z)

    def has(self, link):
        if link == ("z", 1):
            return self.z < DEPTH - 1
        if link == ("z", -1):
            return self.z > 0
        return None

    def source(self, src):
        x = 1 - self.x if src.get("x") else self.x
        y = 1 - self.y if src.get("y") else self.y
        return x, y, self.z + src.get("z", 0)

    def exists(self, src):
        off = src.get("z", 0)
        if off < 0:
            return self.z >= -off
        if off > 0:
            return self.z < DEPTH - off
        return None


def arrivals(order):
    events = []
    for k, axis in enumerate(order):
        sources = [{}]
        for a in order[:k]:
            choice = (0, -1, 1, -2, 2, -3, 3) if a == "z" else (0, 1)
            sources = [dict(b, **{a: o}) for o in choice for b in sources]
        for o in (-1, 1, -2, 2, -3, 3) if axis == "z" else (1,):
            for b in sources:
                src = dict(b, **{axis: o})
                d = 0 if axis != "z" else (1 if o < 0 else -1)
                events.append((k, sum(abs(v) for v in src.values()), src, d))
    return events


def onward(order, k, d):
    out = [("z", d)] if k >= 0 and order[k] == "z" else []
    for a in order[k + 1 :]:
        out += [("z", 1), ("z", -1)] if a == "z" else [(a, 0)]
    return out


def when(cond, action):
    if cond is None:
        action()
    else:
        pl.when(cond)(action)


def number(x, y, z):
    return (x * 2 + y) * DEPTH + z


def greet(place):
    barrier = pltpu.get_barrier_semaphore()

    def signal(link):
        pl.semaphore_signal(
            barrier, inc=1, device_id=place.link(*link), device_id_type=MESH
        )

    for link in LINKS:
        when(place.has(link), functools.partial(signal, link))
    ends = jnp.where(place.z < DEPTH - 1, 1, 0) + jnp.where(place.z > 0, 1, 0)
    pl.semaphore_wait(barrier, ends + 3)


def remote(src, dst, send, recv, device):
    return pltpu.make_async_remote_copy(
        src_ref=src, dst_ref=dst, send_sem=send, recv_sem=recv,
        device_id=device, device_id_type=MESH,
    )


class Gather:
    def __init__(self, place, orders, rows, ins, outs, sems):
        self.place, self.orders, self.rows, self.ins, self.outs = place, orders, rows, ins, outs
        self.send, self.recv, self.core_recv, self.local_sem = sems
        self.me = (place.x, place.y, place.z)
        self.arrivals = [
            (k, hops, j, src, d)
            for j in range(len(orders))
            for k, hops, src, d in arrivals(orders[j])
        ]
        self.arrivals.sort(key=lambda e: (e[0], e[1]))

    @staticmethod
    def scratch(count):
        dma = pltpu.SemaphoreType.DMA
        return [
            dma((count, 4 * DEPTH, 5)), dma((count, 4 * DEPTH)), dma((count, 4 * DEPTH)),
            dma((count,)),
        ]

    def slot(self, j, xyz, c):
        x, y, z = xyz
        if len(self.orders[j]) == 1:
            return self.outs[j].at[y if self.orders[j] == "y" else z]
        at = ((x * 2 + c) * 2 + y) * self.rows[j]
        return self.outs[j].at[z, pl.ds(pl.multiple_of(at, self.rows[j]), self.rows[j]), :]

    def copy(self, j, xyz, link, own):
        here = self.slot(j, xyz, self.place.c)
        arrived = self.core_recv if link[0] == "c" else self.recv
        i = number(*xyz)
        return remote(
            self.ins[j] if own else here, here, self.send.at[j, i, LINKS[link]],
            arrived.at[j, i], self.place.link(*link),
        )

    def routes(self, j, k, d):
        links = onward(self.orders[j], k, d)
        return links + [("c", 0)] if len(self.orders[j]) == 3 else links

    def local(self, j):
        return pltpu.make_async_copy(
            self.ins[j], self.slot(j, self.me, self.place.c), self.local_sem.at[j]
        )

    def start(self, which=None):
        which = range(len(self.orders)) if which is None else which
        for stage in range(2):
            for j in which:
                for link in self.routes(j, -1, 0):
                    if (link[0] == "c") == (stage == 1):
                        when(self.place.has(link), self.copy(j, self.me, link, True).start)
        for j in which:
            self.local(j).start()

    def steps(self, wanted=None):
        for e, (k, hops, j, src, d) in enumerate(self.arrivals):
            xyz = self.place.source(src)
            if wanted is not None and not wanted(j, k):
                continue

            def step(k=k, j=j, d=d, xyz=xyz, src=src):
                def run():
                    self.copy(j, xyz, ("x", 0), True).wait_recv()
                    for link in self.routes(j, k, d):
                        when(self.place.has(link), self.copy(j, xyz, link, False).start)

                when(self.place.exists(src), run)

            yield (e + 1) / len(self.arrivals), step

    def settle(self, which):
        for j in which:
            self.local(j).wait()
            if len(self.orders[j]) == 3:

                def from_core(i, carry):
                    xyz = (
                        lax.div(i, 2 * DEPTH), lax.rem(lax.div(i, DEPTH), 2), lax.rem(i, DEPTH)
                    )
                    remote(
                        self.ins[j], self.slot(j, xyz, 1 - self.place.c), self.send.at[j, i, 4],
                        self.core_recv.at[j, i], self.place.link("c", 0),
                    ).wait_recv()
                    return carry

                lax.fori_loop(0, 4 * DEPTH, from_core, 0)

    def sent(self):
        for j in range(len(self.orders)):
            for link in self.routes(j, -1, 0):
                when(self.place.has(link), self.copy(j, self.me, link, True).wait_send)
        for k, hops, j, src, d in self.arrivals:
            xyz = self.place.source(src)

            def run():
                for link in self.routes(j, k, d):
                    when(self.place.has(link), self.copy(j, xyz, link, False).wait_send)

            when(self.place.exists(src), run)

    def finish(self):
        self.settle(range(len(self.orders)))
        self.sent()


def child_slots(order):
    starts, total, before = [], 0, 1
    for a in order:
        starts.append(total)
        total += before * (DEPTH + 1 if a == "z" else 1)
        before *= SIZES[a]
    return starts, total


def child_slot(order, starts, m, xyz, tail):
    at = 0
    for a in order[:m]:
        at = at * SIZES[a] + xyz["xyz".index(a)]
    if order[m] == "z":
        at = at * (DEPTH + 1) + tail
    return starts[m] + at


def add_rows(out, terms, rows):
    step = min(rows, 16)

    def body(q, carry):
        at = pl.ds(pl.multiple_of(q * step, step), step)
        value = terms[0][at, :].astype(jnp.float32)
        for term in terms[1:]:
            value = value + term[at, :].astype(jnp.float32)
        out[at, :] = value.astype(out.dtype)
        return carry

    lax.fori_loop(0, rows // step, body, 0)


class Scatter:
    def __init__(self, place, orders, rows, ins, outs, scratch):
        self.place, self.orders, self.rows, self.ins, self.outs = place, orders, rows, ins, outs
        n = len(orders)
        self.sums, self.gifts, self.kids = (scratch[i * n : (i + 1) * n] for i in range(3))
        self.load_sem, self.give_sem, self.gift_sem, self.up_sem, self.kid_sem = scratch[3 * n :]
        self.me = (place.x, place.y, place.z)
        self.plans = [child_slots(o) for o in orders]
        self.partner = place.link("c", 0)
        self.events = [
            (k, hops, j, src, d)
            for j in range(n)
            for k, hops, src, d in arrivals(orders[j])
        ]
        self.events.sort(key=lambda e: (-e[0], -e[1]))

    @staticmethod
    def scratch(arrays, rows, orders):
        plans = [child_slots(o)[1] for o in orders]
        count = len(arrays)
        dma = pltpu.SemaphoreType.DMA

        def room(slots):
            return [
                pltpu.VMEM((n, r, a.shape[2]), a.dtype) for n, r, a in zip(slots, rows, arrays)
            ]

        full = [4 * DEPTH] * count
        return (
            room(full) + room(full) + room(plans)
            + [dma((count, 4 * DEPTH))] * 4 + [dma((count, max(plans)))]
        )

    def slot(self, j, xyz, c):
        x, y, z = xyz
        at = ((x * 2 + c) * 2 + y) * self.rows[j]
        return self.ins[j].at[z, pl.ds(pl.multiple_of(at, self.rows[j]), self.rows[j]), :]

    def load(self, j, xyz):
        i = number(*xyz)
        return pltpu.make_async_copy(
            self.slot(j, xyz, self.place.c), self.sums[j].at[i], self.load_sem.at[j, i]
        )

    def give(self, j, xyz):
        i = number(*xyz)
        return remote(
            self.slot(j, xyz, 1 - self.place.c), self.gifts[j].at[i], self.give_sem.at[j, i],
            self.gift_sem.at[j, i], self.partner,
        )

    def up(self, j, xyz, k, d):
        axis = self.orders[j][k]
        tail = xyz[2]
        if axis == "z" and d < 0:
            tail = jnp.where(xyz[2] == self.place.z - d, DEPTH, xyz[2])
        at = child_slot(self.orders[j], self.plans[j][0], k, xyz, tail)
        i = number(*xyz)
        return remote(
            self.sums[j].at[i], self.kids[j].at[at], self.up_sem.at[j, i],
            self.kid_sem.at[j, at], self.place.link(axis, -d),
        )

    def kid(self, j, m, xyz, tail):
        at = child_slot(self.orders[j], self.plans[j][0], m, xyz, tail)
        ref = self.kids[j].at[at]
        remote(ref, ref, self.up_sem.at[j, 0], self.kid_sem.at[j, at], self.partner).wait_recv()
        return ref

    def collect(self, j, xyz, k, d, out=None):
        i = number(*xyz)
        order = self.orders[j]
        total = self.sums[j].at[i]
        self.load(j, xyz).wait()
        self.give(j, xyz).wait_recv()
        always, sometimes = [], []
        if k >= 0 and order[k] == "z":
            sometimes.append((k, ("z", d), xyz[2]))
        for m in range(k + 1, len(order)):
            if order[m] == "z":
                sometimes += [(m, ("z", 1), xyz[2]), (m, ("z", -1), DEPTH)]
            else:
                always.append(m)
        for m, link, tail in sometimes:

            def more():
                add_rows(total, [total, self.kid(j, m, xyz, tail)], self.rows[j])

            when(self.place.has(link), more)
        terms = [total, self.gifts[j].at[i]] + [self.kid(j, m, xyz, 0) for m in always]
        add_rows(total if out is None else out, terms, self.rows[j])

    def start(self):
        for k, hops, j, src, d in self.events:
            xyz = self.place.source(src)

            def begin():
                self.give(j, xyz).start()
                self.load(j, xyz).start()

            when(self.place.exists(src), begin)
        for j in range(len(self.orders)):
            self.give(j, self.me).start()
            self.load(j, self.me).start()

    def steps(self):
        count = len(self.events)
        for e, (k, hops, j, src, d) in enumerate(self.events):
            xyz = self.place.source(src)

            def step(k=k, j=j, d=d, xyz=xyz, src=src):
                def run():
                    self.collect(j, xyz, k, d)
                    self.up(j, xyz, k, d).start()

                when(self.place.exists(src), run)

            yield (e + 1) / (count + 1), step
        for j in range(len(self.orders)):

            def last(j=j):
                self.collect(j, self.me, -1, 0, self.outs[j])

            yield 1.0, last

    def finish(self):
        for k, hops, j, src, d in self.events:
            xyz = self.place.source(src)

            def run():
                self.up(j, xyz, k, d).wait_send()
                self.give(j, xyz).wait_send()

            when(self.place.exists(src), run)
        for j in range(len(self.orders)):
            self.give(j, self.me).wait_send()


class Share:
    def __init__(self, place, rows, ins, outs, scratch):
        self.place, self.rows, self.ins, self.outs = place, rows, ins, outs
        n = len(rows)
        self.first, self.second, self.sums = (scratch[i * n : (i + 1) * n] for i in range(3))
        self.send, self.recv = scratch[3 * n :]
        self.half = lax.rem(place.z, 2)
        self.over_y = place.link("y", 0)
        self.over_z = place.link("z", 1 - 2 * self.half)

    @staticmethod
    def scratch(rows):
        dma = pltpu.SemaphoreType.DMA
        out = []
        for slots in (8, 4, 4):
            out += [pltpu.VMEM((slots, n, 256), jnp.bfloat16) for n in rows]
        return out + [dma((len(rows), 12)), dma((len(rows), 12))]

    def block(self, j, t, y, half):
        n = self.rows[j]
        return self.ins[j].at[t, pl.ds(pl.multiple_of((y * 2 + half) * n, n), n), :]

    def early(self, j, t, s):
        if t < 2:
            src, device = self.block(j, t, 1 - self.place.y, s), self.over_y
        else:
            src, device = self.block(j, t, s, 1 - self.half), self.over_z
        i = t * 2 + s
        return remote(src, self.first[j].at[i], self.send.at[j, i], self.recv.at[j, i], device)

    def late(self, j, t):
        return remote(
            self.sums[j].at[t], self.second[j].at[t], self.send.at[j, 8 + t],
            self.recv.at[j, 8 + t], self.over_z if t < 2 else self.over_y,
        )

    def start(self):
        for j in range(len(self.rows)):
            for s in range(2):
                for t in range(4):
                    self.early(j, t, s).start()

    def steps(self):
        for j in range(len(self.rows)):
            for t in range(4):

                def pass_on(j=j, t=t):
                    for s in range(2):
                        self.early(j, t, s).wait_recv()
                    if t < 2:
                        away = 1 - self.half
                        mine = self.block(j, t, self.place.y, away)
                    else:
                        away = 1 - self.place.y
                        mine = self.block(j, t, away, self.half)
                    add_rows(
                        self.sums[j].at[t], [mine, self.first[j].at[t * 2 + away]], self.rows[j]
                    )
                    self.late(j, t).start()

                yield 0.25, pass_on
        for j in range(len(self.rows)):
            for t in range(4):

                def total(j=j, t=t):
                    self.late(j, t).wait_recv()
                    kept = self.half if t < 2 else self.place.y
                    mine = self.block(j, t, self.place.y, self.half)
                    add_rows(
                        self.outs[j].at[t],
                        [mine, self.first[j].at[t * 2 + kept], self.second[j].at[t]],
                        self.rows[j],
                    )

                yield 0.5, total

    def finish(self):
        for j in range(len(self.rows)):
            for t in range(4):
                for s in range(2):
                    self.early(j, t, s).wait_send()
                self.late(j, t).wait_send()


def run_steps(parts):
    steps = []
    for plan, begin, length in parts:
        steps += [(begin + length * at, step) for at, step in plan.steps()]
    steps.sort(key=lambda s: s[0])
    for _, step in steps:
        step()


HBM = pl.BlockSpec(memory_space=pl.ANY)
INSIDE = pl.BlockSpec(memory_space=pltpu.VMEM)


def comm_call(kernel, name, number_id, ins, in_specs, outs, out_specs, scratch):
    return pl.pallas_call(
        kernel,
        out_shape=outs,
        in_specs=in_specs,
        out_specs=out_specs,
        scratch_shapes=scratch,
        compiler_params=pltpu.CompilerParams(
            collective_id=number_id, has_side_effects=True, vmem_limit_bytes=67043328
        ),
        name=name,
    )(*ins)


def gathered(a, order):
    if len(order) == 1:
        return jax.ShapeDtypeStruct((SIZES[order],) + a.shape, a.dtype)
    return jax.ShapeDtypeStruct((DEPTH, 8 * a.shape[0], a.shape[1]), a.dtype)


def scattered(arrays):
    return [
        jax.ShapeDtypeStruct((a.shape[1] // 8, a.shape[2]), jnp.float32) for a in arrays
    ]


def scatter_and_share(arrays, orders, shared, name):
    n, m = len(arrays), len(shared)
    rows = [a.shape[1] // 8 for a in arrays]
    own = [a.shape[1] // 4 for a in shared]
    room = Scatter.scratch(arrays, rows, orders)

    def kernel(*refs):
        place = Place()
        ins, outs, scratch = refs[: n + m], refs[n + m : 2 * (n + m)], refs[2 * (n + m) :]
        plan = Scatter(place, orders, rows, ins[:n], outs[:n], scratch[: len(room)])
        share = Share(place, own, ins[n:], outs[n:], scratch[len(room) :])
        greet(place)
        share.start()
        plan.start()
        run_steps([(plan, 0.0, 80.0), (share, 0.0, 80.0)])
        share.finish()
        plan.finish()

    return comm_call(
        kernel, name, 2, arrays + shared, [HBM] * n + [INSIDE] * m,
        scattered(arrays)
        + [jax.ShapeDtypeStruct((4, r, 256), jnp.bfloat16) for r in own],
        [INSIDE] * (n + m), room + Share.scratch(own),
    )


def scatter_and_rows(arrays, orders, rows_in, name):
    n, m = len(arrays), len(rows_in)
    rows = [a.shape[1] // 8 for a in arrays]
    room = Scatter.scratch(arrays, rows, orders)

    def kernel(*refs):
        place = Place()
        ins, outs, scratch = refs[: n + m], refs[n + m : 2 * (n + m)], refs[2 * (n + m) :]
        plan = Scatter(place, orders, rows, ins[:n], outs[:n], scratch[: len(room)])
        lines = Gather(
            place, ["z"] * m, [a.shape[0] for a in rows_in], ins[n:], outs[n:],
            scratch[len(room) :],
        )
        greet(place)
        lines.start()
        plan.start()
        run_steps([(plan, 0.0, 70.0), (lines, 0.0, 60.0)])
        lines.finish()
        plan.finish()

    return comm_call(
        kernel, name, 3, arrays + rows_in, [HBM] * n + [INSIDE] * m,
        scattered(arrays) + [gathered(a, "z") for a in rows_in],
        [INSIDE] * n + [HBM] * m, room + Gather.scratch(m),
    )


WIDTH = 1024
QROWS = 256
KEYS = 1024
ENC_ROWS = 512
SPAN = 1280
CHUNK = 128
VMEM_MOST = 64000000
ROWS_OF = (((0,), (0,)), ((), ()))
LAST = (((1,), (1,)), ((), ()))
PLAIN = (((1,), (0,)), ((), ()))


def mm(a, b, dims=PLAIN):
    return lax.dot_general(a, b, dims, preferred_element_type=jnp.float32)


def norm_rows(v, gain):
    return v * lax.rsqrt(jnp.mean(v * v, axis=-1, keepdims=True) + EPSILON) * gain


def norm_back(v, gain, e):
    r = lax.rsqrt(jnp.mean(v * v, axis=-1, keepdims=True) + EPSILON)
    ev = e * v
    gain_grad = jnp.sum(ev * r, axis=0, keepdims=True)
    back = r * gain * e - v * (r * r * r) * jnp.mean(ev * gain, axis=-1, keepdims=True)
    return back, gain_grad


def head_rows(cols, a):
    return jnp.concatenate(
        [cols[:, a * 128 : a * 128 + 64], cols[:, a * 128 + 64 : a * 128 + 128]], axis=0
    )


def attend(q, kv, p_ref, s_ref, ot_ref, keys, add_bias):
    for a in range(2):
        q2 = head_rows(q, a)
        k = kv[:, a * 64 : a * 64 + 64]
        v = kv[:, 128 + a * 64 : 192 + a * 64]
        if add_bias is not None:
            add_bias(a, None, None)
        peak = None
        for c in range(keys // CHUNK):
            rows = pl.ds(c * CHUNK, CHUNK)
            s = mm(k[c * CHUNK : (c + 1) * CHUNK], q2, LAST)
            if add_bias is not None:
                s = add_bias(a, c, s)
            s_ref[rows, :] = s
            top = jnp.max(s, axis=0, keepdims=True)
            peak = top if peak is None else jnp.maximum(peak, top)
        total = jnp.zeros_like(peak)
        for c in range(keys // CHUNK):
            rows = pl.ds(c * CHUNK, CHUNK)
            e = jnp.exp(s_ref[rows, :] - peak)
            s_ref[rows, :] = e
            total = total + jnp.sum(e, axis=0, keepdims=True)
        inverse = 1.0 / total
        for c in range(keys // CHUNK):
            rows = pl.ds(c * CHUNK, CHUNK)
            p_ref[0, a, rows, :] = (s_ref[rows, :] * inverse).astype(jnp.bfloat16)
        ot = mm(v, p_ref[0, a], ROWS_OF)
        ot_ref[a * 128 : a * 128 + 64, :] = ot[:, :QROWS]
        ot_ref[a * 128 + 64 : a * 128 + 128, :] = ot[:, QROWS:]
    return jnp.transpose(ot_ref[...]).astype(jnp.bfloat16)


def attend_back(q, kv, p_ref, do, dkv_ref, d_ref, ds_ref, qt_ref, keys, take_bias):
    for a in range(2):
        q2 = head_rows(q, a)
        do2 = head_rows(do, a)
        k = kv[:, a * 64 : a * 64 + 64]
        v = kv[:, 128 + a * 64 : 192 + a * 64]
        total = jnp.zeros((1, 2 * QROWS), jnp.float32)
        for c in range(keys // CHUNK):
            rows = pl.ds(c * CHUNK, CHUNK)
            dp = mm(v[c * CHUNK : (c + 1) * CHUNK], do2, LAST)
            d_ref[rows, :] = dp
            total = total + jnp.sum(
                dp * p_ref[0, a, rows, :].astype(jnp.float32), axis=0, keepdims=True
            )
        for c in range(keys // CHUNK):
            rows = pl.ds(c * CHUNK, CHUNK)
            ds = p_ref[0, a, rows, :].astype(jnp.float32) * (d_ref[rows, :] - total)
            if take_bias is not None:
                take_bias(a, c, ds)
            ds_ref[rows, :] = ds.astype(jnp.bfloat16)
        if take_bias is not None:
            take_bias(a, None, None)
        dkv_ref[0, :, a * 64 : a * 64 + 64] = mm(ds_ref[...], q2).astype(jnp.bfloat16)
        dkv_ref[0, :, 128 + a * 64 : 192 + a * 64] = mm(p_ref[0, a], do2).astype(jnp.bfloat16)
        qt = mm(k, ds_ref[...], ROWS_OF)
        qt_ref[a * 128 : a * 128 + 64, :] = qt[:, :QROWS]
        qt_ref[a * 128 + 64 : a * 128 + 128, :] = qt[:, QROWS:]
    return jnp.transpose(qt_ref[...]).astype(jnp.bfloat16)


def self_step(first, length, h1_ref, w_ref, wkv_ref, near_of, q_ref, kv_ref, p_ref, o_ref, work):
    s_ref, strip_ref, ot_ref = work
    kv = mm(h1_ref[...], wkv_ref[0]).astype(jnp.bfloat16)
    kv_ref[0] = kv
    q = mm(h1_ref[pl.ds(first, QROWS), :], w_ref[0, :, :QROWS]).astype(jnp.bfloat16)
    q_ref[0] = q
    lane = lax.broadcasted_iota(jnp.int32, (1, 2 * QROWS), 1)
    lane = jnp.where(lane < QROWS, lane, lane - QROWS)
    last_key = jnp.minimum(lane + first, length - 1)

    def add_bias(a, c, s):
        if c is None:
            for b in range(2):
                near = near_of(2 * a + b)
                for g in range(16):
                    shift = (SPAN - (120 - 8 * g)) % SPAN
                    strip_ref[b, 8 * g : 8 * g + 8, :] = (
                        pltpu.roll(near, shift, 1) if shift else near
                    )
            return None
        cols = pl.ds(CHUNK * (7 - c), QROWS)
        bias = jnp.concatenate([strip_ref[0, :, cols], strip_ref[1, :, cols]], axis=1)
        key = lax.broadcasted_iota(jnp.int32, s.shape, 0) + c * CHUNK
        return jnp.where(key <= last_key, s + bias, MASKED)

    o = attend(q, kv, p_ref, s_ref, ot_ref, KEYS, add_bias)
    o_ref[0] = o
    return mm(o, w_ref[0, :, QROWS:], LAST)


def cross_step(h_ref, enc, w_ref, wkv_ref, q_ref, kv_ref, p_ref, o_ref, work):
    s_ref, ot_ref = work
    kv = mm(enc, wkv_ref[0]).astype(jnp.bfloat16)
    kv_ref[0] = kv
    q = mm(h_ref[...], w_ref[0, :, :QROWS]).astype(jnp.bfloat16)
    q_ref[0] = q
    o = attend(q, kv, p_ref, s_ref, ot_ref, ENC_ROWS, None)
    o_ref[0] = o
    return mm(o, w_ref[0, :, QROWS:], LAST)


def feed_kernel(
    info, x3_ref, cot_ref, gain_ref, wg_ref, wu_ref, wo_ref,
    out_ref, g3_ref, gg_ref, gu_ref, go_ref, gn_ref,
    h_ref, ht_ref, g_ref, gt_ref, y_ref, dh_ref,
):
    step = pl.program_id(0)

    @pl.when(step == 0)
    def _():
        h = norm_rows(x3_ref[...], gain_ref[...]).astype(jnp.bfloat16)
        h_ref[...] = h
        ht_ref[...] = jnp.transpose(h)
        row = lax.broadcasted_iota(jnp.int32, (QROWS, 1), 0) + info[0]
        g4 = jnp.where(row < info[1], cot_ref[...].astype(jnp.float32), 0.0)
        g = g4.astype(jnp.bfloat16)
        g_ref[...] = g
        gt_ref[...] = jnp.transpose(g)
        y_ref[...] = x3_ref[...]
        dh_ref[...] = jnp.zeros_like(dh_ref)

    gate = mm(h_ref[...], wg_ref[0])
    up = mm(h_ref[...], wu_ref[0])
    root = math.sqrt(2.0 / math.pi)
    square = gate * gate
    th = jnp.tanh(root * (gate + 0.044715 * gate * square))
    half = 0.5 * (1.0 + th)
    gelu = gate * half
    slope = half + 0.5 * gate * (1.0 - th * th) * (root * (1.0 + 3 * 0.044715 * square))
    hidden = (gelu * up).astype(jnp.bfloat16)
    y_ref[...] += mm(hidden, wo_ref[0], LAST)
    go_ref[0] = mm(gt_ref[...], hidden).astype(jnp.bfloat16)
    dhid = mm(g_ref[...], wo_ref[0])
    dup = (dhid * gelu).astype(jnp.bfloat16)
    dgate = (dhid * up * slope).astype(jnp.bfloat16)
    gg_ref[0] = mm(ht_ref[...], dgate).astype(jnp.bfloat16)
    gu_ref[0] = mm(ht_ref[...], dup).astype(jnp.bfloat16)
    dh_ref[...] += mm(dgate, wg_ref[0], LAST) + mm(dup, wu_ref[0], LAST)

    @pl.when(step == pl.num_programs(0) - 1)
    def _():
        out_ref[...] = y_ref[...].astype(jnp.bfloat16)
        back, gain_grad = norm_back(x3_ref[...], gain_ref[...], dh_ref[...])
        g3_ref[...] = g_ref[...].astype(jnp.float32) + back
        gn_ref[...] = gain_grad


def cross_backward_kernel(
    g3_ref, x2_ref, h_ref, gain_ref, w_ref, q_ref, kv_ref, p_ref, o_ref,
    g2_ref, dkv_ref, gw_ref, gn_ref,
    g_ref, gt_ref, ht_ref, dh_ref, d_ref, ds_ref, qt_ref,
):
    step = pl.program_id(0)

    @pl.when(step == 0)
    def _():
        g = g3_ref[...].astype(jnp.bfloat16)
        g_ref[...] = g
        gt_ref[...] = jnp.transpose(g)
        ht_ref[...] = jnp.transpose(h_ref[...])
        dh_ref[...] = jnp.zeros_like(dh_ref)

    do = mm(g_ref[...], w_ref[0, :, QROWS:]).astype(jnp.bfloat16)
    gw_ref[0, :, QROWS:] = mm(gt_ref[...], o_ref[0]).astype(jnp.bfloat16)
    dq = attend_back(
        q_ref[0], kv_ref[0], p_ref, do, dkv_ref, d_ref, ds_ref, qt_ref, ENC_ROWS, None
    )
    gw_ref[0, :, :QROWS] = mm(ht_ref[...], dq).astype(jnp.bfloat16)
    dh_ref[...] += mm(dq, w_ref[0, :, :QROWS], LAST)

    @pl.when(step == pl.num_programs(0) - 1)
    def _():
        back, gain_grad = norm_back(x2_ref[...], gain_ref[...], dh_ref[...])
        g2_ref[...] = g3_ref[...] + back
        gn_ref[...] = gain_grad


def self_backward_kernel(
    g2_ref, h_ref, w_ref, q_ref, kv_ref, p_ref, o_ref,
    dh_ref, dkv_ref, gw_ref, near_ref,
    g_ref, gt_ref, ht_ref, d_ref, ds_ref, qt_ref, strip_ref,
):
    @pl.when(pl.program_id(0) == 0)
    def _():
        g = g2_ref[...].astype(jnp.bfloat16)
        g_ref[...] = g
        gt_ref[...] = jnp.transpose(g)
        ht_ref[...] = jnp.transpose(h_ref[...])
        dh_ref[...] = jnp.zeros_like(dh_ref)

    def take_bias(a, c, ds):
        if c is None:
            for b in range(2):
                total = jnp.zeros((8, SPAN), jnp.float32)
                for g in range(16):
                    part = strip_ref[b, 8 * g : 8 * g + 8, :]
                    shift = 120 - 8 * g
                    total = total + (pltpu.roll(part, shift, 1) if shift else part)
                near_ref[0, 2 * a + b] = total
            return
        if c == 0:
            strip_ref[...] = jnp.zeros_like(strip_ref)
        cols = pl.ds(CHUNK * (7 - c), QROWS)
        strip_ref[0, :, cols] += ds[:, :QROWS]
        strip_ref[1, :, cols] += ds[:, QROWS:]

    do = mm(g_ref[...], w_ref[0, :, QROWS:]).astype(jnp.bfloat16)
    gw_ref[0, :, QROWS:] = mm(gt_ref[...], o_ref[0]).astype(jnp.bfloat16)
    dq = attend_back(
        q_ref[0], kv_ref[0], p_ref, do, dkv_ref, d_ref, ds_ref, qt_ref, KEYS, take_bias
    )
    gw_ref[0, :, :QROWS] = mm(ht_ref[...], dq).astype(jnp.bfloat16)
    dh_ref[...] += mm(dq, w_ref[0, :, :QROWS], LAST)


def last_kernel(
    dh_part_ref, dkv_ref, x_ref, h_ref, gain_ref, g2_ref, ws_ref, wc_ref, dkvc_ref, enc_ref,
    gx_ref, genc_ref, gw_ref, gn_ref,
    ht_ref, et_ref, dh_ref, de_ref,
):
    step = pl.program_id(0)

    @pl.when(step == 0)
    def _():
        ht_ref[...] = jnp.transpose(h_ref[...])
        et_ref[...] = jnp.transpose(enc_ref[...])
        dh_ref[...] = dh_part_ref[...]
        de_ref[...] = jnp.zeros_like(de_ref)

    dkv = dkv_ref[0]
    dkvc = dkvc_ref[0]
    gw_ref[0, :, :QROWS] = mm(ht_ref[...], dkv).astype(jnp.bfloat16)
    gw_ref[0, :, QROWS:] = mm(et_ref[...], dkvc).astype(jnp.bfloat16)
    dh_ref[...] += mm(dkv, ws_ref[0], LAST)
    de_ref[...] += mm(dkvc, wc_ref[0], LAST)

    @pl.when(step == pl.num_programs(0) - 1)
    def _():
        back, gain_grad = norm_back(
            x_ref[...].astype(jnp.float32), gain_ref[...], dh_ref[...]
        )
        gx_ref[...] = (g2_ref[...] + back).astype(jnp.bfloat16)
        genc_ref[...] = de_ref[...].astype(jnp.bfloat16)
        gn_ref[...] = gain_grad


def whole(shape):
    zeros = (0,) * len(shape)
    return pl.BlockSpec(shape, lambda t: zeros)


def part(shape, column=0):
    tail = (0,) * (len(shape) - 2)
    return pl.BlockSpec(shape, lambda t: (t,) + tail + (column,))


SCALARS = pl.BlockSpec(memory_space=pltpu.SMEM)
F32 = jnp.float32
LOW = jnp.bfloat16


def run_heads(kernel, name, ins, specs, outs, out_specs, scratch, flops, steps=4):
    moved = sum(math.prod(a.shape) * a.dtype.itemsize for a in list(ins) + list(outs))
    return pl.pallas_call(
        kernel,
        grid=(steps,),
        in_specs=specs,
        out_specs=out_specs,
        out_shape=outs,
        scratch_shapes=scratch,
        compiler_params=pltpu.CompilerParams(
            dimension_semantics=("arbitrary",), vmem_limit_bytes=VMEM_MOST
        ),
        cost_estimate=pl.CostEstimate(flops=flops, bytes_accessed=moved, transcendentals=0),
        name=name,
    )(*ins)


def shape_of(shape, dtype):
    return jax.ShapeDtypeStruct(shape, dtype)


def feed(info, x3, cot, gain, wg, wu, wo):
    units = wg.shape[2]
    wide = part((1, WIDTH, units))
    return run_heads(
        feed_kernel, "feed",
        (info, x3, cot, gain, wg, wu, wo),
        [SCALARS, whole((QROWS, WIDTH)), whole((QROWS, WIDTH)), whole((1, WIDTH)),
         wide, wide, wide],
        [shape_of((QROWS, WIDTH), LOW), shape_of((QROWS, WIDTH), F32)]
        + [shape_of((4, WIDTH, units), LOW)] * 3
        + [shape_of((1, WIDTH), F32)],
        [whole((QROWS, WIDTH)), whole((QROWS, WIDTH)), wide, wide, wide, whole((1, WIDTH))],
        [pltpu.VMEM((QROWS, WIDTH), LOW), pltpu.VMEM((WIDTH, QROWS), LOW),
         pltpu.VMEM((QROWS, WIDTH), LOW), pltpu.VMEM((WIDTH, QROWS), LOW),
         pltpu.VMEM((QROWS, WIDTH), F32), pltpu.VMEM((QROWS, WIDTH), F32)],
        13 * 10**9,
    )


def cross_backward(g3, x2, h, gain, w2, q, kv, p, o):
    return run_heads(
        cross_backward_kernel, "cross_backward",
        (g3, x2, h, gain, w2, q, kv, p, o),
        [whole((QROWS, WIDTH)), whole((QROWS, WIDTH)), whole((QROWS, WIDTH)),
         whole((1, WIDTH)), part((1, WIDTH, 512)), part((1, QROWS, 256)),
         part((1, ENC_ROWS, 256)), part((1, 2, ENC_ROWS, 512)), part((1, QROWS, 256))],
        [shape_of((QROWS, WIDTH), F32), shape_of((4, ENC_ROWS, 256), LOW),
         shape_of((4, WIDTH, 512), LOW), shape_of((1, WIDTH), F32)],
        [whole((QROWS, WIDTH)), part((1, ENC_ROWS, 256)), part((1, WIDTH, 512)),
         whole((1, WIDTH))],
        [pltpu.VMEM((QROWS, WIDTH), LOW), pltpu.VMEM((WIDTH, QROWS), LOW),
         pltpu.VMEM((WIDTH, QROWS), LOW), pltpu.VMEM((QROWS, WIDTH), F32),
         pltpu.VMEM((ENC_ROWS, 512), F32), pltpu.VMEM((ENC_ROWS, 512), LOW),
         pltpu.VMEM((256, QROWS), F32)],
        5 * 10**9,
    )


def self_backward(g2, h, w1, q, kv, p, o):
    return run_heads(
        self_backward_kernel, "self_backward",
        (g2, h, w1, q, kv, p, o),
        [whole((QROWS, WIDTH)), whole((QROWS, WIDTH)), part((1, WIDTH, 512)),
         part((1, QROWS, 256)), part((1, KEYS, 256)), part((1, 2, KEYS, 512)),
         part((1, QROWS, 256))],
        [shape_of((QROWS, WIDTH), F32), shape_of((4, KEYS, 256), LOW),
         shape_of((4, WIDTH, 512), LOW), shape_of((4, 4, 8, SPAN), F32)],
        [whole((QROWS, WIDTH)), part((1, KEYS, 256)), part((1, WIDTH, 512)),
         part((1, 4, 8, SPAN))],
        [pltpu.VMEM((QROWS, WIDTH), LOW), pltpu.VMEM((WIDTH, QROWS), LOW),
         pltpu.VMEM((WIDTH, QROWS), LOW), pltpu.VMEM((KEYS, 512), F32),
         pltpu.VMEM((KEYS, 512), LOW), pltpu.VMEM((256, QROWS), F32),
         pltpu.VMEM((2, CHUNK, SPAN), F32)],
        6 * 10**9,
    )


def last_grads(dh, dkv, x, h, gain, g2, w3, dkvc, enc):
    rows = enc.shape[0]
    return run_heads(
        last_kernel, "last_grads",
        (dh, dkv, x, h, gain, g2, w3, w3, dkvc, enc),
        [whole((QROWS, WIDTH)), part((1, QROWS, 256)), whole((QROWS, WIDTH)),
         whole((QROWS, WIDTH)), whole((1, WIDTH)), whole((QROWS, WIDTH)),
         part((1, WIDTH, 256)), part((1, WIDTH, 256), 1), part((1, rows, 256)),
         whole((rows, WIDTH))],
        [shape_of((QROWS, WIDTH), LOW), shape_of((rows, WIDTH), LOW),
         shape_of((4, WIDTH, 512), LOW), shape_of((1, WIDTH), F32)],
        [whole((QROWS, WIDTH)), whole((rows, WIDTH)), part((1, WIDTH, 512)),
         whole((1, WIDTH))],
        [pltpu.VMEM((WIDTH, QROWS), LOW), pltpu.VMEM((WIDTH, rows), LOW),
         pltpu.VMEM((QROWS, WIDTH), F32), pltpu.VMEM((rows, WIDTH), F32)],
        3 * 10**9,
    )


GATHER_ORDERS = ("zyx", "zyx", "xzy", "yzx", "zxy", "yzx", "zxy", "y", "y")
SMALL_ROWS = 16
LANES = 128


def split_steps(steps, parts, low, high):
    ends = [int(len(steps) * (low + (high - low) * (i + 1) / parts)) for i in range(parts)]
    return [steps[a:b] for a, b in zip([0] + ends, ends)], steps[ends[-1] :]


def at_step(t, chunks):
    for i, chunk in enumerate(chunks):

        def run():
            for step in chunk:
                step()

        if chunk:
            pl.when(t == i)(run)


def forward_kernel(rows, *refs):
    lengths, ins = refs[0], refs[1:10]
    weights, refs = refs[10:16], refs[16:]
    gains_ref, x2_ref, x3_ref, h1_out, h2_ref = refs[:5]
    q1_out, kv1_out, p1_out, o1_out, q2_out, kv2_out, p2_out, o2_out = refs[5:13]
    small, x_all, enc_all, bucket_ref, h1_ref, s_ref, strip_ref, ot_ref = refs[13:21]
    place = Place()
    plan = Gather(place, GATHER_ORDERS, rows, ins, weights + (small, x_all, enc_all), refs[21:])
    greet(place)
    half = lax.rem(place.z, 2)
    first = pl.multiple_of(place.y * (2 * QROWS) + half * QROWS, QROWS)
    length = lengths[lax.div(place.z, 2)]
    plan.start(range(3, 9))
    row = lax.broadcasted_iota(jnp.int32, (8, SPAN), 0)
    col = lax.broadcasted_iota(jnp.int32, (8, SPAN), 1)
    bucket_ref[...] = bucket_index(jnp.maximum(first + col - (SPAN - 264) - row, 0))
    for _, step in plan.steps(lambda j, k: 3 <= j < 7 and k < 2):
        step()
    plan.start(range(3))
    for _, step in plan.steps(lambda j, k: j >= 7 or (j >= 3 and k == 2)):
        step()
    plan.settle(range(3, 9))
    feed_steps = [step for _, step in plan.steps(lambda j, k: j < 3)]
    chunks, rest = split_steps(feed_steps, 8, 0.0, 0.7)

    for k in range(3):
        gains_ref[pl.ds(k, 1), :] = jnp.concatenate(
            [small[0, pl.ds(r * SMALL_ROWS + k, 1), :] for r in range(8)], axis=1
        )
    gain = gains_ref[pl.ds(0, 1), :]
    for y in range(2):
        for c in range(2):
            at = pl.ds(c * QROWS, QROWS)
            h1_ref[pl.ds(y * 512 + c * QROWS, QROWS), :] = norm_rows(
                x_all[y, at, :].astype(jnp.float32), gain
            ).astype(jnp.bfloat16)
    x2_ref[...] = ins[7][pl.ds(half * QROWS, QROWS), :].astype(jnp.float32)
    h1_out[...] = h1_ref[pl.ds(first, QROWS), :]

    def self_body(w_ref, wkv_ref, q_ref, kv_ref, p_ref, o_ref):
        t = pl.program_id(0)

        def near_of(head):
            rows_of = [small[t, pl.ds(r * SMALL_ROWS + 3, 1), :] for r in range(8)]
            bucket = bucket_ref[...]
            near = jnp.zeros((8, SPAN), jnp.float32)
            for i in range(BUCKETS):
                lane = (i % 4) * 4 + head
                value = rows_of[i // 4][:, lane : lane + 1]
                near = jnp.where(bucket == i, value, near)
            return near

        x2_ref[...] += self_step(
            first, length, h1_ref, w_ref, wkv_ref, near_of, q_ref, kv_ref, p_ref, o_ref,
            (s_ref, strip_ref, ot_ref),
        )
        at_step(t, chunks[:4])

    pltpu.emit_pipeline(
        self_body,
        grid=(4,),
        in_specs=[part((1, WIDTH, 512)), part((1, WIDTH, 256))],
        out_specs=[
            part((1, QROWS, 256)), part((1, KEYS, 256)), part((1, 2, KEYS, 512)),
            part((1, QROWS, 256)),
        ],
    )(weights[3], weights[5], q1_out, kv1_out, p1_out, o1_out)
    x3_ref[...] = x2_ref[...]
    h2_ref[...] = norm_rows(x2_ref[...], gains_ref[pl.ds(1, 1), :]).astype(jnp.bfloat16)

    def cross_body(w_ref, wkv_ref, q_ref, kv_ref, p_ref, o_ref):
        enc = jnp.concatenate([enc_all[0], enc_all[1]], axis=0)
        x3_ref[...] += cross_step(
            h2_ref, enc, w_ref, wkv_ref, q_ref, kv_ref, p_ref, o_ref, (s_ref, ot_ref)
        )
        at_step(pl.program_id(0), chunks[4:])

    pltpu.emit_pipeline(
        cross_body,
        grid=(4,),
        in_specs=[part((1, WIDTH, 512)), part((1, WIDTH, 256), 1)],
        out_specs=[
            part((1, QROWS, 256)), part((1, ENC_ROWS, 256)), part((1, 2, ENC_ROWS, 512)),
            part((1, QROWS, 256)),
        ],
    )(weights[4], weights[5], q2_out, kv2_out, p2_out, o2_out)
    for step in rest:
        step()
    plan.settle(range(3))
    plan.sent()


def forward(lengths, arrays):
    rows = [a.shape[0] for a in arrays]
    wide = [gathered(a, o) for a, o in zip(arrays, GATHER_ORDERS)]
    vm = pltpu.VMEM
    return comm_call(
        functools.partial(forward_kernel, rows), "forward", 1,
        (lengths,) + tuple(arrays), [SCALARS] + [INSIDE] * 9,
        wide[:6]
        + [shape_of((8, WIDTH), F32), shape_of((QROWS, WIDTH), F32),
           shape_of((QROWS, WIDTH), F32), shape_of((QROWS, WIDTH), LOW),
           shape_of((QROWS, WIDTH), LOW),
           shape_of((4, QROWS, 256), LOW), shape_of((4, KEYS, 256), LOW),
           shape_of((4, 2, KEYS, 512), LOW), shape_of((4, QROWS, 256), LOW),
           shape_of((4, QROWS, 256), LOW), shape_of((4, ENC_ROWS, 256), LOW),
           shape_of((4, 2, ENC_ROWS, 512), LOW), shape_of((4, QROWS, 256), LOW)],
        [HBM] * 6 + [INSIDE] * 5 + [HBM] * 8,
        [vm(w.shape, w.dtype) for w in wide[6:]]
        + [vm((8, SPAN), jnp.int32), vm((KEYS, WIDTH), LOW), vm((KEYS, 512), F32),
           vm((2, CHUNK, SPAN), F32), vm((256, QROWS), F32)]
        + Gather.scratch(9),
    )


FEED_ORDERS = ("xzy", "zyx", "yzx")
HEAD_ORDERS = ("zyx", "zxy", "zyx", "zxy")


def small_rows(gains, table):
    flat = jnp.pad(table.reshape(1, -1).astype(F32), ((0, 0), (0, LANES - table.size)))
    rows = jnp.concatenate([g.reshape(1, LANES).astype(F32) for g in gains] + [flat], axis=0)
    return jnp.pad(rows, ((0, SMALL_ROWS - 4), (0, 0)))


def rows_along_tp(own, t):
    found = [own]
    for k in range(1, DEPTH):
        found.append(lax.ppermute(own, "tp", [(i, (i + k) % DEPTH) for i in range(DEPTH)]))
    found = jnp.stack(found)
    return jnp.stack(
        [lax.dynamic_index_in_dim(found, (t - i + DEPTH) % DEPTH, 0, False) for i in range(DEPTH)]
    )


def tokens_split(
    inputs, encoder, lengths, cotangent,
    norm_self, self_query, self_key_matrix, self_value_matrix, self_out, bias_table,
    norm_cross, cross_query, cross_key_matrix, cross_value_matrix, cross_out,
    norm_feed, feed_gate, feed_up, feed_out,
):
    y = lax.axis_index("ctx")
    t = lax.axis_index("tp")
    seq, half = lax.div(t, 2), lax.rem(t, 2)
    first = y * (2 * QROWS) + half * QROWS
    info = jnp.stack([first, lax.dynamic_index_in_dim(lengths, seq, 0, False)])
    x_seq = lax.dynamic_index_in_dim(inputs, seq, 0, False)
    enc_seq = lax.dynamic_index_in_dim(encoder, seq, 0, False)
    x_own = lax.dynamic_slice_in_dim(x_seq, half * QROWS, QROWS, 0)
    cot = lax.dynamic_slice(cotangent, (seq, half * QROWS, 0), (1, QROWS, WIDTH))[0]
    packed = (
        feed_gate, feed_up, feed_out,
        jnp.concatenate([self_query, self_out], axis=1),
        jnp.concatenate([cross_query, cross_out], axis=1),
        jnp.concatenate(
            [self_key_matrix, self_value_matrix, cross_key_matrix, cross_value_matrix], axis=1
        ),
        small_rows((norm_self, norm_cross, norm_feed), bias_table),
        x_seq, enc_seq,
    )
    (
        wg, wu, wo, w1, w2, w3, gains, x2, x3, h1, h2, q1, kv1, p1, o1, q2, kv2, p2, o2,
    ) = forward(lengths, packed)
    gains = gains[:3].reshape(3, 1, WIDTH)
    distance = jnp.maximum(
        first + jnp.arange(SPAN)[None, :] - (SPAN - 264) - jnp.arange(8)[:, None], 0
    )
    bucket = bucket_index(distance)
    out, g3, gg, gu, go, gn3 = feed(info, x3, cot, gains[2], wg, wu, wo)
    out = rows_along_tp(out, t)
    g2, dkv2, gw2, gn2 = cross_backward(g3, x2, h2, gains[1], w2, q2, kv2, p2, o2)
    dh, dkv1, gw1, near = self_backward(g2, h1, w1, q1, kv1, p1, o1)
    gg, gu, go, dkv, dkvc = scatter_and_share(
        (gg, gu, go), FEED_ORDERS, (dkv1, dkv2), "scatter_feed"
    )
    enc_own = lax.dynamic_slice_in_dim(enc_seq, half * (QROWS // 2), QROWS // 2, 0)
    gx, genc, gw3, gn1 = last_grads(
        dh, dkv, x_own, h1, gains[0], g2, w3, dkvc, enc_own
    )
    one_hot = (bucket[:, :, None] == jnp.arange(BUCKETS, dtype=jnp.int32)).astype(F32)
    grad_table = jnp.einsum(
        "hrm,rmb->bh", near.reshape(16, 8, SPAN), one_hot, precision=TOP_PRECISION
    )
    gain_grads = jnp.concatenate([gn1, gn2, gn3], axis=0).reshape(3, 8, LANES)
    gain_grads = jnp.broadcast_to(jnp.transpose(gain_grads, (1, 0, 2))[None], (4, 8, 3, LANES))
    table_grads = jnp.transpose(grad_table.reshape(8, 4, 4, 4), (2, 0, 1, 3)).reshape(4, 8, 1, 16)
    table_grads = jnp.pad(table_grads, ((0, 0), (0, 0), (0, 0), (0, LANES - 16)))
    small_grads = jnp.pad(
        jnp.concatenate([gain_grads, table_grads], axis=2),
        ((0, 0), (0, 0), (0, SMALL_ROWS - 4), (0, 0)),
    ).reshape(4, 8 * SMALL_ROWS, LANES)
    gw1, gw2, gw3, gs, gx, genc = scatter_and_rows(
        (gw1, gw2, gw3, small_grads), HEAD_ORDERS, (gx, genc), "scatter_heads"
    )
    return (
        out.reshape(inputs.shape),
        gx.reshape(inputs.shape).astype(F32),
        genc.reshape(encoder.shape).astype(F32),
        gs[0], gw1[:, :256], gw3[:, :128], gw3[:, 128:256], gw1[:, 256:],
        gs[3, :16].reshape(4, 4),
        gs[1], gw2[:, :256], gw3[:, 256:384], gw3[:, 384:], gw2[:, 256:],
        gs[2], gg, gu, go,
    )


def solution(mesh):
    sizes = (mesh.shape["fsdp"], mesh.shape["ctx"], mesh.shape["tp"])
    return jax.shard_map(
        tokens_split if sizes == (4, 2, DEPTH) else shards,
        mesh=mesh,
        in_specs=(
            P("fsdp", "ctx", None),
            P("fsdp", "ctx", None),
            P("fsdp"),
            P("fsdp", "ctx", None),
            P(("fsdp", "ctx")),
            P(("fsdp", "ctx"), "tp"),
            P(("fsdp", "ctx"), "tp"),
            P(("fsdp", "ctx"), "tp"),
            P(("fsdp", "ctx"), "tp"),
            P(("fsdp", "ctx"), "tp"),
            P(("fsdp", "ctx")),
            P(("fsdp", "ctx"), "tp"),
            P(("fsdp", "ctx"), "tp"),
            P(("fsdp", "ctx"), "tp"),
            P(("fsdp", "ctx"), "tp"),
            P(("fsdp", "ctx")),
            P(("fsdp", "ctx"), "tp"),
            P(("fsdp", "ctx"), "tp"),
            P(("fsdp", "ctx"), "tp"),
        ),
        out_specs=(
            P("fsdp", "ctx", None),
            P("fsdp", "ctx", None),
            P("fsdp", "ctx", None),
            P(("fsdp", "ctx")),
            P(("fsdp", "ctx"), "tp"),
            P(("fsdp", "ctx"), "tp"),
            P(("fsdp", "ctx"), "tp"),
            P(("fsdp", "ctx"), "tp"),
            P(("fsdp", "ctx"), "tp"),
            P(("fsdp", "ctx")),
            P(("fsdp", "ctx"), "tp"),
            P(("fsdp", "ctx"), "tp"),
            P(("fsdp", "ctx"), "tp"),
            P(("fsdp", "ctx"), "tp"),
            P(("fsdp", "ctx")),
            P(("fsdp", "ctx"), "tp"),
            P(("fsdp", "ctx"), "tp"),
            P(("fsdp", "ctx"), "tp"),
        ),
        check_vma=False,
    )
```

```python
import functools
import math

import jax
import jax.numpy as jnp
from jax import lax
from jax.experimental import pallas as pl
from jax.experimental.pallas import tpu as pltpu
from jax.sharding import PartitionSpec as P

HEAD_SIZE = 64
BUCKETS = 32
MAXDIST = 128


EPSILON = 1e-06
MASKED = -1000000000.0
TOP_PRECISION = lax.Precision.HIGHEST


def rms_scale(values, gain_row):
    inverse = lax.rsqrt(jnp.mean(values * values, axis=-1, keepdims=True) + EPSILON)
    return values * inverse * gain_row


def gated_product(gate_in, up_in):
    return jax.nn.gelu(gate_in, approximate=True) * up_in


def project(operand_array, weight_arrays):
    return jnp.einsum(
        "spd,dk->spk", operand_array, weight_arrays, preferred_element_type=jnp.float32
    )


def project_back(grad_cols, weight_arrays):
    return jnp.einsum("spk,dk->spd", grad_cols, weight_arrays, preferred_element_type=jnp.float32)


def weight_grad(operand_array, grad_cols):
    return jnp.einsum("spd,spk->dk", operand_array, grad_cols, preferred_element_type=jnp.float32)


def bucket_index(distance):
    exact_count = BUCKETS // 2
    counter = jnp.zeros(distance.shape, jnp.int32)
    for level_index in range(1, BUCKETS - exact_count):
        border = math.ceil(
            exact_count * (MAXDIST / exact_count) ** (level_index / (BUCKETS - exact_count))
        )
        counter = counter + (distance >= border).astype(jnp.int32)
    return jnp.where(distance < exact_count, distance, exact_count + counter)


def reduce_rows(partial_sum):
    return lax.psum(partial_sum, "tp")


def block_scores(queries, key_rows, bias_rows, allowed):
    scores = jnp.einsum("gpkrd,gjkd->gkrpj", queries, key_rows, preferred_element_type=jnp.float32)
    if bias_rows is not None:
        scores = jnp.where(allowed[:, None, None], scores + bias_rows[None], MASKED)
    return scores


def forward_block(queries, key_rows, value_rows, bias_rows, allowed):
    scores = block_scores(queries, key_rows, bias_rows, allowed)
    row_peak = jnp.max(scores, axis=-1, keepdims=True)
    log_total = row_peak + jnp.log(jnp.sum(jnp.exp(scores - row_peak), axis=-1, keepdims=True))
    weights_low = jnp.exp(scores - log_total).astype(jnp.bfloat16)
    output = jnp.einsum(
        "gkrpj,gjkd->gpkrd", weights_low, value_rows, preferred_element_type=jnp.float32
    )
    return (output.astype(jnp.bfloat16), log_total)


def backward_block(queries, key_rows, value_rows, bias_rows, allowed, log_total, grad_out):
    scores = block_scores(queries, key_rows, bias_rows, allowed)
    softmax_rows = jnp.exp(scores - log_total)
    grad_probs = jnp.einsum(
        "gpkrd,gjkd->gkrpj", grad_out, value_rows, preferred_element_type=jnp.float32
    )
    grad_scores = softmax_rows * (
        grad_probs - jnp.sum(grad_probs * softmax_rows, axis=-1, keepdims=True)
    )
    scores_low = grad_scores.astype(jnp.bfloat16)
    grad_query = jnp.einsum(
        "gkrpj,gjkd->gpkrd", scores_low, key_rows, preferred_element_type=jnp.float32
    )
    grad_key = jnp.einsum(
        "gkrpj,gpkrd->gjkd", scores_low, queries, preferred_element_type=jnp.float32
    )
    grad_value = jnp.einsum(
        "gkrpj,gpkrd->gjkd",
        softmax_rows.astype(jnp.bfloat16),
        grad_out,
        preferred_element_type=jnp.float32,
    )
    if bias_rows is None:
        grad_bias = jnp.zeros((1,), jnp.float32)
    else:
        grad_bias = jnp.sum(grad_scores, axis=0)
    return (grad_query.astype(jnp.bfloat16), grad_key, grad_value, grad_bias)


def block_shapes(queries, key_rows, block_seqs):
    seq_count, row_total_count, query_cols = queries.shape
    key_total_count, key_cols = (key_rows.shape[1], key_rows.shape[2])
    kv_heads = key_cols // HEAD_SIZE
    repeats = query_cols // key_cols
    blocks = seq_count // block_seqs
    query_shape = (blocks, block_seqs, row_total_count, kv_heads, repeats, HEAD_SIZE)
    key_shape = (blocks, block_seqs, key_total_count, kv_heads, HEAD_SIZE)
    mask_shape = (blocks, block_seqs, row_total_count, key_total_count)
    return (query_shape, key_shape, mask_shape)


def attention_forward(queries, key_rows, value_rows, bias_rows, allowed, block_seqs):
    query_shape, key_shape, mask_shape = block_shapes(queries, key_rows, block_seqs)
    sources = (
        queries.reshape(query_shape),
        key_rows.reshape(key_shape),
        value_rows.reshape(key_shape),
    )
    if allowed is not None:
        sources = sources + (allowed.reshape(mask_shape),)

    def one_block(piece_list):
        mask_block = piece_list[3] if allowed is not None else None
        return forward_block(piece_list[0], piece_list[1], piece_list[2], bias_rows, mask_block)

    outputs, log_totals = lax.map(one_block, sources)
    return (outputs.reshape(queries.shape), log_totals)


def attention_backward(
    queries, key_rows, value_rows, bias_rows, allowed, log_totals, grad_out, block_seqs
):
    query_shape, key_shape, mask_shape = block_shapes(queries, key_rows, block_seqs)
    sources = (
        queries.reshape(query_shape),
        key_rows.reshape(key_shape),
        value_rows.reshape(key_shape),
        log_totals,
        grad_out.reshape(query_shape),
    )
    if allowed is not None:
        sources = sources + (allowed.reshape(mask_shape),)
    if bias_rows is None:
        initial = jnp.zeros((1,), jnp.float32)
    else:
        initial = jnp.zeros(bias_rows.shape, jnp.float32)

    def one_block(running, piece_list):
        mask_block = piece_list[5] if allowed is not None else None
        grad_query, grad_key, grad_value, grad_bias = backward_block(
            piece_list[0],
            piece_list[1],
            piece_list[2],
            bias_rows,
            mask_block,
            piece_list[3],
            piece_list[4],
        )
        return (running + grad_bias, (grad_query, grad_key, grad_value))

    bias_total, grad_list = lax.scan(one_block, initial, sources)
    return (
        grad_list[0].reshape(queries.shape),
        grad_list[1].reshape(key_rows.shape),
        grad_list[2].reshape(value_rows.shape),
        bias_total,
    )


def shards(
    inputs,
    encoder,
    lengths,
    cotangent,
    norm_self,
    self_query,
    self_key_matrix,
    self_value_matrix,
    self_out,
    bias_table,
    norm_cross,
    cross_query,
    cross_key_matrix,
    cross_value_matrix,
    cross_out,
    norm_feed,
    feed_gate,
    feed_up,
    feed_out,
):
    self_group = (
        lax.all_gather(norm_self, ("fsdp", "ctx"), axis=0, tiled=True),
        lax.all_gather(self_query, ("fsdp", "ctx"), axis=0, tiled=True),
        lax.all_gather(self_key_matrix, ("fsdp", "ctx"), axis=0, tiled=True),
        lax.all_gather(self_value_matrix, ("fsdp", "ctx"), axis=0, tiled=True),
        lax.all_gather(self_out, ("fsdp", "ctx"), axis=0, tiled=True),
        lax.all_gather(bias_table, ("fsdp", "ctx"), axis=0, tiled=True),
    )
    seq_count, row_total_count = (inputs.shape[0], inputs.shape[1])
    block_seqs = max((trial for trial in (1, 2, 3, 4) if seq_count % trial == 0))
    start_row = lax.axis_index("ctx") * row_total_count
    key_total_count = row_total_count * lax.axis_size("ctx")
    row_pos = start_row + jnp.arange(row_total_count, dtype=jnp.int32)
    col_pos = jnp.arange(key_total_count, dtype=jnp.int32)
    buckets = bucket_index(jnp.maximum(row_pos[:, None] - col_pos[None, :], 0))
    one_hot = (buckets[:, :, None] == jnp.arange(BUCKETS, dtype=jnp.int32)[None, None, :]).astype(
        jnp.float32
    )
    causal = col_pos[None, :] <= row_pos[:, None]
    allowed = causal[None] & (col_pos[None, None, :] < lengths[:, None, None])
    hidden_in = inputs.astype(jnp.float32)
    normed_one, norm_pull_one = jax.vjp(rms_scale, hidden_in, self_group[0].astype(jnp.float32))
    self_in = normed_one.astype(jnp.bfloat16)
    self_q = project(self_in, self_group[1]).astype(jnp.bfloat16)
    self_k = project(self_in, self_group[2]).astype(jnp.bfloat16)
    self_v = project(self_in, self_group[3]).astype(jnp.bfloat16)
    keys_self, values_self = (
        lax.all_gather(self_k, "ctx", axis=1, tiled=True),
        lax.all_gather(self_v, "ctx", axis=1, tiled=True),
    )
    heads_local = self_group[1].shape[1] // HEAD_SIZE
    kv_local = self_group[2].shape[1] // HEAD_SIZE
    table_rows = self_group[5].astype(jnp.float32)
    bias_rows = jnp.einsum("ijb,bh->hij", one_hot, table_rows, precision=TOP_PRECISION).reshape(
        kv_local, heads_local // kv_local, row_total_count, key_total_count
    )
    self_att, lse_self = attention_forward(
        self_q, keys_self, values_self, bias_rows, allowed, block_seqs
    )
    hidden_two = hidden_in + reduce_rows(project_back(self_att, self_group[4]))
    cross_group = (
        lax.all_gather(norm_cross, ("fsdp", "ctx"), axis=0, tiled=True),
        lax.all_gather(cross_query, ("fsdp", "ctx"), axis=0, tiled=True),
        lax.all_gather(cross_key_matrix, ("fsdp", "ctx"), axis=0, tiled=True),
        lax.all_gather(cross_value_matrix, ("fsdp", "ctx"), axis=0, tiled=True),
        lax.all_gather(cross_out, ("fsdp", "ctx"), axis=0, tiled=True),
    )
    normed_two, norm_pull_two = jax.vjp(rms_scale, hidden_two, cross_group[0].astype(jnp.float32))
    cross_in = normed_two.astype(jnp.bfloat16)
    cross_q = project(cross_in, cross_group[1]).astype(jnp.bfloat16)
    enc_keys = project(encoder, cross_group[2]).astype(jnp.bfloat16)
    enc_values = project(encoder, cross_group[3]).astype(jnp.bfloat16)
    keys_cross, values_cross = (
        lax.all_gather(enc_keys, "ctx", axis=1, tiled=True),
        lax.all_gather(enc_values, "ctx", axis=1, tiled=True),
    )
    cross_att, lse_cross = attention_forward(
        cross_q, keys_cross, values_cross, None, None, block_seqs
    )
    hidden_three = hidden_two + reduce_rows(project_back(cross_att, cross_group[4]))
    feed_group = (
        lax.all_gather(norm_feed, ("fsdp", "ctx"), axis=0, tiled=True),
        lax.all_gather(feed_gate, ("fsdp", "ctx"), axis=0, tiled=True),
        lax.all_gather(feed_up, ("fsdp", "ctx"), axis=0, tiled=True),
        lax.all_gather(feed_out, ("fsdp", "ctx"), axis=0, tiled=True),
    )
    normed_three, norm_pull_three = jax.vjp(
        rms_scale, hidden_three, feed_group[0].astype(jnp.float32)
    )
    feed_in = normed_three.astype(jnp.bfloat16)
    gate_value = project(feed_in, feed_group[1])
    up_value = project(feed_in, feed_group[2])
    gated_value, gated_pull = jax.vjp(gated_product, gate_value, up_value)
    feed_hidden = gated_value.astype(jnp.bfloat16)
    hidden_four = hidden_three + reduce_rows(project_back(feed_hidden, feed_group[3]))
    output = hidden_four.astype(jnp.bfloat16)
    valid_rows = (row_pos[None, :] < lengths[:, None]).astype(jnp.float32)
    grad_full = cotangent.astype(jnp.float32) * valid_rows[:, :, None]
    branch_low = grad_full.astype(jnp.bfloat16)
    grad_hidden = grad_full
    grad_feed_out = weight_grad(branch_low, feed_hidden)
    grad_gated = project(branch_low, feed_group[3])
    grad_gate, grad_up = gated_pull(grad_gated)
    gate_low = grad_gate.astype(jnp.bfloat16)
    up_low = grad_up.astype(jnp.bfloat16)
    grad_feed_gate = weight_grad(feed_in, gate_low)
    grad_feed_up = weight_grad(feed_in, up_low)
    grad_feed_in = reduce_rows(
        project_back(gate_low, feed_group[1]) + project_back(up_low, feed_group[2])
    )
    grad_three, grad_gain_three = norm_pull_three(grad_feed_in)
    grad_hidden = grad_hidden + grad_three
    feed_grads = (
        lax.psum_scatter(
            grad_gain_three.astype(jnp.bfloat16), ("fsdp", "ctx"), scatter_dimension=0, tiled=True
        ).astype(jnp.float32),
        lax.psum_scatter(
            grad_feed_gate.astype(jnp.bfloat16), ("fsdp", "ctx"), scatter_dimension=0, tiled=True
        ).astype(jnp.float32),
        lax.psum_scatter(
            grad_feed_up.astype(jnp.bfloat16), ("fsdp", "ctx"), scatter_dimension=0, tiled=True
        ).astype(jnp.float32),
        lax.psum_scatter(
            grad_feed_out.astype(jnp.bfloat16), ("fsdp", "ctx"), scatter_dimension=0, tiled=True
        ).astype(jnp.float32),
    )
    cross_low = grad_hidden.astype(jnp.bfloat16)
    grad_cross_out = weight_grad(cross_low, cross_att)
    grad_cross_att = project(cross_low, cross_group[4]).astype(jnp.bfloat16)
    grad_cq, grad_ck_part, grad_cv_part, unused_bias = attention_backward(
        cross_q, keys_cross, values_cross, None, None, lse_cross, grad_cross_att, block_seqs
    )
    grad_ck, grad_cv = (
        lax.psum_scatter(
            grad_ck_part.astype(jnp.bfloat16), "ctx", scatter_dimension=1, tiled=True
        ).astype(jnp.float32),
        lax.psum_scatter(
            grad_cv_part.astype(jnp.bfloat16), "ctx", scatter_dimension=1, tiled=True
        ).astype(jnp.float32),
    )
    ck_low = grad_ck.astype(jnp.bfloat16)
    cv_low = grad_cv.astype(jnp.bfloat16)
    grad_cross_query = weight_grad(cross_in, grad_cq)
    grad_cross_key = weight_grad(encoder, ck_low)
    grad_cross_value = weight_grad(encoder, cv_low)
    grad_cross_in, grad_encoder = reduce_rows(
        (
            project_back(grad_cq, cross_group[1]),
            project_back(ck_low, cross_group[2]) + project_back(cv_low, cross_group[3]),
        )
    )
    grad_two, grad_gain_two = norm_pull_two(grad_cross_in)
    grad_hidden = grad_hidden + grad_two
    cross_grads = (
        lax.psum_scatter(
            grad_gain_two.astype(jnp.bfloat16), ("fsdp", "ctx"), scatter_dimension=0, tiled=True
        ).astype(jnp.float32),
        lax.psum_scatter(
            grad_cross_query.astype(jnp.bfloat16), ("fsdp", "ctx"), scatter_dimension=0, tiled=True
        ).astype(jnp.float32),
        lax.psum_scatter(
            grad_cross_key.astype(jnp.bfloat16), ("fsdp", "ctx"), scatter_dimension=0, tiled=True
        ).astype(jnp.float32),
        lax.psum_scatter(
            grad_cross_value.astype(jnp.bfloat16), ("fsdp", "ctx"), scatter_dimension=0, tiled=True
        ).astype(jnp.float32),
        lax.psum_scatter(
            grad_cross_out.astype(jnp.bfloat16), ("fsdp", "ctx"), scatter_dimension=0, tiled=True
        ).astype(jnp.float32),
    )
    self_low = grad_hidden.astype(jnp.bfloat16)
    grad_self_out = weight_grad(self_low, self_att)
    grad_self_att = project(self_low, self_group[4]).astype(jnp.bfloat16)
    grad_sq, grad_sk_part, grad_sv_part, bias_total = attention_backward(
        self_q, keys_self, values_self, bias_rows, allowed, lse_self, grad_self_att, block_seqs
    )
    grad_sk, grad_sv = (
        lax.psum_scatter(
            grad_sk_part.astype(jnp.bfloat16), "ctx", scatter_dimension=1, tiled=True
        ).astype(jnp.float32),
        lax.psum_scatter(
            grad_sv_part.astype(jnp.bfloat16), "ctx", scatter_dimension=1, tiled=True
        ).astype(jnp.float32),
    )
    sk_low = grad_sk.astype(jnp.bfloat16)
    sv_low = grad_sv.astype(jnp.bfloat16)
    grad_table = jnp.einsum(
        "ijb,hij->bh",
        one_hot,
        bias_total.reshape(heads_local, row_total_count, key_total_count),
        precision=TOP_PRECISION,
    )
    grad_self_query = weight_grad(self_in, grad_sq)
    grad_self_key = weight_grad(self_in, sk_low)
    grad_self_value = weight_grad(self_in, sv_low)
    grad_self_in = reduce_rows(
        project_back(grad_sq, self_group[1])
        + project_back(sk_low, self_group[2])
        + project_back(sv_low, self_group[3])
    )
    grad_one, grad_gain_one = norm_pull_one(grad_self_in)
    grad_inputs = grad_hidden + grad_one
    self_grads = (
        lax.psum_scatter(
            grad_gain_one.astype(jnp.bfloat16), ("fsdp", "ctx"), scatter_dimension=0, tiled=True
        ).astype(jnp.float32),
        lax.psum_scatter(
            grad_self_query.astype(jnp.bfloat16), ("fsdp", "ctx"), scatter_dimension=0, tiled=True
        ).astype(jnp.float32),
        lax.psum_scatter(
            grad_self_key.astype(jnp.bfloat16), ("fsdp", "ctx"), scatter_dimension=0, tiled=True
        ).astype(jnp.float32),
        lax.psum_scatter(
            grad_self_value.astype(jnp.bfloat16), ("fsdp", "ctx"), scatter_dimension=0, tiled=True
        ).astype(jnp.float32),
        lax.psum_scatter(
            grad_self_out.astype(jnp.bfloat16), ("fsdp", "ctx"), scatter_dimension=0, tiled=True
        ).astype(jnp.float32),
        lax.psum_scatter(
            grad_table.astype(jnp.bfloat16), ("fsdp", "ctx"), scatter_dimension=0, tiled=True
        ).astype(jnp.float32),
    )
    gain_shares = jnp.stack((self_grads[0], cross_grads[0], feed_grads[0]), axis=0)
    return (
        output,
        grad_inputs,
        grad_encoder,
        gain_shares[0],
        self_grads[1],
        self_grads[2],
        self_grads[3],
        self_grads[4],
        self_grads[5],
        gain_shares[1],
        cross_grads[1],
        cross_grads[2],
        cross_grads[3],
        cross_grads[4],
        gain_shares[2],
        feed_grads[1],
        feed_grads[2],
        feed_grads[3],
    )


MESH = pl.DeviceIdType.MESH
DEPTH = 4
LINKS = {("x", 0): 0, ("y", 0): 1, ("z", 1): 2, ("z", -1): 3, ("c", 0): 4}
SIZES = {"x": 2, "y": 2, "z": DEPTH}


class Place:
    def __init__(self):
        row = lax.axis_index("fsdp")
        self.y = lax.axis_index("ctx")
        self.z = lax.axis_index("tp")
        self.x = lax.div(row, 2)
        self.c = lax.rem(row, 2)

    def link(self, axis, d):
        x, y, z, c = self.x, self.y, self.z, self.c
        if axis == "x":
            x = 1 - x
        elif axis == "y":
            y = 1 - y
        elif axis == "z":
            z = z + d
        else:
            c = 1 - c
        return (x * 2 + c, y, z)

    def has(self, link):
        if link == ("z", 1):
            return self.z < DEPTH - 1
        if link == ("z", -1):
            return self.z > 0
        return None

    def source(self, src):
        x = 1 - self.x if src.get("x") else self.x
        y = 1 - self.y if src.get("y") else self.y
        return x, y, self.z + src.get("z", 0)

    def exists(self, src):
        off = src.get("z", 0)
        if off < 0:
            return self.z >= -off
        if off > 0:
            return self.z < DEPTH - off
        return None


def arrivals(order):
    events = []
    for k, axis in enumerate(order):
        sources = [{}]
        for a in order[:k]:
            choice = (0, -1, 1, -2, 2, -3, 3) if a == "z" else (0, 1)
            sources = [dict(b, **{a: o}) for o in choice for b in sources]
        for o in (-1, 1, -2, 2, -3, 3) if axis == "z" else (1,):
            for b in sources:
                src = dict(b, **{axis: o})
                d = 0 if axis != "z" else (1 if o < 0 else -1)
                events.append((k, sum(abs(v) for v in src.values()), src, d))
    return events


def onward(order, k, d):
    out = [("z", d)] if k >= 0 and order[k] == "z" else []
    for a in order[k + 1 :]:
        out += [("z", 1), ("z", -1)] if a == "z" else [(a, 0)]
    return out


def when(cond, action):
    if cond is None:
        action()
    else:
        pl.when(cond)(action)


def number(x, y, z):
    return (x * 2 + y) * DEPTH + z


def greet(place):
    barrier = pltpu.get_barrier_semaphore()

    def signal(link):
        pl.semaphore_signal(
            barrier, inc=1, device_id=place.link(*link), device_id_type=MESH
        )

    for link in LINKS:
        when(place.has(link), functools.partial(signal, link))
    ends = jnp.where(place.z < DEPTH - 1, 1, 0) + jnp.where(place.z > 0, 1, 0)
    pl.semaphore_wait(barrier, ends + 3)


def remote(src, dst, send, recv, device):
    return pltpu.make_async_remote_copy(
        src_ref=src, dst_ref=dst, send_sem=send, recv_sem=recv,
        device_id=device, device_id_type=MESH,
    )


class Gather:
    def __init__(self, place, orders, rows, ins, outs, sems):
        self.place, self.orders, self.rows, self.ins, self.outs = place, orders, rows, ins, outs
        self.send, self.recv, self.core_recv, self.local_sem = sems
        self.me = (place.x, place.y, place.z)
        self.arrivals = [
            (k, hops, j, src, d)
            for j in range(len(orders))
            for k, hops, src, d in arrivals(orders[j])
        ]
        self.arrivals.sort(key=lambda e: (e[0], e[1]))

    @staticmethod
    def scratch(count):
        dma = pltpu.SemaphoreType.DMA
        return [
            dma((count, 4 * DEPTH, 5)), dma((count, 4 * DEPTH)), dma((count, 4 * DEPTH)),
            dma((count,)),
        ]

    def slot(self, j, xyz, c):
        x, y, z = xyz
        if len(self.orders[j]) == 1:
            return self.outs[j].at[y if self.orders[j] == "y" else z]
        at = ((x * 2 + c) * 2 + y) * self.rows[j]
        return self.outs[j].at[z, pl.ds(pl.multiple_of(at, self.rows[j]), self.rows[j]), :]

    def copy(self, j, xyz, link, own):
        here = self.slot(j, xyz, self.place.c)
        arrived = self.core_recv if link[0] == "c" else self.recv
        i = number(*xyz)
        return remote(
            self.ins[j] if own else here, here, self.send.at[j, i, LINKS[link]],
            arrived.at[j, i], self.place.link(*link),
        )

    def routes(self, j, k, d):
        links = onward(self.orders[j], k, d)
        return links + [("c", 0)] if len(self.orders[j]) == 3 else links

    def local(self, j):
        return pltpu.make_async_copy(
            self.ins[j], self.slot(j, self.me, self.place.c), self.local_sem.at[j]
        )

    def start(self, which=None):
        which = range(len(self.orders)) if which is None else which
        for stage in range(2):
            for j in which:
                for link in self.routes(j, -1, 0):
                    if (link[0] == "c") == (stage == 1):
                        when(self.place.has(link), self.copy(j, self.me, link, True).start)
        for j in which:
            self.local(j).start()

    def steps(self, wanted=None):
        for e, (k, hops, j, src, d) in enumerate(self.arrivals):
            xyz = self.place.source(src)
            if wanted is not None and not wanted(j, k):
                continue

            def step(k=k, j=j, d=d, xyz=xyz, src=src):
                def run():
                    self.copy(j, xyz, ("x", 0), True).wait_recv()
                    for link in self.routes(j, k, d):
                        when(self.place.has(link), self.copy(j, xyz, link, False).start)

                when(self.place.exists(src), run)

            yield (e + 1) / len(self.arrivals), step

    def settle(self, which):
        for j in which:
            self.local(j).wait()
            if len(self.orders[j]) == 3:

                def from_core(i, carry):
                    xyz = (
                        lax.div(i, 2 * DEPTH), lax.rem(lax.div(i, DEPTH), 2), lax.rem(i, DEPTH)
                    )
                    remote(
                        self.ins[j], self.slot(j, xyz, 1 - self.place.c), self.send.at[j, i, 4],
                        self.core_recv.at[j, i], self.place.link("c", 0),
                    ).wait_recv()
                    return carry

                lax.fori_loop(0, 4 * DEPTH, from_core, 0)

    def sent(self):
        for j in range(len(self.orders)):
            for link in self.routes(j, -1, 0):
                when(self.place.has(link), self.copy(j, self.me, link, True).wait_send)
        for k, hops, j, src, d in self.arrivals:
            xyz = self.place.source(src)

            def run():
                for link in self.routes(j, k, d):
                    when(self.place.has(link), self.copy(j, xyz, link, False).wait_send)

            when(self.place.exists(src), run)

    def finish(self):
        self.settle(range(len(self.orders)))
        self.sent()


def child_slots(order):
    starts, total, before = [], 0, 1
    for a in order:
        starts.append(total)
        total += before * (DEPTH + 1 if a == "z" else 1)
        before *= SIZES[a]
    return starts, total


def child_slot(order, starts, m, xyz, tail):
    at = 0
    for a in order[:m]:
        at = at * SIZES[a] + xyz["xyz".index(a)]
    if order[m] == "z":
        at = at * (DEPTH + 1) + tail
    return starts[m] + at


def add_rows(out, terms, rows):
    step = min(rows, 16)

    def body(q, carry):
        at = pl.ds(pl.multiple_of(q * step, step), step)
        value = terms[0][at, :].astype(jnp.float32)
        for term in terms[1:]:
            value = value + term[at, :].astype(jnp.float32)
        out[at, :] = value.astype(out.dtype)
        return carry

    lax.fori_loop(0, rows // step, body, 0)


class Scatter:
    def __init__(self, place, orders, rows, ins, outs, scratch):
        self.place, self.orders, self.rows, self.ins, self.outs = place, orders, rows, ins, outs
        n = len(orders)
        self.sums, self.gifts, self.kids = (scratch[i * n : (i + 1) * n] for i in range(3))
        self.load_sem, self.give_sem, self.gift_sem, self.up_sem, self.kid_sem = scratch[3 * n :]
        self.me = (place.x, place.y, place.z)
        self.plans = [child_slots(o) for o in orders]
        self.partner = place.link("c", 0)
        self.events = [
            (k, hops, j, src, d)
            for j in range(n)
            for k, hops, src, d in arrivals(orders[j])
        ]
        self.events.sort(key=lambda e: (-e[0], -e[1]))

    @staticmethod
    def scratch(arrays, rows, orders):
        plans = [child_slots(o)[1] for o in orders]
        count = len(arrays)
        dma = pltpu.SemaphoreType.DMA

        def room(slots):
            return [
                pltpu.VMEM((n, r, a.shape[2]), a.dtype) for n, r, a in zip(slots, rows, arrays)
            ]

        full = [4 * DEPTH] * count
        return (
            room(full) + room(full) + room(plans)
            + [dma((count, 4 * DEPTH))] * 4 + [dma((count, max(plans)))]
        )

    def slot(self, j, xyz, c):
        x, y, z = xyz
        at = ((x * 2 + c) * 2 + y) * self.rows[j]
        return self.ins[j].at[z, pl.ds(pl.multiple_of(at, self.rows[j]), self.rows[j]), :]

    def load(self, j, xyz):
        i = number(*xyz)
        return pltpu.make_async_copy(
            self.slot(j, xyz, self.place.c), self.sums[j].at[i], self.load_sem.at[j, i]
        )

    def give(self, j, xyz):
        i = number(*xyz)
        return remote(
            self.slot(j, xyz, 1 - self.place.c), self.gifts[j].at[i], self.give_sem.at[j, i],
            self.gift_sem.at[j, i], self.partner,
        )

    def up(self, j, xyz, k, d):
        axis = self.orders[j][k]
        tail = xyz[2]
        if axis == "z" and d < 0:
            tail = jnp.where(xyz[2] == self.place.z - d, DEPTH, xyz[2])
        at = child_slot(self.orders[j], self.plans[j][0], k, xyz, tail)
        i = number(*xyz)
        return remote(
            self.sums[j].at[i], self.kids[j].at[at], self.up_sem.at[j, i],
            self.kid_sem.at[j, at], self.place.link(axis, -d),
        )

    def kid(self, j, m, xyz, tail):
        at = child_slot(self.orders[j], self.plans[j][0], m, xyz, tail)
        ref = self.kids[j].at[at]
        remote(ref, ref, self.up_sem.at[j, 0], self.kid_sem.at[j, at], self.partner).wait_recv()
        return ref

    def collect(self, j, xyz, k, d, out=None):
        i = number(*xyz)
        order = self.orders[j]
        total = self.sums[j].at[i]
        self.load(j, xyz).wait()
        self.give(j, xyz).wait_recv()
        always, sometimes = [], []
        if k >= 0 and order[k] == "z":
            sometimes.append((k, ("z", d), xyz[2]))
        for m in range(k + 1, len(order)):
            if order[m] == "z":
                sometimes += [(m, ("z", 1), xyz[2]), (m, ("z", -1), DEPTH)]
            else:
                always.append(m)
        for m, link, tail in sometimes:

            def more():
                add_rows(total, [total, self.kid(j, m, xyz, tail)], self.rows[j])

            when(self.place.has(link), more)
        terms = [total, self.gifts[j].at[i]] + [self.kid(j, m, xyz, 0) for m in always]
        add_rows(total if out is None else out, terms, self.rows[j])

    def start(self):
        for k, hops, j, src, d in self.events:
            xyz = self.place.source(src)

            def begin():
                self.give(j, xyz).start()
                self.load(j, xyz).start()

            when(self.place.exists(src), begin)
        for j in range(len(self.orders)):
            self.give(j, self.me).start()
            self.load(j, self.me).start()

    def steps(self):
        count = len(self.events)
        for e, (k, hops, j, src, d) in enumerate(self.events):
            xyz = self.place.source(src)

            def step(k=k, j=j, d=d, xyz=xyz, src=src):
                def run():
                    self.collect(j, xyz, k, d)
                    self.up(j, xyz, k, d).start()

                when(self.place.exists(src), run)

            yield (e + 1) / (count + 1), step
        for j in range(len(self.orders)):

            def last(j=j):
                self.collect(j, self.me, -1, 0, self.outs[j])

            yield 1.0, last

    def finish(self):
        for k, hops, j, src, d in self.events:
            xyz = self.place.source(src)

            def run():
                self.up(j, xyz, k, d).wait_send()
                self.give(j, xyz).wait_send()

            when(self.place.exists(src), run)
        for j in range(len(self.orders)):
            self.give(j, self.me).wait_send()


class Share:
    def __init__(self, place, rows, ins, outs, scratch):
        self.place, self.rows, self.ins, self.outs = place, rows, ins, outs
        n = len(rows)
        self.first, self.second, self.sums = (scratch[i * n : (i + 1) * n] for i in range(3))
        self.send, self.recv = scratch[3 * n :]
        self.half = lax.rem(place.z, 2)
        self.over_y = place.link("y", 0)
        self.over_z = place.link("z", 1 - 2 * self.half)

    @staticmethod
    def scratch(rows):
        dma = pltpu.SemaphoreType.DMA
        out = []
        for slots in (8, 4, 4):
            out += [pltpu.VMEM((slots, n, 256), jnp.bfloat16) for n in rows]
        return out + [dma((len(rows), 12)), dma((len(rows), 12))]

    def block(self, j, t, y, half):
        n = self.rows[j]
        return self.ins[j].at[t, pl.ds(pl.multiple_of((y * 2 + half) * n, n), n), :]

    def early(self, j, t, s):
        if t < 2:
            src, device = self.block(j, t, 1 - self.place.y, s), self.over_y
        else:
            src, device = self.block(j, t, s, 1 - self.half), self.over_z
        i = t * 2 + s
        return remote(src, self.first[j].at[i], self.send.at[j, i], self.recv.at[j, i], device)

    def late(self, j, t):
        return remote(
            self.sums[j].at[t], self.second[j].at[t], self.send.at[j, 8 + t],
            self.recv.at[j, 8 + t], self.over_z if t < 2 else self.over_y,
        )

    def start(self):
        for j in range(len(self.rows)):
            for s in range(2):
                for t in range(4):
                    self.early(j, t, s).start()

    def steps(self):
        for j in range(len(self.rows)):
            for t in range(4):

                def pass_on(j=j, t=t):
                    for s in range(2):
                        self.early(j, t, s).wait_recv()
                    if t < 2:
                        away = 1 - self.half
                        mine = self.block(j, t, self.place.y, away)
                    else:
                        away = 1 - self.place.y
                        mine = self.block(j, t, away, self.half)
                    add_rows(
                        self.sums[j].at[t], [mine, self.first[j].at[t * 2 + away]], self.rows[j]
                    )
                    self.late(j, t).start()

                yield 0.25, pass_on
        for j in range(len(self.rows)):
            for t in range(4):

                def total(j=j, t=t):
                    self.late(j, t).wait_recv()
                    kept = self.half if t < 2 else self.place.y
                    mine = self.block(j, t, self.place.y, self.half)
                    add_rows(
                        self.outs[j].at[t],
                        [mine, self.first[j].at[t * 2 + kept], self.second[j].at[t]],
                        self.rows[j],
                    )

                yield 0.5, total

    def finish(self):
        for j in range(len(self.rows)):
            for t in range(4):
                for s in range(2):
                    self.early(j, t, s).wait_send()
                self.late(j, t).wait_send()


def run_steps(parts):
    steps = []
    for plan, begin, length in parts:
        steps += [(begin + length * at, step) for at, step in plan.steps()]
    steps.sort(key=lambda s: s[0])
    for _, step in steps:
        step()


HBM = pl.BlockSpec(memory_space=pl.ANY)
INSIDE = pl.BlockSpec(memory_space=pltpu.VMEM)


def comm_call(kernel, name, number_id, ins, in_specs, outs, out_specs, scratch):
    return pl.pallas_call(
        kernel,
        out_shape=outs,
        in_specs=in_specs,
        out_specs=out_specs,
        scratch_shapes=scratch,
        compiler_params=pltpu.CompilerParams(
            collective_id=number_id, has_side_effects=True, vmem_limit_bytes=67043328
        ),
        name=name,
    )(*ins)


def gathered(a, order):
    if len(order) == 1:
        return jax.ShapeDtypeStruct((SIZES[order],) + a.shape, a.dtype)
    return jax.ShapeDtypeStruct((DEPTH, 8 * a.shape[0], a.shape[1]), a.dtype)


def scattered(arrays):
    return [
        jax.ShapeDtypeStruct((a.shape[1] // 8, a.shape[2]), jnp.float32) for a in arrays
    ]


def scatter_and_rows(arrays, orders, rows_in, name):
    n, m = len(arrays), len(rows_in)
    rows = [a.shape[1] // 8 for a in arrays]
    room = Scatter.scratch(arrays, rows, orders)

    def kernel(*refs):
        place = Place()
        ins, outs, scratch = refs[: n + m], refs[n + m : 2 * (n + m)], refs[2 * (n + m) :]
        plan = Scatter(place, orders, rows, ins[:n], outs[:n], scratch[: len(room)])
        lines = Gather(
            place, ["z"] * m, [a.shape[0] for a in rows_in], ins[n:], outs[n:],
            scratch[len(room) :],
        )
        greet(place)
        lines.start()
        plan.start()
        run_steps([(plan, 0.0, 70.0), (lines, 0.0, 60.0)])
        lines.finish()
        plan.finish()

    return comm_call(
        kernel, name, 3, arrays + rows_in, [HBM] * n + [INSIDE] * m,
        scattered(arrays) + [gathered(a, "z") for a in rows_in],
        [INSIDE] * n + [HBM] * m, room + Gather.scratch(m),
    )


WIDTH = 1024
QROWS = 256
KEYS = 1024
ENC_ROWS = 512
SPAN = 1280
CHUNK = 128
VMEM_MOST = 64000000
ROWS_OF = (((0,), (0,)), ((), ()))
LAST = (((1,), (1,)), ((), ()))
PLAIN = (((1,), (0,)), ((), ()))


def mm(a, b, dims=PLAIN):
    return lax.dot_general(a, b, dims, preferred_element_type=jnp.float32)


def norm_rows(v, gain):
    return v * lax.rsqrt(jnp.mean(v * v, axis=-1, keepdims=True) + EPSILON) * gain


def norm_back(v, gain, e):
    r = lax.rsqrt(jnp.mean(v * v, axis=-1, keepdims=True) + EPSILON)
    ev = e * v
    gain_grad = jnp.sum(ev * r, axis=0, keepdims=True)
    back = r * gain * e - v * (r * r * r) * jnp.mean(ev * gain, axis=-1, keepdims=True)
    return back, gain_grad


def head_rows(cols, a):
    return jnp.concatenate(
        [cols[:, a * 128 : a * 128 + 64], cols[:, a * 128 + 64 : a * 128 + 128]], axis=0
    )


def attend(q, kv, p_ref, s_ref, ot_ref, keys, add_bias):
    for a in range(2):
        q2 = head_rows(q, a)
        k = kv[:, a * 64 : a * 64 + 64]
        v = kv[:, 128 + a * 64 : 192 + a * 64]
        if add_bias is not None:
            add_bias(a, None, None)
        peak = None
        for c in range(keys // CHUNK):
            rows = pl.ds(c * CHUNK, CHUNK)
            s = mm(k[c * CHUNK : (c + 1) * CHUNK], q2, LAST)
            if add_bias is not None:
                s = add_bias(a, c, s)
            s_ref[rows, :] = s
            top = jnp.max(s, axis=0, keepdims=True)
            peak = top if peak is None else jnp.maximum(peak, top)
        total = jnp.zeros_like(peak)
        for c in range(keys // CHUNK):
            rows = pl.ds(c * CHUNK, CHUNK)
            e = jnp.exp(s_ref[rows, :] - peak)
            s_ref[rows, :] = e
            total = total + jnp.sum(e, axis=0, keepdims=True)
        inverse = 1.0 / total
        for c in range(keys // CHUNK):
            rows = pl.ds(c * CHUNK, CHUNK)
            p_ref[0, a, rows, :] = (s_ref[rows, :] * inverse).astype(jnp.bfloat16)
        ot = mm(v, p_ref[0, a], ROWS_OF)
        ot_ref[a * 128 : a * 128 + 64, :] = ot[:, :QROWS]
        ot_ref[a * 128 + 64 : a * 128 + 128, :] = ot[:, QROWS:]
    return jnp.transpose(ot_ref[...]).astype(jnp.bfloat16)


def attend_back(q, kv, p_ref, do, dkv_ref, d_ref, ds_ref, qt_ref, keys, take_bias):
    for a in range(2):
        q2 = head_rows(q, a)
        do2 = head_rows(do, a)
        k = kv[:, a * 64 : a * 64 + 64]
        v = kv[:, 128 + a * 64 : 192 + a * 64]
        total = jnp.zeros((1, 2 * QROWS), jnp.float32)
        for c in range(keys // CHUNK):
            rows = pl.ds(c * CHUNK, CHUNK)
            dp = mm(v[c * CHUNK : (c + 1) * CHUNK], do2, LAST)
            d_ref[rows, :] = dp
            total = total + jnp.sum(
                dp * p_ref[0, a, rows, :].astype(jnp.float32), axis=0, keepdims=True
            )
        for c in range(keys // CHUNK):
            rows = pl.ds(c * CHUNK, CHUNK)
            ds = p_ref[0, a, rows, :].astype(jnp.float32) * (d_ref[rows, :] - total)
            if take_bias is not None:
                take_bias(a, c, ds)
            ds_ref[rows, :] = ds.astype(jnp.bfloat16)
        if take_bias is not None:
            take_bias(a, None, None)
        dkv_ref[0, :, a * 64 : a * 64 + 64] = mm(ds_ref[pl.ds(0, keys), :], q2).astype(jnp.bfloat16)
        dkv_ref[0, :, 128 + a * 64 : 192 + a * 64] = mm(p_ref[0, a], do2).astype(jnp.bfloat16)
        qt = mm(k, ds_ref[pl.ds(0, keys), :], ROWS_OF)
        qt_ref[a * 128 : a * 128 + 64, :] = qt[:, :QROWS]
        qt_ref[a * 128 + 64 : a * 128 + 128, :] = qt[:, QROWS:]
    return jnp.transpose(qt_ref[...]).astype(jnp.bfloat16)


def self_step(first, length, h1_ref, w_ref, wkv_ref, near_of, q_ref, kv_ref, p_ref, o_ref, work):
    s_ref, strip_ref, ot_ref = work
    kv = mm(h1_ref[...], wkv_ref[0]).astype(jnp.bfloat16)
    kv_ref[0] = kv
    q = mm(h1_ref[pl.ds(first, QROWS), :], w_ref[0, :, :QROWS]).astype(jnp.bfloat16)
    q_ref[0] = q
    lane = lax.broadcasted_iota(jnp.int32, (1, 2 * QROWS), 1)
    lane = jnp.where(lane < QROWS, lane, lane - QROWS)
    last_key = jnp.minimum(lane + first, length - 1)

    def add_bias(a, c, s):
        if c is None:
            for b in range(2):
                near = near_of(2 * a + b)
                for g in range(16):
                    shift = (SPAN - (120 - 8 * g)) % SPAN
                    strip_ref[b, 8 * g : 8 * g + 8, :] = (
                        pltpu.roll(near, shift, 1) if shift else near
                    )
            return None
        cols = pl.ds(CHUNK * (7 - c), QROWS)
        bias = jnp.concatenate([strip_ref[0, :, cols], strip_ref[1, :, cols]], axis=1)
        key = lax.broadcasted_iota(jnp.int32, s.shape, 0) + c * CHUNK
        return jnp.where(key <= last_key, s + bias, MASKED)

    o = attend(q, kv, p_ref, s_ref, ot_ref, KEYS, add_bias)
    o_ref[0] = o
    return mm(o, w_ref[0, :, QROWS:], LAST)


def cross_step(h_ref, enc, w_ref, wkv_ref, q_ref, kv_ref, p_ref, o_ref, work):
    s_ref, ot_ref = work
    kv = mm(enc, wkv_ref[0]).astype(jnp.bfloat16)
    kv_ref[0] = kv
    q = mm(h_ref[...], w_ref[0, :, :QROWS]).astype(jnp.bfloat16)
    q_ref[0] = q
    o = attend(q, kv, p_ref, s_ref, ot_ref, ENC_ROWS, None)
    o_ref[0] = o
    return mm(o, w_ref[0, :, QROWS:], LAST)


def feed_kernel(
    info, x3_ref, cot_ref, gain_ref, wg_ref, wu_ref, wo_ref,
    out_ref, g3_ref, gg_ref, gu_ref, go_ref, gn_ref,
    h_ref, ht_ref, g_ref, gt_ref, y_ref, dh_ref,
):
    step = pl.program_id(0)

    @pl.when(step == 0)
    def _():
        h = norm_rows(x3_ref[...], gain_ref[pl.ds(2, 1), :]).astype(jnp.bfloat16)
        h_ref[...] = h
        ht_ref[...] = jnp.transpose(h)
        row = lax.broadcasted_iota(jnp.int32, (QROWS, 1), 0) + info[0]
        g4 = jnp.where(row < info[1], cot_ref[...].astype(jnp.float32), 0.0)
        g = g4.astype(jnp.bfloat16)
        g_ref[...] = g
        gt_ref[...] = jnp.transpose(g)
        y_ref[...] = x3_ref[...]
        dh_ref[...] = jnp.zeros_like(dh_ref)

    gate = mm(h_ref[...], wg_ref[0])
    up = mm(h_ref[...], wu_ref[0])
    root = math.sqrt(2.0 / math.pi)
    square = gate * gate
    th = jnp.tanh(root * (gate + 0.044715 * gate * square))
    half = 0.5 * (1.0 + th)
    gelu = gate * half
    slope = half + 0.5 * gate * (1.0 - th * th) * (root * (1.0 + 3 * 0.044715 * square))
    hidden = (gelu * up).astype(jnp.bfloat16)
    y_ref[...] += mm(hidden, wo_ref[0], LAST)
    go_ref[0] = mm(gt_ref[...], hidden).astype(jnp.bfloat16)
    dhid = mm(g_ref[...], wo_ref[0])
    dup = (dhid * gelu).astype(jnp.bfloat16)
    dgate = (dhid * up * slope).astype(jnp.bfloat16)
    gg_ref[0] = mm(ht_ref[...], dgate).astype(jnp.bfloat16)
    gu_ref[0] = mm(ht_ref[...], dup).astype(jnp.bfloat16)
    dh_ref[...] += mm(dgate, wg_ref[0], LAST) + mm(dup, wu_ref[0], LAST)

    @pl.when(step == pl.num_programs(0) - 1)
    def _():
        out_ref[...] = y_ref[...].astype(jnp.bfloat16)
        back, gain_grad = norm_back(x3_ref[...], gain_ref[pl.ds(2, 1), :], dh_ref[...])
        g3_ref[...] = g_ref[...].astype(jnp.float32) + back
        gn_ref[...] = gain_grad


def last_kernel(
    dh_part_ref, dkv_ref, x_ref, h_ref, gain_ref, g2_ref, ws_ref, wc_ref, dkvc_ref, enc_ref,
    gx_ref, genc_ref, gw_ref, gn_ref,
    ht_ref, et_ref, dh_ref, de_ref,
):
    step = pl.program_id(0)

    @pl.when(step == 0)
    def _():
        ht_ref[...] = jnp.transpose(h_ref[...])
        et_ref[...] = jnp.transpose(enc_ref[...])
        dh_ref[...] = dh_part_ref[...]
        de_ref[...] = jnp.zeros_like(de_ref)

    dkv = dkv_ref[0]
    dkvc = dkvc_ref[0]
    gw_ref[0, :, :QROWS] = mm(ht_ref[...], dkv).astype(jnp.bfloat16)
    gw_ref[0, :, QROWS:] = mm(et_ref[...], dkvc).astype(jnp.bfloat16)
    dh_ref[...] += mm(dkv, ws_ref[0], LAST)
    de_ref[...] += mm(dkvc, wc_ref[0], LAST)

    @pl.when(step == pl.num_programs(0) - 1)
    def _():
        back, gain_grad = norm_back(
            x_ref[...].astype(jnp.float32), gain_ref[pl.ds(0, 1), :], dh_ref[...]
        )
        gx_ref[...] = (g2_ref[pl.ds(0, QROWS), :] + back).astype(jnp.bfloat16)
        genc_ref[...] = de_ref[...].astype(jnp.bfloat16)
        gn_ref[...] = gain_grad


def whole(shape):
    zeros = (0,) * len(shape)
    return pl.BlockSpec(shape, lambda t: zeros)


def part(shape, column=0):
    tail = (0,) * (len(shape) - 2)
    return pl.BlockSpec(shape, lambda t: (t,) + tail + (column,))


SCALARS = pl.BlockSpec(memory_space=pltpu.SMEM)
F32 = jnp.float32
LOW = jnp.bfloat16


def run_heads(kernel, name, ins, specs, outs, out_specs, scratch, flops, steps=4):
    moved = sum(math.prod(a.shape) * a.dtype.itemsize for a in list(ins) + list(outs))
    return pl.pallas_call(
        kernel,
        grid=(steps,),
        in_specs=specs,
        out_specs=out_specs,
        out_shape=outs,
        scratch_shapes=scratch,
        compiler_params=pltpu.CompilerParams(
            dimension_semantics=("arbitrary",), vmem_limit_bytes=VMEM_MOST
        ),
        cost_estimate=pl.CostEstimate(flops=flops, bytes_accessed=moved, transcendentals=0),
        name=name,
    )(*ins)


def shape_of(shape, dtype):
    return jax.ShapeDtypeStruct(shape, dtype)


def feed(info, x3, cot, gain, wg, wu, wo):
    units = wg.shape[2]
    wide = part((1, WIDTH, units))
    return run_heads(
        feed_kernel, "feed",
        (info, x3, cot, gain, wg, wu, wo),
        [SCALARS, whole((QROWS, WIDTH)), whole((QROWS, WIDTH)), whole((8, WIDTH)),
         wide, wide, wide],
        [shape_of((QROWS, WIDTH), LOW), shape_of((QROWS, WIDTH), F32)]
        + [shape_of((4, WIDTH, units), LOW)] * 3
        + [shape_of((1, WIDTH), F32)],
        [whole((QROWS, WIDTH)), whole((QROWS, WIDTH)), wide, wide, wide, whole((1, WIDTH))],
        [pltpu.VMEM((QROWS, WIDTH), LOW), pltpu.VMEM((WIDTH, QROWS), LOW),
         pltpu.VMEM((QROWS, WIDTH), LOW), pltpu.VMEM((WIDTH, QROWS), LOW),
         pltpu.VMEM((QROWS, WIDTH), F32), pltpu.VMEM((QROWS, WIDTH), F32)],
        13 * 10**9,
    )


def last_grads(dh, dkv, x, h, gain, g2, w3, dkvc, enc):
    rows = enc.shape[0]
    return run_heads(
        last_kernel, "last_grads",
        (dh, dkv, x, h, gain, g2, w3, w3, dkvc, enc),
        [whole((QROWS, WIDTH)), part((1, QROWS, 256)), whole((QROWS, WIDTH)),
         whole((QROWS, WIDTH)), whole((8, WIDTH)), whole((QROWS + 8, WIDTH)),
         part((1, WIDTH, 256)), part((1, WIDTH, 256), 1), part((1, rows, 256)),
         whole((rows, WIDTH))],
        [shape_of((QROWS, WIDTH), LOW), shape_of((rows, WIDTH), LOW),
         shape_of((4, WIDTH, 512), LOW), shape_of((1, WIDTH), F32)],
        [whole((QROWS, WIDTH)), whole((rows, WIDTH)), part((1, WIDTH, 512)),
         whole((1, WIDTH))],
        [pltpu.VMEM((WIDTH, QROWS), LOW), pltpu.VMEM((WIDTH, rows), LOW),
         pltpu.VMEM((QROWS, WIDTH), F32), pltpu.VMEM((rows, WIDTH), F32)],
        3 * 10**9,
    )


GATHER_ORDERS = ("zyx", "zyx", "xzy", "yzx", "zxy", "yzx", "zxy", "y", "y")
SMALL_ROWS = 16
LANES = 128


def split_steps(steps, parts, low, high):
    ends = [int(len(steps) * (low + (high - low) * (i + 1) / parts)) for i in range(parts)]
    return [steps[a:b] for a, b in zip([0] + ends, ends)], steps[ends[-1] :]


def at_step(t, chunks):
    for i, chunk in enumerate(chunks):

        def run():
            for step in chunk:
                step()

        if chunk:
            pl.when(t == i)(run)


def forward_kernel(rows, *refs):
    lengths, ins = refs[0], refs[1:10]
    weights, refs = refs[10:16], refs[16:]
    gains_ref, x2_ref, x3_ref, h1_out, h2_ref = refs[:5]
    q1_out, kv1_out, p1_out, o1_out, q2_out, kv2_out, p2_out, o2_out = refs[5:13]
    small, x_all, enc_all, bucket_ref, h1_ref, s_ref, strip_ref, ot_ref = refs[13:21]
    place = Place()
    plan = Gather(place, GATHER_ORDERS, rows, ins, weights + (small, x_all, enc_all), refs[21:])
    greet(place)
    half = lax.rem(place.z, 2)
    first = pl.multiple_of(place.y * (2 * QROWS) + half * QROWS, QROWS)
    length = lengths[lax.div(place.z, 2)]
    plan.start(range(3, 9))
    row = lax.broadcasted_iota(jnp.int32, (8, SPAN), 0)
    col = lax.broadcasted_iota(jnp.int32, (8, SPAN), 1)
    bucket_ref[...] = bucket_index(jnp.maximum(first + col - (SPAN - 264) - row, 0))
    for _, step in plan.steps(lambda j, k: 3 <= j < 7 and k < 2):
        step()
    plan.start(range(3))
    for _, step in plan.steps(lambda j, k: j >= 7 or (j >= 3 and k == 2)):
        step()
    plan.settle(range(3, 9))
    feed_steps = [step for _, step in plan.steps(lambda j, k: j < 3)]
    chunks, rest = split_steps(feed_steps, 8, 0.0, 0.7)

    for k in range(3):
        gains_ref[pl.ds(k, 1), :] = jnp.concatenate(
            [small[0, pl.ds(r * SMALL_ROWS + k, 1), :] for r in range(8)], axis=1
        )
    gain = gains_ref[pl.ds(0, 1), :]
    for y in range(2):
        for c in range(2):
            at = pl.ds(c * QROWS, QROWS)
            h1_ref[pl.ds(y * 512 + c * QROWS, QROWS), :] = norm_rows(
                x_all[y, at, :].astype(jnp.float32), gain
            ).astype(jnp.bfloat16)
    x2_ref[...] = ins[7][pl.ds(half * QROWS, QROWS), :].astype(jnp.float32)
    h1_out[...] = h1_ref[pl.ds(first, QROWS), :]

    def self_body(w_ref, wkv_ref, q_ref, kv_ref, p_ref, o_ref):
        t = pl.program_id(0)

        def near_of(head):
            rows_of = [small[t, pl.ds(r * SMALL_ROWS + 3, 1), :] for r in range(8)]
            bucket = bucket_ref[...]
            near = jnp.zeros((8, SPAN), jnp.float32)
            for i in range(BUCKETS):
                lane = (i % 4) * 4 + head
                value = rows_of[i // 4][:, lane : lane + 1]
                near = jnp.where(bucket == i, value, near)
            return near

        x2_ref[...] += self_step(
            first, length, h1_ref, w_ref, wkv_ref, near_of, q_ref, kv_ref, p_ref, o_ref,
            (s_ref, strip_ref, ot_ref),
        )
        at_step(t, chunks[:4])

    pltpu.emit_pipeline(
        self_body,
        grid=(4,),
        in_specs=[part((1, WIDTH, 512)), part((1, WIDTH, 256))],
        out_specs=[
            part((1, QROWS, 256)), part((1, KEYS, 256)), part((1, 2, KEYS, 512)),
            part((1, QROWS, 256)),
        ],
    )(weights[3], weights[5], q1_out, kv1_out, p1_out, o1_out)
    x3_ref[...] = x2_ref[...]
    h2_ref[...] = norm_rows(x2_ref[...], gains_ref[pl.ds(1, 1), :]).astype(jnp.bfloat16)

    def cross_body(w_ref, wkv_ref, q_ref, kv_ref, p_ref, o_ref):
        enc = jnp.concatenate([enc_all[0], enc_all[1]], axis=0)
        x3_ref[...] += cross_step(
            h2_ref, enc, w_ref, wkv_ref, q_ref, kv_ref, p_ref, o_ref, (s_ref, ot_ref)
        )
        at_step(pl.program_id(0), chunks[4:])

    pltpu.emit_pipeline(
        cross_body,
        grid=(4,),
        in_specs=[part((1, WIDTH, 512)), part((1, WIDTH, 256), 1)],
        out_specs=[
            part((1, QROWS, 256)), part((1, ENC_ROWS, 256)), part((1, 2, ENC_ROWS, 512)),
            part((1, QROWS, 256)),
        ],
    )(weights[4], weights[5], q2_out, kv2_out, p2_out, o2_out)
    for step in rest:
        step()
    plan.settle(range(3))
    plan.sent()


def forward(lengths, arrays):
    rows = [a.shape[0] for a in arrays]
    wide = [gathered(a, o) for a, o in zip(arrays, GATHER_ORDERS)]
    vm = pltpu.VMEM
    return comm_call(
        functools.partial(forward_kernel, rows), "forward", 1,
        (lengths,) + tuple(arrays), [SCALARS] + [INSIDE] * 9,
        wide[:6]
        + [shape_of((8, WIDTH), F32), shape_of((QROWS, WIDTH), F32),
           shape_of((QROWS, WIDTH), F32), shape_of((QROWS, WIDTH), LOW),
           shape_of((QROWS, WIDTH), LOW),
           shape_of((4, QROWS, 256), LOW), shape_of((4, KEYS, 256), LOW),
           shape_of((4, 2, KEYS, 512), LOW), shape_of((4, QROWS, 256), LOW),
           shape_of((4, QROWS, 256), LOW), shape_of((4, ENC_ROWS, 256), LOW),
           shape_of((4, 2, ENC_ROWS, 512), LOW), shape_of((4, QROWS, 256), LOW)],
        [HBM] * 6 + [INSIDE] * 5 + [HBM] * 8,
        [vm(w.shape, w.dtype) for w in wide[6:]]
        + [vm((8, SPAN), jnp.int32), vm((KEYS, WIDTH), LOW), vm((KEYS, 512), F32),
           vm((2, CHUNK, SPAN), F32), vm((256, QROWS), F32)]
        + Gather.scratch(9),
    )


FEED_ORDERS = ("zxy", "zyx", "zyx")


def backward_kernel(rows, own, room, *refs):
    grads, refs = refs[:3], refs[3:]
    out_ref, g3_ref, x2_ref, h2_ref, h1_ref, gains_ref = refs[:6]
    w1, w2, q1, kv1, p1, o1, q2, kv2, p2, o2 = refs[6:16]
    shards, refs = refs[16:19], refs[19:]
    dkv1_out, dkv2_out, rows_out, g2_ref, dh_ref, near_ref, gw1, gw2 = refs[:8]
    dkv1, dkv2, g_ref, gt_ref, ht_ref, dc_ref, d_ref, ds_ref, qt_ref, strip_ref = refs[8:18]
    scratch = refs[18:]
    place = Place()
    plan = Scatter(place, FEED_ORDERS, rows, grads, shards, scratch[: len(room)])
    scratch = scratch[len(room) :]
    share = Share(place, own, (dkv1, dkv2), (dkv1_out, dkv2_out), scratch[:8])
    lines = Gather(place, ("z",), (QROWS,), (out_ref,), (rows_out,), scratch[8:])
    greet(place)
    lines.start()
    plan.start()
    steps = [step for _, step in plan.steps()]
    begin = len(steps) // 10
    for step in steps[:begin]:
        step()
    chunks, rest = split_steps(steps[begin:], 8, 0.0, 0.6)

    def load_grad(ref, h_ref):
        g = ref[...].astype(jnp.bfloat16)
        g_ref[...] = g
        gt_ref[...] = jnp.transpose(g)
        ht_ref[...] = jnp.transpose(h_ref[...])

    def heads(t, w_ref, q_ref, kv_ref, p_ref, o_ref, gw_ref, dkv, d_sum, keys, take_bias):
        do = mm(g_ref[...], w_ref[0, :, QROWS:]).astype(jnp.bfloat16)
        gw_ref[0, :, QROWS:] = mm(gt_ref[...], o_ref[0]).astype(jnp.bfloat16)
        dq = attend_back(
            q_ref[0], kv_ref[0], p_ref, do, dkv.at[pl.ds(t, 1)], d_ref, ds_ref, qt_ref, keys,
            take_bias,
        )
        gw_ref[0, :, :QROWS] = mm(ht_ref[...], dq).astype(jnp.bfloat16)
        d_sum[...] += mm(dq, w_ref[0, :, :QROWS], LAST)

    def specs(keys):
        return [
            part((1, WIDTH, 512)), part((1, QROWS, 256)), part((1, keys, 256)),
            part((1, 2, keys, 512)), part((1, QROWS, 256)),
        ]

    load_grad(g3_ref, h2_ref)
    dc_ref[...] = jnp.zeros_like(dc_ref)

    def cross_body(w_ref, q_ref, kv_ref, p_ref, o_ref, gw_ref):
        t = pl.program_id(0)
        heads(t, w_ref, q_ref, kv_ref, p_ref, o_ref, gw_ref, dkv2, dc_ref, ENC_ROWS, None)
        at_step(t, chunks[:4])

    pltpu.emit_pipeline(
        cross_body, grid=(4,), in_specs=specs(ENC_ROWS), out_specs=[part((1, WIDTH, 512))]
    )(w2, q2, kv2, p2, o2, gw2)
    back, gain_grad = norm_back(x2_ref[...], gains_ref[pl.ds(1, 1), :], dc_ref[...])
    g2_ref[pl.ds(0, QROWS), :] = g3_ref[...] + back
    g2_ref[pl.ds(QROWS, 1), :] = gain_grad
    load_grad(g2_ref.at[pl.ds(0, QROWS)], h1_ref)
    dh_ref[...] = jnp.zeros_like(dh_ref)

    def self_body(w_ref, q_ref, kv_ref, p_ref, o_ref, gw_ref):
        t = pl.program_id(0)

        def take_bias(a, c, ds):
            if c is None:
                for b in range(2):
                    total = jnp.zeros((8, SPAN), jnp.float32)
                    for g in range(16):
                        piece = strip_ref[b, 8 * g : 8 * g + 8, :]
                        shift = 120 - 8 * g
                        total = total + (pltpu.roll(piece, shift, 1) if shift else piece)
                    near_ref[t, 2 * a + b] = total
                return
            if c == 0:
                strip_ref[...] = jnp.zeros_like(strip_ref)
            cols = pl.ds(CHUNK * (7 - c), QROWS)
            strip_ref[0, :, cols] += ds[:, :QROWS]
            strip_ref[1, :, cols] += ds[:, QROWS:]

        heads(t, w_ref, q_ref, kv_ref, p_ref, o_ref, gw_ref, dkv1, dh_ref, KEYS, take_bias)
        at_step(t, chunks[4:])

    pltpu.emit_pipeline(
        self_body, grid=(4,), in_specs=specs(KEYS), out_specs=[part((1, WIDTH, 512))]
    )(w1, q1, kv1, p1, o1, gw1)
    share.start()
    ordered = [(i / max(len(rest), 1), step) for i, step in enumerate(rest)]
    ordered += [(0.05 + 0.9 * at, step) for at, step in share.steps()]
    ordered += [(0.1 * at, step) for at, step in lines.steps()]
    ordered.sort(key=lambda s: s[0])
    for _, step in ordered:
        step()
    lines.finish()
    share.finish()
    plan.finish()


def backward(grads, out, g3, x2, h2, h1, gains, w1, w2, saved1, saved2):
    rows = [a.shape[1] // 8 for a in grads]
    own = [KEYS // 4, ENC_ROWS // 4]
    room = Scatter.scratch(grads, rows, FEED_ORDERS)
    vm = pltpu.VMEM
    return comm_call(
        functools.partial(backward_kernel, rows, own, room), "backward", 2,
        tuple(grads) + (out, g3, x2, h2, h1, gains, w1, w2) + tuple(saved1) + tuple(saved2),
        [HBM] * 3 + [INSIDE] * 6 + [HBM] * 10,
        scattered(grads)
        + [shape_of((4, r, 256), LOW) for r in own]
        + [gathered(out, "z"), shape_of((QROWS + 8, WIDTH), F32), shape_of((QROWS, WIDTH), F32),
           shape_of((4, 4, 8, SPAN), F32), shape_of(w1.shape, LOW), shape_of(w2.shape, LOW)],
        [INSIDE] * 5 + [HBM] + [INSIDE] * 3 + [HBM] * 2,
        [vm((4, KEYS, 256), LOW), vm((4, ENC_ROWS, 256), LOW), vm((QROWS, WIDTH), LOW),
         vm((WIDTH, QROWS), LOW), vm((WIDTH, QROWS), LOW), vm((QROWS, WIDTH), F32),
         vm((KEYS, 512), F32), vm((KEYS, 512), LOW), vm((256, QROWS), F32),
         vm((2, CHUNK, SPAN), F32)]
        + room + Share.scratch(own) + Gather.scratch(1),
    )


HEAD_ORDERS = ("zyx", "zxy", "zyx", "zxy")


def small_rows(gains, table):
    flat = jnp.pad(table.reshape(1, -1).astype(F32), ((0, 0), (0, LANES - table.size)))
    rows = jnp.concatenate([g.reshape(1, LANES).astype(F32) for g in gains] + [flat], axis=0)
    return jnp.pad(rows, ((0, SMALL_ROWS - 4), (0, 0)))


def tokens_split(
    inputs, encoder, lengths, cotangent,
    norm_self, self_query, self_key_matrix, self_value_matrix, self_out, bias_table,
    norm_cross, cross_query, cross_key_matrix, cross_value_matrix, cross_out,
    norm_feed, feed_gate, feed_up, feed_out,
):
    y = lax.axis_index("ctx")
    t = lax.axis_index("tp")
    seq, half = lax.div(t, 2), lax.rem(t, 2)
    first = y * (2 * QROWS) + half * QROWS
    info = jnp.stack([first, lax.dynamic_index_in_dim(lengths, seq, 0, False)])
    x_seq = lax.dynamic_index_in_dim(inputs, seq, 0, False)
    enc_seq = lax.dynamic_index_in_dim(encoder, seq, 0, False)
    x_own = lax.dynamic_slice_in_dim(x_seq, half * QROWS, QROWS, 0)
    cot = lax.dynamic_slice(cotangent, (seq, half * QROWS, 0), (1, QROWS, WIDTH))[0]
    packed = (
        feed_gate, feed_up, feed_out,
        jnp.concatenate([self_query, self_out], axis=1),
        jnp.concatenate([cross_query, cross_out], axis=1),
        jnp.concatenate(
            [self_key_matrix, self_value_matrix, cross_key_matrix, cross_value_matrix], axis=1
        ),
        small_rows((norm_self, norm_cross, norm_feed), bias_table),
        x_seq, enc_seq,
    )
    (
        wg, wu, wo, w1, w2, w3, gains, x2, x3, h1, h2, q1, kv1, p1, o1, q2, kv2, p2, o2,
    ) = forward(lengths, packed)
    distance = jnp.maximum(
        first + jnp.arange(SPAN)[None, :] - (SPAN - 264) - jnp.arange(8)[:, None], 0
    )
    bucket = bucket_index(distance)
    out, g3, gg, gu, go, gn3 = feed(info, x3, cot, gains, wg, wu, wo)
    gg, gu, go, dkv, dkvc, out, g2, dh, near, gw1, gw2 = backward(
        (gg, gu, go), out, g3, x2, h2, h1, gains, w1, w2, (q1, kv1, p1, o1), (q2, kv2, p2, o2)
    )
    gn2 = g2[QROWS : QROWS + 1]
    enc_own = lax.dynamic_slice_in_dim(enc_seq, half * (QROWS // 2), QROWS // 2, 0)
    gx, genc, gw3, gn1 = last_grads(
        dh, dkv, x_own, h1, gains, g2, w3, dkvc, enc_own
    )
    one_hot = (bucket[:, :, None] == jnp.arange(BUCKETS, dtype=jnp.int32)).astype(F32)
    grad_table = jnp.einsum(
        "hrm,rmb->bh", near.reshape(16, 8, SPAN), one_hot, precision=TOP_PRECISION
    )
    gain_grads = jnp.concatenate([gn1, gn2, gn3], axis=0).reshape(3, 8, LANES)
    gain_grads = jnp.broadcast_to(jnp.transpose(gain_grads, (1, 0, 2))[None], (4, 8, 3, LANES))
    table_grads = jnp.transpose(grad_table.reshape(8, 4, 4, 4), (2, 0, 1, 3)).reshape(4, 8, 1, 16)
    table_grads = jnp.pad(table_grads, ((0, 0), (0, 0), (0, 0), (0, LANES - 16)))
    small_grads = jnp.pad(
        jnp.concatenate([gain_grads, table_grads], axis=2),
        ((0, 0), (0, 0), (0, SMALL_ROWS - 4), (0, 0)),
    ).reshape(4, 8 * SMALL_ROWS, LANES)
    gw1, gw2, gw3, gs, gx, genc = scatter_and_rows(
        (gw1, gw2, gw3, small_grads), HEAD_ORDERS, (gx, genc), "scatter_heads"
    )
    return (
        out.reshape(inputs.shape),
        gx.reshape(inputs.shape).astype(F32),
        genc.reshape(encoder.shape).astype(F32),
        gs[0], gw1[:, :256], gw3[:, :128], gw3[:, 128:256], gw1[:, 256:],
        gs[3, :16].reshape(4, 4),
        gs[1], gw2[:, :256], gw3[:, 256:384], gw3[:, 384:], gw2[:, 256:],
        gs[2], gg, gu, go,
    )


def solution(mesh):
    sizes = (mesh.shape["fsdp"], mesh.shape["ctx"], mesh.shape["tp"])
    return jax.shard_map(
        tokens_split if sizes == (4, 2, DEPTH) else shards,
        mesh=mesh,
        in_specs=(
            P("fsdp", "ctx", None),
            P("fsdp", "ctx", None),
            P("fsdp"),
            P("fsdp", "ctx", None),
            P(("fsdp", "ctx")),
            P(("fsdp", "ctx"), "tp"),
            P(("fsdp", "ctx"), "tp"),
            P(("fsdp", "ctx"), "tp"),
            P(("fsdp", "ctx"), "tp"),
            P(("fsdp", "ctx"), "tp"),
            P(("fsdp", "ctx")),
            P(("fsdp", "ctx"), "tp"),
            P(("fsdp", "ctx"), "tp"),
            P(("fsdp", "ctx"), "tp"),
            P(("fsdp", "ctx"), "tp"),
            P(("fsdp", "ctx")),
            P(("fsdp", "ctx"), "tp"),
            P(("fsdp", "ctx"), "tp"),
            P(("fsdp", "ctx"), "tp"),
        ),
        out_specs=(
            P("fsdp", "ctx", None),
            P("fsdp", "ctx", None),
            P("fsdp", "ctx", None),
            P(("fsdp", "ctx")),
            P(("fsdp", "ctx"), "tp"),
            P(("fsdp", "ctx"), "tp"),
            P(("fsdp", "ctx"), "tp"),
            P(("fsdp", "ctx"), "tp"),
            P(("fsdp", "ctx"), "tp"),
            P(("fsdp", "ctx")),
            P(("fsdp", "ctx"), "tp"),
            P(("fsdp", "ctx"), "tp"),
            P(("fsdp", "ctx"), "tp"),
            P(("fsdp", "ctx"), "tp"),
            P(("fsdp", "ctx")),
            P(("fsdp", "ctx"), "tp"),
            P(("fsdp", "ctx"), "tp"),
            P(("fsdp", "ctx"), "tp"),
        ),
        check_vma=False,
    )
```

```python
import functools
import math

import jax
import jax.numpy as jnp
from jax import lax
from jax.experimental import pallas as pl
from jax.experimental.pallas import tpu as pltpu
from jax.sharding import PartitionSpec as P

HEAD_SIZE = 64
BUCKETS = 32
MAXDIST = 128


EPSILON = 1e-06
MASKED = -1000000000.0
TOP_PRECISION = lax.Precision.HIGHEST


def rms_scale(values, gain_row):
    inverse = lax.rsqrt(jnp.mean(values * values, axis=-1, keepdims=True) + EPSILON)
    return values * inverse * gain_row


def gated_product(gate_in, up_in):
    return jax.nn.gelu(gate_in, approximate=True) * up_in


def project(operand_array, weight_arrays):
    return jnp.einsum(
        "spd,dk->spk", operand_array, weight_arrays, preferred_element_type=jnp.float32
    )


def project_back(grad_cols, weight_arrays):
    return jnp.einsum("spk,dk->spd", grad_cols, weight_arrays, preferred_element_type=jnp.float32)


def weight_grad(operand_array, grad_cols):
    return jnp.einsum("spd,spk->dk", operand_array, grad_cols, preferred_element_type=jnp.float32)


def bucket_index(distance):
    exact_count = BUCKETS // 2
    counter = jnp.zeros(distance.shape, jnp.int32)
    for level_index in range(1, BUCKETS - exact_count):
        border = math.ceil(
            exact_count * (MAXDIST / exact_count) ** (level_index / (BUCKETS - exact_count))
        )
        counter = counter + (distance >= border).astype(jnp.int32)
    return jnp.where(distance < exact_count, distance, exact_count + counter)


def reduce_rows(partial_sum):
    return lax.psum(partial_sum, "tp")


def block_scores(queries, key_rows, bias_rows, allowed):
    scores = jnp.einsum("gpkrd,gjkd->gkrpj", queries, key_rows, preferred_element_type=jnp.float32)
    if bias_rows is not None:
        scores = jnp.where(allowed[:, None, None], scores + bias_rows[None], MASKED)
    return scores


def forward_block(queries, key_rows, value_rows, bias_rows, allowed):
    scores = block_scores(queries, key_rows, bias_rows, allowed)
    row_peak = jnp.max(scores, axis=-1, keepdims=True)
    log_total = row_peak + jnp.log(jnp.sum(jnp.exp(scores - row_peak), axis=-1, keepdims=True))
    weights_low = jnp.exp(scores - log_total).astype(jnp.bfloat16)
    output = jnp.einsum(
        "gkrpj,gjkd->gpkrd", weights_low, value_rows, preferred_element_type=jnp.float32
    )
    return (output.astype(jnp.bfloat16), log_total)


def backward_block(queries, key_rows, value_rows, bias_rows, allowed, log_total, grad_out):
    scores = block_scores(queries, key_rows, bias_rows, allowed)
    softmax_rows = jnp.exp(scores - log_total)
    grad_probs = jnp.einsum(
        "gpkrd,gjkd->gkrpj", grad_out, value_rows, preferred_element_type=jnp.float32
    )
    grad_scores = softmax_rows * (
        grad_probs - jnp.sum(grad_probs * softmax_rows, axis=-1, keepdims=True)
    )
    scores_low = grad_scores.astype(jnp.bfloat16)
    grad_query = jnp.einsum(
        "gkrpj,gjkd->gpkrd", scores_low, key_rows, preferred_element_type=jnp.float32
    )
    grad_key = jnp.einsum(
        "gkrpj,gpkrd->gjkd", scores_low, queries, preferred_element_type=jnp.float32
    )
    grad_value = jnp.einsum(
        "gkrpj,gpkrd->gjkd",
        softmax_rows.astype(jnp.bfloat16),
        grad_out,
        preferred_element_type=jnp.float32,
    )
    if bias_rows is None:
        grad_bias = jnp.zeros((1,), jnp.float32)
    else:
        grad_bias = jnp.sum(grad_scores, axis=0)
    return (grad_query.astype(jnp.bfloat16), grad_key, grad_value, grad_bias)


def block_shapes(queries, key_rows, block_seqs):
    seq_count, row_total_count, query_cols = queries.shape
    key_total_count, key_cols = (key_rows.shape[1], key_rows.shape[2])
    kv_heads = key_cols // HEAD_SIZE
    repeats = query_cols // key_cols
    blocks = seq_count // block_seqs
    query_shape = (blocks, block_seqs, row_total_count, kv_heads, repeats, HEAD_SIZE)
    key_shape = (blocks, block_seqs, key_total_count, kv_heads, HEAD_SIZE)
    mask_shape = (blocks, block_seqs, row_total_count, key_total_count)
    return (query_shape, key_shape, mask_shape)


def attention_forward(queries, key_rows, value_rows, bias_rows, allowed, block_seqs):
    query_shape, key_shape, mask_shape = block_shapes(queries, key_rows, block_seqs)
    sources = (
        queries.reshape(query_shape),
        key_rows.reshape(key_shape),
        value_rows.reshape(key_shape),
    )
    if allowed is not None:
        sources = sources + (allowed.reshape(mask_shape),)

    def one_block(piece_list):
        mask_block = piece_list[3] if allowed is not None else None
        return forward_block(piece_list[0], piece_list[1], piece_list[2], bias_rows, mask_block)

    outputs, log_totals = lax.map(one_block, sources)
    return (outputs.reshape(queries.shape), log_totals)


def attention_backward(
    queries, key_rows, value_rows, bias_rows, allowed, log_totals, grad_out, block_seqs
):
    query_shape, key_shape, mask_shape = block_shapes(queries, key_rows, block_seqs)
    sources = (
        queries.reshape(query_shape),
        key_rows.reshape(key_shape),
        value_rows.reshape(key_shape),
        log_totals,
        grad_out.reshape(query_shape),
    )
    if allowed is not None:
        sources = sources + (allowed.reshape(mask_shape),)
    if bias_rows is None:
        initial = jnp.zeros((1,), jnp.float32)
    else:
        initial = jnp.zeros(bias_rows.shape, jnp.float32)

    def one_block(running, piece_list):
        mask_block = piece_list[5] if allowed is not None else None
        grad_query, grad_key, grad_value, grad_bias = backward_block(
            piece_list[0],
            piece_list[1],
            piece_list[2],
            bias_rows,
            mask_block,
            piece_list[3],
            piece_list[4],
        )
        return (running + grad_bias, (grad_query, grad_key, grad_value))

    bias_total, grad_list = lax.scan(one_block, initial, sources)
    return (
        grad_list[0].reshape(queries.shape),
        grad_list[1].reshape(key_rows.shape),
        grad_list[2].reshape(value_rows.shape),
        bias_total,
    )


def shards(
    inputs,
    encoder,
    lengths,
    cotangent,
    norm_self,
    self_query,
    self_key_matrix,
    self_value_matrix,
    self_out,
    bias_table,
    norm_cross,
    cross_query,
    cross_key_matrix,
    cross_value_matrix,
    cross_out,
    norm_feed,
    feed_gate,
    feed_up,
    feed_out,
):
    self_group = (
        lax.all_gather(norm_self, ("fsdp", "ctx"), axis=0, tiled=True),
        lax.all_gather(self_query, ("fsdp", "ctx"), axis=0, tiled=True),
        lax.all_gather(self_key_matrix, ("fsdp", "ctx"), axis=0, tiled=True),
        lax.all_gather(self_value_matrix, ("fsdp", "ctx"), axis=0, tiled=True),
        lax.all_gather(self_out, ("fsdp", "ctx"), axis=0, tiled=True),
        lax.all_gather(bias_table, ("fsdp", "ctx"), axis=0, tiled=True),
    )
    seq_count, row_total_count = (inputs.shape[0], inputs.shape[1])
    block_seqs = max((trial for trial in (1, 2, 3, 4) if seq_count % trial == 0))
    start_row = lax.axis_index("ctx") * row_total_count
    key_total_count = row_total_count * lax.axis_size("ctx")
    row_pos = start_row + jnp.arange(row_total_count, dtype=jnp.int32)
    col_pos = jnp.arange(key_total_count, dtype=jnp.int32)
    buckets = bucket_index(jnp.maximum(row_pos[:, None] - col_pos[None, :], 0))
    one_hot = (buckets[:, :, None] == jnp.arange(BUCKETS, dtype=jnp.int32)[None, None, :]).astype(
        jnp.float32
    )
    causal = col_pos[None, :] <= row_pos[:, None]
    allowed = causal[None] & (col_pos[None, None, :] < lengths[:, None, None])
    hidden_in = inputs.astype(jnp.float32)
    normed_one, norm_pull_one = jax.vjp(rms_scale, hidden_in, self_group[0].astype(jnp.float32))
    self_in = normed_one.astype(jnp.bfloat16)
    self_q = project(self_in, self_group[1]).astype(jnp.bfloat16)
    self_k = project(self_in, self_group[2]).astype(jnp.bfloat16)
    self_v = project(self_in, self_group[3]).astype(jnp.bfloat16)
    keys_self, values_self = (
        lax.all_gather(self_k, "ctx", axis=1, tiled=True),
        lax.all_gather(self_v, "ctx", axis=1, tiled=True),
    )
    heads_local = self_group[1].shape[1] // HEAD_SIZE
    kv_local = self_group[2].shape[1] // HEAD_SIZE
    table_rows = self_group[5].astype(jnp.float32)
    bias_rows = jnp.einsum("ijb,bh->hij", one_hot, table_rows, precision=TOP_PRECISION).reshape(
        kv_local, heads_local // kv_local, row_total_count, key_total_count
    )
    self_att, lse_self = attention_forward(
        self_q, keys_self, values_self, bias_rows, allowed, block_seqs
    )
    hidden_two = hidden_in + reduce_rows(project_back(self_att, self_group[4]))
    cross_group = (
        lax.all_gather(norm_cross, ("fsdp", "ctx"), axis=0, tiled=True),
        lax.all_gather(cross_query, ("fsdp", "ctx"), axis=0, tiled=True),
        lax.all_gather(cross_key_matrix, ("fsdp", "ctx"), axis=0, tiled=True),
        lax.all_gather(cross_value_matrix, ("fsdp", "ctx"), axis=0, tiled=True),
        lax.all_gather(cross_out, ("fsdp", "ctx"), axis=0, tiled=True),
    )
    normed_two, norm_pull_two = jax.vjp(rms_scale, hidden_two, cross_group[0].astype(jnp.float32))
    cross_in = normed_two.astype(jnp.bfloat16)
    cross_q = project(cross_in, cross_group[1]).astype(jnp.bfloat16)
    enc_keys = project(encoder, cross_group[2]).astype(jnp.bfloat16)
    enc_values = project(encoder, cross_group[3]).astype(jnp.bfloat16)
    keys_cross, values_cross = (
        lax.all_gather(enc_keys, "ctx", axis=1, tiled=True),
        lax.all_gather(enc_values, "ctx", axis=1, tiled=True),
    )
    cross_att, lse_cross = attention_forward(
        cross_q, keys_cross, values_cross, None, None, block_seqs
    )
    hidden_three = hidden_two + reduce_rows(project_back(cross_att, cross_group[4]))
    feed_group = (
        lax.all_gather(norm_feed, ("fsdp", "ctx"), axis=0, tiled=True),
        lax.all_gather(feed_gate, ("fsdp", "ctx"), axis=0, tiled=True),
        lax.all_gather(feed_up, ("fsdp", "ctx"), axis=0, tiled=True),
        lax.all_gather(feed_out, ("fsdp", "ctx"), axis=0, tiled=True),
    )
    normed_three, norm_pull_three = jax.vjp(
        rms_scale, hidden_three, feed_group[0].astype(jnp.float32)
    )
    feed_in = normed_three.astype(jnp.bfloat16)
    gate_value = project(feed_in, feed_group[1])
    up_value = project(feed_in, feed_group[2])
    gated_value, gated_pull = jax.vjp(gated_product, gate_value, up_value)
    feed_hidden = gated_value.astype(jnp.bfloat16)
    hidden_four = hidden_three + reduce_rows(project_back(feed_hidden, feed_group[3]))
    output = hidden_four.astype(jnp.bfloat16)
    valid_rows = (row_pos[None, :] < lengths[:, None]).astype(jnp.float32)
    grad_full = cotangent.astype(jnp.float32) * valid_rows[:, :, None]
    branch_low = grad_full.astype(jnp.bfloat16)
    grad_hidden = grad_full
    grad_feed_out = weight_grad(branch_low, feed_hidden)
    grad_gated = project(branch_low, feed_group[3])
    grad_gate, grad_up = gated_pull(grad_gated)
    gate_low = grad_gate.astype(jnp.bfloat16)
    up_low = grad_up.astype(jnp.bfloat16)
    grad_feed_gate = weight_grad(feed_in, gate_low)
    grad_feed_up = weight_grad(feed_in, up_low)
    grad_feed_in = reduce_rows(
        project_back(gate_low, feed_group[1]) + project_back(up_low, feed_group[2])
    )
    grad_three, grad_gain_three = norm_pull_three(grad_feed_in)
    grad_hidden = grad_hidden + grad_three
    feed_grads = (
        lax.psum_scatter(
            grad_gain_three.astype(jnp.bfloat16), ("fsdp", "ctx"), scatter_dimension=0, tiled=True
        ).astype(jnp.float32),
        lax.psum_scatter(
            grad_feed_gate.astype(jnp.bfloat16), ("fsdp", "ctx"), scatter_dimension=0, tiled=True
        ).astype(jnp.float32),
        lax.psum_scatter(
            grad_feed_up.astype(jnp.bfloat16), ("fsdp", "ctx"), scatter_dimension=0, tiled=True
        ).astype(jnp.float32),
        lax.psum_scatter(
            grad_feed_out.astype(jnp.bfloat16), ("fsdp", "ctx"), scatter_dimension=0, tiled=True
        ).astype(jnp.float32),
    )
    cross_low = grad_hidden.astype(jnp.bfloat16)
    grad_cross_out = weight_grad(cross_low, cross_att)
    grad_cross_att = project(cross_low, cross_group[4]).astype(jnp.bfloat16)
    grad_cq, grad_ck_part, grad_cv_part, unused_bias = attention_backward(
        cross_q, keys_cross, values_cross, None, None, lse_cross, grad_cross_att, block_seqs
    )
    grad_ck, grad_cv = (
        lax.psum_scatter(
            grad_ck_part.astype(jnp.bfloat16), "ctx", scatter_dimension=1, tiled=True
        ).astype(jnp.float32),
        lax.psum_scatter(
            grad_cv_part.astype(jnp.bfloat16), "ctx", scatter_dimension=1, tiled=True
        ).astype(jnp.float32),
    )
    ck_low = grad_ck.astype(jnp.bfloat16)
    cv_low = grad_cv.astype(jnp.bfloat16)
    grad_cross_query = weight_grad(cross_in, grad_cq)
    grad_cross_key = weight_grad(encoder, ck_low)
    grad_cross_value = weight_grad(encoder, cv_low)
    grad_cross_in, grad_encoder = reduce_rows(
        (
            project_back(grad_cq, cross_group[1]),
            project_back(ck_low, cross_group[2]) + project_back(cv_low, cross_group[3]),
        )
    )
    grad_two, grad_gain_two = norm_pull_two(grad_cross_in)
    grad_hidden = grad_hidden + grad_two
    cross_grads = (
        lax.psum_scatter(
            grad_gain_two.astype(jnp.bfloat16), ("fsdp", "ctx"), scatter_dimension=0, tiled=True
        ).astype(jnp.float32),
        lax.psum_scatter(
            grad_cross_query.astype(jnp.bfloat16), ("fsdp", "ctx"), scatter_dimension=0, tiled=True
        ).astype(jnp.float32),
        lax.psum_scatter(
            grad_cross_key.astype(jnp.bfloat16), ("fsdp", "ctx"), scatter_dimension=0, tiled=True
        ).astype(jnp.float32),
        lax.psum_scatter(
            grad_cross_value.astype(jnp.bfloat16), ("fsdp", "ctx"), scatter_dimension=0, tiled=True
        ).astype(jnp.float32),
        lax.psum_scatter(
            grad_cross_out.astype(jnp.bfloat16), ("fsdp", "ctx"), scatter_dimension=0, tiled=True
        ).astype(jnp.float32),
    )
    self_low = grad_hidden.astype(jnp.bfloat16)
    grad_self_out = weight_grad(self_low, self_att)
    grad_self_att = project(self_low, self_group[4]).astype(jnp.bfloat16)
    grad_sq, grad_sk_part, grad_sv_part, bias_total = attention_backward(
        self_q, keys_self, values_self, bias_rows, allowed, lse_self, grad_self_att, block_seqs
    )
    grad_sk, grad_sv = (
        lax.psum_scatter(
            grad_sk_part.astype(jnp.bfloat16), "ctx", scatter_dimension=1, tiled=True
        ).astype(jnp.float32),
        lax.psum_scatter(
            grad_sv_part.astype(jnp.bfloat16), "ctx", scatter_dimension=1, tiled=True
        ).astype(jnp.float32),
    )
    sk_low = grad_sk.astype(jnp.bfloat16)
    sv_low = grad_sv.astype(jnp.bfloat16)
    grad_table = jnp.einsum(
        "ijb,hij->bh",
        one_hot,
        bias_total.reshape(heads_local, row_total_count, key_total_count),
        precision=TOP_PRECISION,
    )
    grad_self_query = weight_grad(self_in, grad_sq)
    grad_self_key = weight_grad(self_in, sk_low)
    grad_self_value = weight_grad(self_in, sv_low)
    grad_self_in = reduce_rows(
        project_back(grad_sq, self_group[1])
        + project_back(sk_low, self_group[2])
        + project_back(sv_low, self_group[3])
    )
    grad_one, grad_gain_one = norm_pull_one(grad_self_in)
    grad_inputs = grad_hidden + grad_one
    self_grads = (
        lax.psum_scatter(
            grad_gain_one.astype(jnp.bfloat16), ("fsdp", "ctx"), scatter_dimension=0, tiled=True
        ).astype(jnp.float32),
        lax.psum_scatter(
            grad_self_query.astype(jnp.bfloat16), ("fsdp", "ctx"), scatter_dimension=0, tiled=True
        ).astype(jnp.float32),
        lax.psum_scatter(
            grad_self_key.astype(jnp.bfloat16), ("fsdp", "ctx"), scatter_dimension=0, tiled=True
        ).astype(jnp.float32),
        lax.psum_scatter(
            grad_self_value.astype(jnp.bfloat16), ("fsdp", "ctx"), scatter_dimension=0, tiled=True
        ).astype(jnp.float32),
        lax.psum_scatter(
            grad_self_out.astype(jnp.bfloat16), ("fsdp", "ctx"), scatter_dimension=0, tiled=True
        ).astype(jnp.float32),
        lax.psum_scatter(
            grad_table.astype(jnp.bfloat16), ("fsdp", "ctx"), scatter_dimension=0, tiled=True
        ).astype(jnp.float32),
    )
    gain_shares = jnp.stack((self_grads[0], cross_grads[0], feed_grads[0]), axis=0)
    return (
        output,
        grad_inputs,
        grad_encoder,
        gain_shares[0],
        self_grads[1],
        self_grads[2],
        self_grads[3],
        self_grads[4],
        self_grads[5],
        gain_shares[1],
        cross_grads[1],
        cross_grads[2],
        cross_grads[3],
        cross_grads[4],
        gain_shares[2],
        feed_grads[1],
        feed_grads[2],
        feed_grads[3],
    )


MESH = pl.DeviceIdType.MESH
LANES = 128
DEPTH = 4
LINKS = {("x", 0): 0, ("y", 0): 1, ("z", 1): 2, ("z", -1): 3, ("c", 0): 4}
SIZES = {"x": 2, "y": 2, "z": DEPTH}


class Place:
    def __init__(self):
        row = lax.axis_index("fsdp")
        self.y = lax.axis_index("ctx")
        self.z = lax.axis_index("tp")
        self.x = lax.div(row, 2)
        self.c = lax.rem(row, 2)

    def link(self, axis, d):
        x, y, z, c = self.x, self.y, self.z, self.c
        if axis == "x":
            x = 1 - x
        elif axis == "y":
            y = 1 - y
        elif axis == "z":
            z = z + d
        else:
            c = 1 - c
        return (x * 2 + c, y, z)

    def has(self, link):
        if link == ("z", 1):
            return self.z < DEPTH - 1
        if link == ("z", -1):
            return self.z > 0
        return None

    def source(self, src):
        x = 1 - self.x if src.get("x") else self.x
        y = 1 - self.y if src.get("y") else self.y
        return x, y, self.z + src.get("z", 0)

    def exists(self, src):
        off = src.get("z", 0)
        if off < 0:
            return self.z >= -off
        if off > 0:
            return self.z < DEPTH - off
        return None


def arrivals(order):
    events = []
    for k, axis in enumerate(order):
        sources = [{}]
        for a in order[:k]:
            choice = (0, -1, 1, -2, 2, -3, 3) if a == "z" else (0, 1)
            sources = [dict(b, **{a: o}) for o in choice for b in sources]
        for o in (-1, 1, -2, 2, -3, 3) if axis == "z" else (1,):
            for b in sources:
                src = dict(b, **{axis: o})
                d = 0 if axis != "z" else (1 if o < 0 else -1)
                events.append((k, sum(abs(v) for v in src.values()), src, d))
    return events


def onward(order, k, d):
    out = [("z", d)] if k >= 0 and order[k] == "z" else []
    for a in order[k + 1 :]:
        out += [("z", 1), ("z", -1)] if a == "z" else [(a, 0)]
    return out


def when(cond, action):
    if cond is None:
        action()
    else:
        pl.when(cond)(action)


def number(x, y, z):
    return (x * 2 + y) * DEPTH + z


def greet(place):
    barrier = pltpu.get_barrier_semaphore()

    def signal(link):
        pl.semaphore_signal(
            barrier, inc=1, device_id=place.link(*link), device_id_type=MESH
        )

    for link in LINKS:
        when(place.has(link), functools.partial(signal, link))
    ends = jnp.where(place.z < DEPTH - 1, 1, 0) + jnp.where(place.z > 0, 1, 0)
    pl.semaphore_wait(barrier, ends + 3)


def remote(src, dst, send, recv, device):
    return pltpu.make_async_remote_copy(
        src_ref=src, dst_ref=dst, send_sem=send, recv_sem=recv,
        device_id=device, device_id_type=MESH,
    )


def shard(ref, z, r, rows):
    if ref.shape[1] == rows:
        return ref.at[z, :, pl.ds(pl.multiple_of(r * LANES, LANES), LANES)]
    return ref.at[z, pl.ds(pl.multiple_of(r * rows, rows), rows), :]


class Gather:
    def __init__(self, place, orders, rows, ins, outs, sems):
        self.place, self.orders, self.rows, self.ins, self.outs = place, orders, rows, ins, outs
        self.send, self.recv, self.core_recv, self.local_sem = sems
        self.me = (place.x, place.y, place.z)
        self.arrivals = [
            (k, hops, j, src, d)
            for j in range(len(orders))
            for k, hops, src, d in arrivals(orders[j])
        ]
        self.arrivals.sort(key=lambda e: (e[0], e[1]))

    @staticmethod
    def scratch(count):
        dma = pltpu.SemaphoreType.DMA
        return [
            dma((count, 4 * DEPTH, 5)), dma((count, 4 * DEPTH)), dma((count, 4 * DEPTH)),
            dma((count,)),
        ]

    def slot(self, j, xyz, c):
        x, y, z = xyz
        if len(self.orders[j]) == 1:
            return self.outs[j].at[y if self.orders[j] == "y" else z]
        return shard(self.outs[j], z, (x * 2 + c) * 2 + y, self.rows[j])

    def copy(self, j, xyz, link, own):
        here = self.slot(j, xyz, self.place.c)
        arrived = self.core_recv if link[0] == "c" else self.recv
        i = number(*xyz)
        return remote(
            self.ins[j] if own else here, here, self.send.at[j, i, LINKS[link]],
            arrived.at[j, i], self.place.link(*link),
        )

    def routes(self, j, k, d):
        links = onward(self.orders[j], k, d)
        return links + [("c", 0)] if len(self.orders[j]) == 3 else links

    def local(self, j):
        return pltpu.make_async_copy(
            self.ins[j], self.slot(j, self.me, self.place.c), self.local_sem.at[j]
        )

    def start(self, which=None):
        which = range(len(self.orders)) if which is None else which
        for stage in range(2):
            for j in which:
                for link in self.routes(j, -1, 0):
                    if (link[0] == "c") == (stage == 1):
                        when(self.place.has(link), self.copy(j, self.me, link, True).start)
        for j in which:
            self.local(j).start()

    def steps(self, wanted=None):
        for e, (k, hops, j, src, d) in enumerate(self.arrivals):
            xyz = self.place.source(src)
            if wanted is not None and not wanted(j, k):
                continue

            def step(k=k, j=j, d=d, xyz=xyz, src=src):
                def run():
                    self.copy(j, xyz, ("x", 0), True).wait_recv()
                    for link in self.routes(j, k, d):
                        when(self.place.has(link), self.copy(j, xyz, link, False).start)

                when(self.place.exists(src), run)

            yield (e + 1) / len(self.arrivals), step

    def settle(self, which):
        for j in which:
            self.local(j).wait()
            if len(self.orders[j]) == 3:

                def from_core(i, carry):
                    xyz = (
                        lax.div(i, 2 * DEPTH), lax.rem(lax.div(i, DEPTH), 2), lax.rem(i, DEPTH)
                    )
                    remote(
                        self.ins[j], self.slot(j, xyz, 1 - self.place.c), self.send.at[j, i, 4],
                        self.core_recv.at[j, i], self.place.link("c", 0),
                    ).wait_recv()
                    return carry

                lax.fori_loop(0, 4 * DEPTH, from_core, 0)

    def sent(self):
        place = self.place
        for j, order in enumerate(self.orders):

            def wait(i, carry):
                xyz = (lax.div(i, 2 * DEPTH), lax.rem(lax.div(i, DEPTH), 2), lax.rem(i, DEPTH))
                same = {a: xyz["xyz".index(a)] == self.me["xyz".index(a)] for a in "xyz"}
                if len(order) == 3:
                    for m, a in enumerate(order):
                        after = True
                        for b in order[m + 1 :]:
                            after = same[b] & after
                        for link in ((a, 0),) if a != "z" else (("z", 1), ("z", -1)):
                            if a == "z":
                                d = link[1]
                                near = (xyz[2] - place.z) * d <= 0
                                cond = near & after & place.has(link)
                            else:
                                cond = same[a] & after
                            pl.when(cond)(self.copy(j, xyz, link, False).wait_send)
                    self.copy(j, xyz, ("c", 0), False).wait_send()
                elif order == "z":
                    column = same["x"] & same["y"]
                    for link in (("z", 1), ("z", -1)):
                        near = (xyz[2] - place.z) * link[1] <= 0
                        pl.when(column & near & place.has(link))(
                            self.copy(j, xyz, link, False).wait_send
                        )
                else:
                    pl.when(same["x"] & same["y"] & same["z"])(
                        self.copy(j, xyz, (order, 0), False).wait_send
                    )
                return carry

            lax.fori_loop(0, 4 * DEPTH, wait, 0)

    def finish(self):
        self.settle(range(len(self.orders)))
        self.sent()


def child_slots(order):
    starts, total, before = [], 0, 1
    for a in order:
        starts.append(total)
        total += before * (DEPTH + 1 if a == "z" else 1)
        before *= SIZES[a]
    return starts, total


def child_slot(order, starts, m, xyz, tail):
    at = 0
    for a in order[:m]:
        at = at * SIZES[a] + xyz["xyz".index(a)]
    if order[m] == "z":
        at = at * (DEPTH + 1) + tail
    return starts[m] + at


def add_rows(out, terms, rows):
    step = min(rows, 64 if out.shape[-1] <= LANES else 32)

    def body(q, carry):
        at = pl.ds(pl.multiple_of(q * step, step), step)
        value = terms[0][at, :].astype(jnp.float32)
        for term in terms[1:]:
            value = value + term[at, :].astype(jnp.float32)
        out[at, :] = value.astype(out.dtype)
        return carry

    lax.fori_loop(0, rows // step, body, 0)


class Scatter:
    def __init__(self, place, orders, rows, ins, outs, scratch):
        self.place, self.orders, self.rows, self.ins, self.outs = place, orders, rows, ins, outs
        n = len(orders)
        self.sums, self.gifts, self.kids = (scratch[i * n : (i + 1) * n] for i in range(3))
        self.load_sem, self.give_sem, self.gift_sem, self.up_sem, self.kid_sem = scratch[3 * n :]
        self.me = (place.x, place.y, place.z)
        self.plans = [child_slots(o) for o in orders]
        self.partner = place.link("c", 0)
        self.events = [
            (k, hops, j, src, d)
            for j in range(n)
            for k, hops, src, d in arrivals(orders[j])
        ]
        self.events.sort(key=lambda e: (-e[0], -e[1]))

    @staticmethod
    def scratch(arrays, orders):
        plans = [child_slots(o)[1] for o in orders]
        count = len(arrays)
        dma = pltpu.SemaphoreType.DMA

        def room(slots):
            return [pltpu.VMEM((n,) + shard_shape(a), a.dtype) for n, a in zip(slots, arrays)]

        full = [4 * DEPTH] * count
        return (
            room(full) + room(full) + room(plans)
            + [dma((count, 4 * DEPTH))] * 4 + [dma((count, max(plans)))]
        )

    def slot(self, j, xyz, c):
        x, y, z = xyz
        return shard(self.ins[j], z, (x * 2 + c) * 2 + y, self.rows[j])

    def load(self, j, xyz):
        i = number(*xyz)
        return pltpu.make_async_copy(
            self.slot(j, xyz, self.place.c), self.sums[j].at[i], self.load_sem.at[j, i]
        )

    def give(self, j, xyz):
        i = number(*xyz)
        return remote(
            self.slot(j, xyz, 1 - self.place.c), self.gifts[j].at[i], self.give_sem.at[j, i],
            self.gift_sem.at[j, i], self.partner,
        )

    def up(self, j, xyz, k, d):
        axis = self.orders[j][k]
        tail = xyz[2]
        if axis == "z" and d < 0:
            tail = jnp.where(xyz[2] == self.place.z - d, DEPTH, xyz[2])
        at = child_slot(self.orders[j], self.plans[j][0], k, xyz, tail)
        i = number(*xyz)
        return remote(
            self.sums[j].at[i], self.kids[j].at[at], self.up_sem.at[j, i],
            self.kid_sem.at[j, at], self.place.link(axis, -d),
        )

    def kid(self, j, m, xyz, tail):
        at = child_slot(self.orders[j], self.plans[j][0], m, xyz, tail)
        ref = self.kids[j].at[at]
        remote(ref, ref, self.up_sem.at[j, 0], self.kid_sem.at[j, at], self.partner).wait_recv()
        return ref

    def collect(self, j, xyz, k, d, out=None):
        i = number(*xyz)
        order = self.orders[j]
        total = self.sums[j].at[i]
        self.load(j, xyz).wait()
        self.give(j, xyz).wait_recv()
        always, sometimes = [], []
        if k >= 0 and order[k] == "z":
            sometimes.append((k, ("z", d), xyz[2]))
        for m in range(k + 1, len(order)):
            if order[m] == "z":
                sometimes += [(m, ("z", 1), xyz[2]), (m, ("z", -1), DEPTH)]
            else:
                always.append(m)
        for m, link, tail in sometimes:

            def more():
                add_rows(total, [total, self.kid(j, m, xyz, tail)], self.rows[j])

            when(self.place.has(link), more)
        terms = [total, self.gifts[j].at[i]] + [self.kid(j, m, xyz, 0) for m in always]
        add_rows(total if out is None else out, terms, self.rows[j])

    def start(self, which=None):
        for j in range(len(self.orders)) if which is None else which:
            order = self.orders[j]

            def begin(e, carry):
                left = 4 * DEPTH - 1 - e
                at = {}
                for a in order:
                    at[a] = lax.rem(left, SIZES[a])
                    left = lax.div(left, SIZES[a])
                xyz = tuple(
                    lax.rem(self.me["xyz".index(a)] + at[a], SIZES[a]) for a in "xyz"
                )
                self.give(j, xyz).start()
                self.load(j, xyz).start()
                return carry

            lax.fori_loop(0, 4 * DEPTH, begin, 0)

    def steps(self, wanted=None):
        count = len(self.events)
        for e, (k, hops, j, src, d) in enumerate(self.events):
            xyz = self.place.source(src)
            if wanted is not None and not wanted(j):
                continue

            def step(k=k, j=j, d=d, xyz=xyz, src=src):
                def run():
                    self.collect(j, xyz, k, d)
                    self.up(j, xyz, k, d).start()

                when(self.place.exists(src), run)

            yield (e + 1) / (count + 1), step
        for j in range(len(self.orders)):
            if wanted is not None and not wanted(j):
                continue

            def last(j=j):
                self.collect(j, self.me, -1, 0, self.outs[j])

            yield 1.0, last

    def finish(self):
        me = number(*self.me)
        for j in range(len(self.orders)):

            def wait(i, carry):
                xyz = (lax.div(i, 2 * DEPTH), lax.rem(lax.div(i, DEPTH), 2), lax.rem(i, DEPTH))
                self.give(j, xyz).wait_send()

                def sent():
                    mine = self.sums[j].at[i]
                    remote(
                        mine, mine, self.up_sem.at[j, i], self.kid_sem.at[j, 0], self.partner
                    ).wait_send()

                pl.when(i != me)(sent)
                return carry

            lax.fori_loop(0, 4 * DEPTH, wait, 0)


class Share:
    def __init__(self, place, rows, ins, outs, scratch):
        self.place, self.rows, self.ins, self.outs = place, rows, ins, outs
        n = len(rows)
        self.first, self.second, self.sums = (scratch[i * n : (i + 1) * n] for i in range(3))
        self.send, self.recv = scratch[3 * n :]
        self.half = lax.rem(place.z, 2)
        self.over_y = place.link("y", 0)
        self.over_z = place.link("z", 1 - 2 * self.half)

    @staticmethod
    def scratch(rows):
        dma = pltpu.SemaphoreType.DMA
        out = []
        for slots in (8, 4, 4):
            out += [pltpu.VMEM((slots, n, 256), jnp.bfloat16) for n in rows]
        return out + [dma((len(rows), 12)), dma((len(rows), 12))]

    def block(self, j, t, y, half):
        n = self.rows[j]
        return self.ins[j].at[t, pl.ds(pl.multiple_of((y * 2 + half) * n, n), n), :]

    def early(self, j, t, s):
        if t < 2:
            src, device = self.block(j, t, 1 - self.place.y, s), self.over_y
        else:
            src, device = self.block(j, t, s, 1 - self.half), self.over_z
        i = t * 2 + s
        return remote(src, self.first[j].at[i], self.send.at[j, i], self.recv.at[j, i], device)

    def late(self, j, t):
        return remote(
            self.sums[j].at[t], self.second[j].at[t], self.send.at[j, 8 + t],
            self.recv.at[j, 8 + t], self.over_z if t < 2 else self.over_y,
        )

    def start(self):
        for j in range(len(self.rows)):
            for s in range(2):
                for t in range(4):
                    self.early(j, t, s).start()

    def steps(self):
        for j in range(len(self.rows)):
            for t in range(4):

                def pass_on(j=j, t=t):
                    for s in range(2):
                        self.early(j, t, s).wait_recv()
                    if t < 2:
                        away = 1 - self.half
                        mine = self.block(j, t, self.place.y, away)
                    else:
                        away = 1 - self.place.y
                        mine = self.block(j, t, away, self.half)
                    add_rows(
                        self.sums[j].at[t], [mine, self.first[j].at[t * 2 + away]], self.rows[j]
                    )
                    self.late(j, t).start()

                yield 0.25, pass_on
        for j in range(len(self.rows)):
            for t in range(4):

                def total(j=j, t=t):
                    self.late(j, t).wait_recv()
                    kept = self.half if t < 2 else self.place.y
                    mine = self.block(j, t, self.place.y, self.half)
                    add_rows(
                        self.outs[j].at[t],
                        [mine, self.first[j].at[t * 2 + kept], self.second[j].at[t]],
                        self.rows[j],
                    )

                yield 0.5, total

    def finish(self):
        for j in range(len(self.rows)):
            for t in range(4):
                for s in range(2):
                    self.early(j, t, s).wait_send()
                self.late(j, t).wait_send()


HBM = pl.BlockSpec(memory_space=pl.ANY)
INSIDE = pl.BlockSpec(memory_space=pltpu.VMEM)


def comm_call(kernel, name, number_id, ins, in_specs, outs, out_specs, scratch):
    return pl.pallas_call(
        kernel,
        out_shape=outs,
        in_specs=in_specs,
        out_specs=out_specs,
        scratch_shapes=scratch,
        compiler_params=pltpu.CompilerParams(
            collective_id=number_id, has_side_effects=True, vmem_limit_bytes=67043328
        ),
        name=name,
    )(*ins)


def gathered(a, order):
    if len(order) == 1:
        return jax.ShapeDtypeStruct((SIZES[order],) + a.shape, a.dtype)
    if a.shape[0] > a.shape[1] == LANES:
        return jax.ShapeDtypeStruct((DEPTH, a.shape[0], 8 * LANES), a.dtype)
    return jax.ShapeDtypeStruct((DEPTH, 8 * a.shape[0], a.shape[1]), a.dtype)


def shard_shape(a):
    if a.shape[2] == 8 * LANES:
        return (a.shape[1], LANES)
    return (a.shape[1] // 8, a.shape[2])


def scattered(arrays):
    return [jax.ShapeDtypeStruct(shard_shape(a), jnp.float32) for a in arrays]


WIDTH = 1024
QROWS = 256
KEYS = 1024
ENC_ROWS = 512
SPAN = 1280
CHUNK = 128
VMEM_MOST = 64000000
ROWS_OF = (((0,), (0,)), ((), ()))
LAST = (((1,), (1,)), ((), ()))
PLAIN = (((1,), (0,)), ((), ()))


def mm(a, b, dims=PLAIN):
    return lax.dot_general(a, b, dims, preferred_element_type=jnp.float32)


def norm_rows(v, gain):
    return v * lax.rsqrt(jnp.mean(v * v, axis=-1, keepdims=True) + EPSILON) * gain


def norm_back(v, gain, e):
    r = lax.rsqrt(jnp.mean(v * v, axis=-1, keepdims=True) + EPSILON)
    ev = e * v
    gain_grad = jnp.sum(ev * r, axis=0, keepdims=True)
    back = r * gain * e - v * (r * r * r) * jnp.mean(ev * gain, axis=-1, keepdims=True)
    return back, gain_grad


def head_rows(cols, a):
    return jnp.concatenate(
        [cols[:, a * 128 : a * 128 + 64], cols[:, a * 128 + 64 : a * 128 + 128]], axis=0
    )


def attend(q, kv, p_ref, s_ref, ot_ref, keys, add_bias):
    for a in range(2):
        q2 = head_rows(q, a)
        k = kv[:, a * 64 : a * 64 + 64]
        v = kv[:, 128 + a * 64 : 192 + a * 64]
        if add_bias is not None:
            add_bias(a, None, None)
        peak = None
        for c in range(keys // CHUNK):
            rows = pl.ds(c * CHUNK, CHUNK)
            s = mm(k[c * CHUNK : (c + 1) * CHUNK], q2, LAST)
            if add_bias is not None:
                s = add_bias(a, c, s)
            s_ref[rows, :] = s
            top = jnp.max(s, axis=0, keepdims=True)
            peak = top if peak is None else jnp.maximum(peak, top)
        total = jnp.zeros_like(peak)
        for c in range(keys // CHUNK):
            rows = pl.ds(c * CHUNK, CHUNK)
            e = jnp.exp(s_ref[rows, :] - peak)
            s_ref[rows, :] = e
            total = total + jnp.sum(e, axis=0, keepdims=True)
        inverse = 1.0 / total
        for c in range(keys // CHUNK):
            rows = pl.ds(c * CHUNK, CHUNK)
            p_ref[0, a, rows, :] = (s_ref[rows, :] * inverse).astype(jnp.bfloat16)
        ot = mm(v, p_ref[0, a], ROWS_OF)
        ot_ref[a * 128 : a * 128 + 64, :] = ot[:, :QROWS]
        ot_ref[a * 128 + 64 : a * 128 + 128, :] = ot[:, QROWS:]
    return jnp.transpose(ot_ref[...]).astype(jnp.bfloat16)


def attend_back(q, kv, p_ref, do, dkv_ref, d_ref, ds_ref, qt_ref, keys, take_bias):
    for a in range(2):
        q2 = head_rows(q, a)
        do2 = head_rows(do, a)
        k = kv[:, a * 64 : a * 64 + 64]
        v = kv[:, 128 + a * 64 : 192 + a * 64]
        total = jnp.zeros((1, 2 * QROWS), jnp.float32)
        for c in range(keys // CHUNK):
            rows = pl.ds(c * CHUNK, CHUNK)
            dp = mm(v[c * CHUNK : (c + 1) * CHUNK], do2, LAST)
            d_ref[rows, :] = dp
            total = total + jnp.sum(
                dp * p_ref[0, a, rows, :].astype(jnp.float32), axis=0, keepdims=True
            )
        for c in range(keys // CHUNK):
            rows = pl.ds(c * CHUNK, CHUNK)
            ds = p_ref[0, a, rows, :].astype(jnp.float32) * (d_ref[rows, :] - total)
            if take_bias is not None:
                take_bias(a, c, ds)
            ds_ref[rows, :] = ds.astype(jnp.bfloat16)
        if take_bias is not None:
            take_bias(a, None, None)
        dkv_ref[0, :, a * 64 : a * 64 + 64] = mm(ds_ref[pl.ds(0, keys), :], q2).astype(jnp.bfloat16)
        dkv_ref[0, :, 128 + a * 64 : 192 + a * 64] = mm(p_ref[0, a], do2).astype(jnp.bfloat16)
        qt = mm(k, ds_ref[pl.ds(0, keys), :], ROWS_OF)
        qt_ref[a * 128 : a * 128 + 64, :] = qt[:, :QROWS]
        qt_ref[a * 128 + 64 : a * 128 + 128, :] = qt[:, QROWS:]
    return jnp.transpose(qt_ref[...]).astype(jnp.bfloat16)


def self_step(first, length, h1_ref, w_ref, wkv_ref, near_of, q_ref, kv_ref, p_ref, o_ref, work):
    s_ref, strip_ref, ot_ref = work
    kv = mm(h1_ref[...], wkv_ref[0]).astype(jnp.bfloat16)
    kv_ref[0] = kv
    q = mm(h1_ref[pl.ds(first, QROWS), :], w_ref[0, :, :QROWS]).astype(jnp.bfloat16)
    q_ref[0] = q
    lane = lax.broadcasted_iota(jnp.int32, (1, 2 * QROWS), 1)
    lane = jnp.where(lane < QROWS, lane, lane - QROWS)
    last_key = jnp.minimum(lane + first, length - 1)

    def add_bias(a, c, s):
        if c is None:
            for b in range(2):
                near = near_of(2 * a + b)
                for g in range(16):
                    shift = (SPAN - (120 - 8 * g)) % SPAN
                    strip_ref[b, 8 * g : 8 * g + 8, :] = (
                        pltpu.roll(near, shift, 1) if shift else near
                    )
            return None
        cols = pl.ds(CHUNK * (7 - c), QROWS)
        bias = jnp.concatenate([strip_ref[0, :, cols], strip_ref[1, :, cols]], axis=1)
        key = lax.broadcasted_iota(jnp.int32, s.shape, 0) + c * CHUNK
        return jnp.where(key <= last_key, s + bias, MASKED)

    o = attend(q, kv, p_ref, s_ref, ot_ref, KEYS, add_bias)
    o_ref[0] = o
    return mm(o, w_ref[0, :, QROWS:], LAST)


def cross_step(h_ref, enc, w_ref, wkv_ref, q_ref, kv_ref, p_ref, o_ref, work):
    s_ref, ot_ref = work
    kv = mm(enc, wkv_ref[0]).astype(jnp.bfloat16)
    kv_ref[0] = kv
    q = mm(h_ref[...], w_ref[0, :, :QROWS]).astype(jnp.bfloat16)
    q_ref[0] = q
    o = attend(q, kv, p_ref, s_ref, ot_ref, ENC_ROWS, None)
    o_ref[0] = o
    return mm(o, w_ref[0, :, QROWS:], LAST)


def here():
    z = lax.axis_index("tp")
    half = lax.rem(z, 2)
    return lax.div(z, 2), half, lax.axis_index("ctx") * (2 * QROWS) + half * QROWS


def feed_kernel(
    at, lengths, x3_ref, cot_ref, gain_ref, wg_ref, wu_ref, wo_ref,
    out_ref, g3_ref, gg_ref, gu_ref, go_ref, gn_ref,
    h_ref, g_ref, y_ref, dh_ref,
):
    step = pl.program_id(0)

    @pl.when(step == 0)
    def _():
        h_ref[...] = norm_rows(x3_ref[...], gain_ref[pl.ds(2, 1), :]).astype(jnp.bfloat16)
        row = lax.broadcasted_iota(jnp.int32, (QROWS, 1), 0) + at[2]
        g4 = jnp.where(row < lengths[at[0]], cot_ref[0].astype(jnp.float32), 0.0)
        g_ref[...] = g4.astype(jnp.bfloat16)
        y_ref[...] = x3_ref[...]
        dh_ref[...] = jnp.zeros_like(dh_ref)

    gate = mm(h_ref[...], wg_ref[0], LAST)
    up = mm(h_ref[...], wu_ref[0], LAST)
    root = math.sqrt(2.0 / math.pi)
    square = gate * gate
    th = jnp.tanh(root * (gate + 0.044715 * gate * square))
    half = 0.5 * (1.0 + th)
    gelu = gate * half
    slope = half + 0.5 * gate * (1.0 - th * th) * (root * (1.0 + 3 * 0.044715 * square))
    hidden = (gelu * up).astype(jnp.bfloat16)
    y_ref[...] += mm(hidden, wo_ref[0])
    go_ref[0] = mm(hidden, g_ref[...], ROWS_OF).astype(jnp.bfloat16)
    dhid = mm(g_ref[...], wo_ref[0], LAST)
    dup = (dhid * gelu).astype(jnp.bfloat16)
    dgate = (dhid * up * slope).astype(jnp.bfloat16)
    gg_ref[0] = mm(dgate, h_ref[...], ROWS_OF).astype(jnp.bfloat16)
    gu_ref[0] = mm(dup, h_ref[...], ROWS_OF).astype(jnp.bfloat16)
    dh_ref[...] += mm(dgate, wg_ref[0]) + mm(dup, wu_ref[0])

    @pl.when(step == pl.num_programs(0) - 1)
    def _():
        out_ref[...] = y_ref[...].astype(jnp.bfloat16)
        back, gain_grad = norm_back(x3_ref[...], gain_ref[pl.ds(2, 1), :], dh_ref[...])
        g3_ref[...] = g_ref[...].astype(jnp.float32) + back
        gn_ref[...] = gain_grad


def whole(shape):
    zeros = (0,) * len(shape)
    return pl.BlockSpec(shape, lambda t: zeros)


def part(shape, column=0):
    tail = (0,) * (len(shape) - 2)
    return pl.BlockSpec(shape, lambda t: (t,) + tail + (column,))


SCALARS = pl.BlockSpec(memory_space=pltpu.SMEM)
F32 = jnp.float32
LOW = jnp.bfloat16


def shape_of(shape, dtype):
    return jax.ShapeDtypeStruct(shape, dtype)


def feed(at, lengths, x3, cot, gains, wg, wu, wo):
    units = wg.shape[1]

    def fixed(shape):
        return pl.BlockSpec(shape, lambda t, at: (0,) * len(shape))

    wide = pl.BlockSpec((1, units, WIDTH), lambda t, at: (t, 0, 0))
    outs = (
        [shape_of((QROWS, WIDTH), LOW), shape_of((QROWS, WIDTH), F32)]
        + [shape_of((4, units, WIDTH), LOW)] * 3
        + [shape_of((1, WIDTH), F32)]
    )
    return pl.pallas_call(
        feed_kernel,
        grid_spec=pltpu.PrefetchScalarGridSpec(
            num_scalar_prefetch=1,
            grid=(4,),
            in_specs=[
                SCALARS, fixed((QROWS, WIDTH)),
                pl.BlockSpec((1, QROWS, WIDTH), lambda t, at: (at[0], at[1], 0)),
                fixed((8, WIDTH)), wide, wide, wide,
            ],
            out_specs=[fixed((QROWS, WIDTH)), fixed((QROWS, WIDTH)), wide, wide, wide,
                       fixed((1, WIDTH))],
            scratch_shapes=[
                pltpu.VMEM((QROWS, WIDTH), LOW), pltpu.VMEM((QROWS, WIDTH), LOW),
                pltpu.VMEM((QROWS, WIDTH), F32), pltpu.VMEM((QROWS, WIDTH), F32),
            ],
        ),
        out_shape=outs,
        compiler_params=pltpu.CompilerParams(
            dimension_semantics=("arbitrary",), vmem_limit_bytes=VMEM_MOST
        ),
        cost_estimate=pl.CostEstimate(
            flops=13 * 10**9, bytes_accessed=4 * 10**7, transcendentals=0
        ),
        name="feed",
    )(at, lengths, x3, cot, gains, wg, wu, wo)


FORWARD_SPLIT = (0.0, 0.7)
BACKWARD_SPLIT = (0.1, 0.0, 0.6)
FINISH_SPLIT = (0.0, 0.0)
GATHER_ORDERS = ("zyx", "zyx", "xzy", "yzx", "zxy", "yzx", "zxy", "y", "y")
SMALL_ROWS = 16


def split_steps(steps, parts, low, high):
    ends = [int(len(steps) * (low + (high - low) * (i + 1) / parts)) for i in range(parts)]
    return [steps[a:b] for a, b in zip([0] + ends, ends)], steps[ends[-1] :]


def at_step(t, chunks):
    for i, chunk in enumerate(chunks):

        def run():
            for step in chunk:
                step()

        if chunk:
            pl.when(t == i)(run)


def forward_kernel(rows, *refs):
    lengths, feeds, packs, inputs, encoder = refs[0], refs[1:4], refs[4:8], refs[8], refs[9]
    weights, refs = refs[10:16], refs[16:]
    gains_ref, x2_ref, x3_ref, h1_out, h2_ref, x_out, enc_out = refs[:7]
    q1_out, kv1_out, p1_out, o1_out, q2_out, kv2_out, p2_out, o2_out = refs[7:15]
    small, x_all, enc_all, bucket_ref, h1_ref, s_ref, strip_ref, ot_ref = refs[15:23]
    own_feeds, own_x, own_enc, own_sem = refs[23:26], refs[26], refs[27], refs[28]
    place = Place()
    half = lax.rem(place.z, 2)
    seq = lax.div(place.z, 2)
    ins = own_feeds + packs + (own_x, own_enc)
    loads = [
        pltpu.make_async_copy(src, dst, own_sem.at[i])
        for i, (src, dst) in enumerate(
            [(inputs.at[seq], own_x), (encoder.at[seq], own_enc)] + list(zip(feeds, own_feeds))
        )
    ]
    for load in loads:
        load.start()
    plan = Gather(place, GATHER_ORDERS, rows, ins, weights + (small, x_all, enc_all), refs[29:])
    greet(place)
    first = pl.multiple_of(place.y * (2 * QROWS) + half * QROWS, QROWS)
    length = lengths[seq]
    for load in loads:
        load.wait()
    plan.start(range(3, 9))
    row = lax.broadcasted_iota(jnp.int32, (8, SPAN), 0)
    col = lax.broadcasted_iota(jnp.int32, (8, SPAN), 1)
    bucket_ref[...] = bucket_index(jnp.maximum(first + col - (SPAN - 264) - row, 0))
    for _, step in plan.steps(lambda j, k: 3 <= j < 7 and k < 2):
        step()
    plan.start(range(3))
    for _, step in plan.steps(lambda j, k: j >= 7 or (j >= 3 and k == 2)):
        step()
    plan.settle(range(3, 9))
    feed_steps = [step for _, step in plan.steps(lambda j, k: j < 3)]
    chunks, rest = split_steps(feed_steps, 8, *FORWARD_SPLIT)

    for k in range(3):
        gains_ref[pl.ds(k, 1), :] = jnp.concatenate(
            [small[0, pl.ds(r * SMALL_ROWS + k, 1), :] for r in range(8)], axis=1
        )
    gain = gains_ref[pl.ds(0, 1), :]
    for y in range(2):
        for c in range(2):
            at = pl.ds(c * QROWS, QROWS)
            h1_ref[pl.ds(y * 512 + c * QROWS, QROWS), :] = norm_rows(
                x_all[y, at, :].astype(jnp.float32), gain
            ).astype(jnp.bfloat16)
    own = own_x[pl.ds(pl.multiple_of(half * QROWS, QROWS), QROWS), :]
    x_out[...] = own
    x2_ref[...] = own.astype(jnp.float32)
    n = QROWS // 2
    enc_out[...] = own_enc[pl.ds(pl.multiple_of(half * n, n), n), :]
    h1_out[...] = h1_ref[pl.ds(first, QROWS), :]

    def self_body(w_ref, wkv_ref, q_ref, kv_ref, p_ref, o_ref):
        t = pl.program_id(0)

        def near_of(head):
            rows_of = [small[t, pl.ds(r * SMALL_ROWS + 3, 1), :] for r in range(8)]
            bucket = bucket_ref[...]
            near = jnp.zeros((8, SPAN), jnp.float32)
            for i in range(BUCKETS):
                lane = (i % 4) * 4 + head
                value = rows_of[i // 4][:, lane : lane + 1]
                near = jnp.where(bucket == i, value, near)
            return near

        x2_ref[...] += self_step(
            first, length, h1_ref, w_ref, wkv_ref, near_of, q_ref, kv_ref, p_ref, o_ref,
            (s_ref, strip_ref, ot_ref),
        )
        at_step(t, chunks[:4])

    pltpu.emit_pipeline(
        self_body,
        grid=(4,),
        in_specs=[part((1, WIDTH, 512)), part((1, WIDTH, 256))],
        out_specs=[
            part((1, QROWS, 256)), part((1, KEYS, 256)), part((1, 2, KEYS, 512)),
            part((1, QROWS, 256)),
        ],
    )(weights[3], weights[5], q1_out, kv1_out, p1_out, o1_out)
    x3_ref[...] = x2_ref[...]
    h2_ref[...] = norm_rows(x2_ref[...], gains_ref[pl.ds(1, 1), :]).astype(jnp.bfloat16)

    def cross_body(w_ref, wkv_ref, q_ref, kv_ref, p_ref, o_ref):
        enc = jnp.concatenate([enc_all[0], enc_all[1]], axis=0)
        x3_ref[...] += cross_step(
            h2_ref, enc, w_ref, wkv_ref, q_ref, kv_ref, p_ref, o_ref, (s_ref, ot_ref)
        )
        at_step(pl.program_id(0), chunks[4:])

    pltpu.emit_pipeline(
        cross_body,
        grid=(4,),
        in_specs=[part((1, WIDTH, 512)), part((1, WIDTH, 256), 1)],
        out_specs=[
            part((1, QROWS, 256)), part((1, ENC_ROWS, 256)), part((1, 2, ENC_ROWS, 512)),
            part((1, QROWS, 256)),
        ],
    )(weights[4], weights[5], q2_out, kv2_out, p2_out, o2_out)
    for step in rest:
        step()
    plan.settle(range(3))
    plan.sent()


def forward(lengths, feeds, packs, inputs, encoder):
    x, enc = shape_of(inputs.shape[1:], LOW), shape_of(encoder.shape[1:], LOW)
    arrays = list(feeds) + list(packs) + [x, enc]
    rows = [a.shape[0] for a in arrays]
    wide = [gathered(a, o) for a, o in zip(arrays, GATHER_ORDERS)]
    vm = pltpu.VMEM
    return comm_call(
        functools.partial(forward_kernel, rows), "forward", 1,
        (lengths,) + tuple(feeds) + tuple(packs) + (inputs, encoder),
        [SCALARS] + [HBM] * 3 + [INSIDE] * 4 + [HBM] * 2,
        wide[:6]
        + [shape_of((8, WIDTH), F32), shape_of((QROWS, WIDTH), F32),
           shape_of((QROWS, WIDTH), F32), shape_of((QROWS, WIDTH), LOW),
           shape_of((QROWS, WIDTH), LOW), shape_of((QROWS, WIDTH), LOW),
           shape_of((QROWS // 2, WIDTH), LOW),
           shape_of((4, QROWS, 256), LOW), shape_of((4, KEYS, 256), LOW),
           shape_of((4, 2, KEYS, 512), LOW), shape_of((4, QROWS, 256), LOW),
           shape_of((4, QROWS, 256), LOW), shape_of((4, ENC_ROWS, 256), LOW),
           shape_of((4, 2, ENC_ROWS, 512), LOW), shape_of((4, QROWS, 256), LOW)],
        [HBM] * 6 + [INSIDE] * 7 + [HBM] * 8,
        [vm(w.shape, w.dtype) for w in wide[6:]]
        + [vm((8, SPAN), jnp.int32), vm((KEYS, WIDTH), LOW), vm((KEYS, 512), F32),
           vm((2, CHUNK, SPAN), F32), vm((256, QROWS), F32)]
        + [vm(a.shape, LOW) for a in arrays[:3] + arrays[7:]]
        + [pltpu.SemaphoreType.DMA((5,))]
        + Gather.scratch(9),
    )


FEED_ORDERS = ("zxy", "zyx", "zyx")


def backward_kernel(rows, own, room, *refs):
    grads, refs = refs[:3], refs[3:]
    out_ref, g3_ref, x2_ref, h2_ref, h1_ref, gains_ref = refs[:6]
    w1, w2, q1, kv1, p1, o1, q2, kv2, p2, o2 = refs[6:16]
    shards, refs = refs[16:19], refs[19:]
    dkv1_out, dkv2_out, rows_out, g2_ref, dh_ref, near_ref, gw1, gw2 = refs[:8]
    dkv1, dkv2, g_ref, gt_ref, ht_ref, dc_ref, d_ref, ds_ref, qt_ref, strip_ref = refs[8:18]
    line_ref, scratch = refs[18], refs[19:]
    place = Place()
    plan = Scatter(place, FEED_ORDERS, rows, grads, shards, scratch[: len(room)])
    scratch = scratch[len(room) :]
    share = Share(place, own, (dkv1, dkv2), (dkv1_out, dkv2_out), scratch[:8])
    lines = Gather(place, ("z",), (QROWS,), (out_ref,), (rows_out,), scratch[8:])
    greet(place)
    lines.start()
    plan.start()
    steps = [step for _, step in plan.steps()]
    begin = int(len(steps) * BACKWARD_SPLIT[0])
    for step in steps[:begin]:
        step()
    chunks, rest = split_steps(steps[begin:], 8, *BACKWARD_SPLIT[1:])

    def load_grad(ref, h_ref):
        g = ref[...].astype(jnp.bfloat16)
        g_ref[...] = g
        gt_ref[...] = jnp.transpose(g)
        ht_ref[...] = jnp.transpose(h_ref[...])

    def heads(t, w_ref, q_ref, kv_ref, p_ref, o_ref, gw_ref, dkv, d_sum, keys, take_bias):
        do = mm(g_ref[...], w_ref[0, :, QROWS:]).astype(jnp.bfloat16)
        gw_ref[0, :, QROWS:] = mm(gt_ref[...], o_ref[0]).astype(jnp.bfloat16)
        dq = attend_back(
            q_ref[0], kv_ref[0], p_ref, do, dkv.at[pl.ds(t, 1)], d_ref, ds_ref, qt_ref, keys,
            take_bias,
        )
        gw_ref[0, :, :QROWS] = mm(ht_ref[...], dq).astype(jnp.bfloat16)
        d_sum[...] += mm(dq, w_ref[0, :, :QROWS], LAST)

    def specs(keys):
        return [
            part((1, WIDTH, 512)), part((1, QROWS, 256)), part((1, keys, 256)),
            part((1, 2, keys, 512)), part((1, QROWS, 256)),
        ]

    load_grad(g3_ref, h2_ref)
    dc_ref[...] = jnp.zeros_like(dc_ref)

    def cross_body(w_ref, q_ref, kv_ref, p_ref, o_ref, gw_ref):
        t = pl.program_id(0)
        heads(t, w_ref, q_ref, kv_ref, p_ref, o_ref, gw_ref, dkv2, dc_ref, ENC_ROWS, None)
        at_step(t, chunks[:4])

    pltpu.emit_pipeline(
        cross_body, grid=(4,), in_specs=specs(ENC_ROWS), out_specs=[part((1, WIDTH, 512))]
    )(w2, q2, kv2, p2, o2, gw2)
    back, gain_grad = norm_back(x2_ref[...], gains_ref[pl.ds(1, 1), :], dc_ref[...])
    g2_ref[pl.ds(0, QROWS), :] = g3_ref[...] + back
    g2_ref[pl.ds(QROWS, 1), :] = gain_grad
    load_grad(g2_ref.at[pl.ds(0, QROWS)], h1_ref)
    dh_ref[...] = jnp.zeros_like(dh_ref)

    def self_body(w_ref, q_ref, kv_ref, p_ref, o_ref, gw_ref):
        t = pl.program_id(0)

        def take_bias(a, c, ds):
            if c is None:
                for b in range(2):
                    total = jnp.zeros((8, SPAN), jnp.float32)
                    for g in range(16):
                        piece = strip_ref[b, 8 * g : 8 * g + 8, :]
                        shift = 120 - 8 * g
                        total = total + (pltpu.roll(piece, shift, 1) if shift else piece)
                    line = total[0:1]
                    for r in range(1, 8):
                        line = line + pltpu.roll(total[r : r + 1], SPAN - r, 1)
                    line_ref[pl.ds(t * 4 + 2 * a + b, 1), :] = line
                return
            if c == 0:
                strip_ref[...] = jnp.zeros_like(strip_ref)
            cols = pl.ds(CHUNK * (7 - c), QROWS)
            strip_ref[0, :, cols] += ds[:, :QROWS]
            strip_ref[1, :, cols] += ds[:, QROWS:]

        heads(t, w_ref, q_ref, kv_ref, p_ref, o_ref, gw_ref, dkv1, dh_ref, KEYS, take_bias)
        at_step(t, chunks[4:])

    pltpu.emit_pipeline(
        self_body, grid=(4,), in_specs=specs(KEYS), out_specs=[part((1, WIDTH, 512))]
    )(w1, q1, kv1, p1, o1, gw1)
    share.start()
    distance = lax.broadcasted_iota(jnp.int32, (1, SPAN), 1) - (SPAN - 264) + here()[2]
    bucket = bucket_index(jnp.maximum(distance, 0))
    chosen = lax.broadcasted_iota(jnp.int32, (LANES, SPAN), 0) == bucket
    near_ref[...] = lax.dot_general(
        line_ref[...], chosen.astype(jnp.float32), LAST, precision=TOP_PRECISION,
        preferred_element_type=jnp.float32,
    )
    ordered = [(i / max(len(rest), 1), step) for i, step in enumerate(rest)]
    ordered += [(0.05 + 0.9 * at, step) for at, step in share.steps()]
    ordered += [(0.1 * at, step) for at, step in lines.steps()]
    ordered.sort(key=lambda s: s[0])
    for _, step in ordered:
        step()
    lines.finish()
    share.finish()
    plan.finish()


def backward(grads, out, g3, x2, h2, h1, gains, w1, w2, saved1, saved2):
    rows = [shard_shape(a)[0] for a in grads]
    own = [KEYS // 4, ENC_ROWS // 4]
    room = Scatter.scratch(grads, FEED_ORDERS)
    vm = pltpu.VMEM
    return comm_call(
        functools.partial(backward_kernel, rows, own, room), "backward", 2,
        tuple(grads) + (out, g3, x2, h2, h1, gains, w1, w2) + tuple(saved1) + tuple(saved2),
        [HBM] * 3 + [INSIDE] * 6 + [HBM] * 10,
        scattered(grads)
        + [shape_of((4, r, 256), LOW) for r in own]
        + [gathered(out, "z"), shape_of((QROWS + 8, WIDTH), F32), shape_of((QROWS, WIDTH), F32),
           shape_of((16, LANES), F32), shape_of(w1.shape, LOW), shape_of(w2.shape, LOW)],
        [INSIDE] * 5 + [HBM] + [INSIDE] * 3 + [HBM] * 2,
        [vm((4, KEYS, 256), LOW), vm((4, ENC_ROWS, 256), LOW), vm((QROWS, WIDTH), LOW),
         vm((WIDTH, QROWS), LOW), vm((WIDTH, QROWS), LOW), vm((QROWS, WIDTH), F32),
         vm((KEYS, 512), F32), vm((KEYS, 512), LOW), vm((256, QROWS), F32),
         vm((2, CHUNK, SPAN), F32), vm((16, SPAN), F32)]
        + room + Share.scratch(own) + Gather.scratch(1),
    )


HEAD_ORDERS = ("zyx", "zxy", "zyx", "zxy")


def finish_kernel(rows, room, *refs):
    gw1, gw2, w3 = refs[:3]
    dkv, dkvc, dh_ref, g2_ref, x_ref, h1_ref, enc_ref, gains_ref, gn3_ref, table_ref = refs[3:13]
    shards, (gx_out, genc_out) = refs[13:17], refs[17:19]
    gw3, small, gx_ref, genc_ref, ht_ref, et_ref, dsum_ref, de_ref = refs[19:27]
    scratch = refs[27:]
    place = Place()
    plan = Scatter(
        place, HEAD_ORDERS, rows, (gw1, gw2, gw3, small), shards, scratch[: len(room)]
    )
    lines = Gather(
        place, ("z", "z"), (QROWS, QROWS // 2), (gx_ref, genc_ref), (gx_out, genc_out),
        scratch[len(room) :],
    )
    greet(place)
    plan.start(range(2))
    ready = [step for _, step in plan.steps(lambda j: j < 2)]
    chunks, rest = split_steps(ready, 4, *FINISH_SPLIT)
    ht_ref[...] = jnp.transpose(h1_ref[...])
    et_ref[...] = jnp.transpose(enc_ref[...])
    dsum_ref[...] = dh_ref[...]
    de_ref[...] = jnp.zeros_like(de_ref)

    def body(ws_ref, wc_ref):
        t = pl.program_id(0)
        gw3[t, :, pl.ds(0, 256)] = mm(ht_ref[...], dkv[t]).astype(jnp.bfloat16)
        gw3[t, :, pl.ds(256, 256)] = mm(et_ref[...], dkvc[t]).astype(jnp.bfloat16)
        dsum_ref[...] += mm(dkv[t], ws_ref[0], LAST)
        de_ref[...] += mm(dkvc[t], wc_ref[0], LAST)
        at_step(t, chunks)

    pltpu.emit_pipeline(
        body, grid=(4,), in_specs=[part((1, WIDTH, 256)), part((1, WIDTH, 256), 1)]
    )(w3, w3)
    back, gn1 = norm_back(
        x_ref[...].astype(jnp.float32), gains_ref[pl.ds(0, 1), :], dsum_ref[...]
    )
    gx_ref[...] = (g2_ref[pl.ds(0, QROWS), :] + back).astype(jnp.bfloat16)
    genc_ref[...] = de_ref[...].astype(jnp.bfloat16)
    lines.start()
    small[...] = jnp.zeros_like(small)
    gain_grads = (gn1, g2_ref[pl.ds(QROWS, 1), :], gn3_ref[...])
    table = table_ref[...]
    for r in range(8):
        shifted = pltpu.roll(table, (LANES - 4 * r) % LANES, 1) if r else table
        for t in range(4):
            for k in range(3):
                small[t, pl.ds(r * SMALL_ROWS + k, 1), :] = gain_grads[k][
                    :, r * LANES : (r + 1) * LANES
                ]
            small[t, pl.ds(r * SMALL_ROWS + 4, 4), :] = shifted[4 * t : 4 * t + 4]
    plan.start(range(2, 4))
    ordered = [(0.6 * i / len(rest), step) for i, step in enumerate(rest)]
    ordered += [(0.1 + 0.9 * at, step) for at, step in plan.steps(lambda j: j >= 2)]
    ordered += [(0.9 * at, step) for at, step in lines.steps()]
    ordered.sort(key=lambda s: s[0])
    for _, step in ordered:
        step()
    lines.finish()
    plan.finish()


def finish(gw1, gw2, w3, dkv, dkvc, dh, g2, x, h1, enc, gains, gn3, table):
    whole_small = shape_of((4, 8 * SMALL_ROWS, LANES), F32)
    arrays = (gw1, gw2, shape_of(w3.shape, LOW), whole_small)
    rows = [shard_shape(a)[0] for a in arrays]
    room = Scatter.scratch(arrays, HEAD_ORDERS)
    vm = pltpu.VMEM
    lines = [shape_of(a.shape, LOW) for a in (x, enc)]
    return comm_call(
        functools.partial(finish_kernel, rows, room), "finish", 3,
        (gw1, gw2, w3, dkv, dkvc, dh, g2, x, h1, enc, gains, gn3, table),
        [HBM] * 3 + [INSIDE] * 10,
        scattered(arrays) + [gathered(a, "z") for a in lines],
        [INSIDE] * 4 + [HBM] * 2,
        [vm(a.shape, a.dtype) for a in arrays[2:]] + [vm(a.shape, a.dtype) for a in lines]
        + [vm((WIDTH, QROWS), LOW), vm((WIDTH, QROWS // 2), LOW), vm((QROWS, WIDTH), F32),
           vm((QROWS // 2, WIDTH), F32)]
        + room + Gather.scratch(2),
    )


def small_rows(gains, table):
    flat = jnp.pad(table.reshape(1, -1).astype(F32), ((0, 0), (0, LANES - table.size)))
    rows = jnp.concatenate([g.reshape(1, LANES).astype(F32) for g in gains] + [flat], axis=0)
    return jnp.pad(rows, ((0, SMALL_ROWS - 4), (0, 0)))


def tokens_split(
    inputs, encoder, lengths, cotangent,
    norm_self, self_query, self_key_matrix, self_value_matrix, self_out, bias_table,
    norm_cross, cross_query, cross_key_matrix, cross_value_matrix, cross_out,
    norm_feed, feed_gate, feed_up, feed_out,
):
    packs = (
        jnp.concatenate([self_query, self_out], axis=1),
        jnp.concatenate([cross_query, cross_out], axis=1),
        jnp.concatenate(
            [self_key_matrix, self_value_matrix, cross_key_matrix, cross_value_matrix], axis=1
        ),
        small_rows((norm_self, norm_cross, norm_feed), bias_table),
    )
    (
        wg, wu, wo, w1, w2, w3, gains, x2, x3, h1, h2, x_own, enc_own,
        q1, kv1, p1, o1, q2, kv2, p2, o2,
    ) = forward(lengths, (feed_gate.T, feed_up.T, feed_out.T), packs, inputs, encoder)
    out, g3, gg, gu, go, gn3 = feed(
        jnp.stack(here()), lengths, x3, cotangent, gains, wg, wu, wo
    )
    gg, gu, go, dkv, dkvc, out, g2, dh, table, gw1, gw2 = backward(
        (gg, gu, go), out, g3, x2, h2, h1, gains, w1, w2, (q1, kv1, p1, o1), (q2, kv2, p2, o2)
    )
    gw1, gw2, gw3, gs, gx, genc = finish(
        gw1, gw2, w3, dkv, dkvc, dh, g2, x_own, h1, enc_own, gains, gn3, table
    )
    return (
        out.reshape(inputs.shape),
        gx.reshape(inputs.shape).astype(F32),
        genc.reshape(encoder.shape).astype(F32),
        gs[0], gw1[:, :256], gw3[:, :128], gw3[:, 128:256], gw1[:, 256:],
        jnp.transpose(gs[4:8, :4]),
        gs[1], gw2[:, :256], gw3[:, 256:384], gw3[:, 384:], gw2[:, 256:],
        gs[2], gg.T, gu.T, go.T,
    )


def solution(mesh):
    sizes = (mesh.shape["fsdp"], mesh.shape["ctx"], mesh.shape["tp"])
    return jax.shard_map(
        tokens_split if sizes == (4, 2, DEPTH) else shards,
        mesh=mesh,
        in_specs=(
            P("fsdp", "ctx", None),
            P("fsdp", "ctx", None),
            P("fsdp"),
            P("fsdp", "ctx", None),
            P(("fsdp", "ctx")),
            P(("fsdp", "ctx"), "tp"),
            P(("fsdp", "ctx"), "tp"),
            P(("fsdp", "ctx"), "tp"),
            P(("fsdp", "ctx"), "tp"),
            P(("fsdp", "ctx"), "tp"),
            P(("fsdp", "ctx")),
            P(("fsdp", "ctx"), "tp"),
            P(("fsdp", "ctx"), "tp"),
            P(("fsdp", "ctx"), "tp"),
            P(("fsdp", "ctx"), "tp"),
            P(("fsdp", "ctx")),
            P(("fsdp", "ctx"), "tp"),
            P(("fsdp", "ctx"), "tp"),
            P(("fsdp", "ctx"), "tp"),
        ),
        out_specs=(
            P("fsdp", "ctx", None),
            P("fsdp", "ctx", None),
            P("fsdp", "ctx", None),
            P(("fsdp", "ctx")),
            P(("fsdp", "ctx"), "tp"),
            P(("fsdp", "ctx"), "tp"),
            P(("fsdp", "ctx"), "tp"),
            P(("fsdp", "ctx"), "tp"),
            P(("fsdp", "ctx"), "tp"),
            P(("fsdp", "ctx")),
            P(("fsdp", "ctx"), "tp"),
            P(("fsdp", "ctx"), "tp"),
            P(("fsdp", "ctx"), "tp"),
            P(("fsdp", "ctx"), "tp"),
            P(("fsdp", "ctx")),
            P(("fsdp", "ctx"), "tp"),
            P(("fsdp", "ctx"), "tp"),
            P(("fsdp", "ctx"), "tp"),
        ),
        check_vma=False,
    )
```

```python
import functools
import math

import jax
import jax.numpy as jnp
from jax import lax
from jax.experimental import pallas as pl
from jax.experimental.pallas import tpu as pltpu
from jax.sharding import PartitionSpec as P

HEAD_SIZE = 64
BUCKETS = 32
MAXDIST = 128


EPSILON = 1e-06
MASKED = -1000000000.0
TOP_PRECISION = lax.Precision.HIGHEST


def rms_scale(values, gain_row):
    inverse = lax.rsqrt(jnp.mean(values * values, axis=-1, keepdims=True) + EPSILON)
    return values * inverse * gain_row


def gated_product(gate_in, up_in):
    return jax.nn.gelu(gate_in, approximate=True) * up_in


def project(operand_array, weight_arrays):
    return jnp.einsum(
        "spd,dk->spk", operand_array, weight_arrays, preferred_element_type=jnp.float32
    )


def project_back(grad_cols, weight_arrays):
    return jnp.einsum("spk,dk->spd", grad_cols, weight_arrays, preferred_element_type=jnp.float32)


def weight_grad(operand_array, grad_cols):
    return jnp.einsum("spd,spk->dk", operand_array, grad_cols, preferred_element_type=jnp.float32)


def bucket_index(distance):
    exact_count = BUCKETS // 2
    counter = jnp.zeros(distance.shape, jnp.int32)
    for level_index in range(1, BUCKETS - exact_count):
        border = math.ceil(
            exact_count * (MAXDIST / exact_count) ** (level_index / (BUCKETS - exact_count))
        )
        counter = counter + (distance >= border).astype(jnp.int32)
    return jnp.where(distance < exact_count, distance, exact_count + counter)


def reduce_rows(partial_sum):
    return lax.psum(partial_sum, "tp")


def block_scores(queries, key_rows, bias_rows, allowed):
    scores = jnp.einsum("gpkrd,gjkd->gkrpj", queries, key_rows, preferred_element_type=jnp.float32)
    if bias_rows is not None:
        scores = jnp.where(allowed[:, None, None], scores + bias_rows[None], MASKED)
    return scores


def forward_block(queries, key_rows, value_rows, bias_rows, allowed):
    scores = block_scores(queries, key_rows, bias_rows, allowed)
    row_peak = jnp.max(scores, axis=-1, keepdims=True)
    log_total = row_peak + jnp.log(jnp.sum(jnp.exp(scores - row_peak), axis=-1, keepdims=True))
    weights_low = jnp.exp(scores - log_total).astype(jnp.bfloat16)
    output = jnp.einsum(
        "gkrpj,gjkd->gpkrd", weights_low, value_rows, preferred_element_type=jnp.float32
    )
    return (output.astype(jnp.bfloat16), log_total)


def backward_block(queries, key_rows, value_rows, bias_rows, allowed, log_total, grad_out):
    scores = block_scores(queries, key_rows, bias_rows, allowed)
    softmax_rows = jnp.exp(scores - log_total)
    grad_probs = jnp.einsum(
        "gpkrd,gjkd->gkrpj", grad_out, value_rows, preferred_element_type=jnp.float32
    )
    grad_scores = softmax_rows * (
        grad_probs - jnp.sum(grad_probs * softmax_rows, axis=-1, keepdims=True)
    )
    scores_low = grad_scores.astype(jnp.bfloat16)
    grad_query = jnp.einsum(
        "gkrpj,gjkd->gpkrd", scores_low, key_rows, preferred_element_type=jnp.float32
    )
    grad_key = jnp.einsum(
        "gkrpj,gpkrd->gjkd", scores_low, queries, preferred_element_type=jnp.float32
    )
    grad_value = jnp.einsum(
        "gkrpj,gpkrd->gjkd",
        softmax_rows.astype(jnp.bfloat16),
        grad_out,
        preferred_element_type=jnp.float32,
    )
    if bias_rows is None:
        grad_bias = jnp.zeros((1,), jnp.float32)
    else:
        grad_bias = jnp.sum(grad_scores, axis=0)
    return (grad_query.astype(jnp.bfloat16), grad_key, grad_value, grad_bias)


def block_shapes(queries, key_rows, block_seqs):
    seq_count, row_total_count, query_cols = queries.shape
    key_total_count, key_cols = (key_rows.shape[1], key_rows.shape[2])
    kv_heads = key_cols // HEAD_SIZE
    repeats = query_cols // key_cols
    blocks = seq_count // block_seqs
    query_shape = (blocks, block_seqs, row_total_count, kv_heads, repeats, HEAD_SIZE)
    key_shape = (blocks, block_seqs, key_total_count, kv_heads, HEAD_SIZE)
    mask_shape = (blocks, block_seqs, row_total_count, key_total_count)
    return (query_shape, key_shape, mask_shape)


def attention_forward(queries, key_rows, value_rows, bias_rows, allowed, block_seqs):
    query_shape, key_shape, mask_shape = block_shapes(queries, key_rows, block_seqs)
    sources = (
        queries.reshape(query_shape),
        key_rows.reshape(key_shape),
        value_rows.reshape(key_shape),
    )
    if allowed is not None:
        sources = sources + (allowed.reshape(mask_shape),)

    def one_block(piece_list):
        mask_block = piece_list[3] if allowed is not None else None
        return forward_block(piece_list[0], piece_list[1], piece_list[2], bias_rows, mask_block)

    outputs, log_totals = lax.map(one_block, sources)
    return (outputs.reshape(queries.shape), log_totals)


def attention_backward(
    queries, key_rows, value_rows, bias_rows, allowed, log_totals, grad_out, block_seqs
):
    query_shape, key_shape, mask_shape = block_shapes(queries, key_rows, block_seqs)
    sources = (
        queries.reshape(query_shape),
        key_rows.reshape(key_shape),
        value_rows.reshape(key_shape),
        log_totals,
        grad_out.reshape(query_shape),
    )
    if allowed is not None:
        sources = sources + (allowed.reshape(mask_shape),)
    if bias_rows is None:
        initial = jnp.zeros((1,), jnp.float32)
    else:
        initial = jnp.zeros(bias_rows.shape, jnp.float32)

    def one_block(running, piece_list):
        mask_block = piece_list[5] if allowed is not None else None
        grad_query, grad_key, grad_value, grad_bias = backward_block(
            piece_list[0],
            piece_list[1],
            piece_list[2],
            bias_rows,
            mask_block,
            piece_list[3],
            piece_list[4],
        )
        return (running + grad_bias, (grad_query, grad_key, grad_value))

    bias_total, grad_list = lax.scan(one_block, initial, sources)
    return (
        grad_list[0].reshape(queries.shape),
        grad_list[1].reshape(key_rows.shape),
        grad_list[2].reshape(value_rows.shape),
        bias_total,
    )


def shards(
    inputs,
    encoder,
    lengths,
    cotangent,
    norm_self,
    self_query,
    self_key_matrix,
    self_value_matrix,
    self_out,
    bias_table,
    norm_cross,
    cross_query,
    cross_key_matrix,
    cross_value_matrix,
    cross_out,
    norm_feed,
    feed_gate,
    feed_up,
    feed_out,
):
    self_group = (
        lax.all_gather(norm_self, ("fsdp", "ctx"), axis=0, tiled=True),
        lax.all_gather(self_query, ("fsdp", "ctx"), axis=0, tiled=True),
        lax.all_gather(self_key_matrix, ("fsdp", "ctx"), axis=0, tiled=True),
        lax.all_gather(self_value_matrix, ("fsdp", "ctx"), axis=0, tiled=True),
        lax.all_gather(self_out, ("fsdp", "ctx"), axis=0, tiled=True),
        lax.all_gather(bias_table, ("fsdp", "ctx"), axis=0, tiled=True),
    )
    seq_count, row_total_count = (inputs.shape[0], inputs.shape[1])
    block_seqs = max((trial for trial in (1, 2, 3, 4) if seq_count % trial == 0))
    start_row = lax.axis_index("ctx") * row_total_count
    key_total_count = row_total_count * lax.axis_size("ctx")
    row_pos = start_row + jnp.arange(row_total_count, dtype=jnp.int32)
    col_pos = jnp.arange(key_total_count, dtype=jnp.int32)
    buckets = bucket_index(jnp.maximum(row_pos[:, None] - col_pos[None, :], 0))
    one_hot = (buckets[:, :, None] == jnp.arange(BUCKETS, dtype=jnp.int32)[None, None, :]).astype(
        jnp.float32
    )
    causal = col_pos[None, :] <= row_pos[:, None]
    allowed = causal[None] & (col_pos[None, None, :] < lengths[:, None, None])
    hidden_in = inputs.astype(jnp.float32)
    normed_one, norm_pull_one = jax.vjp(rms_scale, hidden_in, self_group[0].astype(jnp.float32))
    self_in = normed_one.astype(jnp.bfloat16)
    self_q = project(self_in, self_group[1]).astype(jnp.bfloat16)
    self_k = project(self_in, self_group[2]).astype(jnp.bfloat16)
    self_v = project(self_in, self_group[3]).astype(jnp.bfloat16)
    keys_self, values_self = (
        lax.all_gather(self_k, "ctx", axis=1, tiled=True),
        lax.all_gather(self_v, "ctx", axis=1, tiled=True),
    )
    heads_local = self_group[1].shape[1] // HEAD_SIZE
    kv_local = self_group[2].shape[1] // HEAD_SIZE
    table_rows = self_group[5].astype(jnp.float32)
    bias_rows = jnp.einsum("ijb,bh->hij", one_hot, table_rows, precision=TOP_PRECISION).reshape(
        kv_local, heads_local // kv_local, row_total_count, key_total_count
    )
    self_att, lse_self = attention_forward(
        self_q, keys_self, values_self, bias_rows, allowed, block_seqs
    )
    hidden_two = hidden_in + reduce_rows(project_back(self_att, self_group[4]))
    cross_group = (
        lax.all_gather(norm_cross, ("fsdp", "ctx"), axis=0, tiled=True),
        lax.all_gather(cross_query, ("fsdp", "ctx"), axis=0, tiled=True),
        lax.all_gather(cross_key_matrix, ("fsdp", "ctx"), axis=0, tiled=True),
        lax.all_gather(cross_value_matrix, ("fsdp", "ctx"), axis=0, tiled=True),
        lax.all_gather(cross_out, ("fsdp", "ctx"), axis=0, tiled=True),
    )
    normed_two, norm_pull_two = jax.vjp(rms_scale, hidden_two, cross_group[0].astype(jnp.float32))
    cross_in = normed_two.astype(jnp.bfloat16)
    cross_q = project(cross_in, cross_group[1]).astype(jnp.bfloat16)
    enc_keys = project(encoder, cross_group[2]).astype(jnp.bfloat16)
    enc_values = project(encoder, cross_group[3]).astype(jnp.bfloat16)
    keys_cross, values_cross = (
        lax.all_gather(enc_keys, "ctx", axis=1, tiled=True),
        lax.all_gather(enc_values, "ctx", axis=1, tiled=True),
    )
    cross_att, lse_cross = attention_forward(
        cross_q, keys_cross, values_cross, None, None, block_seqs
    )
    hidden_three = hidden_two + reduce_rows(project_back(cross_att, cross_group[4]))
    feed_group = (
        lax.all_gather(norm_feed, ("fsdp", "ctx"), axis=0, tiled=True),
        lax.all_gather(feed_gate, ("fsdp", "ctx"), axis=0, tiled=True),
        lax.all_gather(feed_up, ("fsdp", "ctx"), axis=0, tiled=True),
        lax.all_gather(feed_out, ("fsdp", "ctx"), axis=0, tiled=True),
    )
    normed_three, norm_pull_three = jax.vjp(
        rms_scale, hidden_three, feed_group[0].astype(jnp.float32)
    )
    feed_in = normed_three.astype(jnp.bfloat16)
    gate_value = project(feed_in, feed_group[1])
    up_value = project(feed_in, feed_group[2])
    gated_value, gated_pull = jax.vjp(gated_product, gate_value, up_value)
    feed_hidden = gated_value.astype(jnp.bfloat16)
    hidden_four = hidden_three + reduce_rows(project_back(feed_hidden, feed_group[3]))
    output = hidden_four.astype(jnp.bfloat16)
    valid_rows = (row_pos[None, :] < lengths[:, None]).astype(jnp.float32)
    grad_full = cotangent.astype(jnp.float32) * valid_rows[:, :, None]
    branch_low = grad_full.astype(jnp.bfloat16)
    grad_hidden = grad_full
    grad_feed_out = weight_grad(branch_low, feed_hidden)
    grad_gated = project(branch_low, feed_group[3])
    grad_gate, grad_up = gated_pull(grad_gated)
    gate_low = grad_gate.astype(jnp.bfloat16)
    up_low = grad_up.astype(jnp.bfloat16)
    grad_feed_gate = weight_grad(feed_in, gate_low)
    grad_feed_up = weight_grad(feed_in, up_low)
    grad_feed_in = reduce_rows(
        project_back(gate_low, feed_group[1]) + project_back(up_low, feed_group[2])
    )
    grad_three, grad_gain_three = norm_pull_three(grad_feed_in)
    grad_hidden = grad_hidden + grad_three
    feed_grads = (
        lax.psum_scatter(
            grad_gain_three.astype(jnp.bfloat16), ("fsdp", "ctx"), scatter_dimension=0, tiled=True
        ).astype(jnp.float32),
        lax.psum_scatter(
            grad_feed_gate.astype(jnp.bfloat16), ("fsdp", "ctx"), scatter_dimension=0, tiled=True
        ).astype(jnp.float32),
        lax.psum_scatter(
            grad_feed_up.astype(jnp.bfloat16), ("fsdp", "ctx"), scatter_dimension=0, tiled=True
        ).astype(jnp.float32),
        lax.psum_scatter(
            grad_feed_out.astype(jnp.bfloat16), ("fsdp", "ctx"), scatter_dimension=0, tiled=True
        ).astype(jnp.float32),
    )
    cross_low = grad_hidden.astype(jnp.bfloat16)
    grad_cross_out = weight_grad(cross_low, cross_att)
    grad_cross_att = project(cross_low, cross_group[4]).astype(jnp.bfloat16)
    grad_cq, grad_ck_part, grad_cv_part, unused_bias = attention_backward(
        cross_q, keys_cross, values_cross, None, None, lse_cross, grad_cross_att, block_seqs
    )
    grad_ck, grad_cv = (
        lax.psum_scatter(
            grad_ck_part.astype(jnp.bfloat16), "ctx", scatter_dimension=1, tiled=True
        ).astype(jnp.float32),
        lax.psum_scatter(
            grad_cv_part.astype(jnp.bfloat16), "ctx", scatter_dimension=1, tiled=True
        ).astype(jnp.float32),
    )
    ck_low = grad_ck.astype(jnp.bfloat16)
    cv_low = grad_cv.astype(jnp.bfloat16)
    grad_cross_query = weight_grad(cross_in, grad_cq)
    grad_cross_key = weight_grad(encoder, ck_low)
    grad_cross_value = weight_grad(encoder, cv_low)
    grad_cross_in, grad_encoder = reduce_rows(
        (
            project_back(grad_cq, cross_group[1]),
            project_back(ck_low, cross_group[2]) + project_back(cv_low, cross_group[3]),
        )
    )
    grad_two, grad_gain_two = norm_pull_two(grad_cross_in)
    grad_hidden = grad_hidden + grad_two
    cross_grads = (
        lax.psum_scatter(
            grad_gain_two.astype(jnp.bfloat16), ("fsdp", "ctx"), scatter_dimension=0, tiled=True
        ).astype(jnp.float32),
        lax.psum_scatter(
            grad_cross_query.astype(jnp.bfloat16), ("fsdp", "ctx"), scatter_dimension=0, tiled=True
        ).astype(jnp.float32),
        lax.psum_scatter(
            grad_cross_key.astype(jnp.bfloat16), ("fsdp", "ctx"), scatter_dimension=0, tiled=True
        ).astype(jnp.float32),
        lax.psum_scatter(
            grad_cross_value.astype(jnp.bfloat16), ("fsdp", "ctx"), scatter_dimension=0, tiled=True
        ).astype(jnp.float32),
        lax.psum_scatter(
            grad_cross_out.astype(jnp.bfloat16), ("fsdp", "ctx"), scatter_dimension=0, tiled=True
        ).astype(jnp.float32),
    )
    self_low = grad_hidden.astype(jnp.bfloat16)
    grad_self_out = weight_grad(self_low, self_att)
    grad_self_att = project(self_low, self_group[4]).astype(jnp.bfloat16)
    grad_sq, grad_sk_part, grad_sv_part, bias_total = attention_backward(
        self_q, keys_self, values_self, bias_rows, allowed, lse_self, grad_self_att, block_seqs
    )
    grad_sk, grad_sv = (
        lax.psum_scatter(
            grad_sk_part.astype(jnp.bfloat16), "ctx", scatter_dimension=1, tiled=True
        ).astype(jnp.float32),
        lax.psum_scatter(
            grad_sv_part.astype(jnp.bfloat16), "ctx", scatter_dimension=1, tiled=True
        ).astype(jnp.float32),
    )
    sk_low = grad_sk.astype(jnp.bfloat16)
    sv_low = grad_sv.astype(jnp.bfloat16)
    grad_table = jnp.einsum(
        "ijb,hij->bh",
        one_hot,
        bias_total.reshape(heads_local, row_total_count, key_total_count),
        precision=TOP_PRECISION,
    )
    grad_self_query = weight_grad(self_in, grad_sq)
    grad_self_key = weight_grad(self_in, sk_low)
    grad_self_value = weight_grad(self_in, sv_low)
    grad_self_in = reduce_rows(
        project_back(grad_sq, self_group[1])
        + project_back(sk_low, self_group[2])
        + project_back(sv_low, self_group[3])
    )
    grad_one, grad_gain_one = norm_pull_one(grad_self_in)
    grad_inputs = grad_hidden + grad_one
    self_grads = (
        lax.psum_scatter(
            grad_gain_one.astype(jnp.bfloat16), ("fsdp", "ctx"), scatter_dimension=0, tiled=True
        ).astype(jnp.float32),
        lax.psum_scatter(
            grad_self_query.astype(jnp.bfloat16), ("fsdp", "ctx"), scatter_dimension=0, tiled=True
        ).astype(jnp.float32),
        lax.psum_scatter(
            grad_self_key.astype(jnp.bfloat16), ("fsdp", "ctx"), scatter_dimension=0, tiled=True
        ).astype(jnp.float32),
        lax.psum_scatter(
            grad_self_value.astype(jnp.bfloat16), ("fsdp", "ctx"), scatter_dimension=0, tiled=True
        ).astype(jnp.float32),
        lax.psum_scatter(
            grad_self_out.astype(jnp.bfloat16), ("fsdp", "ctx"), scatter_dimension=0, tiled=True
        ).astype(jnp.float32),
        lax.psum_scatter(
            grad_table.astype(jnp.bfloat16), ("fsdp", "ctx"), scatter_dimension=0, tiled=True
        ).astype(jnp.float32),
    )
    gain_shares = jnp.stack((self_grads[0], cross_grads[0], feed_grads[0]), axis=0)
    return (
        output,
        grad_inputs,
        grad_encoder,
        gain_shares[0],
        self_grads[1],
        self_grads[2],
        self_grads[3],
        self_grads[4],
        self_grads[5],
        gain_shares[1],
        cross_grads[1],
        cross_grads[2],
        cross_grads[3],
        cross_grads[4],
        gain_shares[2],
        feed_grads[1],
        feed_grads[2],
        feed_grads[3],
    )


MESH = pl.DeviceIdType.MESH
LANES = 128
DEPTH = 4
LINKS = {("x", 0): 0, ("y", 0): 1, ("z", 1): 2, ("z", -1): 3, ("c", 0): 4}
SIZES = {"x": 2, "y": 2, "z": DEPTH}


class Place:
    def __init__(self):
        row = lax.axis_index("fsdp")
        self.y = lax.axis_index("ctx")
        self.z = lax.axis_index("tp")
        self.x = lax.div(row, 2)
        self.c = lax.rem(row, 2)

    def link(self, axis, d):
        x, y, z, c = self.x, self.y, self.z, self.c
        if axis == "x":
            x = 1 - x
        elif axis == "y":
            y = 1 - y
        elif axis == "z":
            z = z + d
        else:
            c = 1 - c
        return (x * 2 + c, y, z)

    def has(self, link):
        if link == ("z", 1):
            return self.z < DEPTH - 1
        if link == ("z", -1):
            return self.z > 0
        return None

    def source(self, src):
        x = 1 - self.x if src.get("x") else self.x
        y = 1 - self.y if src.get("y") else self.y
        return x, y, self.z + src.get("z", 0)

    def exists(self, src):
        off = src.get("z", 0)
        if off < 0:
            return self.z >= -off
        if off > 0:
            return self.z < DEPTH - off
        return None


def arrivals(order):
    events = []
    for k, axis in enumerate(order):
        sources = [{}]
        for a in order[:k]:
            choice = (0, -1, 1, -2, 2, -3, 3) if a == "z" else (0, 1)
            sources = [dict(b, **{a: o}) for o in choice for b in sources]
        for o in (-1, 1, -2, 2, -3, 3) if axis == "z" else (1,):
            for b in sources:
                src = dict(b, **{axis: o})
                d = 0 if axis != "z" else (1 if o < 0 else -1)
                events.append((k, sum(abs(v) for v in src.values()), src, d))
    return events


def onward(order, k, d):
    out = [("z", d)] if k >= 0 and order[k] == "z" else []
    for a in order[k + 1 :]:
        out += [("z", 1), ("z", -1)] if a == "z" else [(a, 0)]
    return out


def when(cond, action):
    if cond is None:
        action()
    else:
        pl.when(cond)(action)


def number(x, y, z):
    return (x * 2 + y) * DEPTH + z


def greet(place):
    barrier = pltpu.get_barrier_semaphore()

    def signal(link):
        pl.semaphore_signal(
            barrier, inc=1, device_id=place.link(*link), device_id_type=MESH
        )

    for link in LINKS:
        when(place.has(link), functools.partial(signal, link))
    ends = jnp.where(place.z < DEPTH - 1, 1, 0) + jnp.where(place.z > 0, 1, 0)
    pl.semaphore_wait(barrier, ends + 3)


def remote(src, dst, send, recv, device):
    return pltpu.make_async_remote_copy(
        src_ref=src, dst_ref=dst, send_sem=send, recv_sem=recv,
        device_id=device, device_id_type=MESH,
    )


def shard(ref, z, r, rows):
    if ref.shape[1] == rows:
        return ref.at[z, :, pl.ds(pl.multiple_of(r * LANES, LANES), LANES)]
    return ref.at[z, pl.ds(pl.multiple_of(r * rows, rows), rows), :]


class Gather:
    def __init__(self, place, orders, rows, ins, outs, sems):
        self.place, self.orders, self.rows, self.ins, self.outs = place, orders, rows, ins, outs
        self.send, self.recv, self.core_recv, self.local_sem = sems
        self.me = (place.x, place.y, place.z)
        self.arrivals = [
            (k, hops, j, src, d)
            for j in range(len(orders))
            for k, hops, src, d in arrivals(orders[j])
        ]
        self.arrivals.sort(key=lambda e: (e[0], e[1]))

    @staticmethod
    def scratch(count):
        dma = pltpu.SemaphoreType.DMA
        return [
            dma((count, 4 * DEPTH, 5)), dma((count, 4 * DEPTH)), dma((count, 4 * DEPTH)),
            dma((count,)),
        ]

    def slot(self, j, xyz, c):
        x, y, z = xyz
        if len(self.orders[j]) == 1:
            return self.outs[j].at[y if self.orders[j] == "y" else z]
        return shard(self.outs[j], z, (x * 2 + c) * 2 + y, self.rows[j])

    def copy(self, j, xyz, link, own):
        here = self.slot(j, xyz, self.place.c)
        arrived = self.core_recv if link[0] == "c" else self.recv
        i = number(*xyz)
        return remote(
            self.ins[j] if own else here, here, self.send.at[j, i, LINKS[link]],
            arrived.at[j, i], self.place.link(*link),
        )

    def routes(self, j, k, d):
        links = onward(self.orders[j], k, d)
        return links + [("c", 0)] if len(self.orders[j]) == 3 else links

    def local(self, j):
        return pltpu.make_async_copy(
            self.ins[j], self.slot(j, self.me, self.place.c), self.local_sem.at[j]
        )

    def start(self, which=None):
        which = range(len(self.orders)) if which is None else which
        for stage in range(2):
            for j in which:
                for link in self.routes(j, -1, 0):
                    if (link[0] == "c") == (stage == 1):
                        when(self.place.has(link), self.copy(j, self.me, link, True).start)
        for j in which:
            self.local(j).start()

    def steps(self, wanted=None):
        for e, (k, hops, j, src, d) in enumerate(self.arrivals):
            xyz = self.place.source(src)
            if wanted is not None and not wanted(j, k):
                continue

            def step(k=k, j=j, d=d, xyz=xyz, src=src):
                def run():
                    self.copy(j, xyz, ("x", 0), True).wait_recv()
                    for link in self.routes(j, k, d):
                        when(self.place.has(link), self.copy(j, xyz, link, False).start)

                when(self.place.exists(src), run)

            yield (e + 1) / len(self.arrivals), step

    def settle(self, which):
        for j in which:
            self.local(j).wait()
            if len(self.orders[j]) == 3:

                def from_core(i, carry):
                    xyz = (
                        lax.div(i, 2 * DEPTH), lax.rem(lax.div(i, DEPTH), 2), lax.rem(i, DEPTH)
                    )
                    remote(
                        self.ins[j], self.slot(j, xyz, 1 - self.place.c), self.send.at[j, i, 4],
                        self.core_recv.at[j, i], self.place.link("c", 0),
                    ).wait_recv()
                    return carry

                lax.fori_loop(0, 4 * DEPTH, from_core, 0)

    def sent(self):
        place = self.place
        for j, order in enumerate(self.orders):

            def wait(i, carry):
                xyz = (lax.div(i, 2 * DEPTH), lax.rem(lax.div(i, DEPTH), 2), lax.rem(i, DEPTH))
                same = {a: xyz["xyz".index(a)] == self.me["xyz".index(a)] for a in "xyz"}
                if len(order) == 3:
                    for m, a in enumerate(order):
                        after = True
                        for b in order[m + 1 :]:
                            after = same[b] & after
                        for link in ((a, 0),) if a != "z" else (("z", 1), ("z", -1)):
                            if a == "z":
                                d = link[1]
                                near = (xyz[2] - place.z) * d <= 0
                                cond = near & after & place.has(link)
                            else:
                                cond = same[a] & after
                            pl.when(cond)(self.copy(j, xyz, link, False).wait_send)
                    self.copy(j, xyz, ("c", 0), False).wait_send()
                elif order == "z":
                    column = same["x"] & same["y"]
                    for link in (("z", 1), ("z", -1)):
                        near = (xyz[2] - place.z) * link[1] <= 0
                        pl.when(column & near & place.has(link))(
                            self.copy(j, xyz, link, False).wait_send
                        )
                else:
                    pl.when(same["x"] & same["y"] & same["z"])(
                        self.copy(j, xyz, (order, 0), False).wait_send
                    )
                return carry

            lax.fori_loop(0, 4 * DEPTH, wait, 0)

    def finish(self):
        self.settle(range(len(self.orders)))
        self.sent()


def child_slots(order):
    starts, total, before = [], 0, 1
    for a in order:
        starts.append(total)
        total += before * (DEPTH + 1 if a == "z" else 1)
        before *= SIZES[a]
    return starts, total


def child_slot(order, starts, m, xyz, tail):
    at = 0
    for a in order[:m]:
        at = at * SIZES[a] + xyz["xyz".index(a)]
    if order[m] == "z":
        at = at * (DEPTH + 1) + tail
    return starts[m] + at


def add_rows(out, terms, rows):
    step = min(rows, 64 if out.shape[-1] <= LANES else 32)

    def body(q, carry):
        at = pl.ds(pl.multiple_of(q * step, step), step)
        value = terms[0][at, :].astype(jnp.float32)
        for term in terms[1:]:
            value = value + term[at, :].astype(jnp.float32)
        out[at, :] = value.astype(out.dtype)
        return carry

    lax.fori_loop(0, rows // step, body, 0)


class Scatter:
    def __init__(self, place, orders, rows, ins, outs, scratch):
        self.place, self.orders, self.rows, self.ins, self.outs = place, orders, rows, ins, outs
        n = len(orders)
        self.sums, self.gifts, self.kids = (scratch[i * n : (i + 1) * n] for i in range(3))
        self.load_sem, self.give_sem, self.gift_sem, self.up_sem, self.kid_sem = scratch[3 * n :]
        self.me = (place.x, place.y, place.z)
        self.plans = [child_slots(o) for o in orders]
        self.partner = place.link("c", 0)
        self.events = [
            (k, hops, j, src, d)
            for j in range(n)
            for k, hops, src, d in arrivals(orders[j])
        ]
        self.events.sort(key=lambda e: (-e[0], -e[1]))

    @staticmethod
    def scratch(arrays, orders):
        plans = [child_slots(o)[1] for o in orders]
        count = len(arrays)
        dma = pltpu.SemaphoreType.DMA

        def room(slots):
            return [pltpu.VMEM((n,) + shard_shape(a), a.dtype) for n, a in zip(slots, arrays)]

        full = [4 * DEPTH] * count
        return (
            room(full) + room(full) + room(plans)
            + [dma((count, 4 * DEPTH))] * 4 + [dma((count, max(plans)))]
        )

    def slot(self, j, xyz, c):
        x, y, z = xyz
        return shard(self.ins[j], z, (x * 2 + c) * 2 + y, self.rows[j])

    def load(self, j, xyz):
        i = number(*xyz)
        return pltpu.make_async_copy(
            self.slot(j, xyz, self.place.c), self.sums[j].at[i], self.load_sem.at[j, i]
        )

    def give(self, j, xyz):
        i = number(*xyz)
        return remote(
            self.slot(j, xyz, 1 - self.place.c), self.gifts[j].at[i], self.give_sem.at[j, i],
            self.gift_sem.at[j, i], self.partner,
        )

    def up(self, j, xyz, k, d):
        axis = self.orders[j][k]
        tail = xyz[2]
        if axis == "z" and d < 0:
            tail = jnp.where(xyz[2] == self.place.z - d, DEPTH, xyz[2])
        at = child_slot(self.orders[j], self.plans[j][0], k, xyz, tail)
        i = number(*xyz)
        return remote(
            self.sums[j].at[i], self.kids[j].at[at], self.up_sem.at[j, i],
            self.kid_sem.at[j, at], self.place.link(axis, -d),
        )

    def kid(self, j, m, xyz, tail):
        at = child_slot(self.orders[j], self.plans[j][0], m, xyz, tail)
        ref = self.kids[j].at[at]
        remote(ref, ref, self.up_sem.at[j, 0], self.kid_sem.at[j, at], self.partner).wait_recv()
        return ref

    def collect(self, j, xyz, k, d, out=None):
        i = number(*xyz)
        order = self.orders[j]
        total = self.sums[j].at[i]
        self.load(j, xyz).wait()
        self.give(j, xyz).wait_recv()
        always, sometimes = [], []
        if k >= 0 and order[k] == "z":
            sometimes.append((k, ("z", d), xyz[2]))
        for m in range(k + 1, len(order)):
            if order[m] == "z":
                sometimes += [(m, ("z", 1), xyz[2]), (m, ("z", -1), DEPTH)]
            else:
                always.append(m)
        for m, link, tail in sometimes:

            def more():
                add_rows(total, [total, self.kid(j, m, xyz, tail)], self.rows[j])

            when(self.place.has(link), more)
        terms = [total, self.gifts[j].at[i]] + [self.kid(j, m, xyz, 0) for m in always]
        add_rows(total if out is None else out, terms, self.rows[j])

    def start(self, which=None):
        for j in range(len(self.orders)) if which is None else which:
            order = self.orders[j]

            def begin(e, carry):
                left = 4 * DEPTH - 1 - e
                at = {}
                for a in order:
                    at[a] = lax.rem(left, SIZES[a])
                    left = lax.div(left, SIZES[a])
                xyz = tuple(
                    lax.rem(self.me["xyz".index(a)] + at[a], SIZES[a]) for a in "xyz"
                )
                self.give(j, xyz).start()
                self.load(j, xyz).start()
                return carry

            lax.fori_loop(0, 4 * DEPTH, begin, 0)

    def steps(self, wanted=None):
        count = len(self.events)
        for e, (k, hops, j, src, d) in enumerate(self.events):
            xyz = self.place.source(src)
            if wanted is not None and not wanted(j):
                continue

            def step(k=k, j=j, d=d, xyz=xyz, src=src):
                def run():
                    self.collect(j, xyz, k, d)
                    self.up(j, xyz, k, d).start()

                when(self.place.exists(src), run)

            yield (e + 1) / (count + 1), step
        for j in range(len(self.orders)):
            if wanted is not None and not wanted(j):
                continue

            def last(j=j):
                self.collect(j, self.me, -1, 0, self.outs[j])

            yield 1.0, last

    def finish(self):
        me = number(*self.me)
        for j in range(len(self.orders)):

            def wait(i, carry):
                xyz = (lax.div(i, 2 * DEPTH), lax.rem(lax.div(i, DEPTH), 2), lax.rem(i, DEPTH))
                self.give(j, xyz).wait_send()

                def sent():
                    mine = self.sums[j].at[i]
                    remote(
                        mine, mine, self.up_sem.at[j, i], self.kid_sem.at[j, 0], self.partner
                    ).wait_send()

                pl.when(i != me)(sent)
                return carry

            lax.fori_loop(0, 4 * DEPTH, wait, 0)


class Share:
    def __init__(self, place, rows, ins, outs, scratch):
        self.place, self.rows, self.ins, self.outs = place, rows, ins, outs
        n = len(rows)
        self.first, self.second, self.sums = (scratch[i * n : (i + 1) * n] for i in range(3))
        self.send, self.recv = scratch[3 * n :]
        self.half = lax.rem(place.z, 2)
        self.over_y = place.link("y", 0)
        self.over_z = place.link("z", 1 - 2 * self.half)

    @staticmethod
    def scratch(rows):
        dma = pltpu.SemaphoreType.DMA
        out = []
        for slots in (8, 4, 4):
            out += [pltpu.VMEM((slots, n, 256), jnp.bfloat16) for n in rows]
        return out + [dma((len(rows), 12)), dma((len(rows), 12))]

    def block(self, j, t, y, half):
        n = self.rows[j]
        return self.ins[j].at[t, pl.ds(pl.multiple_of((y * 2 + half) * n, n), n), :]

    def early(self, j, t, s):
        if t < 2:
            src, device = self.block(j, t, 1 - self.place.y, s), self.over_y
        else:
            src, device = self.block(j, t, s, 1 - self.half), self.over_z
        i = t * 2 + s
        return remote(src, self.first[j].at[i], self.send.at[j, i], self.recv.at[j, i], device)

    def late(self, j, t):
        return remote(
            self.sums[j].at[t], self.second[j].at[t], self.send.at[j, 8 + t],
            self.recv.at[j, 8 + t], self.over_z if t < 2 else self.over_y,
        )

    def start(self):
        for j in range(len(self.rows)):
            for s in range(2):
                for t in range(4):
                    self.early(j, t, s).start()

    def steps(self):
        for j in range(len(self.rows)):
            for t in range(4):

                def pass_on(j=j, t=t):
                    for s in range(2):
                        self.early(j, t, s).wait_recv()
                    if t < 2:
                        away = 1 - self.half
                        mine = self.block(j, t, self.place.y, away)
                    else:
                        away = 1 - self.place.y
                        mine = self.block(j, t, away, self.half)
                    add_rows(
                        self.sums[j].at[t], [mine, self.first[j].at[t * 2 + away]], self.rows[j]
                    )
                    self.late(j, t).start()

                yield 0.25, pass_on
        for j in range(len(self.rows)):
            for t in range(4):

                def total(j=j, t=t):
                    self.late(j, t).wait_recv()
                    kept = self.half if t < 2 else self.place.y
                    mine = self.block(j, t, self.place.y, self.half)
                    add_rows(
                        self.outs[j].at[t],
                        [mine, self.first[j].at[t * 2 + kept], self.second[j].at[t]],
                        self.rows[j],
                    )

                yield 0.5, total

    def finish(self):
        for j in range(len(self.rows)):
            for t in range(4):
                for s in range(2):
                    self.early(j, t, s).wait_send()
                self.late(j, t).wait_send()


HBM = pl.BlockSpec(memory_space=pl.ANY)
INSIDE = pl.BlockSpec(memory_space=pltpu.VMEM)


def comm_call(kernel, name, number_id, ins, in_specs, outs, out_specs, scratch):
    return pl.pallas_call(
        kernel,
        out_shape=outs,
        in_specs=in_specs,
        out_specs=out_specs,
        scratch_shapes=scratch,
        compiler_params=pltpu.CompilerParams(
            collective_id=number_id, has_side_effects=True, vmem_limit_bytes=67043328
        ),
        name=name,
    )(*ins)


def gathered(a, order):
    if len(order) == 1:
        return jax.ShapeDtypeStruct((SIZES[order],) + a.shape, a.dtype)
    if a.shape[0] > a.shape[1] == LANES:
        return jax.ShapeDtypeStruct((DEPTH, a.shape[0], 8 * LANES), a.dtype)
    return jax.ShapeDtypeStruct((DEPTH, 8 * a.shape[0], a.shape[1]), a.dtype)


def shard_shape(a):
    if a.shape[2] == 8 * LANES:
        return (a.shape[1], LANES)
    return (a.shape[1] // 8, a.shape[2])


def scattered(arrays):
    return [jax.ShapeDtypeStruct(shard_shape(a), jnp.float32) for a in arrays]


WIDTH = 1024
QROWS = 256
KEYS = 1024
ENC_ROWS = 512
SPAN = 1280
CHUNK = 128
VMEM_MOST = 64000000
ROWS_OF = (((0,), (0,)), ((), ()))
LAST = (((1,), (1,)), ((), ()))
PLAIN = (((1,), (0,)), ((), ()))


def mm(a, b, dims=PLAIN):
    return lax.dot_general(a, b, dims, preferred_element_type=jnp.float32)


def norm_rows(v, gain):
    return v * lax.rsqrt(jnp.mean(v * v, axis=-1, keepdims=True) + EPSILON) * gain


def norm_back(v, gain, e):
    r = lax.rsqrt(jnp.mean(v * v, axis=-1, keepdims=True) + EPSILON)
    ev = e * v
    gain_grad = jnp.sum(ev * r, axis=0, keepdims=True)
    back = r * gain * e - v * (r * r * r) * jnp.mean(ev * gain, axis=-1, keepdims=True)
    return back, gain_grad


def head_rows(cols, a):
    return jnp.concatenate(
        [cols[:, a * 128 : a * 128 + 64], cols[:, a * 128 + 64 : a * 128 + 128]], axis=0
    )


def attend(q, kv, p_ref, s_ref, ot_ref, keys, add_bias):
    for a in range(2):
        q2 = head_rows(q, a)
        k = kv[:, a * 64 : a * 64 + 64]
        v = kv[:, 128 + a * 64 : 192 + a * 64]
        if add_bias is not None:
            add_bias(a, None, None)
        peak = None
        for c in range(keys // CHUNK):
            rows = pl.ds(c * CHUNK, CHUNK)
            s = mm(k[c * CHUNK : (c + 1) * CHUNK], q2, LAST)
            if add_bias is not None:
                s = add_bias(a, c, s)
            s_ref[rows, :] = s
            top = jnp.max(s, axis=0, keepdims=True)
            peak = top if peak is None else jnp.maximum(peak, top)
        total = jnp.zeros_like(peak)
        for c in range(keys // CHUNK):
            rows = pl.ds(c * CHUNK, CHUNK)
            e = jnp.exp(s_ref[rows, :] - peak)
            s_ref[rows, :] = e
            total = total + jnp.sum(e, axis=0, keepdims=True)
        inverse = 1.0 / total
        for c in range(keys // CHUNK):
            rows = pl.ds(c * CHUNK, CHUNK)
            p_ref[0, a, rows, :] = (s_ref[rows, :] * inverse).astype(jnp.bfloat16)
        ot = mm(v, p_ref[0, a], ROWS_OF)
        ot_ref[a * 128 : a * 128 + 64, :] = ot[:, :QROWS]
        ot_ref[a * 128 + 64 : a * 128 + 128, :] = ot[:, QROWS:]
    return jnp.transpose(ot_ref[...]).astype(jnp.bfloat16)


def attend_back(q, kv, p_ref, do, dkv_ref, d_ref, ds_ref, qt_ref, keys, take_bias):
    for a in range(2):
        q2 = head_rows(q, a)
        do2 = head_rows(do, a)
        k = kv[:, a * 64 : a * 64 + 64]
        v = kv[:, 128 + a * 64 : 192 + a * 64]
        total = jnp.zeros((1, 2 * QROWS), jnp.float32)
        for c in range(keys // CHUNK):
            rows = pl.ds(c * CHUNK, CHUNK)
            dp = mm(v[c * CHUNK : (c + 1) * CHUNK], do2, LAST)
            d_ref[rows, :] = dp
            total = total + jnp.sum(
                dp * p_ref[0, a, rows, :].astype(jnp.float32), axis=0, keepdims=True
            )
        for c in range(keys // CHUNK):
            rows = pl.ds(c * CHUNK, CHUNK)
            ds = p_ref[0, a, rows, :].astype(jnp.float32) * (d_ref[rows, :] - total)
            if take_bias is not None:
                take_bias(a, c, ds)
            ds_ref[rows, :] = ds.astype(jnp.bfloat16)
        if take_bias is not None:
            take_bias(a, None, None)
        dkv_ref[0, :, a * 64 : a * 64 + 64] = mm(ds_ref[pl.ds(0, keys), :], q2).astype(jnp.bfloat16)
        dkv_ref[0, :, 128 + a * 64 : 192 + a * 64] = mm(p_ref[0, a], do2).astype(jnp.bfloat16)
        qt = mm(k, ds_ref[pl.ds(0, keys), :], ROWS_OF)
        qt_ref[a * 128 : a * 128 + 64, :] = qt[:, :QROWS]
        qt_ref[a * 128 + 64 : a * 128 + 128, :] = qt[:, QROWS:]
    return jnp.transpose(qt_ref[...]).astype(jnp.bfloat16)


def self_step(first, length, h1_ref, w_ref, wkv_ref, near_of, q_ref, kv_ref, p_ref, o_ref, work):
    s_ref, strip_ref, ot_ref = work
    kv = mm(h1_ref[...], wkv_ref[0]).astype(jnp.bfloat16)
    kv_ref[0] = kv
    q = mm(h1_ref[pl.ds(first, QROWS), :], w_ref[0, :, :QROWS]).astype(jnp.bfloat16)
    q_ref[0] = q
    lane = lax.broadcasted_iota(jnp.int32, (1, 2 * QROWS), 1)
    lane = jnp.where(lane < QROWS, lane, lane - QROWS)
    last_key = jnp.minimum(lane + first, length - 1)

    def add_bias(a, c, s):
        if c is None:
            for b in range(2):
                near = near_of(2 * a + b)
                for g in range(16):
                    shift = (SPAN - (120 - 8 * g)) % SPAN
                    strip_ref[b, 8 * g : 8 * g + 8, :] = (
                        pltpu.roll(near, shift, 1) if shift else near
                    )
            return None
        cols = pl.ds(CHUNK * (7 - c), QROWS)
        bias = jnp.concatenate([strip_ref[0, :, cols], strip_ref[1, :, cols]], axis=1)
        key = lax.broadcasted_iota(jnp.int32, s.shape, 0) + c * CHUNK
        return jnp.where(key <= last_key, s + bias, MASKED)

    o = attend(q, kv, p_ref, s_ref, ot_ref, KEYS, add_bias)
    o_ref[0] = o
    return mm(o, w_ref[0, :, QROWS:], LAST)


def cross_step(h_ref, enc, w_ref, wkv_ref, q_ref, kv_ref, p_ref, o_ref, work):
    s_ref, ot_ref = work
    kv = mm(enc, wkv_ref[0]).astype(jnp.bfloat16)
    kv_ref[0] = kv
    q = mm(h_ref[...], w_ref[0, :, :QROWS]).astype(jnp.bfloat16)
    q_ref[0] = q
    o = attend(q, kv, p_ref, s_ref, ot_ref, ENC_ROWS, None)
    o_ref[0] = o
    return mm(o, w_ref[0, :, QROWS:], LAST)


def here():
    z = lax.axis_index("tp")
    half = lax.rem(z, 2)
    return lax.div(z, 2), half, lax.axis_index("ctx") * (2 * QROWS) + half * QROWS


def feed_kernel(
    at, lengths, x3_ref, cot_ref, gain_ref, wg_ref, wu_ref, wo_ref,
    out_ref, g3_ref, gg_ref, gu_ref, go_ref, gn_ref,
    h_ref, g_ref, y_ref, dh_ref,
):
    step = pl.program_id(0)

    @pl.when(step == 0)
    def _():
        h_ref[...] = norm_rows(x3_ref[...], gain_ref[pl.ds(2, 1), :]).astype(jnp.bfloat16)
        row = lax.broadcasted_iota(jnp.int32, (QROWS, 1), 0) + at[2]
        g4 = jnp.where(row < lengths[at[0]], cot_ref[0].astype(jnp.float32), 0.0)
        g_ref[...] = g4.astype(jnp.bfloat16)
        y_ref[...] = x3_ref[...]
        dh_ref[...] = jnp.zeros_like(dh_ref)

    gate = mm(h_ref[...], wg_ref[0], LAST)
    up = mm(h_ref[...], wu_ref[0], LAST)
    root = math.sqrt(2.0 / math.pi)
    square = gate * gate
    th = jnp.tanh(root * (gate + 0.044715 * gate * square))
    half = 0.5 * (1.0 + th)
    gelu = gate * half
    slope = half + 0.5 * gate * (1.0 - th * th) * (root * (1.0 + 3 * 0.044715 * square))
    hidden = (gelu * up).astype(jnp.bfloat16)
    y_ref[...] += mm(hidden, wo_ref[0])
    go_ref[0] = mm(hidden, g_ref[...], ROWS_OF).astype(jnp.bfloat16)
    dhid = mm(g_ref[...], wo_ref[0], LAST)
    dup = (dhid * gelu).astype(jnp.bfloat16)
    dgate = (dhid * up * slope).astype(jnp.bfloat16)
    gg_ref[0] = mm(dgate, h_ref[...], ROWS_OF).astype(jnp.bfloat16)
    gu_ref[0] = mm(dup, h_ref[...], ROWS_OF).astype(jnp.bfloat16)
    dh_ref[...] += mm(dgate, wg_ref[0]) + mm(dup, wu_ref[0])

    @pl.when(step == pl.num_programs(0) - 1)
    def _():
        out_ref[...] = y_ref[...].astype(jnp.bfloat16)
        back, gain_grad = norm_back(x3_ref[...], gain_ref[pl.ds(2, 1), :], dh_ref[...])
        g3_ref[...] = g_ref[...].astype(jnp.float32) + back
        gn_ref[...] = gain_grad


def whole(shape):
    zeros = (0,) * len(shape)
    return pl.BlockSpec(shape, lambda t: zeros)


def part(shape, column=0):
    tail = (0,) * (len(shape) - 2)
    return pl.BlockSpec(shape, lambda t: (t,) + tail + (column,))


SCALARS = pl.BlockSpec(memory_space=pltpu.SMEM)
F32 = jnp.float32
LOW = jnp.bfloat16


def shape_of(shape, dtype):
    return jax.ShapeDtypeStruct(shape, dtype)


def feed(at, lengths, x3, cot, gains, wg, wu, wo):
    units = wg.shape[1]

    def fixed(shape):
        return pl.BlockSpec(shape, lambda t, at: (0,) * len(shape))

    wide = pl.BlockSpec((1, units, WIDTH), lambda t, at: (t, 0, 0))
    outs = (
        [shape_of((QROWS, WIDTH), LOW), shape_of((QROWS, WIDTH), F32)]
        + [shape_of((4, units, WIDTH), LOW)] * 3
        + [shape_of((1, WIDTH), F32)]
    )
    return pl.pallas_call(
        feed_kernel,
        grid_spec=pltpu.PrefetchScalarGridSpec(
            num_scalar_prefetch=1,
            grid=(4,),
            in_specs=[
                SCALARS, fixed((QROWS, WIDTH)),
                pl.BlockSpec((1, QROWS, WIDTH), lambda t, at: (at[0], at[1], 0)),
                fixed((8, WIDTH)), wide, wide, wide,
            ],
            out_specs=[fixed((QROWS, WIDTH)), fixed((QROWS, WIDTH)), wide, wide, wide,
                       fixed((1, WIDTH))],
            scratch_shapes=[
                pltpu.VMEM((QROWS, WIDTH), LOW), pltpu.VMEM((QROWS, WIDTH), LOW),
                pltpu.VMEM((QROWS, WIDTH), F32), pltpu.VMEM((QROWS, WIDTH), F32),
            ],
        ),
        out_shape=outs,
        compiler_params=pltpu.CompilerParams(
            dimension_semantics=("arbitrary",), vmem_limit_bytes=VMEM_MOST
        ),
        cost_estimate=pl.CostEstimate(
            flops=13 * 10**9, bytes_accessed=4 * 10**7, transcendentals=0
        ),
        name="feed",
    )(at, lengths, x3, cot, gains, wg, wu, wo)


FORWARD_SPLIT = (0.0, 0.7)
BACKWARD_SPLIT = (0.1, 0.0, 0.6)
SHARED = 0.5
LAST_SPLIT = (0.0, 0.6)
GATHER_ORDERS = ("zyx", "zyx", "xzy", "yzx", "zxy", "yzx", "zxy", "y", "y")
SMALL_ROWS = 16


def split_steps(steps, parts, low, high):
    ends = [int(len(steps) * (low + (high - low) * (i + 1) / parts)) for i in range(parts)]
    return [steps[a:b] for a, b in zip([0] + ends, ends)], steps[ends[-1] :]


def at_step(t, chunks):
    for i, chunk in enumerate(chunks):

        def run():
            for step in chunk:
                step()

        if chunk:
            pl.when(t == i)(run)


def forward_kernel(rows, *refs):
    lengths, feeds, packs, inputs, encoder = refs[0], refs[1:4], refs[4:8], refs[8], refs[9]
    weights, refs = refs[10:16], refs[16:]
    gains_ref, x2_ref, x3_ref, h1_out, h2_ref, x_out, enc_out = refs[:7]
    q1_out, kv1_out, p1_out, o1_out, q2_out, kv2_out, p2_out, o2_out = refs[7:15]
    small, x_all, enc_all, bucket_ref, h1_ref, s_ref, strip_ref, ot_ref = refs[15:23]
    own_feeds, own_x, own_enc, own_sem = refs[23:26], refs[26], refs[27], refs[28]
    place = Place()
    half = lax.rem(place.z, 2)
    seq = lax.div(place.z, 2)
    ins = own_feeds + packs + (own_x, own_enc)
    loads = [
        pltpu.make_async_copy(src, dst, own_sem.at[i])
        for i, (src, dst) in enumerate(
            [(inputs.at[seq], own_x), (encoder.at[seq], own_enc)] + list(zip(feeds, own_feeds))
        )
    ]
    for load in loads:
        load.start()
    plan = Gather(place, GATHER_ORDERS, rows, ins, weights + (small, x_all, enc_all), refs[29:])
    greet(place)
    first = pl.multiple_of(place.y * (2 * QROWS) + half * QROWS, QROWS)
    length = lengths[seq]
    for load in loads:
        load.wait()
    plan.start(range(3, 9))
    row = lax.broadcasted_iota(jnp.int32, (8, SPAN), 0)
    col = lax.broadcasted_iota(jnp.int32, (8, SPAN), 1)
    bucket_ref[...] = bucket_index(jnp.maximum(first + col - (SPAN - 264) - row, 0))
    for _, step in plan.steps(lambda j, k: 3 <= j < 7 and k < 2):
        step()
    plan.start(range(3))
    for _, step in plan.steps(lambda j, k: j >= 7 or (j >= 3 and k == 2)):
        step()
    plan.settle(range(3, 9))
    feed_steps = [step for _, step in plan.steps(lambda j, k: j < 3)]
    chunks, rest = split_steps(feed_steps, 8, *FORWARD_SPLIT)

    for k in range(3):
        gains_ref[pl.ds(k, 1), :] = jnp.concatenate(
            [small[0, pl.ds(r * SMALL_ROWS + k, 1), :] for r in range(8)], axis=1
        )
    gain = gains_ref[pl.ds(0, 1), :]
    for y in range(2):
        for c in range(2):
            at = pl.ds(c * QROWS, QROWS)
            h1_ref[pl.ds(y * 512 + c * QROWS, QROWS), :] = norm_rows(
                x_all[y, at, :].astype(jnp.float32), gain
            ).astype(jnp.bfloat16)
    own = own_x[pl.ds(pl.multiple_of(half * QROWS, QROWS), QROWS), :]
    x_out[...] = own
    x2_ref[...] = own.astype(jnp.float32)
    n = QROWS // 2
    enc_out[...] = own_enc[pl.ds(pl.multiple_of(half * n, n), n), :]
    h1_out[...] = h1_ref[pl.ds(first, QROWS), :]

    def self_body(w_ref, wkv_ref, q_ref, kv_ref, p_ref, o_ref):
        t = pl.program_id(0)

        def near_of(head):
            rows_of = [small[t, pl.ds(r * SMALL_ROWS + 3, 1), :] for r in range(8)]
            bucket = bucket_ref[...]
            near = jnp.zeros((8, SPAN), jnp.float32)
            for i in range(BUCKETS):
                lane = (i % 4) * 4 + head
                value = rows_of[i // 4][:, lane : lane + 1]
                near = jnp.where(bucket == i, value, near)
            return near

        x2_ref[...] += self_step(
            first, length, h1_ref, w_ref, wkv_ref, near_of, q_ref, kv_ref, p_ref, o_ref,
            (s_ref, strip_ref, ot_ref),
        )
        at_step(t, chunks[:4])

    pltpu.emit_pipeline(
        self_body,
        grid=(4,),
        in_specs=[part((1, WIDTH, 512)), part((1, WIDTH, 256))],
        out_specs=[
            part((1, QROWS, 256)), part((1, KEYS, 256)), part((1, 2, KEYS, 512)),
            part((1, QROWS, 256)),
        ],
    )(weights[3], weights[5], q1_out, kv1_out, p1_out, o1_out)
    x3_ref[...] = x2_ref[...]
    h2_ref[...] = norm_rows(x2_ref[...], gains_ref[pl.ds(1, 1), :]).astype(jnp.bfloat16)

    def cross_body(w_ref, wkv_ref, q_ref, kv_ref, p_ref, o_ref):
        enc = jnp.concatenate([enc_all[0], enc_all[1]], axis=0)
        x3_ref[...] += cross_step(
            h2_ref, enc, w_ref, wkv_ref, q_ref, kv_ref, p_ref, o_ref, (s_ref, ot_ref)
        )
        at_step(pl.program_id(0), chunks[4:])

    pltpu.emit_pipeline(
        cross_body,
        grid=(4,),
        in_specs=[part((1, WIDTH, 512)), part((1, WIDTH, 256), 1)],
        out_specs=[
            part((1, QROWS, 256)), part((1, ENC_ROWS, 256)), part((1, 2, ENC_ROWS, 512)),
            part((1, QROWS, 256)),
        ],
    )(weights[4], weights[5], q2_out, kv2_out, p2_out, o2_out)
    for step in rest:
        step()
    plan.settle(range(3))
    plan.sent()


def forward(lengths, feeds, packs, inputs, encoder):
    x, enc = shape_of(inputs.shape[1:], LOW), shape_of(encoder.shape[1:], LOW)
    arrays = list(feeds) + list(packs) + [x, enc]
    rows = [a.shape[0] for a in arrays]
    wide = [gathered(a, o) for a, o in zip(arrays, GATHER_ORDERS)]
    vm = pltpu.VMEM
    return comm_call(
        functools.partial(forward_kernel, rows), "forward", 1,
        (lengths,) + tuple(feeds) + tuple(packs) + (inputs, encoder),
        [SCALARS] + [HBM] * 3 + [INSIDE] * 4 + [HBM] * 2,
        wide[:6]
        + [shape_of((8, WIDTH), F32), shape_of((QROWS, WIDTH), F32),
           shape_of((QROWS, WIDTH), F32), shape_of((QROWS, WIDTH), LOW),
           shape_of((QROWS, WIDTH), LOW), shape_of((QROWS, WIDTH), LOW),
           shape_of((QROWS // 2, WIDTH), LOW),
           shape_of((4, QROWS, 256), LOW), shape_of((4, KEYS, 256), LOW),
           shape_of((4, 2, KEYS, 512), LOW), shape_of((4, QROWS, 256), LOW),
           shape_of((4, QROWS, 256), LOW), shape_of((4, ENC_ROWS, 256), LOW),
           shape_of((4, 2, ENC_ROWS, 512), LOW), shape_of((4, QROWS, 256), LOW)],
        [HBM] * 6 + [INSIDE] * 7 + [HBM] * 8,
        [vm(w.shape, w.dtype) for w in wide[6:]]
        + [vm((8, SPAN), jnp.int32), vm((KEYS, WIDTH), LOW), vm((KEYS, 512), F32),
           vm((2, CHUNK, SPAN), F32), vm((256, QROWS), F32)]
        + [vm(a.shape, LOW) for a in arrays[:3] + arrays[7:]]
        + [pltpu.SemaphoreType.DMA((5,))]
        + Gather.scratch(9),
    )


FEED_ORDERS = ("zxy", "zyx", "zyx")


def backward_kernel(rows, own, room, *refs):
    grads, refs = refs[:3], refs[3:]
    out_ref, g3_ref, x2_ref, h2_ref, h1_ref, gains_ref, x_ref, enc_ref, gn3_ref = refs[:9]
    w1, w2, w3, q1, kv1, p1, o1, q2, kv2, p2, o2 = refs[9:20]
    shards, refs = refs[20:23], refs[23:]
    rows_out, gx_ref, genc_ref, small, gw1, gw2, gw3 = refs[:7]
    dkv1, dkv2, g_ref, gt_ref, ht_ref, dc_ref, d_ref, ds_ref, qt_ref, strip_ref = refs[7:17]
    line_ref, g2_ref, dh_ref, dkv1_out, dkv2_out, et_ref, scratch = *refs[17:23], refs[23:]
    place = Place()
    plan = Scatter(place, FEED_ORDERS, rows, grads, shards, scratch[: len(room)])
    scratch = scratch[len(room) :]
    share = Share(place, own, (dkv1, dkv2), (dkv1_out, dkv2_out), scratch[:8])
    lines = Gather(place, ("z",), (QROWS,), (out_ref,), (rows_out,), scratch[8:])
    greet(place)
    lines.start()
    plan.start()
    steps = [step for _, step in plan.steps()]
    begin = int(len(steps) * BACKWARD_SPLIT[0])
    for step in steps[:begin]:
        step()
    chunks, rest = split_steps(steps[begin:], 8, *BACKWARD_SPLIT[1:])

    def load_grad(ref, h_ref):
        g = ref[...].astype(jnp.bfloat16)
        g_ref[...] = g
        gt_ref[...] = jnp.transpose(g)
        ht_ref[...] = jnp.transpose(h_ref[...])

    def heads(t, w_ref, q_ref, kv_ref, p_ref, o_ref, gw_ref, dkv, d_sum, keys, take_bias):
        do = mm(g_ref[...], w_ref[0, :, QROWS:]).astype(jnp.bfloat16)
        gw_ref[0, :, QROWS:] = mm(gt_ref[...], o_ref[0]).astype(jnp.bfloat16)
        dq = attend_back(
            q_ref[0], kv_ref[0], p_ref, do, dkv.at[pl.ds(t, 1)], d_ref, ds_ref, qt_ref, keys,
            take_bias,
        )
        gw_ref[0, :, :QROWS] = mm(ht_ref[...], dq).astype(jnp.bfloat16)
        d_sum[...] += mm(dq, w_ref[0, :, :QROWS], LAST)

    def specs(keys):
        return [
            part((1, WIDTH, 512)), part((1, QROWS, 256)), part((1, keys, 256)),
            part((1, 2, keys, 512)), part((1, QROWS, 256)),
        ]

    load_grad(g3_ref, h2_ref)
    dc_ref[...] = jnp.zeros_like(dc_ref)

    def cross_body(w_ref, q_ref, kv_ref, p_ref, o_ref, gw_ref):
        t = pl.program_id(0)
        heads(t, w_ref, q_ref, kv_ref, p_ref, o_ref, gw_ref, dkv2, dc_ref, ENC_ROWS, None)
        at_step(t, chunks[:4])

    pltpu.emit_pipeline(
        cross_body, grid=(4,), in_specs=specs(ENC_ROWS), out_specs=[part((1, WIDTH, 512))]
    )(w2, q2, kv2, p2, o2, gw2)
    back, gain_grad = norm_back(x2_ref[...], gains_ref[pl.ds(1, 1), :], dc_ref[...])
    g2_ref[...] = g3_ref[...] + back
    gain_grads = [None, gain_grad, gn3_ref[...]]
    load_grad(g2_ref, h1_ref)
    dh_ref[...] = jnp.zeros_like(dh_ref)

    def self_body(w_ref, q_ref, kv_ref, p_ref, o_ref, gw_ref):
        t = pl.program_id(0)

        def take_bias(a, c, ds):
            if c is None:
                for b in range(2):
                    total = jnp.zeros((8, SPAN), jnp.float32)
                    for g in range(16):
                        piece = strip_ref[b, 8 * g : 8 * g + 8, :]
                        shift = 120 - 8 * g
                        total = total + (pltpu.roll(piece, shift, 1) if shift else piece)
                    line = total[0:1]
                    for r in range(1, 8):
                        line = line + pltpu.roll(total[r : r + 1], SPAN - r, 1)
                    line_ref[pl.ds(t * 4 + 2 * a + b, 1), :] = line
                return
            if c == 0:
                strip_ref[...] = jnp.zeros_like(strip_ref)
            cols = pl.ds(CHUNK * (7 - c), QROWS)
            strip_ref[0, :, cols] += ds[:, :QROWS]
            strip_ref[1, :, cols] += ds[:, QROWS:]

        heads(t, w_ref, q_ref, kv_ref, p_ref, o_ref, gw_ref, dkv1, dh_ref, KEYS, take_bias)
        at_step(t, chunks[4:])

    pltpu.emit_pipeline(
        self_body, grid=(4,), in_specs=specs(KEYS), out_specs=[part((1, WIDTH, 512))]
    )(w1, q1, kv1, p1, o1, gw1)
    share.start()
    distance = lax.broadcasted_iota(jnp.int32, (1, SPAN), 1) - (SPAN - 264) + here()[2]
    bucket = bucket_index(jnp.maximum(distance, 0))
    chosen = lax.broadcasted_iota(jnp.int32, (LANES, SPAN), 0) == bucket
    table = lax.dot_general(
        line_ref[...], chosen.astype(jnp.float32), LAST, precision=TOP_PRECISION,
        preferred_element_type=jnp.float32,
    )
    ordered = [(i / max(len(rest), 1), step) for i, step in enumerate(rest)]
    ordered += [(0.05 + 0.9 * at, step) for at, step in share.steps()]
    ordered += [(0.1 * at, step) for at, step in lines.steps()]
    ordered.sort(key=lambda s: s[0])
    for _, step in [s for s in ordered if s[0] <= SHARED]:
        step()
    chunks, rest = split_steps([s[1] for s in ordered if s[0] > SHARED], 4, *LAST_SPLIT)
    et_ref[...] = jnp.transpose(enc_ref[...])
    n = QROWS // 2
    dc_ref[pl.ds(0, n), :] = jnp.zeros((n, WIDTH), jnp.float32)

    def last_body(ws_ref, wc_ref, gw_ref):
        t = pl.program_id(0)
        dkv, dkvc = dkv1_out[t], dkv2_out[t]
        gw_ref[0, :, :256] = mm(ht_ref[...], dkv).astype(jnp.bfloat16)
        gw_ref[0, :, 256:] = mm(et_ref[...], dkvc).astype(jnp.bfloat16)
        dh_ref[...] += mm(dkv, ws_ref[0], LAST)
        dc_ref[pl.ds(0, n), :] += mm(dkvc, wc_ref[0], LAST)
        at_step(t, chunks)

    pltpu.emit_pipeline(
        last_body, grid=(4,), in_specs=[part((1, WIDTH, 256)), part((1, WIDTH, 256), 1)],
        out_specs=[part((1, WIDTH, 512))],
    )(w3, w3, gw3)
    back, gain_grads[0] = norm_back(
        x_ref[...].astype(jnp.float32), gains_ref[pl.ds(0, 1), :], dh_ref[...]
    )
    gx_ref[...] = (g2_ref[...] + back).astype(jnp.bfloat16)
    genc_ref[...] = dc_ref[pl.ds(0, n), :].astype(jnp.bfloat16)
    small[...] = jnp.zeros_like(small)
    for r in range(8):
        shifted = pltpu.roll(table, (LANES - 4 * r) % LANES, 1) if r else table
        for t in range(4):
            for k in range(3):
                small[t, pl.ds(r * SMALL_ROWS + k, 1), :] = gain_grads[k][
                    :, r * LANES : (r + 1) * LANES
                ]
            small[t, pl.ds(r * SMALL_ROWS + 4, 4), :] = shifted[4 * t : 4 * t + 4]
    for step in rest:
        step()
    lines.finish()
    share.finish()
    plan.finish()


def backward(grads, out, g3, x2, h2, h1, gains, x, enc, gn3, w1, w2, w3, saved1, saved2):
    rows = [shard_shape(a)[0] for a in grads]
    own = [KEYS // 4, ENC_ROWS // 4]
    room = Scatter.scratch(grads, FEED_ORDERS)
    vm = pltpu.VMEM
    return comm_call(
        functools.partial(backward_kernel, rows, own, room), "backward", 2,
        tuple(grads) + (out, g3, x2, h2, h1, gains, x, enc, gn3, w1, w2, w3)
        + tuple(saved1) + tuple(saved2),
        [HBM] * 3 + [INSIDE] * 9 + [HBM] * 11,
        scattered(grads)
        + [gathered(out, "z"), shape_of(x.shape, LOW), shape_of(enc.shape, LOW),
           shape_of((4, 8 * SMALL_ROWS, LANES), F32), shape_of(w1.shape, LOW),
           shape_of(w2.shape, LOW), shape_of(w3.shape, LOW)],
        [INSIDE] * 3 + [HBM] + [INSIDE] * 3 + [HBM] * 3,
        [vm((4, KEYS, 256), LOW), vm((4, ENC_ROWS, 256), LOW), vm((QROWS, WIDTH), LOW),
         vm((WIDTH, QROWS), LOW), vm((WIDTH, QROWS), LOW), vm((QROWS, WIDTH), F32),
         vm((KEYS, 512), F32), vm((KEYS, 512), LOW), vm((256, QROWS), F32),
         vm((2, CHUNK, SPAN), F32), vm((16, SPAN), F32), vm((QROWS, WIDTH), F32),
         vm((QROWS, WIDTH), F32)]
        + [vm((4, r, 256), LOW) for r in own] + [vm((WIDTH, enc.shape[0]), LOW)]
        + room + Share.scratch(own) + Gather.scratch(1),
    )


HEAD_ORDERS = ("zyx", "zxy", "zyx", "zxy")


def finish_kernel(rows, room, *refs):
    ins, sent, out, landed, scratch = refs[:4], refs[4:6], refs[6], refs[7:9], refs[9:]
    place = Place()
    shards = [out.at[j] for j in range(3)]
    shards.append(out.at[3, pl.ds(0, SMALL_ROWS), pl.ds(0, LANES)])
    plan = Scatter(place, HEAD_ORDERS, rows, ins, shards, scratch[: len(room)])
    lines = Gather(
        place, ("z", "z"), (QROWS, QROWS // 2), sent, landed, scratch[len(room) :]
    )
    greet(place)
    lines.start()
    plan.start()
    steps = list(plan.steps()) + [(0.8 * at, step) for at, step in lines.steps()]
    steps.sort(key=lambda s: s[0])
    for _, step in steps:
        step()
    lines.finish()
    plan.finish()


def finish(arrays, lines):
    rows = [shard_shape(a)[0] for a in arrays]
    room = Scatter.scratch(arrays, HEAD_ORDERS)
    return comm_call(
        functools.partial(finish_kernel, rows, room), "finish", 3,
        tuple(arrays) + tuple(lines), [HBM] * 4 + [INSIDE] * 2,
        [shape_of((4, LANES, 512), F32)] + [gathered(a, "z") for a in lines],
        [INSIDE] + [HBM] * 2,
        room + Gather.scratch(2),
    )


def small_rows(gains, table):
    flat = jnp.pad(table.reshape(1, -1).astype(F32), ((0, 0), (0, LANES - table.size)))
    rows = jnp.concatenate([g.reshape(1, LANES).astype(F32) for g in gains] + [flat], axis=0)
    return jnp.pad(rows, ((0, SMALL_ROWS - 4), (0, 0)))


def tokens_split(
    inputs, encoder, lengths, cotangent,
    norm_self, self_query, self_key_matrix, self_value_matrix, self_out, bias_table,
    norm_cross, cross_query, cross_key_matrix, cross_value_matrix, cross_out,
    norm_feed, feed_gate, feed_up, feed_out,
):
    packs = (
        jnp.concatenate([self_query, self_out], axis=1),
        jnp.concatenate([cross_query, cross_out], axis=1),
        jnp.concatenate(
            [self_key_matrix, self_value_matrix, cross_key_matrix, cross_value_matrix], axis=1
        ),
        small_rows((norm_self, norm_cross, norm_feed), bias_table),
    )
    (
        wg, wu, wo, w1, w2, w3, gains, x2, x3, h1, h2, x_own, enc_own,
        q1, kv1, p1, o1, q2, kv2, p2, o2,
    ) = forward(lengths, (feed_gate.T, feed_up.T, feed_out.T), packs, inputs, encoder)
    out, g3, gg, gu, go, gn3 = feed(
        jnp.stack(here()), lengths, x3, cotangent, gains, wg, wu, wo
    )
    gg, gu, go, out, gx, genc, small, gw1, gw2, gw3 = backward(
        (gg, gu, go), out, g3, x2, h2, h1, gains, x_own, enc_own, gn3, w1, w2, w3,
        (q1, kv1, p1, o1), (q2, kv2, p2, o2),
    )
    heads, gx, genc = finish((gw1, gw2, gw3, small), (gx, genc))
    return (
        out.reshape(inputs.shape),
        gx.reshape(inputs.shape).astype(F32),
        genc.reshape(encoder.shape).astype(F32),
        heads[3, 0, :128], heads[0, :, :256], heads[2, :, :128], heads[2, :, 128:256],
        heads[0, :, 256:], jnp.transpose(heads[3, 4:8, :4]),
        heads[3, 1, :128], heads[1, :, :256], heads[2, :, 256:384], heads[2, :, 384:],
        heads[1, :, 256:],
        heads[3, 2, :128], gg.T, gu.T, go.T,
    )


def solution(mesh):
    sizes = (mesh.shape["fsdp"], mesh.shape["ctx"], mesh.shape["tp"])
    return jax.shard_map(
        tokens_split if sizes == (4, 2, DEPTH) else shards,
        mesh=mesh,
        in_specs=(
            P("fsdp", "ctx", None),
            P("fsdp", "ctx", None),
            P("fsdp"),
            P("fsdp", "ctx", None),
            P(("fsdp", "ctx")),
            P(("fsdp", "ctx"), "tp"),
            P(("fsdp", "ctx"), "tp"),
            P(("fsdp", "ctx"), "tp"),
            P(("fsdp", "ctx"), "tp"),
            P(("fsdp", "ctx"), "tp"),
            P(("fsdp", "ctx")),
            P(("fsdp", "ctx"), "tp"),
            P(("fsdp", "ctx"), "tp"),
            P(("fsdp", "ctx"), "tp"),
            P(("fsdp", "ctx"), "tp"),
            P(("fsdp", "ctx")),
            P(("fsdp", "ctx"), "tp"),
            P(("fsdp", "ctx"), "tp"),
            P(("fsdp", "ctx"), "tp"),
        ),
        out_specs=(
            P("fsdp", "ctx", None),
            P("fsdp", "ctx", None),
            P("fsdp", "ctx", None),
            P(("fsdp", "ctx")),
            P(("fsdp", "ctx"), "tp"),
            P(("fsdp", "ctx"), "tp"),
            P(("fsdp", "ctx"), "tp"),
            P(("fsdp", "ctx"), "tp"),
            P(("fsdp", "ctx"), "tp"),
            P(("fsdp", "ctx")),
            P(("fsdp", "ctx"), "tp"),
            P(("fsdp", "ctx"), "tp"),
            P(("fsdp", "ctx"), "tp"),
            P(("fsdp", "ctx"), "tp"),
            P(("fsdp", "ctx")),
            P(("fsdp", "ctx"), "tp"),
            P(("fsdp", "ctx"), "tp"),
            P(("fsdp", "ctx"), "tp"),
        ),
        check_vma=False,
    )
```

```python
import functools
import math

import jax
import jax.numpy as jnp
from jax import lax
from jax.experimental import pallas as pl
from jax.experimental.pallas import tpu as pltpu
from jax.sharding import PartitionSpec as P

HEAD_SIZE = 64
BUCKETS = 32
MAXDIST = 128


EPSILON = 1e-06
MASKED = -1000000000.0
TOP_PRECISION = lax.Precision.HIGHEST


def rms_scale(values, gain_row):
    inverse = lax.rsqrt(jnp.mean(values * values, axis=-1, keepdims=True) + EPSILON)
    return values * inverse * gain_row


def gated_product(gate_in, up_in):
    return jax.nn.gelu(gate_in, approximate=True) * up_in


def project(operand_array, weight_arrays):
    return jnp.einsum(
        "spd,dk->spk", operand_array, weight_arrays, preferred_element_type=jnp.float32
    )


def project_back(grad_cols, weight_arrays):
    return jnp.einsum("spk,dk->spd", grad_cols, weight_arrays, preferred_element_type=jnp.float32)


def weight_grad(operand_array, grad_cols):
    return jnp.einsum("spd,spk->dk", operand_array, grad_cols, preferred_element_type=jnp.float32)


def bucket_index(distance):
    exact_count = BUCKETS // 2
    counter = jnp.zeros(distance.shape, jnp.int32)
    for level_index in range(1, BUCKETS - exact_count):
        border = math.ceil(
            exact_count * (MAXDIST / exact_count) ** (level_index / (BUCKETS - exact_count))
        )
        counter = counter + (distance >= border).astype(jnp.int32)
    return jnp.where(distance < exact_count, distance, exact_count + counter)


def reduce_rows(partial_sum):
    return lax.psum(partial_sum, "tp")


def block_scores(queries, key_rows, bias_rows, allowed):
    scores = jnp.einsum("gpkrd,gjkd->gkrpj", queries, key_rows, preferred_element_type=jnp.float32)
    if bias_rows is not None:
        scores = jnp.where(allowed[:, None, None], scores + bias_rows[None], MASKED)
    return scores


def forward_block(queries, key_rows, value_rows, bias_rows, allowed):
    scores = block_scores(queries, key_rows, bias_rows, allowed)
    row_peak = jnp.max(scores, axis=-1, keepdims=True)
    log_total = row_peak + jnp.log(jnp.sum(jnp.exp(scores - row_peak), axis=-1, keepdims=True))
    weights_low = jnp.exp(scores - log_total).astype(jnp.bfloat16)
    output = jnp.einsum(
        "gkrpj,gjkd->gpkrd", weights_low, value_rows, preferred_element_type=jnp.float32
    )
    return (output.astype(jnp.bfloat16), log_total)


def backward_block(queries, key_rows, value_rows, bias_rows, allowed, log_total, grad_out):
    scores = block_scores(queries, key_rows, bias_rows, allowed)
    softmax_rows = jnp.exp(scores - log_total)
    grad_probs = jnp.einsum(
        "gpkrd,gjkd->gkrpj", grad_out, value_rows, preferred_element_type=jnp.float32
    )
    grad_scores = softmax_rows * (
        grad_probs - jnp.sum(grad_probs * softmax_rows, axis=-1, keepdims=True)
    )
    scores_low = grad_scores.astype(jnp.bfloat16)
    grad_query = jnp.einsum(
        "gkrpj,gjkd->gpkrd", scores_low, key_rows, preferred_element_type=jnp.float32
    )
    grad_key = jnp.einsum(
        "gkrpj,gpkrd->gjkd", scores_low, queries, preferred_element_type=jnp.float32
    )
    grad_value = jnp.einsum(
        "gkrpj,gpkrd->gjkd",
        softmax_rows.astype(jnp.bfloat16),
        grad_out,
        preferred_element_type=jnp.float32,
    )
    if bias_rows is None:
        grad_bias = jnp.zeros((1,), jnp.float32)
    else:
        grad_bias = jnp.sum(grad_scores, axis=0)
    return (grad_query.astype(jnp.bfloat16), grad_key, grad_value, grad_bias)


def block_shapes(queries, key_rows, block_seqs):
    seq_count, row_total_count, query_cols = queries.shape
    key_total_count, key_cols = (key_rows.shape[1], key_rows.shape[2])
    kv_heads = key_cols // HEAD_SIZE
    repeats = query_cols // key_cols
    blocks = seq_count // block_seqs
    query_shape = (blocks, block_seqs, row_total_count, kv_heads, repeats, HEAD_SIZE)
    key_shape = (blocks, block_seqs, key_total_count, kv_heads, HEAD_SIZE)
    mask_shape = (blocks, block_seqs, row_total_count, key_total_count)
    return (query_shape, key_shape, mask_shape)


def attention_forward(queries, key_rows, value_rows, bias_rows, allowed, block_seqs):
    query_shape, key_shape, mask_shape = block_shapes(queries, key_rows, block_seqs)
    sources = (
        queries.reshape(query_shape),
        key_rows.reshape(key_shape),
        value_rows.reshape(key_shape),
    )
    if allowed is not None:
        sources = sources + (allowed.reshape(mask_shape),)

    def one_block(piece_list):
        mask_block = piece_list[3] if allowed is not None else None
        return forward_block(piece_list[0], piece_list[1], piece_list[2], bias_rows, mask_block)

    outputs, log_totals = lax.map(one_block, sources)
    return (outputs.reshape(queries.shape), log_totals)


def attention_backward(
    queries, key_rows, value_rows, bias_rows, allowed, log_totals, grad_out, block_seqs
):
    query_shape, key_shape, mask_shape = block_shapes(queries, key_rows, block_seqs)
    sources = (
        queries.reshape(query_shape),
        key_rows.reshape(key_shape),
        value_rows.reshape(key_shape),
        log_totals,
        grad_out.reshape(query_shape),
    )
    if allowed is not None:
        sources = sources + (allowed.reshape(mask_shape),)
    if bias_rows is None:
        initial = jnp.zeros((1,), jnp.float32)
    else:
        initial = jnp.zeros(bias_rows.shape, jnp.float32)

    def one_block(running, piece_list):
        mask_block = piece_list[5] if allowed is not None else None
        grad_query, grad_key, grad_value, grad_bias = backward_block(
            piece_list[0],
            piece_list[1],
            piece_list[2],
            bias_rows,
            mask_block,
            piece_list[3],
            piece_list[4],
        )
        return (running + grad_bias, (grad_query, grad_key, grad_value))

    bias_total, grad_list = lax.scan(one_block, initial, sources)
    return (
        grad_list[0].reshape(queries.shape),
        grad_list[1].reshape(key_rows.shape),
        grad_list[2].reshape(value_rows.shape),
        bias_total,
    )


def shards(
    inputs,
    encoder,
    lengths,
    cotangent,
    norm_self,
    self_query,
    self_key_matrix,
    self_value_matrix,
    self_out,
    bias_table,
    norm_cross,
    cross_query,
    cross_key_matrix,
    cross_value_matrix,
    cross_out,
    norm_feed,
    feed_gate,
    feed_up,
    feed_out,
):
    self_group = (
        lax.all_gather(norm_self, ("fsdp", "ctx"), axis=0, tiled=True),
        lax.all_gather(self_query, ("fsdp", "ctx"), axis=0, tiled=True),
        lax.all_gather(self_key_matrix, ("fsdp", "ctx"), axis=0, tiled=True),
        lax.all_gather(self_value_matrix, ("fsdp", "ctx"), axis=0, tiled=True),
        lax.all_gather(self_out, ("fsdp", "ctx"), axis=0, tiled=True),
        lax.all_gather(bias_table, ("fsdp", "ctx"), axis=0, tiled=True),
    )
    seq_count, row_total_count = (inputs.shape[0], inputs.shape[1])
    block_seqs = max((trial for trial in (1, 2, 3, 4) if seq_count % trial == 0))
    start_row = lax.axis_index("ctx") * row_total_count
    key_total_count = row_total_count * lax.axis_size("ctx")
    row_pos = start_row + jnp.arange(row_total_count, dtype=jnp.int32)
    col_pos = jnp.arange(key_total_count, dtype=jnp.int32)
    buckets = bucket_index(jnp.maximum(row_pos[:, None] - col_pos[None, :], 0))
    one_hot = (buckets[:, :, None] == jnp.arange(BUCKETS, dtype=jnp.int32)[None, None, :]).astype(
        jnp.float32
    )
    causal = col_pos[None, :] <= row_pos[:, None]
    allowed = causal[None] & (col_pos[None, None, :] < lengths[:, None, None])
    hidden_in = inputs.astype(jnp.float32)
    normed_one, norm_pull_one = jax.vjp(rms_scale, hidden_in, self_group[0].astype(jnp.float32))
    self_in = normed_one.astype(jnp.bfloat16)
    self_q = project(self_in, self_group[1]).astype(jnp.bfloat16)
    self_k = project(self_in, self_group[2]).astype(jnp.bfloat16)
    self_v = project(self_in, self_group[3]).astype(jnp.bfloat16)
    keys_self, values_self = (
        lax.all_gather(self_k, "ctx", axis=1, tiled=True),
        lax.all_gather(self_v, "ctx", axis=1, tiled=True),
    )
    heads_local = self_group[1].shape[1] // HEAD_SIZE
    kv_local = self_group[2].shape[1] // HEAD_SIZE
    table_rows = self_group[5].astype(jnp.float32)
    bias_rows = jnp.einsum("ijb,bh->hij", one_hot, table_rows, precision=TOP_PRECISION).reshape(
        kv_local, heads_local // kv_local, row_total_count, key_total_count
    )
    self_att, lse_self = attention_forward(
        self_q, keys_self, values_self, bias_rows, allowed, block_seqs
    )
    hidden_two = hidden_in + reduce_rows(project_back(self_att, self_group[4]))
    cross_group = (
        lax.all_gather(norm_cross, ("fsdp", "ctx"), axis=0, tiled=True),
        lax.all_gather(cross_query, ("fsdp", "ctx"), axis=0, tiled=True),
        lax.all_gather(cross_key_matrix, ("fsdp", "ctx"), axis=0, tiled=True),
        lax.all_gather(cross_value_matrix, ("fsdp", "ctx"), axis=0, tiled=True),
        lax.all_gather(cross_out, ("fsdp", "ctx"), axis=0, tiled=True),
    )
    normed_two, norm_pull_two = jax.vjp(rms_scale, hidden_two, cross_group[0].astype(jnp.float32))
    cross_in = normed_two.astype(jnp.bfloat16)
    cross_q = project(cross_in, cross_group[1]).astype(jnp.bfloat16)
    enc_keys = project(encoder, cross_group[2]).astype(jnp.bfloat16)
    enc_values = project(encoder, cross_group[3]).astype(jnp.bfloat16)
    keys_cross, values_cross = (
        lax.all_gather(enc_keys, "ctx", axis=1, tiled=True),
        lax.all_gather(enc_values, "ctx", axis=1, tiled=True),
    )
    cross_att, lse_cross = attention_forward(
        cross_q, keys_cross, values_cross, None, None, block_seqs
    )
    hidden_three = hidden_two + reduce_rows(project_back(cross_att, cross_group[4]))
    feed_group = (
        lax.all_gather(norm_feed, ("fsdp", "ctx"), axis=0, tiled=True),
        lax.all_gather(feed_gate, ("fsdp", "ctx"), axis=0, tiled=True),
        lax.all_gather(feed_up, ("fsdp", "ctx"), axis=0, tiled=True),
        lax.all_gather(feed_out, ("fsdp", "ctx"), axis=0, tiled=True),
    )
    normed_three, norm_pull_three = jax.vjp(
        rms_scale, hidden_three, feed_group[0].astype(jnp.float32)
    )
    feed_in = normed_three.astype(jnp.bfloat16)
    gate_value = project(feed_in, feed_group[1])
    up_value = project(feed_in, feed_group[2])
    gated_value, gated_pull = jax.vjp(gated_product, gate_value, up_value)
    feed_hidden = gated_value.astype(jnp.bfloat16)
    hidden_four = hidden_three + reduce_rows(project_back(feed_hidden, feed_group[3]))
    output = hidden_four.astype(jnp.bfloat16)
    valid_rows = (row_pos[None, :] < lengths[:, None]).astype(jnp.float32)
    grad_full = cotangent.astype(jnp.float32) * valid_rows[:, :, None]
    branch_low = grad_full.astype(jnp.bfloat16)
    grad_hidden = grad_full
    grad_feed_out = weight_grad(branch_low, feed_hidden)
    grad_gated = project(branch_low, feed_group[3])
    grad_gate, grad_up = gated_pull(grad_gated)
    gate_low = grad_gate.astype(jnp.bfloat16)
    up_low = grad_up.astype(jnp.bfloat16)
    grad_feed_gate = weight_grad(feed_in, gate_low)
    grad_feed_up = weight_grad(feed_in, up_low)
    grad_feed_in = reduce_rows(
        project_back(gate_low, feed_group[1]) + project_back(up_low, feed_group[2])
    )
    grad_three, grad_gain_three = norm_pull_three(grad_feed_in)
    grad_hidden = grad_hidden + grad_three
    feed_grads = (
        lax.psum_scatter(
            grad_gain_three.astype(jnp.bfloat16), ("fsdp", "ctx"), scatter_dimension=0, tiled=True
        ).astype(jnp.float32),
        lax.psum_scatter(
            grad_feed_gate.astype(jnp.bfloat16), ("fsdp", "ctx"), scatter_dimension=0, tiled=True
        ).astype(jnp.float32),
        lax.psum_scatter(
            grad_feed_up.astype(jnp.bfloat16), ("fsdp", "ctx"), scatter_dimension=0, tiled=True
        ).astype(jnp.float32),
        lax.psum_scatter(
            grad_feed_out.astype(jnp.bfloat16), ("fsdp", "ctx"), scatter_dimension=0, tiled=True
        ).astype(jnp.float32),
    )
    cross_low = grad_hidden.astype(jnp.bfloat16)
    grad_cross_out = weight_grad(cross_low, cross_att)
    grad_cross_att = project(cross_low, cross_group[4]).astype(jnp.bfloat16)
    grad_cq, grad_ck_part, grad_cv_part, unused_bias = attention_backward(
        cross_q, keys_cross, values_cross, None, None, lse_cross, grad_cross_att, block_seqs
    )
    grad_ck, grad_cv = (
        lax.psum_scatter(
            grad_ck_part.astype(jnp.bfloat16), "ctx", scatter_dimension=1, tiled=True
        ).astype(jnp.float32),
        lax.psum_scatter(
            grad_cv_part.astype(jnp.bfloat16), "ctx", scatter_dimension=1, tiled=True
        ).astype(jnp.float32),
    )
    ck_low = grad_ck.astype(jnp.bfloat16)
    cv_low = grad_cv.astype(jnp.bfloat16)
    grad_cross_query = weight_grad(cross_in, grad_cq)
    grad_cross_key = weight_grad(encoder, ck_low)
    grad_cross_value = weight_grad(encoder, cv_low)
    grad_cross_in, grad_encoder = reduce_rows(
        (
            project_back(grad_cq, cross_group[1]),
            project_back(ck_low, cross_group[2]) + project_back(cv_low, cross_group[3]),
        )
    )
    grad_two, grad_gain_two = norm_pull_two(grad_cross_in)
    grad_hidden = grad_hidden + grad_two
    cross_grads = (
        lax.psum_scatter(
            grad_gain_two.astype(jnp.bfloat16), ("fsdp", "ctx"), scatter_dimension=0, tiled=True
        ).astype(jnp.float32),
        lax.psum_scatter(
            grad_cross_query.astype(jnp.bfloat16), ("fsdp", "ctx"), scatter_dimension=0, tiled=True
        ).astype(jnp.float32),
        lax.psum_scatter(
            grad_cross_key.astype(jnp.bfloat16), ("fsdp", "ctx"), scatter_dimension=0, tiled=True
        ).astype(jnp.float32),
        lax.psum_scatter(
            grad_cross_value.astype(jnp.bfloat16), ("fsdp", "ctx"), scatter_dimension=0, tiled=True
        ).astype(jnp.float32),
        lax.psum_scatter(
            grad_cross_out.astype(jnp.bfloat16), ("fsdp", "ctx"), scatter_dimension=0, tiled=True
        ).astype(jnp.float32),
    )
    self_low = grad_hidden.astype(jnp.bfloat16)
    grad_self_out = weight_grad(self_low, self_att)
    grad_self_att = project(self_low, self_group[4]).astype(jnp.bfloat16)
    grad_sq, grad_sk_part, grad_sv_part, bias_total = attention_backward(
        self_q, keys_self, values_self, bias_rows, allowed, lse_self, grad_self_att, block_seqs
    )
    grad_sk, grad_sv = (
        lax.psum_scatter(
            grad_sk_part.astype(jnp.bfloat16), "ctx", scatter_dimension=1, tiled=True
        ).astype(jnp.float32),
        lax.psum_scatter(
            grad_sv_part.astype(jnp.bfloat16), "ctx", scatter_dimension=1, tiled=True
        ).astype(jnp.float32),
    )
    sk_low = grad_sk.astype(jnp.bfloat16)
    sv_low = grad_sv.astype(jnp.bfloat16)
    grad_table = jnp.einsum(
        "ijb,hij->bh",
        one_hot,
        bias_total.reshape(heads_local, row_total_count, key_total_count),
        precision=TOP_PRECISION,
    )
    grad_self_query = weight_grad(self_in, grad_sq)
    grad_self_key = weight_grad(self_in, sk_low)
    grad_self_value = weight_grad(self_in, sv_low)
    grad_self_in = reduce_rows(
        project_back(grad_sq, self_group[1])
        + project_back(sk_low, self_group[2])
        + project_back(sv_low, self_group[3])
    )
    grad_one, grad_gain_one = norm_pull_one(grad_self_in)
    grad_inputs = grad_hidden + grad_one
    self_grads = (
        lax.psum_scatter(
            grad_gain_one.astype(jnp.bfloat16), ("fsdp", "ctx"), scatter_dimension=0, tiled=True
        ).astype(jnp.float32),
        lax.psum_scatter(
            grad_self_query.astype(jnp.bfloat16), ("fsdp", "ctx"), scatter_dimension=0, tiled=True
        ).astype(jnp.float32),
        lax.psum_scatter(
            grad_self_key.astype(jnp.bfloat16), ("fsdp", "ctx"), scatter_dimension=0, tiled=True
        ).astype(jnp.float32),
        lax.psum_scatter(
            grad_self_value.astype(jnp.bfloat16), ("fsdp", "ctx"), scatter_dimension=0, tiled=True
        ).astype(jnp.float32),
        lax.psum_scatter(
            grad_self_out.astype(jnp.bfloat16), ("fsdp", "ctx"), scatter_dimension=0, tiled=True
        ).astype(jnp.float32),
        lax.psum_scatter(
            grad_table.astype(jnp.bfloat16), ("fsdp", "ctx"), scatter_dimension=0, tiled=True
        ).astype(jnp.float32),
    )
    gain_shares = jnp.stack((self_grads[0], cross_grads[0], feed_grads[0]), axis=0)
    return (
        output,
        grad_inputs,
        grad_encoder,
        gain_shares[0],
        self_grads[1],
        self_grads[2],
        self_grads[3],
        self_grads[4],
        self_grads[5],
        gain_shares[1],
        cross_grads[1],
        cross_grads[2],
        cross_grads[3],
        cross_grads[4],
        gain_shares[2],
        feed_grads[1],
        feed_grads[2],
        feed_grads[3],
    )


MESH = pl.DeviceIdType.MESH
LANES = 128
DEPTH = 4
LINKS = {("x", 0): 0, ("y", 0): 1, ("z", 1): 2, ("z", -1): 3, ("c", 0): 4}
SIZES = {"x": 2, "y": 2, "z": DEPTH}


class Place:
    def __init__(self):
        row = lax.axis_index("fsdp")
        self.y = lax.axis_index("ctx")
        self.z = lax.axis_index("tp")
        self.x = lax.div(row, 2)
        self.c = lax.rem(row, 2)

    def link(self, axis, d):
        x, y, z, c = self.x, self.y, self.z, self.c
        if axis == "x":
            x = 1 - x
        elif axis == "y":
            y = 1 - y
        elif axis == "z":
            z = z + d
        else:
            c = 1 - c
        return (x * 2 + c, y, z)

    def has(self, link):
        if link == ("z", 1):
            return self.z < DEPTH - 1
        if link == ("z", -1):
            return self.z > 0
        return None

    def source(self, src):
        x = 1 - self.x if src.get("x") else self.x
        y = 1 - self.y if src.get("y") else self.y
        return x, y, self.z + src.get("z", 0)

    def exists(self, src):
        off = src.get("z", 0)
        if off < 0:
            return self.z >= -off
        if off > 0:
            return self.z < DEPTH - off
        return None


def arrivals(order):
    events = []
    for k, axis in enumerate(order):
        sources = [{}]
        for a in order[:k]:
            choice = (0, -1, 1, -2, 2, -3, 3) if a == "z" else (0, 1)
            sources = [dict(b, **{a: o}) for o in choice for b in sources]
        for o in (-1, 1, -2, 2, -3, 3) if axis == "z" else (1,):
            for b in sources:
                src = dict(b, **{axis: o})
                d = 0 if axis != "z" else (1 if o < 0 else -1)
                events.append((k, sum(abs(v) for v in src.values()), src, d))
    return events


def onward(order, k, d):
    out = [("z", d)] if k >= 0 and order[k] == "z" else []
    for a in order[k + 1 :]:
        out += [("z", 1), ("z", -1)] if a == "z" else [(a, 0)]
    return out


def when(cond, action):
    if cond is None:
        action()
    else:
        pl.when(cond)(action)


def number(x, y, z):
    return (x * 2 + y) * DEPTH + z


def greet(place):
    barrier = pltpu.get_barrier_semaphore()

    def signal(link):
        pl.semaphore_signal(
            barrier, inc=1, device_id=place.link(*link), device_id_type=MESH
        )

    for link in LINKS:
        when(place.has(link), functools.partial(signal, link))
    ends = jnp.where(place.z < DEPTH - 1, 1, 0) + jnp.where(place.z > 0, 1, 0)
    pl.semaphore_wait(barrier, ends + 3)


def remote(src, dst, send, recv, device):
    return pltpu.make_async_remote_copy(
        src_ref=src, dst_ref=dst, send_sem=send, recv_sem=recv,
        device_id=device, device_id_type=MESH,
    )


def shard(ref, z, r, rows):
    if ref.shape[1] == rows:
        return ref.at[z, :, pl.ds(pl.multiple_of(r * LANES, LANES), LANES)]
    return ref.at[z, pl.ds(pl.multiple_of(r * rows, rows), rows), :]


class Gather:
    def __init__(self, place, orders, rows, ins, outs, sems):
        self.place, self.orders, self.rows, self.ins, self.outs = place, orders, rows, ins, outs
        self.send, self.recv, self.core_recv, self.local_sem = sems
        self.me = (place.x, place.y, place.z)
        self.arrivals = [
            (k, hops, j, src, d)
            for j in range(len(orders))
            for k, hops, src, d in arrivals(orders[j])
        ]
        self.arrivals.sort(key=lambda e: (e[0], e[1]))

    @staticmethod
    def scratch(count):
        dma = pltpu.SemaphoreType.DMA
        return [
            dma((count, 4 * DEPTH, 5)), dma((count, 4 * DEPTH)), dma((count, 4 * DEPTH)),
            dma((count,)),
        ]

    def slot(self, j, xyz, c):
        x, y, z = xyz
        if len(self.orders[j]) == 1:
            return self.outs[j].at[y if self.orders[j] == "y" else z]
        return shard(self.outs[j], z, (x * 2 + c) * 2 + y, self.rows[j])

    def copy(self, j, xyz, link, own):
        here = self.slot(j, xyz, self.place.c)
        arrived = self.core_recv if link[0] == "c" else self.recv
        i = number(*xyz)
        return remote(
            self.ins[j] if own else here, here, self.send.at[j, i, LINKS[link]],
            arrived.at[j, i], self.place.link(*link),
        )

    def routes(self, j, k, d):
        links = onward(self.orders[j], k, d)
        return links + [("c", 0)] if len(self.orders[j]) == 3 else links

    def local(self, j):
        return pltpu.make_async_copy(
            self.ins[j], self.slot(j, self.me, self.place.c), self.local_sem.at[j]
        )

    def start(self, which=None):
        which = range(len(self.orders)) if which is None else which
        for stage in range(2):
            for j in which:
                for link in self.routes(j, -1, 0):
                    if (link[0] == "c") == (stage == 1):
                        when(self.place.has(link), self.copy(j, self.me, link, True).start)
        for j in which:
            self.local(j).start()

    def steps(self, wanted=None):
        for e, (k, hops, j, src, d) in enumerate(self.arrivals):
            xyz = self.place.source(src)
            if wanted is not None and not wanted(j, k):
                continue

            def step(k=k, j=j, d=d, xyz=xyz, src=src):
                def run():
                    self.copy(j, xyz, ("x", 0), True).wait_recv()
                    for link in self.routes(j, k, d):
                        when(self.place.has(link), self.copy(j, xyz, link, False).start)

                when(self.place.exists(src), run)

            yield (e + 1) / len(self.arrivals), step

    def settle(self, which):
        for j in which:
            self.local(j).wait()
            if len(self.orders[j]) == 3:

                def from_core(i, carry):
                    xyz = (
                        lax.div(i, 2 * DEPTH), lax.rem(lax.div(i, DEPTH), 2), lax.rem(i, DEPTH)
                    )
                    remote(
                        self.ins[j], self.slot(j, xyz, 1 - self.place.c), self.send.at[j, i, 4],
                        self.core_recv.at[j, i], self.place.link("c", 0),
                    ).wait_recv()
                    return carry

                lax.fori_loop(0, 4 * DEPTH, from_core, 0)

    def sent(self):
        place = self.place
        for j, order in enumerate(self.orders):

            def wait(i, carry):
                xyz = (lax.div(i, 2 * DEPTH), lax.rem(lax.div(i, DEPTH), 2), lax.rem(i, DEPTH))
                same = {a: xyz["xyz".index(a)] == self.me["xyz".index(a)] for a in "xyz"}
                if len(order) == 3:
                    for m, a in enumerate(order):
                        after = True
                        for b in order[m + 1 :]:
                            after = same[b] & after
                        for link in ((a, 0),) if a != "z" else (("z", 1), ("z", -1)):
                            if a == "z":
                                d = link[1]
                                near = (xyz[2] - place.z) * d <= 0
                                cond = near & after & place.has(link)
                            else:
                                cond = same[a] & after
                            pl.when(cond)(self.copy(j, xyz, link, False).wait_send)
                    self.copy(j, xyz, ("c", 0), False).wait_send()
                elif order == "z":
                    column = same["x"] & same["y"]
                    for link in (("z", 1), ("z", -1)):
                        near = (xyz[2] - place.z) * link[1] <= 0
                        pl.when(column & near & place.has(link))(
                            self.copy(j, xyz, link, False).wait_send
                        )
                else:
                    pl.when(same["x"] & same["y"] & same["z"])(
                        self.copy(j, xyz, (order, 0), False).wait_send
                    )
                return carry

            lax.fori_loop(0, 4 * DEPTH, wait, 0)

    def finish(self):
        self.settle(range(len(self.orders)))
        self.sent()


def child_slots(order):
    starts, total, before = [], 0, 1
    for a in order:
        starts.append(total)
        total += before * (DEPTH + 1 if a == "z" else 1)
        before *= SIZES[a]
    return starts, total


def child_slot(order, starts, m, xyz, tail):
    at = 0
    for a in order[:m]:
        at = at * SIZES[a] + xyz["xyz".index(a)]
    if order[m] == "z":
        at = at * (DEPTH + 1) + tail
    return starts[m] + at


def add_rows(out, terms, rows):
    step = min(rows, 32)

    def body(q, carry):
        at = pl.ds(pl.multiple_of(q * step, step), step)
        value = terms[0][at, :].astype(jnp.float32)
        for term in terms[1:]:
            value = value + term[at, :].astype(jnp.float32)
        out[at, :] = value.astype(out.dtype)
        return carry

    lax.fori_loop(0, rows // step, body, 0)


class Scatter:
    def __init__(self, place, orders, rows, ins, outs, scratch):
        self.place, self.orders, self.rows, self.ins, self.outs = place, orders, rows, ins, outs
        n = len(orders)
        self.sums, self.gifts, self.kids = (scratch[i * n : (i + 1) * n] for i in range(3))
        self.load_sem, self.give_sem, self.gift_sem, self.up_sem, self.kid_sem = scratch[3 * n :]
        self.me = (place.x, place.y, place.z)
        self.plans = [child_slots(o) for o in orders]
        self.partner = place.link("c", 0)
        self.events = [
            (k, hops, j, src, d)
            for j in range(n)
            for k, hops, src, d in arrivals(orders[j])
        ]
        self.events.sort(key=lambda e: (-e[0], -e[1]))

    @staticmethod
    def scratch(arrays, orders):
        plans = [child_slots(o)[1] for o in orders]
        count = len(arrays)
        dma = pltpu.SemaphoreType.DMA

        def room(slots):
            return [pltpu.VMEM((n,) + shard_shape(a), a.dtype) for n, a in zip(slots, arrays)]

        full = [4 * DEPTH] * count
        return (
            room(full) + room(full) + room(plans)
            + [dma((count, 4 * DEPTH))] * 4 + [dma((count, max(plans)))]
        )

    def slot(self, j, xyz, c):
        x, y, z = xyz
        return shard(self.ins[j], z, (x * 2 + c) * 2 + y, self.rows[j])

    def load(self, j, xyz):
        i = number(*xyz)
        return pltpu.make_async_copy(
            self.slot(j, xyz, self.place.c), self.sums[j].at[i], self.load_sem.at[j, i]
        )

    def give(self, j, xyz):
        i = number(*xyz)
        return remote(
            self.slot(j, xyz, 1 - self.place.c), self.gifts[j].at[i], self.give_sem.at[j, i],
            self.gift_sem.at[j, i], self.partner,
        )

    def up(self, j, xyz, k, d):
        axis = self.orders[j][k]
        tail = xyz[2]
        if axis == "z" and d < 0:
            tail = jnp.where(xyz[2] == self.place.z - d, DEPTH, xyz[2])
        at = child_slot(self.orders[j], self.plans[j][0], k, xyz, tail)
        i = number(*xyz)
        return remote(
            self.sums[j].at[i], self.kids[j].at[at], self.up_sem.at[j, i],
            self.kid_sem.at[j, at], self.place.link(axis, -d),
        )

    def kid(self, j, m, xyz, tail):
        at = child_slot(self.orders[j], self.plans[j][0], m, xyz, tail)
        ref = self.kids[j].at[at]
        remote(ref, ref, self.up_sem.at[j, 0], self.kid_sem.at[j, at], self.partner).wait_recv()
        return ref

    def collect(self, j, xyz, k, d, out=None):
        i = number(*xyz)
        order = self.orders[j]
        total = self.sums[j].at[i]
        self.load(j, xyz).wait()
        self.give(j, xyz).wait_recv()
        always, sometimes = [], []
        if k >= 0 and order[k] == "z":
            sometimes.append((k, ("z", d), xyz[2]))
        for m in range(k + 1, len(order)):
            if order[m] == "z":
                sometimes += [(m, ("z", 1), xyz[2]), (m, ("z", -1), DEPTH)]
            else:
                always.append(m)
        for m, link, tail in sometimes:

            def more():
                add_rows(total, [total, self.kid(j, m, xyz, tail)], self.rows[j])

            when(self.place.has(link), more)
        terms = [total, self.gifts[j].at[i]] + [self.kid(j, m, xyz, 0) for m in always]
        add_rows(total if out is None else out, terms, self.rows[j])

    def start(self, which=None):
        for j in range(len(self.orders)) if which is None else which:
            order = self.orders[j]

            def begin(e, carry):
                left = 4 * DEPTH - 1 - e
                at = {}
                for a in order:
                    at[a] = lax.rem(left, SIZES[a])
                    left = lax.div(left, SIZES[a])
                xyz = tuple(
                    lax.rem(self.me["xyz".index(a)] + at[a], SIZES[a]) for a in "xyz"
                )
                self.give(j, xyz).start()
                self.load(j, xyz).start()
                return carry

            lax.fori_loop(0, 4 * DEPTH, begin, 0)

    def steps(self, wanted=None):
        count = len(self.events)
        for e, (k, hops, j, src, d) in enumerate(self.events):
            xyz = self.place.source(src)
            if wanted is not None and not wanted(j):
                continue

            def step(k=k, j=j, d=d, xyz=xyz, src=src):
                def run():
                    self.collect(j, xyz, k, d)
                    self.up(j, xyz, k, d).start()

                when(self.place.exists(src), run)

            yield (e + 1) / (count + 1), step
        for j in range(len(self.orders)):
            if wanted is not None and not wanted(j):
                continue

            def last(j=j):
                self.collect(j, self.me, -1, 0, self.outs[j])

            yield 1.0, last

    def finish(self):
        me = number(*self.me)
        for j in range(len(self.orders)):

            def wait(i, carry):
                xyz = (lax.div(i, 2 * DEPTH), lax.rem(lax.div(i, DEPTH), 2), lax.rem(i, DEPTH))
                self.give(j, xyz).wait_send()

                def sent():
                    mine = self.sums[j].at[i]
                    remote(
                        mine, mine, self.up_sem.at[j, i], self.kid_sem.at[j, 0], self.partner
                    ).wait_send()

                pl.when(i != me)(sent)
                return carry

            lax.fori_loop(0, 4 * DEPTH, wait, 0)


class Share:
    def __init__(self, place, rows, ins, outs, scratch):
        self.place, self.rows, self.ins, self.outs = place, rows, ins, outs
        n = len(rows)
        self.first, self.second, self.sums = (scratch[i * n : (i + 1) * n] for i in range(3))
        self.send, self.recv = scratch[3 * n :]
        self.half = lax.rem(place.z, 2)
        self.over_y = place.link("y", 0)
        self.over_z = place.link("z", 1 - 2 * self.half)

    @staticmethod
    def scratch(rows):
        dma = pltpu.SemaphoreType.DMA
        out = []
        for slots in (8, 4, 4):
            out += [pltpu.VMEM((slots, n, 256), jnp.bfloat16) for n in rows]
        return out + [dma((len(rows), 12)), dma((len(rows), 12))]

    def block(self, j, t, y, half):
        n = self.rows[j]
        return self.ins[j].at[t, pl.ds(pl.multiple_of((y * 2 + half) * n, n), n), :]

    def early(self, j, t, s):
        if t < 2:
            src, device = self.block(j, t, 1 - self.place.y, s), self.over_y
        else:
            src, device = self.block(j, t, s, 1 - self.half), self.over_z
        i = t * 2 + s
        return remote(src, self.first[j].at[i], self.send.at[j, i], self.recv.at[j, i], device)

    def late(self, j, t):
        return remote(
            self.sums[j].at[t], self.second[j].at[t], self.send.at[j, 8 + t],
            self.recv.at[j, 8 + t], self.over_z if t < 2 else self.over_y,
        )

    def start(self):
        for j in range(len(self.rows)):
            for s in range(2):
                for t in range(4):
                    self.early(j, t, s).start()

    def steps(self):
        for j in range(len(self.rows)):
            for t in range(4):

                def pass_on(j=j, t=t):
                    for s in range(2):
                        self.early(j, t, s).wait_recv()
                    if t < 2:
                        away = 1 - self.half
                        mine = self.block(j, t, self.place.y, away)
                    else:
                        away = 1 - self.place.y
                        mine = self.block(j, t, away, self.half)
                    add_rows(
                        self.sums[j].at[t], [mine, self.first[j].at[t * 2 + away]], self.rows[j]
                    )
                    self.late(j, t).start()

                yield 0.25, pass_on
        for j in range(len(self.rows)):
            for t in range(4):

                def total(j=j, t=t):
                    self.late(j, t).wait_recv()
                    kept = self.half if t < 2 else self.place.y
                    mine = self.block(j, t, self.place.y, self.half)
                    add_rows(
                        self.outs[j].at[t],
                        [mine, self.first[j].at[t * 2 + kept], self.second[j].at[t]],
                        self.rows[j],
                    )

                yield 0.5, total

    def finish(self):
        for j in range(len(self.rows)):
            for t in range(4):
                for s in range(2):
                    self.early(j, t, s).wait_send()
                self.late(j, t).wait_send()


HBM = pl.BlockSpec(memory_space=pl.ANY)
INSIDE = pl.BlockSpec(memory_space=pltpu.VMEM)


def comm_call(kernel, name, number_id, ins, in_specs, outs, out_specs, scratch):
    return pl.pallas_call(
        kernel,
        out_shape=outs,
        in_specs=in_specs,
        out_specs=out_specs,
        scratch_shapes=scratch,
        compiler_params=pltpu.CompilerParams(
            collective_id=number_id, has_side_effects=True, vmem_limit_bytes=67043328
        ),
        name=name,
    )(*ins)


def gathered(a, order):
    if len(order) == 1:
        return jax.ShapeDtypeStruct((SIZES[order],) + a.shape, a.dtype)
    if a.shape[0] > a.shape[1] == LANES:
        return jax.ShapeDtypeStruct((DEPTH, a.shape[0], 8 * LANES), a.dtype)
    return jax.ShapeDtypeStruct((DEPTH, 8 * a.shape[0], a.shape[1]), a.dtype)


def shard_shape(a):
    if a.shape[2] == 8 * LANES:
        return (a.shape[1], LANES)
    return (a.shape[1] // 8, a.shape[2])


def scattered(arrays):
    return [jax.ShapeDtypeStruct(shard_shape(a), jnp.float32) for a in arrays]


WIDTH = 1024
QROWS = 256
KEYS = 1024
ENC_ROWS = 512
SPAN = 1280
CHUNK = 128
VMEM_MOST = 64000000
ROWS_OF = (((0,), (0,)), ((), ()))
LAST = (((1,), (1,)), ((), ()))
PLAIN = (((1,), (0,)), ((), ()))


def mm(a, b, dims=PLAIN):
    return lax.dot_general(a, b, dims, preferred_element_type=jnp.float32)


def norm_rows(v, gain):
    return v * lax.rsqrt(jnp.mean(v * v, axis=-1, keepdims=True) + EPSILON) * gain


def norm_back(v, gain, e):
    r = lax.rsqrt(jnp.mean(v * v, axis=-1, keepdims=True) + EPSILON)
    ev = e * v
    gain_grad = jnp.sum(ev * r, axis=0, keepdims=True)
    back = r * gain * e - v * (r * r * r) * jnp.mean(ev * gain, axis=-1, keepdims=True)
    return back, gain_grad


def head_rows(cols, a):
    return jnp.concatenate(
        [cols[:, a * 128 : a * 128 + 64], cols[:, a * 128 + 64 : a * 128 + 128]], axis=0
    )


def attend(q, kv, p_ref, s_ref, ot_ref, keys, add_bias):
    for a in range(2):
        q2 = head_rows(q, a)
        k = kv[:, a * 64 : a * 64 + 64]
        v = kv[:, 128 + a * 64 : 192 + a * 64]
        if add_bias is not None:
            add_bias(a, None, None)
        peak = None
        for c in range(keys // CHUNK):
            rows = pl.ds(c * CHUNK, CHUNK)
            s = mm(k[c * CHUNK : (c + 1) * CHUNK], q2, LAST)
            if add_bias is not None:
                s = add_bias(a, c, s)
            s_ref[rows, :] = s
            top = jnp.max(s, axis=0, keepdims=True)
            peak = top if peak is None else jnp.maximum(peak, top)

        def expose(c, total):
            rows = pl.ds(pl.multiple_of(c * CHUNK, CHUNK), CHUNK)
            e = jnp.exp(s_ref[rows, :] - peak)
            s_ref[rows, :] = e
            return total + jnp.sum(e, axis=0, keepdims=True)

        total = lax.fori_loop(0, keys // CHUNK, expose, jnp.zeros_like(peak))
        inverse = 1.0 / total

        def scale(c, carry):
            rows = pl.ds(pl.multiple_of(c * CHUNK, CHUNK), CHUNK)
            p_ref[0, a, rows, :] = (s_ref[rows, :] * inverse).astype(jnp.bfloat16)
            return carry

        lax.fori_loop(0, keys // CHUNK, scale, 0)
        ot = mm(v, p_ref[0, a], ROWS_OF)
        ot_ref[a * 128 : a * 128 + 64, :] = ot[:, :QROWS]
        ot_ref[a * 128 + 64 : a * 128 + 128, :] = ot[:, QROWS:]
    return jnp.transpose(ot_ref[...]).astype(jnp.bfloat16)


def attend_back(q, kv, p_ref, do, dkv_ref, d_ref, ds_ref, qt_ref, keys, take_bias):
    for a in range(2):
        q2 = head_rows(q, a)
        do2 = head_rows(do, a)
        k = kv[:, a * 64 : a * 64 + 64]
        v = kv[:, 128 + a * 64 : 192 + a * 64]
        total = jnp.zeros((1, 2 * QROWS), jnp.float32)
        for c in range(keys // CHUNK):
            rows = pl.ds(c * CHUNK, CHUNK)
            dp = mm(v[c * CHUNK : (c + 1) * CHUNK], do2, LAST)
            d_ref[rows, :] = dp
            total = total + jnp.sum(
                dp * p_ref[0, a, rows, :].astype(jnp.float32), axis=0, keepdims=True
            )
        for c in range(keys // CHUNK):
            rows = pl.ds(c * CHUNK, CHUNK)
            ds = p_ref[0, a, rows, :].astype(jnp.float32) * (d_ref[rows, :] - total)
            if take_bias is not None:
                take_bias(a, c, ds)
            ds_ref[rows, :] = ds.astype(jnp.bfloat16)
        if take_bias is not None:
            take_bias(a, None, None)
        dkv_ref[0, :, a * 64 : a * 64 + 64] = mm(ds_ref[pl.ds(0, keys), :], q2).astype(jnp.bfloat16)
        dkv_ref[0, :, 128 + a * 64 : 192 + a * 64] = mm(p_ref[0, a], do2).astype(jnp.bfloat16)
        qt = mm(k, ds_ref[pl.ds(0, keys), :], ROWS_OF)
        qt_ref[a * 128 : a * 128 + 64, :] = qt[:, :QROWS]
        qt_ref[a * 128 + 64 : a * 128 + 128, :] = qt[:, QROWS:]
    return jnp.transpose(qt_ref[...]).astype(jnp.bfloat16)


def self_step(first, length, h1_ref, w_ref, wkv_ref, q_ref, kv_ref, p_ref, o_ref, work):
    s_ref, strip_ref, ot_ref = work
    kv = mm(h1_ref[...], wkv_ref[0]).astype(jnp.bfloat16)
    kv_ref[0] = kv
    q = mm(h1_ref[pl.ds(first, QROWS), :], w_ref[0, :, :QROWS]).astype(jnp.bfloat16)
    q_ref[0] = q
    lane = lax.broadcasted_iota(jnp.int32, (1, 2 * QROWS), 1)
    lane = jnp.where(lane < QROWS, lane, lane - QROWS)
    last_key = jnp.minimum(lane + first, length - 1)

    def add_bias(a, c, s):
        if c is None:
            return None
        cols = pl.ds(CHUNK * (7 - c), QROWS)
        bias = jnp.concatenate(
            [strip_ref[2 * a, :, cols], strip_ref[2 * a + 1, :, cols]], axis=1
        )
        key = lax.broadcasted_iota(jnp.int32, s.shape, 0) + c * CHUNK
        return jnp.where(key <= last_key, s + bias, MASKED)

    o = attend(q, kv, p_ref, s_ref, ot_ref, KEYS, add_bias)
    o_ref[0] = o
    return mm(o, w_ref[0, :, QROWS:], LAST)


def cross_step(h_ref, enc, w_ref, wkv_ref, q_ref, kv_ref, p_ref, o_ref, work):
    s_ref, ot_ref = work
    kv = mm(enc, wkv_ref[0]).astype(jnp.bfloat16)
    kv_ref[0] = kv
    q = mm(h_ref[...], w_ref[0, :, :QROWS]).astype(jnp.bfloat16)
    q_ref[0] = q
    o = attend(q, kv, p_ref, s_ref, ot_ref, ENC_ROWS, None)
    o_ref[0] = o
    return mm(o, w_ref[0, :, QROWS:], LAST)


def here():
    z = lax.axis_index("tp")
    half = lax.rem(z, 2)
    return lax.div(z, 2), half, lax.axis_index("ctx") * (2 * QROWS) + half * QROWS


def feed_kernel(
    at, lengths, x3_ref, cot_ref, gain_ref, wg_ref, wu_ref, wo_ref,
    out_ref, g3_ref, gg_ref, gu_ref, go_ref, gn_ref,
    h_ref, g_ref, y_ref, dh_ref,
):
    step = pl.program_id(0)

    @pl.when(step == 0)
    def _():
        h_ref[...] = norm_rows(x3_ref[...], gain_ref[pl.ds(2, 1), :]).astype(jnp.bfloat16)
        row = lax.broadcasted_iota(jnp.int32, (QROWS, 1), 0) + at[2]
        g4 = jnp.where(row < lengths[at[0]], cot_ref[0].astype(jnp.float32), 0.0)
        g_ref[...] = g4.astype(jnp.bfloat16)
        y_ref[...] = x3_ref[...]
        dh_ref[...] = jnp.zeros_like(dh_ref)

    gate = mm(h_ref[...], wg_ref[0], LAST)
    up = mm(h_ref[...], wu_ref[0], LAST)
    root = math.sqrt(2.0 / math.pi)
    square = gate * gate
    th = jnp.tanh(root * (gate + 0.044715 * gate * square))
    half = 0.5 * (1.0 + th)
    gelu = gate * half
    slope = half + 0.5 * gate * (1.0 - th * th) * (root * (1.0 + 3 * 0.044715 * square))
    hidden = (gelu * up).astype(jnp.bfloat16)
    y_ref[...] += mm(hidden, wo_ref[0])
    go_ref[0] = mm(hidden, g_ref[...], ROWS_OF).astype(jnp.bfloat16)
    dhid = mm(g_ref[...], wo_ref[0], LAST)
    dup = (dhid * gelu).astype(jnp.bfloat16)
    dgate = (dhid * up * slope).astype(jnp.bfloat16)
    gg_ref[0] = mm(dgate, h_ref[...], ROWS_OF).astype(jnp.bfloat16)
    gu_ref[0] = mm(dup, h_ref[...], ROWS_OF).astype(jnp.bfloat16)
    dh_ref[...] += mm(dgate, wg_ref[0]) + mm(dup, wu_ref[0])

    @pl.when(step == pl.num_programs(0) - 1)
    def _():
        out_ref[...] = y_ref[...].astype(jnp.bfloat16)
        back, gain_grad = norm_back(x3_ref[...], gain_ref[pl.ds(2, 1), :], dh_ref[...])
        g3_ref[...] = g_ref[...].astype(jnp.float32) + back
        gn_ref[...] = gain_grad


def whole(shape):
    zeros = (0,) * len(shape)
    return pl.BlockSpec(shape, lambda t: zeros)


def part(shape, column=0):
    tail = (0,) * (len(shape) - 2)
    return pl.BlockSpec(shape, lambda t: (t,) + tail + (column,))


SCALARS = pl.BlockSpec(memory_space=pltpu.SMEM)
F32 = jnp.float32
LOW = jnp.bfloat16


def shape_of(shape, dtype):
    return jax.ShapeDtypeStruct(shape, dtype)


def feed(at, lengths, x3, cot, gains, wg, wu, wo):
    units = wg.shape[1]

    def fixed(shape):
        return pl.BlockSpec(shape, lambda t, at: (0,) * len(shape))

    wide = pl.BlockSpec((1, units, WIDTH), lambda t, at: (t, 0, 0))
    outs = (
        [shape_of((QROWS, WIDTH), LOW), shape_of((QROWS, WIDTH), F32)]
        + [shape_of((4, units, WIDTH), LOW)] * 3
        + [shape_of((1, WIDTH), F32)]
    )
    return pl.pallas_call(
        feed_kernel,
        grid_spec=pltpu.PrefetchScalarGridSpec(
            num_scalar_prefetch=1,
            grid=(4,),
            in_specs=[
                SCALARS, fixed((QROWS, WIDTH)),
                pl.BlockSpec((1, QROWS, WIDTH), lambda t, at: (at[0], at[1], 0)),
                fixed((8, WIDTH)), wide, wide, wide,
            ],
            out_specs=[fixed((QROWS, WIDTH)), fixed((QROWS, WIDTH)), wide, wide, wide,
                       fixed((1, WIDTH))],
            scratch_shapes=[
                pltpu.VMEM((QROWS, WIDTH), LOW), pltpu.VMEM((QROWS, WIDTH), LOW),
                pltpu.VMEM((QROWS, WIDTH), F32), pltpu.VMEM((QROWS, WIDTH), F32),
            ],
        ),
        out_shape=outs,
        compiler_params=pltpu.CompilerParams(
            dimension_semantics=("arbitrary",), vmem_limit_bytes=VMEM_MOST
        ),
        cost_estimate=pl.CostEstimate(
            flops=13 * 10**9, bytes_accessed=4 * 10**7, transcendentals=0
        ),
        name="feed",
    )(at, lengths, x3, cot, gains, wg, wu, wo)


FORWARD_SPLIT = (0.0, 0.7)
BACKWARD_SPLIT = (0.1, 0.0, 0.6)
SHARED = 0.5
LAST_SPLIT = (0.0, 0.6)
GATHER_ORDERS = ("zyx", "zyx", "xzy", "yzx", "zxy", "yzx", "zxy", "y", "y")
SMALL_ROWS = 16


def split_steps(steps, parts, low, high):
    ends = [int(len(steps) * (low + (high - low) * (i + 1) / parts)) for i in range(parts)]
    return [steps[a:b] for a, b in zip([0] + ends, ends)], steps[ends[-1] :]


def at_step(t, chunks):
    for i, chunk in enumerate(chunks):

        def run():
            for step in chunk:
                step()

        if chunk:
            pl.when(t == i)(run)


def forward_kernel(rows, *refs):
    lengths, feeds, packs, inputs, encoder = refs[0], refs[1:4], refs[4:8], refs[8], refs[9]
    weights, refs = refs[10:16], refs[16:]
    gains_ref, x2_ref, x3_ref, h1_out, h2_ref, x_out, enc_out = refs[:7]
    q1_out, kv1_out, p1_out, o1_out, q2_out, kv2_out, p2_out, o2_out = refs[7:15]
    small, x_all, enc_all, bucket_ref, h1_ref, s_ref, strip_ref, ot_ref = refs[15:23]
    own_feeds, own_x, own_enc, own_sem = refs[23:26], refs[26], refs[27], refs[28]
    place = Place()
    half = lax.rem(place.z, 2)
    seq = lax.div(place.z, 2)
    ins = own_feeds + packs + (own_x, own_enc)
    loads = [
        pltpu.make_async_copy(src, dst, own_sem.at[i])
        for i, (src, dst) in enumerate(
            [(inputs.at[seq], own_x), (encoder.at[seq], own_enc)] + list(zip(feeds, own_feeds))
        )
    ]
    for load in loads:
        load.start()
    plan = Gather(place, GATHER_ORDERS, rows, ins, weights + (small, x_all, enc_all), refs[29:])
    greet(place)
    first = pl.multiple_of(place.y * (2 * QROWS) + half * QROWS, QROWS)
    length = lengths[seq]
    for load in loads:
        load.wait()
    plan.start(range(3, 9))
    row = lax.broadcasted_iota(jnp.int32, (8, SPAN), 0)
    col = lax.broadcasted_iota(jnp.int32, (8, SPAN), 1)
    bucket_ref[...] = bucket_index(jnp.maximum(first + col - (SPAN - 264) - row, 0))
    for _, step in plan.steps(lambda j, k: 3 <= j < 7 and k < 2):
        step()
    plan.start(range(3))
    for _, step in plan.steps(lambda j, k: j >= 7 or (j >= 3 and k == 2)):
        step()
    plan.settle(range(3, 9))
    feed_steps = [step for _, step in plan.steps(lambda j, k: j < 3)]
    chunks, rest = split_steps(feed_steps, 8, *FORWARD_SPLIT)

    for k in range(3):
        gains_ref[pl.ds(k, 1), :] = jnp.concatenate(
            [small[0, pl.ds(r * SMALL_ROWS + k, 1), :] for r in range(8)], axis=1
        )
    gain = gains_ref[pl.ds(0, 1), :]
    for y in range(2):
        for c in range(2):
            at = pl.ds(c * QROWS, QROWS)
            h1_ref[pl.ds(y * 512 + c * QROWS, QROWS), :] = norm_rows(
                x_all[y, at, :].astype(jnp.float32), gain
            ).astype(jnp.bfloat16)
    own = own_x[pl.ds(pl.multiple_of(half * QROWS, QROWS), QROWS), :]
    x_out[...] = own
    x2_ref[...] = own.astype(jnp.float32)
    n = QROWS // 2
    enc_out[...] = own_enc[pl.ds(pl.multiple_of(half * n, n), n), :]
    h1_out[...] = h1_ref[pl.ds(first, QROWS), :]

    def self_body(w_ref, wkv_ref, q_ref, kv_ref, p_ref, o_ref):
        t = pl.program_id(0)

        def spread(head, carry):
            rows_of = [
                pltpu.roll(small[t, pl.ds(r * SMALL_ROWS + 3, 1), :], LANES - head, 1)
                for r in range(8)
            ]
            bucket = bucket_ref[...]
            near = jnp.zeros((8, SPAN), jnp.float32)
            for i in range(BUCKETS):
                lane = (i % 4) * 4
                near = jnp.where(bucket == i, rows_of[i // 4][:, lane : lane + 1], near)
            for g in range(16):
                shift = (SPAN - (120 - 8 * g)) % SPAN
                strip_ref[head, 8 * g : 8 * g + 8, :] = (
                    pltpu.roll(near, shift, 1) if shift else near
                )
            return carry

        lax.fori_loop(0, 4, spread, 0)
        x2_ref[...] += self_step(
            first, length, h1_ref, w_ref, wkv_ref, q_ref, kv_ref, p_ref, o_ref,
            (s_ref, strip_ref, ot_ref),
        )
        at_step(t, chunks[:4])

    pltpu.emit_pipeline(
        self_body,
        grid=(4,),
        in_specs=[part((1, WIDTH, 512)), part((1, WIDTH, 256))],
        out_specs=[
            part((1, QROWS, 256)), part((1, KEYS, 256)), part((1, 2, KEYS, 512)),
            part((1, QROWS, 256)),
        ],
    )(weights[3], weights[5], q1_out, kv1_out, p1_out, o1_out)
    x3_ref[...] = x2_ref[...]
    h2_ref[...] = norm_rows(x2_ref[...], gains_ref[pl.ds(1, 1), :]).astype(jnp.bfloat16)

    def cross_body(w_ref, wkv_ref, q_ref, kv_ref, p_ref, o_ref):
        t = pl.program_id(0)
        enc = jnp.concatenate([enc_all[0], enc_all[1]], axis=0)
        x3_ref[...] += cross_step(
            h2_ref, enc, w_ref, wkv_ref, q_ref, kv_ref, p_ref, o_ref,
            (s_ref, ot_ref),
        )
        at_step(t, chunks[4:])

    pltpu.emit_pipeline(
        cross_body,
        grid=(4,),
        in_specs=[part((1, WIDTH, 512)), part((1, WIDTH, 256), 1)],
        out_specs=[
            part((1, QROWS, 256)), part((1, ENC_ROWS, 256)), part((1, 2, ENC_ROWS, 512)),
            part((1, QROWS, 256)),
        ],
    )(weights[4], weights[5], q2_out, kv2_out, p2_out, o2_out)
    for step in rest:
        step()
    plan.settle(range(3))
    plan.sent()


def forward(lengths, feeds, packs, inputs, encoder):
    x, enc = shape_of(inputs.shape[1:], LOW), shape_of(encoder.shape[1:], LOW)
    arrays = list(feeds) + list(packs) + [x, enc]
    rows = [a.shape[0] for a in arrays]
    wide = [gathered(a, o) for a, o in zip(arrays, GATHER_ORDERS)]
    vm = pltpu.VMEM
    return comm_call(
        functools.partial(forward_kernel, rows), "forward", 1,
        (lengths,) + tuple(feeds) + tuple(packs) + (inputs, encoder),
        [SCALARS] + [HBM] * 3 + [INSIDE] * 4 + [HBM] * 2,
        wide[:6]
        + [shape_of((8, WIDTH), F32), shape_of((QROWS, WIDTH), F32),
           shape_of((QROWS, WIDTH), F32), shape_of((QROWS, WIDTH), LOW),
           shape_of((QROWS, WIDTH), LOW), shape_of((QROWS, WIDTH), LOW),
           shape_of((QROWS // 2, WIDTH), LOW),
           shape_of((4, QROWS, 256), LOW), shape_of((4, KEYS, 256), LOW),
           shape_of((4, 2, KEYS, 512), LOW), shape_of((4, QROWS, 256), LOW),
           shape_of((4, QROWS, 256), LOW), shape_of((4, ENC_ROWS, 256), LOW),
           shape_of((4, 2, ENC_ROWS, 512), LOW), shape_of((4, QROWS, 256), LOW)],
        [HBM] * 6 + [INSIDE] * 7 + [HBM] * 8,
        [vm(w.shape, w.dtype) for w in wide[6:]]
        + [vm((8, SPAN), jnp.int32), vm((KEYS, WIDTH), LOW), vm((KEYS, 512), F32),
           vm((4, CHUNK, SPAN), F32), vm((256, QROWS), F32)]
        + [vm(a.shape, LOW) for a in arrays[:3] + arrays[7:]]
        + [pltpu.SemaphoreType.DMA((5,))]
        + Gather.scratch(9),
    )


FEED_ORDERS = ("zxy", "zyx", "zyx")


def backward_kernel(rows, own, room, *refs):
    grads, refs = refs[:3], refs[3:]
    out_ref, g3_ref, x2_ref, h2_ref, h1_ref, gains_ref, x_ref, enc_ref, gn3_ref = refs[:9]
    w1, w2, w3, q1, kv1, p1, o1, q2, kv2, p2, o2 = refs[9:20]
    shards, refs = refs[20:23], refs[23:]
    rows_out, gx_ref, genc_ref, small, gw1, gw2, gw3 = refs[:7]
    dkv1, dkv2, g_ref, gt_ref, ht_ref, dc_ref, d_ref, ds_ref, qt_ref, strip_ref = refs[7:17]
    line_ref, g2_ref, dh_ref, dkv1_out, dkv2_out, et_ref, scratch = *refs[17:23], refs[23:]
    place = Place()
    plan = Scatter(place, FEED_ORDERS, rows, grads, shards, scratch[: len(room)])
    scratch = scratch[len(room) :]
    share = Share(place, own, (dkv1, dkv2), (dkv1_out, dkv2_out), scratch[:8])
    lines = Gather(place, ("z",), (QROWS,), (out_ref,), (rows_out,), scratch[8:])
    greet(place)
    lines.start()
    plan.start()
    steps = [step for _, step in plan.steps()]
    begin = int(len(steps) * BACKWARD_SPLIT[0])
    for step in steps[:begin]:
        step()
    chunks, rest = split_steps(steps[begin:], 8, *BACKWARD_SPLIT[1:])

    def load_grad(ref, h_ref):
        g = ref[...].astype(jnp.bfloat16)
        g_ref[...] = g
        gt_ref[...] = jnp.transpose(g)
        ht_ref[...] = jnp.transpose(h_ref[...])

    def heads(t, w_ref, q_ref, kv_ref, p_ref, o_ref, gw_ref, dkv, d_sum, keys, take_bias, todo):
        do = mm(g_ref[...], w_ref[0, :, QROWS:]).astype(jnp.bfloat16)
        gw_ref[0, :, QROWS:] = mm(gt_ref[...], o_ref[0]).astype(jnp.bfloat16)
        dq = attend_back(
            q_ref[0], kv_ref[0], p_ref, do, dkv.at[pl.ds(t, 1)], d_ref, ds_ref, qt_ref, keys,
            take_bias,
        )
        at_step(t, todo)
        gw_ref[0, :, :QROWS] = mm(ht_ref[...], dq).astype(jnp.bfloat16)
        d_sum[...] += mm(dq, w_ref[0, :, :QROWS], LAST)

    def specs(keys):
        return [
            part((1, WIDTH, 512)), part((1, QROWS, 256)), part((1, keys, 256)),
            part((1, 2, keys, 512)), part((1, QROWS, 256)),
        ]

    load_grad(g3_ref, h2_ref)
    dc_ref[...] = jnp.zeros_like(dc_ref)

    def cross_body(w_ref, q_ref, kv_ref, p_ref, o_ref, gw_ref):
        t = pl.program_id(0)
        heads(t, w_ref, q_ref, kv_ref, p_ref, o_ref, gw_ref, dkv2, dc_ref, ENC_ROWS, None, chunks[:4])

    pltpu.emit_pipeline(
        cross_body, grid=(4,), in_specs=specs(ENC_ROWS), out_specs=[part((1, WIDTH, 512))]
    )(w2, q2, kv2, p2, o2, gw2)
    back, gain_grad = norm_back(x2_ref[...], gains_ref[pl.ds(1, 1), :], dc_ref[...])
    g2_ref[...] = g3_ref[...] + back
    gain_grads = [None, gain_grad, gn3_ref[...]]
    load_grad(g2_ref, h1_ref)
    dh_ref[...] = jnp.zeros_like(dh_ref)

    def self_body(w_ref, q_ref, kv_ref, p_ref, o_ref, gw_ref):
        t = pl.program_id(0)

        def take_bias(a, c, ds):
            if c is None:
                for b in range(2):
                    total = jnp.zeros((8, SPAN), jnp.float32)
                    for g in range(16):
                        piece = strip_ref[b, 8 * g : 8 * g + 8, :]
                        shift = 120 - 8 * g
                        total = total + (pltpu.roll(piece, shift, 1) if shift else piece)
                    line = total[0:1]
                    for r in range(1, 8):
                        line = line + pltpu.roll(total[r : r + 1], SPAN - r, 1)
                    line_ref[pl.ds(t * 4 + 2 * a + b, 1), :] = line
                return
            if c == 0:
                strip_ref[...] = jnp.zeros_like(strip_ref)
            cols = pl.ds(CHUNK * (7 - c), QROWS)
            strip_ref[0, :, cols] += ds[:, :QROWS]
            strip_ref[1, :, cols] += ds[:, QROWS:]

        heads(t, w_ref, q_ref, kv_ref, p_ref, o_ref, gw_ref, dkv1, dh_ref, KEYS, take_bias, chunks[4:])

    pltpu.emit_pipeline(
        self_body, grid=(4,), in_specs=specs(KEYS), out_specs=[part((1, WIDTH, 512))]
    )(w1, q1, kv1, p1, o1, gw1)
    share.start()
    distance = lax.broadcasted_iota(jnp.int32, (1, SPAN), 1) - (SPAN - 264) + here()[2]
    bucket = bucket_index(jnp.maximum(distance, 0))
    chosen = lax.broadcasted_iota(jnp.int32, (LANES, SPAN), 0) == bucket
    table = lax.dot_general(
        line_ref[...], chosen.astype(jnp.float32), LAST, precision=TOP_PRECISION,
        preferred_element_type=jnp.float32,
    )
    ordered = [(i / max(len(rest), 1), step) for i, step in enumerate(rest)]
    ordered += [(0.05 + 0.9 * at, step) for at, step in share.steps()]
    ordered += [(0.1 * at, step) for at, step in lines.steps()]
    ordered.sort(key=lambda s: s[0])
    for _, step in [s for s in ordered if s[0] <= SHARED]:
        step()
    chunks, rest = split_steps([s[1] for s in ordered if s[0] > SHARED], 4, *LAST_SPLIT)
    et_ref[...] = jnp.transpose(enc_ref[...])
    n = QROWS // 2
    dc_ref[pl.ds(0, n), :] = jnp.zeros((n, WIDTH), jnp.float32)

    def last_body(ws_ref, wc_ref, gw_ref):
        t = pl.program_id(0)
        dkv, dkvc = dkv1_out[t], dkv2_out[t]
        gw_ref[0, :, :256] = mm(ht_ref[...], dkv).astype(jnp.bfloat16)
        gw_ref[0, :, 256:] = mm(et_ref[...], dkvc).astype(jnp.bfloat16)
        dh_ref[...] += mm(dkv, ws_ref[0], LAST)
        dc_ref[pl.ds(0, n), :] += mm(dkvc, wc_ref[0], LAST)
        at_step(t, chunks)

    pltpu.emit_pipeline(
        last_body, grid=(4,), in_specs=[part((1, WIDTH, 256)), part((1, WIDTH, 256), 1)],
        out_specs=[part((1, WIDTH, 512))],
    )(w3, w3, gw3)
    back, gain_grads[0] = norm_back(
        x_ref[...].astype(jnp.float32), gains_ref[pl.ds(0, 1), :], dh_ref[...]
    )
    gx_ref[...] = (g2_ref[...] + back).astype(jnp.bfloat16)
    genc_ref[...] = dc_ref[pl.ds(0, n), :].astype(jnp.bfloat16)
    small[...] = jnp.zeros_like(small)
    for r in range(8):
        shifted = pltpu.roll(table, (LANES - 4 * r) % LANES, 1) if r else table
        for t in range(4):
            for k in range(3):
                small[t, pl.ds(r * SMALL_ROWS + k, 1), :] = gain_grads[k][
                    :, r * LANES : (r + 1) * LANES
                ]
            small[t, pl.ds(r * SMALL_ROWS + 4, 4), :] = shifted[4 * t : 4 * t + 4]
    for step in rest:
        step()
    lines.finish()
    share.finish()
    plan.finish()


def backward(grads, out, g3, x2, h2, h1, gains, x, enc, gn3, w1, w2, w3, saved1, saved2):
    rows = [shard_shape(a)[0] for a in grads]
    own = [KEYS // 4, ENC_ROWS // 4]
    room = Scatter.scratch(grads, FEED_ORDERS)
    vm = pltpu.VMEM
    return comm_call(
        functools.partial(backward_kernel, rows, own, room), "backward", 2,
        tuple(grads) + (out, g3, x2, h2, h1, gains, x, enc, gn3, w1, w2, w3)
        + tuple(saved1) + tuple(saved2),
        [HBM] * 3 + [INSIDE] * 9 + [HBM] * 11,
        scattered(grads)
        + [gathered(out, "z"), shape_of(x.shape, LOW), shape_of(enc.shape, LOW),
           shape_of((4, 8 * SMALL_ROWS, LANES), F32), shape_of(w1.shape, LOW),
           shape_of(w2.shape, LOW), shape_of(w3.shape, LOW)],
        [INSIDE] * 3 + [HBM] + [INSIDE] * 3 + [HBM] * 3,
        [vm((4, KEYS, 256), LOW), vm((4, ENC_ROWS, 256), LOW), vm((QROWS, WIDTH), LOW),
         vm((WIDTH, QROWS), LOW), vm((WIDTH, QROWS), LOW), vm((QROWS, WIDTH), F32),
         vm((KEYS, 512), F32), vm((KEYS, 512), LOW), vm((256, QROWS), F32),
         vm((2, CHUNK, SPAN), F32), vm((16, SPAN), F32), vm((QROWS, WIDTH), F32),
         vm((QROWS, WIDTH), F32)]
        + [vm((4, r, 256), LOW) for r in own] + [vm((WIDTH, enc.shape[0]), LOW)]
        + room + Share.scratch(own) + Gather.scratch(1),
    )


HEAD_ORDERS = ("zyx", "zxy", "zyx", "zxy")


def finish_kernel(rows, room, *refs):
    ins, sent, out, landed, scratch = refs[:4], refs[4:6], refs[6], refs[7:9], refs[9:]
    place = Place()
    shards = [out.at[j] for j in range(3)]
    shards.append(out.at[3, pl.ds(0, SMALL_ROWS), pl.ds(0, LANES)])
    plan = Scatter(place, HEAD_ORDERS, rows, ins, shards, scratch[: len(room)])
    lines = Gather(
        place, ("z", "z"), (QROWS, QROWS // 2), sent, landed, scratch[len(room) :]
    )
    greet(place)
    lines.start()
    plan.start()
    steps = list(plan.steps()) + [(0.8 * at, step) for at, step in lines.steps()]
    steps.sort(key=lambda s: s[0])
    for _, step in steps:
        step()
    lines.finish()
    plan.finish()


def finish(arrays, lines):
    rows = [shard_shape(a)[0] for a in arrays]
    room = Scatter.scratch(arrays, HEAD_ORDERS)
    return comm_call(
        functools.partial(finish_kernel, rows, room), "finish", 3,
        tuple(arrays) + tuple(lines), [HBM] * 4 + [INSIDE] * 2,
        [shape_of((4, LANES, 512), F32)] + [gathered(a, "z") for a in lines],
        [INSIDE] + [HBM] * 2,
        room + Gather.scratch(2),
    )


def small_rows(gains, table):
    flat = jnp.pad(table.reshape(1, -1).astype(F32), ((0, 0), (0, LANES - table.size)))
    rows = jnp.concatenate([g.reshape(1, LANES).astype(F32) for g in gains] + [flat], axis=0)
    return jnp.pad(rows, ((0, SMALL_ROWS - 4), (0, 0)))


def tokens_split(
    inputs, encoder, lengths, cotangent,
    norm_self, self_query, self_key_matrix, self_value_matrix, self_out, bias_table,
    norm_cross, cross_query, cross_key_matrix, cross_value_matrix, cross_out,
    norm_feed, feed_gate, feed_up, feed_out,
):
    packs = (
        jnp.concatenate([self_query, self_out], axis=1),
        jnp.concatenate([cross_query, cross_out], axis=1),
        jnp.concatenate(
            [self_key_matrix, self_value_matrix, cross_key_matrix, cross_value_matrix], axis=1
        ),
        small_rows((norm_self, norm_cross, norm_feed), bias_table),
    )
    (
        wg, wu, wo, w1, w2, w3, gains, x2, x3, h1, h2, x_own, enc_own,
        q1, kv1, p1, o1, q2, kv2, p2, o2,
    ) = forward(lengths, (feed_gate.T, feed_up.T, feed_out.T), packs, inputs, encoder)
    out, g3, gg, gu, go, gn3 = feed(
        jnp.stack(here()), lengths, x3, cotangent, gains, wg, wu, wo
    )
    gg, gu, go, out, gx, genc, small, gw1, gw2, gw3 = backward(
        (gg, gu, go), out, g3, x2, h2, h1, gains, x_own, enc_own, gn3, w1, w2, w3,
        (q1, kv1, p1, o1), (q2, kv2, p2, o2),
    )
    heads, gx, genc = finish((gw1, gw2, gw3, small), (gx, genc))
    return (
        out.reshape(inputs.shape),
        gx.reshape(inputs.shape).astype(F32),
        genc.reshape(encoder.shape).astype(F32),
        heads[3, 0, :128], heads[0, :, :256], heads[2, :, :128], heads[2, :, 128:256],
        heads[0, :, 256:], jnp.transpose(heads[3, 4:8, :4]),
        heads[3, 1, :128], heads[1, :, :256], heads[2, :, 256:384], heads[2, :, 384:],
        heads[1, :, 256:],
        heads[3, 2, :128], gg.T, gu.T, go.T,
    )


def solution(mesh):
    sizes = (mesh.shape["fsdp"], mesh.shape["ctx"], mesh.shape["tp"])
    return jax.shard_map(
        tokens_split if sizes == (4, 2, DEPTH) else shards,
        mesh=mesh,
        in_specs=(
            P("fsdp", "ctx", None),
            P("fsdp", "ctx", None),
            P("fsdp"),
            P("fsdp", "ctx", None),
            P(("fsdp", "ctx")),
            P(("fsdp", "ctx"), "tp"),
            P(("fsdp", "ctx"), "tp"),
            P(("fsdp", "ctx"), "tp"),
            P(("fsdp", "ctx"), "tp"),
            P(("fsdp", "ctx"), "tp"),
            P(("fsdp", "ctx")),
            P(("fsdp", "ctx"), "tp"),
            P(("fsdp", "ctx"), "tp"),
            P(("fsdp", "ctx"), "tp"),
            P(("fsdp", "ctx"), "tp"),
            P(("fsdp", "ctx")),
            P(("fsdp", "ctx"), "tp"),
            P(("fsdp", "ctx"), "tp"),
            P(("fsdp", "ctx"), "tp"),
        ),
        out_specs=(
            P("fsdp", "ctx", None),
            P("fsdp", "ctx", None),
            P("fsdp", "ctx", None),
            P(("fsdp", "ctx")),
            P(("fsdp", "ctx"), "tp"),
            P(("fsdp", "ctx"), "tp"),
            P(("fsdp", "ctx"), "tp"),
            P(("fsdp", "ctx"), "tp"),
            P(("fsdp", "ctx"), "tp"),
            P(("fsdp", "ctx")),
            P(("fsdp", "ctx"), "tp"),
            P(("fsdp", "ctx"), "tp"),
            P(("fsdp", "ctx"), "tp"),
            P(("fsdp", "ctx"), "tp"),
            P(("fsdp", "ctx")),
            P(("fsdp", "ctx"), "tp"),
            P(("fsdp", "ctx"), "tp"),
            P(("fsdp", "ctx"), "tp"),
        ),
        check_vma=False,
    )
```
